32 devices in a mesh: dp: 8 (over z, y), tensor: 4 (over x, core).
Axes of the slice: x: 2, y: 2, z: 4, core: 2. Of those that a mesh axis runs over, the one named last changes fastest.
Arguments:
- hidden_in: bfloat16 [16384, 1024], P(('dp', 'tensor')), may hold values from -6 to 6
- doc_ids: int32 [32, 512], P('dp'), may hold values from 0 to 5, never falling along the last dimension, each value on 1 to 256 neighbouring positions
- unit_slot: int32 [24], replicated, may hold values from 0 to 31, as said below
- masters: float32 [32, 1024, 1024], P('dp', None, 'tensor')
- first_moment: float32 [32, 1024, 1024], P('dp', None, 'tensor')
- second_moment: float32 [32, 1024, 1024], P('dp', None, 'tensor')
- column_state: float32 [3, 2, 6, 1024], P(None, None, None, 'tensor')
- row_state: float32 [3, 2, 6, 1024], replicated
- out_grad: bfloat16 [16384, 1024], P(('dp', 'tensor')), may hold values from -0.046875 to 0.046875
Outputs:
- block_out: float32 [16384, 1024], P(('dp', 'tensor'))
- input_grad: float32 [16384, 1024], P(('dp', 'tensor'))
- unit_master: float32 [32, 1024, 1024], P('dp', None, 'tensor')
- unit_state: float32 [2, 32, 1024, 1024], P(None, 'dp', None, 'tensor')
- column_out: float32 [4, 2, 6, 1024], P(None, None, None, 'tensor')
- row_out: float32 [4, 2, 6, 1024], replicated
The draws below stay inside these ranges and needn't reach their ends.
Inputs may be any that keep to these rules, and one draw needn't show every extreme that they name: `doc_ids`: within a row the ids never fall; each of the 6 documents covers 1 to 256 tokens, one exactly that many. `unit_slot`: all 24 entries differ; slot s belongs to index s // 4 of dp; some index of dp holds exactly 4 matrices.
All inputs are finite; a program needn't handle non-finite values.
Results may differ from the reference program's by a relative error of at most 0.028.
Values may be sent and summed in bfloat16 or wider, within the bound.
A program may use at most 256 MiB of HBM per device.

```python
import math
import jax
import jax.numpy as jnp
import numpy as np
from jax import lax

D = 1024
HEADS = 16
HEAD_DIM = 64
FF = 4096
SEQ_LEN = 512
LAYERS = 2
DOCS = 6
STEP = 3
UNITS = 24
CAP = 4
SLOTS = 32
SEQS = 32
TOKENS = 16384


def slot_list(key):
    shuffled = jax.random.permutation(jax.random.fold_in(key, 11), SLOTS)
    full_owner = jax.random.randint(jax.random.fold_in(key, 12), (), 0, SLOTS // CAP)
    positions = jnp.arange(SLOTS)
    sort_keys = jnp.where(shuffled // CAP == full_owner, positions - SLOTS, positions)
    chosen = shuffled[jnp.argsort(sort_keys)][:UNITS]
    return chosen[jax.random.permutation(jax.random.fold_in(key, 13), UNITS)].astype(jnp.int32)


def slot_scales(key, kind_scales, empty_scale):
    unit_kinds = jnp.tile(jnp.array(kind_scales, jnp.float32), LAYERS)
    return jnp.full((SLOTS,), empty_scale, jnp.float32).at[slot_list(key)].set(unit_kinds)


def master_kinds():
    blocks = FF // D
    narrow = D ** (-0.5)
    return [narrow] * 3 + [4.0 * narrow] + [narrow] * blocks + [FF ** (-0.5)] * blocks


def grad_kinds():
    blocks = FF // D
    return [0.4, 0.4, 0.45, 0.25] + [0.25] * blocks + [0.6] * blocks


def bounded_normal(key, out_shape):
    return jnp.clip(jax.random.normal(key, out_shape, jnp.float32), -6.0, 6.0)


def spread_factor(key, out_shape):
    return jnp.exp(jax.random.uniform(key, out_shape, jnp.float32, math.log(0.5), math.log(8.0)))


def draw_unit_slot(key, part):
    return slot_list(key)


def draw_masters(key, part):
    scales = slot_scales(key, master_kinds(), D ** (-0.5))
    return bounded_normal(jax.random.fold_in(key, 21), (SLOTS, D, D)) * scales[:, None, None]


def draw_first_moment(key, part):
    scales = slot_scales(key, grad_kinds(), 0.3)
    return bounded_normal(jax.random.fold_in(key, 22), (SLOTS, D, D)) * scales[:, None, None]


def draw_second_moment(key, part):
    scales = slot_scales(key, grad_kinds(), 0.3)
    return spread_factor(jax.random.fold_in(key, 23), (SLOTS, D, D)) * (scales * scales)[:, None, None]


def draw_column_state(key, part):
    blocks = FF // D
    out_shape = (LAYERS, 2 + blocks, D)
    grad_scale = jnp.array([0.45, 0.45] + [0.25] * blocks, jnp.float32)[None, :, None]
    values = 0.3 * bounded_normal(jax.random.fold_in(key, 31), out_shape)
    first_vals = grad_scale * bounded_normal(jax.random.fold_in(key, 32), out_shape)
    second_vals = grad_scale * grad_scale * spread_factor(jax.random.fold_in(key, 33), out_shape)
    return jnp.stack([values, first_vals, second_vals])


def draw_row_state(key, part):
    out_shape = (LAYERS, 6, D)
    centre = jnp.array([0.0, 0.0, 1.0, 0.0, 1.0, 0.0], jnp.float32)[None, :, None]
    spread = jnp.array([0.3, 0.3, 0.15, 0.3, 0.15, 0.3], jnp.float32)[None, :, None]
    values = centre + spread * bounded_normal(jax.random.fold_in(key, 41), out_shape)
    first_vals = bounded_normal(jax.random.fold_in(key, 42), out_shape)
    second_vals = spread_factor(jax.random.fold_in(key, 43), out_shape)
    return jnp.stack([values, first_vals, second_vals])


def block_levels(own_key, dims, pieces, smallest, largest):
    def one(position, blocks):
        steps = jax.random.uniform(jax.random.fold_in(jax.random.fold_in(own_key, 6), position), (blocks,), jnp.float32, smallest / len(pieces), largest / len(pieces))
        return jnp.repeat(jnp.exp(steps), dims[position] // blocks).reshape((-1,) + (1,) * (len(dims) - position - 1))

    loudness = one(*pieces[0])
    for cut in pieces[1:]:
        loudness = loudness * one(*cut)
    return loudness


def profile(amount, total, reach, slope):
    weights = [(1 << 20) // math.isqrt(rank ** slope) + 1 for rank in range(2, amount + 1)]
    surplus, holding = total - reach - (amount - 1), [1] * (amount - 1)
    while surplus > 0:
        free = [i for i in range(amount - 1) if holding[i] < reach]
        mass, left = sum([weights[i] for i in free]), surplus
        for i in free:
            extra = min(reach - holding[i], max(1, left * weights[i] // mass), surplus)
            holding[i] = holding[i] + extra
            surplus = surplus - extra
    return np.array([reach] + holding)


def uneven(rng, count, total, most, skew):
    if count == 2:
        one = jax.random.randint(rng, (), max(1, total - most), min(most, total - 1) + 1)
        return jnp.stack([one, total - one])
    lengths = jnp.asarray(profile(count, total, most, skew), jnp.int32)
    couples = (count - 1) // 2
    giver, taker = lengths[1:1 + 2 * couples:2], lengths[2:2 + 2 * couples:2]
    slack = jnp.minimum(giver - 1, most - taker)
    shifted = jax.random.randint(jax.random.fold_in(rng, 1), (couples,), 0, 1 << 20) % (slack + 1)
    lengths = lengths.at[1:1 + 2 * couples:2].set(giver - shifted).at[2:2 + 2 * couples:2].set(taker + shifted)
    return lengths[jax.random.permutation(jax.random.fold_in(rng, 2), count)]


def bell_draw(rng, shape, scale, limit, split=(), kind=jnp.bfloat16):
    level = block_levels(rng, shape, split, -0.22, 0.18) if split else 1.0
    result = jax.random.normal(rng, shape, jnp.float32) * scale * level
    return jnp.minimum(jnp.maximum(result, -limit), limit).astype(kind)


def setup_inputs(seed: int = 0) -> dict:
    key_of = jax.random.split(jax.random.key(seed), 10)
    hidden_in = bell_draw(key_of[0], (TOKENS, D), 1.0, 6.0, ((0, 32),))
    doc_ids = jax.vmap(lambda own: jnp.searchsorted(jnp.cumsum(uneven(own, DOCS, SEQ_LEN, SEQ_LEN // 2, 1)), jnp.arange(SEQ_LEN), side="right"))(jax.random.split(key_of[1], SEQS)).reshape((SEQS, SEQ_LEN)).astype(jnp.int32)
    unit_slot = draw_unit_slot(jax.random.fold_in(key_of[9], 71), 0)
    masters = draw_masters(jax.random.fold_in(key_of[9], 71), 0)
    first_moment = draw_first_moment(jax.random.fold_in(key_of[9], 71), 0)
    second_moment = draw_second_moment(jax.random.fold_in(key_of[9], 71), 0)
    column_state = draw_column_state(jax.random.fold_in(key_of[9], 71), 0)
    row_state = draw_row_state(jax.random.fold_in(key_of[9], 71), 0)
    out_grad = bell_draw(key_of[8], (TOKENS, D), TOKENS ** -0.5, 0.046875, ((0, 32),))
    return {"hidden_in": hidden_in, "doc_ids": doc_ids, "unit_slot": unit_slot, "masters": masters, "first_moment": first_moment, "second_moment": second_moment, "column_state": column_state, "row_state": row_state, "out_grad": out_grad}


@jax.custom_vjp
def low(v):
    return lax.optimization_barrier(v.astype(jnp.bfloat16)).astype(jnp.float32)

@jax.custom_vjp
def low_back(v):
    return v

def low_keep(v):
    return (low(v), None)

def low_pass(kept, grad):
    return (grad,)

def back_keep(v):
    return (v, None)

def back_low(kept, grad):
    return (low(grad),)
low.defvjp(low_keep, low_pass)
low_back.defvjp(back_keep, back_low)
EPS_NORM = 1e-06
RATE_UNITS = 0.05
RATE_SMALL = 0.2
WEIGHT_DECAY = 0.01
ADAM_EPS = 1e-08
BETA_MOMENT = 0.5
PRECISE = lax.Precision.HIGHEST

def matmul(left, right):
    return jnp.dot(left, right, precision=PRECISE, preferred_element_type=jnp.float32)

def norm_rows(summed, gain, shift):
    row_mean = lax.optimization_barrier(jnp.mean(summed, axis=-1, keepdims=True))
    centred = summed - row_mean
    variance = lax.optimization_barrier(jnp.mean(centred * centred, axis=-1, keepdims=True))
    return centred * lax.rsqrt(variance + EPS_NORM) * gain + shift

def attend_one(packed):
    queries, key_rows, value_rows, doc_row = packed
    raw_scores = jnp.einsum('qhd,khd->hqk', queries, key_rows, precision=PRECISE) * HEAD_DIM ** (-0.5)
    scores = low_back(raw_scores)
    same_doc = doc_row[:, None] == doc_row[None, :]
    scores = jnp.where(same_doc[None], scores, -1e+30)
    soft_probs = low(jax.nn.softmax(scores, axis=-1))
    context = jnp.einsum('hqk,khd->qhd', soft_probs, value_rows, precision=PRECISE)
    return context.reshape(SEQ_LEN, D)

def encoder_layer(hidden, unit_vals, col_vals, row_vals, doc_ids):
    blocks = FF // D
    weights = low(unit_vals)
    hidden_bf = low(hidden)
    queries = low(low_back(matmul(hidden_bf, weights[0]) + col_vals[0]))
    key_rows = low(low_back(matmul(hidden_bf, weights[1])))
    value_rows = low(low_back(matmul(hidden_bf, weights[2]) + col_vals[1]))
    shape_heads = (SEQS, SEQ_LEN, HEADS, HEAD_DIM)
    context = lax.map(jax.checkpoint(attend_one), (queries.reshape(shape_heads), key_rows.reshape(shape_heads), value_rows.reshape(shape_heads), doc_ids))
    context = low(low_back(context.reshape(TOKENS, D)))
    attended = low_back(matmul(context, weights[3].T)) + row_vals[0]
    normed = norm_rows(hidden + attended, row_vals[2], row_vals[3])
    normed_bf = low(normed)
    w_in = jnp.concatenate([weights[4 + block_index] for block_index in range(blocks)], axis=1)
    w_out = jnp.concatenate([weights[4 + blocks + block_index] for block_index in range(blocks)], axis=1)
    pre_act = low_back(matmul(normed_bf, w_in) + col_vals[2:2 + blocks].reshape(FF))
    activated = low(jax.nn.gelu(pre_act, approximate=False))
    mlp_out = low_back(matmul(activated, w_out.T)) + row_vals[1]
    return norm_rows(normed + mlp_out, row_vals[4], row_vals[5])

def adamw_update(old_value, gradient, first_old, second_old, learn_rate):
    first_new = BETA_MOMENT * first_old + (1.0 - BETA_MOMENT) * gradient
    second_new = BETA_MOMENT * second_old + (1.0 - BETA_MOMENT) * gradient * gradient
    correct = 1.0 - BETA_MOMENT ** STEP
    step_size = first_new / correct / (jnp.sqrt(second_new / correct) + ADAM_EPS)
    return (old_value - learn_rate * (step_size + WEIGHT_DECAY * old_value), first_new, second_new)

def reference(hidden_in, doc_ids, unit_slot, masters, first_moment, second_moment, column_state, row_state, out_grad):
    per_layer = UNITS // LAYERS
    unit_mats = masters[unit_slot]

    def forward(start_rows, unit_vals, col_vals, row_vals):
        hidden = start_rows
        for layer_index in range(LAYERS):
            hidden = encoder_layer(hidden, unit_vals[layer_index * per_layer:(layer_index + 1) * per_layer], col_vals[layer_index], row_vals[layer_index], doc_ids)
        return hidden
    block_out, pullback = jax.vjp(forward, hidden_in.astype(jnp.float32), unit_mats, column_state[0], row_state[0])
    input_grad, unit_grads, col_grads, row_grads = pullback(out_grad.astype(jnp.float32))
    slot_grads = jnp.zeros(masters.shape, jnp.float32).at[unit_slot].set(unit_grads)
    occupied = jnp.zeros((SLOTS,), jnp.float32).at[unit_slot].set(1.0)[:, None, None]
    new_master, new_first, new_second = adamw_update(masters, slot_grads, first_moment, second_moment, RATE_UNITS)
    unit_master = new_master * occupied
    unit_state = jnp.stack([new_first * occupied, new_second * occupied])
    new_col, col_first, col_second = adamw_update(column_state[0], col_grads, column_state[1], column_state[2], RATE_SMALL)
    column_out = jnp.stack([col_grads, new_col, col_first, col_second])
    new_row, row_first, row_second = adamw_update(row_state[0], row_grads, row_state[1], row_state[2], RATE_SMALL)
    row_out = jnp.stack([row_grads, new_row, row_first, row_second])
    return (block_out, input_grad, unit_master, unit_state, column_out, row_out)
```

```python
import math

import jax
import jax.numpy as jnp
from jax import lax
from jax.sharding import PartitionSpec as P

HEAD_DIM = 64
LAYERS = 2
STEP = 3

EPS_NORM = 1e-06
RATE_UNITS = 0.05
RATE_SMALL = 0.2
WEIGHT_DECAY = 0.01
ADAM_EPS = 1e-08
BETA_MOMENT = 0.5
BOTH = ("dp", "tensor")


def norm_forward(summed, gain, shift):
    row_mean = jnp.mean(summed, axis=1, keepdims=True)
    centred = summed - row_mean
    inverse = lax.rsqrt(jnp.mean(centred * centred, axis=1, keepdims=True) + EPS_NORM)
    scaled = centred * inverse
    return (scaled * gain + shift, scaled, inverse)


def norm_backward(upstream, scaled, inverse, gain):
    d_scaled = upstream * gain
    mean_one = jnp.mean(d_scaled, axis=1, keepdims=True)
    mean_two = jnp.mean(d_scaled * scaled, axis=1, keepdims=True)
    grad_input = inverse * (d_scaled - mean_one - scaled * mean_two)
    return (grad_input, jnp.sum(upstream * scaled, axis=0), jnp.sum(upstream, axis=0))


def gelu_pair(v):
    z = jnp.abs(v) * (2.0**-0.5)
    t = 1.0 / (1.0 + 0.5 * z)
    poly = 0.17087277
    for coefficient in (
        -0.82215223,
        1.48851587,
        -1.13520398,
        0.27886807,
        -0.18628806,
        0.09678418,
        0.37409196,
        1.00002368,
        -1.26551223,
    ):
        poly = poly * t + coefficient
    bell = jnp.exp(-0.5 * v * v)
    tail = 0.5 * t * jnp.exp(poly) * bell
    cdf = jnp.where(v >= 0.0, 1.0 - tail, tail)
    return (v * cdf, cdf + v * bell * (2.0 * math.pi) ** (-0.5))


def adamw_update(old_value, gradient, first_old, second_old, learn_rate):
    first_new = BETA_MOMENT * first_old + (1.0 - BETA_MOMENT) * gradient
    second_new = BETA_MOMENT * second_old + (1.0 - BETA_MOMENT) * gradient * gradient
    correct = 1.0 - BETA_MOMENT**STEP
    step_size = first_new / correct / (jnp.sqrt(second_new / correct) + ADAM_EPS)
    return (old_value - learn_rate * (step_size + WEIGHT_DECAY * old_value), first_new, second_new)


def dot(left, right, dims):
    return lax.dot_general(left, right, (dims, ((), ())), preferred_element_type=jnp.float32)


def local(
    hidden_in,
    doc_ids,
    unit_slot,
    masters,
    first_moment,
    second_moment,
    column_state,
    row_state,
    out_grad,
):
    slot_count, width, col_width = masters.shape
    units = unit_slot.shape[0]
    per_layer = units // LAYERS
    blocks = (per_layer - 4) // 2
    dp_size = lax.axis_size("dp")
    tensor_size = lax.axis_size("tensor")
    devices = dp_size * tensor_size
    slots = slot_count * dp_size
    rows = hidden_in.shape[0]
    seq_len = doc_ids.shape[1]
    heads = width // HEAD_DIM
    piece = width // devices
    share = seq_len // rows
    tensor_index = lax.axis_index("tensor")
    groups = [list(range(i, i + share)) for i in range(0, tensor_size, share)]
    score_scale = HEAD_DIM ** (-0.5)

    sent = masters.astype(jnp.bfloat16).reshape(slot_count, devices, piece, col_width)
    spread = lax.all_to_all(sent.transpose(1, 0, 2, 3), BOTH, 0, 0)
    spread = spread.reshape(dp_size, tensor_size, slot_count, piece, col_width)
    spread = spread.transpose(0, 2, 3, 1, 4).reshape(slots, piece, width)
    mine = spread[unit_slot]
    layer_mats = []
    for layer in range(LAYERS):
        own = mine[layer * per_layer : (layer + 1) * per_layer].transpose(1, 0, 2)
        full = lax.all_gather(own.reshape(piece, per_layer * width), BOTH, axis=0, tiled=True)
        layer_mats.append(
            (
                full[:, : 3 * width],
                full[:, 3 * width : 4 * width],
                full[:, 4 * width : (4 + blocks) * width],
                full[:, (4 + blocks) * width :],
            )
        )

    row_docs = lax.dynamic_slice_in_dim(doc_ids, tensor_index // share, 1, axis=0)[0]
    my_docs = lax.dynamic_slice_in_dim(row_docs, (tensor_index % share) * rows, rows)
    same_doc = (my_docs[:, None] == row_docs[None, :])[None]

    def whole_row(value):
        if share == 1:
            return value
        return lax.all_gather(value, "tensor", axis=0, tiled=True, axis_index_groups=groups)

    def own_rows(value):
        if share == 1:
            return value
        return lax.psum_scatter(
            value, "tensor", scatter_dimension=0, tiled=True, axis_index_groups=groups
        )

    col_full = lax.all_gather(column_state[0], "tensor", axis=2, tiled=True)
    hidden = hidden_in.astype(jnp.float32)
    saved_layers = []
    for layer in range(LAYERS):
        w_qkv, w_proj, w_in, w_out = layer_mats[layer]
        row_now = row_state[0, layer]
        col_now = col_full[layer]
        hidden_bf = hidden.astype(jnp.bfloat16)
        mixed = dot(hidden_bf, w_qkv, ((1,), (0,)))
        query = (mixed[:, :width] + col_now[0]).astype(jnp.bfloat16)
        key = whole_row(mixed[:, width : 2 * width].astype(jnp.bfloat16))
        value = whole_row((mixed[:, 2 * width :] + col_now[1]).astype(jnp.bfloat16))
        query = query.reshape(rows, heads, HEAD_DIM)
        key = key.reshape(seq_len, heads, HEAD_DIM)
        value = value.reshape(seq_len, heads, HEAD_DIM)
        scores = (
            jnp.einsum("qhd,khd->hqk", query, key, preferred_element_type=jnp.float32) * score_scale
        )
        scores = jnp.where(same_doc, scores, -1e30)
        row_top = jnp.max(scores, axis=-1, keepdims=True)
        log_total = row_top + jnp.log(jnp.sum(jnp.exp(scores - row_top), axis=-1, keepdims=True))
        soft_bf = jnp.exp(scores - log_total).astype(jnp.bfloat16)
        context = jnp.einsum("hqk,khd->qhd", soft_bf, value, preferred_element_type=jnp.float32)
        context = context.reshape(rows, width).astype(jnp.bfloat16)
        attended = dot(context, w_proj, ((1,), (1,)))
        normed, scaled_one, inverse_one = norm_forward(
            hidden + attended + row_now[0], row_now[2], row_now[3]
        )
        normed_bf = normed.astype(jnp.bfloat16)
        pre_act = dot(normed_bf, w_in, ((1,), (0,))) + col_now[2:].reshape(-1)
        activated, slope = gelu_pair(pre_act)
        activated = activated.astype(jnp.bfloat16)
        slope = slope.astype(jnp.bfloat16)
        mlp_out = dot(activated, w_out, ((1,), (1,)))
        output, scaled_two, inverse_two = norm_forward(
            normed + mlp_out + row_now[1], row_now[4], row_now[5]
        )
        saved_layers.append(
            (hidden_bf, query, key, value, log_total, context, scaled_one, inverse_one, normed_bf)
            + (slope, activated, scaled_two, inverse_two)
        )
        hidden = output
    upstream = out_grad.astype(jnp.float32)
    pieces = [None] * LAYERS
    col_parts = [None] * LAYERS
    row_parts = [None] * LAYERS
    for layer in reversed(range(LAYERS)):
        w_qkv, w_proj, w_in, w_out = layer_mats[layer]
        row_now = row_state[0, layer]
        (
            hidden_bf,
            query,
            key,
            value,
            log_total,
            context,
            scaled_one,
            inverse_one,
            normed_bf,
            slope,
            activated,
            scaled_two,
            inverse_two,
        ) = saved_layers[layer]
        d_two, gain_two, shift_two = norm_backward(upstream, scaled_two, inverse_two, row_now[4])
        grad_bias_two = jnp.sum(d_two, axis=0)
        d_two_bf = d_two.astype(jnp.bfloat16)
        grad_w_out = dot(d_two_bf, activated, ((0,), (0,)))
        d_pre = (dot(d_two_bf, w_out, ((1,), (0,))) * slope).astype(jnp.bfloat16)
        grad_bias_in = jnp.sum(d_pre, axis=0, dtype=jnp.float32)
        grad_w_in = dot(normed_bf, d_pre, ((0,), (0,)))
        d_normed = d_two + dot(d_pre, w_in, ((1,), (1,)))
        d_one, gain_one, shift_one = norm_backward(d_normed, scaled_one, inverse_one, row_now[2])
        grad_bias_proj = jnp.sum(d_one, axis=0)
        d_one_bf = d_one.astype(jnp.bfloat16)
        grad_w_proj = dot(d_one_bf, context, ((0,), (0,)))
        d_context = (
            dot(d_one_bf, w_proj, ((1,), (0,))).astype(jnp.bfloat16).reshape(rows, heads, HEAD_DIM)
        )
        scores = (
            jnp.einsum("qhd,khd->hqk", query, key, preferred_element_type=jnp.float32) * score_scale
        )
        scores = jnp.where(same_doc, scores, -1e30)
        soft = jnp.exp(scores - log_total)
        d_values = jnp.einsum(
            "hqk,qhd->khd", soft.astype(jnp.bfloat16), d_context, preferred_element_type=jnp.float32
        )
        d_probs = jnp.einsum("qhd,khd->hqk", d_context, value, preferred_element_type=jnp.float32)
        d_scores = (
            soft * (d_probs - jnp.sum(soft * d_probs, axis=-1, keepdims=True))
        ).astype(jnp.bfloat16)
        d_queries = (
            jnp.einsum("hqk,khd->qhd", d_scores, key, preferred_element_type=jnp.float32)
            * score_scale
        )
        d_keys = (
            jnp.einsum("hqk,qhd->khd", d_scores, query, preferred_element_type=jnp.float32)
            * score_scale
        )
        d_qkv = jnp.concatenate(
            [
                d_queries.reshape(rows, width),
                own_rows(d_keys.reshape(seq_len, width)),
                own_rows(d_values.reshape(seq_len, width)),
            ],
            axis=1,
        ).astype(jnp.bfloat16)
        grad_bias_qkv = jnp.sum(d_qkv, axis=0, dtype=jnp.float32)
        grad_w_qkv = dot(hidden_bf, d_qkv, ((0,), (0,)))
        upstream = d_one + dot(d_qkv, w_qkv, ((1,), (1,)))
        whole = jnp.concatenate([grad_w_qkv, grad_w_proj, grad_w_in, grad_w_out], axis=1)
        pieces[layer] = lax.psum_scatter(
            whole.astype(jnp.bfloat16), BOTH, scatter_dimension=0, tiled=True
        )
        col_parts[layer] = jnp.concatenate(
            [
                grad_bias_qkv[:width][None],
                grad_bias_qkv[2 * width :][None],
                grad_bias_in.reshape(blocks, width),
            ],
            axis=0,
        )
        row_parts[layer] = jnp.stack(
            [grad_bias_proj, grad_bias_two, gain_one, shift_one, gain_two, shift_two]
        )
    small = lax.psum(jnp.stack([jnp.stack(col_parts), jnp.stack(row_parts)]), BOTH)
    row_total = small[1]
    col_total = lax.dynamic_slice_in_dim(small[0], tensor_index * col_width, col_width, axis=2)

    summed = jnp.concatenate(
        [part.reshape(piece, per_layer, width).transpose(1, 0, 2) for part in pieces], axis=0
    )
    slot_ids = jnp.arange(slots, dtype=jnp.int32)
    named = unit_slot[None, :] == slot_ids[:, None]
    holds = jnp.any(named, axis=1)
    unit_of = jnp.argmax(named, axis=1)
    back = jnp.where(holds[:, None, None], summed[unit_of], jnp.zeros((), jnp.bfloat16))
    back = back.reshape(dp_size, slot_count, piece, tensor_size, col_width)
    back = back.transpose(0, 3, 1, 2, 4).reshape(devices, slot_count, piece, col_width)
    owned = lax.all_to_all(back, BOTH, 0, 0)
    owned = owned.transpose(1, 0, 2, 3).reshape(slot_count, width, col_width).astype(jnp.float32)
    occupied = lax.dynamic_slice_in_dim(holds, lax.axis_index("dp") * slot_count, slot_count)
    occupied = occupied.astype(jnp.float32)[:, None, None]
    new_master, new_first, new_second = adamw_update(
        masters, owned, first_moment, second_moment, RATE_UNITS
    )
    unit_master = new_master * occupied
    unit_state = jnp.stack([new_first * occupied, new_second * occupied])
    new_col, col_first, col_second = adamw_update(
        column_state[0], col_total, column_state[1], column_state[2], RATE_SMALL
    )
    column_out = jnp.stack([col_total, new_col, col_first, col_second])
    new_row, row_first, row_second = adamw_update(
        row_state[0], row_total, row_state[1], row_state[2], RATE_SMALL
    )
    row_out = jnp.stack([row_total, new_row, row_first, row_second])
    return (hidden, upstream, unit_master, unit_state, column_out, row_out)


def solution(mesh):
    return jax.shard_map(
        local,
        mesh=mesh,
        in_specs=(
            P(("dp", "tensor"), None),
            P("dp", None),
            P(),
            P("dp", None, "tensor"),
            P("dp", None, "tensor"),
            P("dp", None, "tensor"),
            P(None, None, None, "tensor"),
            P(),
            P(("dp", "tensor"), None),
        ),
        out_specs=(
            P(("dp", "tensor"), None),
            P(("dp", "tensor"), None),
            P("dp", None, "tensor"),
            P(None, "dp", None, "tensor"),
            P(None, None, None, "tensor"),
            P(),
        ),
        check_vma=False,
    )
```

```python
import functools
import math

import jax
import jax.numpy as jnp
from jax import lax
from jax.experimental import pallas as pl
from jax.experimental.pallas import tpu as pltpu
from jax.sharding import PartitionSpec as P

HEAD_DIM = 64
LAYERS = 2
STEP = 3

EPS_NORM = 1e-06
RATE_UNITS = 0.05
RATE_SMALL = 0.2
WEIGHT_DECAY = 0.01
ADAM_EPS = 1e-08
BETA_MOMENT = 0.5
BOTH = ("dp", "tensor")


def norm_forward(summed, gain, shift):
    row_mean = jnp.mean(summed, axis=1, keepdims=True)
    centred = summed - row_mean
    inverse = lax.rsqrt(jnp.mean(centred * centred, axis=1, keepdims=True) + EPS_NORM)
    scaled = centred * inverse
    return (scaled * gain + shift, scaled, inverse)


def norm_backward(upstream, scaled, inverse, gain):
    d_scaled = upstream * gain
    mean_one = jnp.mean(d_scaled, axis=1, keepdims=True)
    mean_two = jnp.mean(d_scaled * scaled, axis=1, keepdims=True)
    grad_input = inverse * (d_scaled - mean_one - scaled * mean_two)
    return (grad_input, jnp.sum(upstream * scaled, axis=0), jnp.sum(upstream, axis=0))


def gelu_pair(v):
    z = jnp.abs(v) * (2.0**-0.5)
    t = 1.0 / (1.0 + 0.5 * z)
    poly = 0.17087277
    for coefficient in (
        -0.82215223,
        1.48851587,
        -1.13520398,
        0.27886807,
        -0.18628806,
        0.09678418,
        0.37409196,
        1.00002368,
        -1.26551223,
    ):
        poly = poly * t + coefficient
    bell = jnp.exp(-0.5 * v * v)
    tail = 0.5 * t * jnp.exp(poly) * bell
    cdf = jnp.where(v >= 0.0, 1.0 - tail, tail)
    return (v * cdf, cdf + v * bell * (2.0 * math.pi) ** (-0.5))


def adamw_update(old_value, gradient, first_old, second_old, learn_rate):
    first_new = BETA_MOMENT * first_old + (1.0 - BETA_MOMENT) * gradient
    second_new = BETA_MOMENT * second_old + (1.0 - BETA_MOMENT) * gradient * gradient
    correct = 1.0 - BETA_MOMENT**STEP
    step_size = first_new / correct / (jnp.sqrt(second_new / correct) + ADAM_EPS)
    return (old_value - learn_rate * (step_size + WEIGHT_DECAY * old_value), first_new, second_new)


def dot(left, right, dims):
    return lax.dot_general(left, right, (dims, ((), ())), preferred_element_type=jnp.float32)


TILE = 256
LAG = 2


def reduce_kernel(units, sources, *refs):
    n_in = 8 * LAYERS + 1
    ins, small_in = refs[: n_in - 1], refs[n_in - 1]
    out_ref, small_out = refs[n_in : n_in + 2]
    (
        a_buf,
        b_buf,
        core_out,
        core_in,
        sum_core,
        first_in,
        sum_first,
        second_in,
        sum_second,
        z_in,
        small_sum,
        small_got,
        a_sem,
        b_sem,
        core_sems,
        first_sems,
        second_sems,
        z_sems,
        small_sems,
    ) = refs[n_in + 2 :]
    dp, tensor = lax.axis_index("dp"), lax.axis_index("tensor")
    z, y, x, c = dp // 2, dp % 2, tensor // 2, tensor % 2
    width = out_ref.shape[2]
    half = width // 2
    per_layer = units // LAYERS
    quarter, eighth, piece = half // 2, half // 4, out_ref.shape[1]
    to_core = (dp, x * 2 + 1 - c)
    to_x = (dp, (1 - x) * 2 + c)
    to_y = (z * 2 + 1 - y, tensor)
    to_z = [(((z + k) % 4) * 2 + y, tensor) for k in (1, 2, 3)]
    to_z1 = ((z + 1 - 2 * (z % 2)) * 2 + y, tensor)
    to_z2 = (((z + 2) % 4) * 2 + y, tensor)
    mesh_id = pl.DeviceIdType.MESH

    barrier = pltpu.get_barrier_semaphore()
    for peer in (to_core, to_x, to_y, *to_z):
        pl.semaphore_signal(barrier, inc=1, device_id=peer, device_id_type=mesh_id)

    def remote(src, dst, sems, send, recv, peer):
        return pltpu.make_async_remote_copy(
            src_ref=src,
            dst_ref=dst,
            send_sem=sems.at[send],
            recv_sem=sems.at[recv],
            device_id=peer,
            device_id_type=mesh_id,
        )

    loads = []
    for layer in range(LAYERS):
        for kind in range(4):
            loads.append(
                pltpu.make_async_copy(
                    ins[layer * 8 + kind], a_buf.at[layer * 4 + kind], a_sem.at[layer * 4 + kind]
                )
            )
    for load in loads:
        load.start()

    def b_copy(unit):
        slot = unit % 3
        for layer in range(LAYERS):
            start = layer * per_layer
            for kind, count in enumerate(sources):
                ref = ins[layer * 8 + 4 + kind]

                @pl.when((unit >= start) & (unit < start + count))
                def _(ref=ref, start=start):
                    cols = pl.ds(pl.multiple_of((unit - start) * width, width), width)
                    pltpu.make_async_copy(ref.at[:, cols], b_buf.at[slot], b_sem.at[slot]).start()

                start = start + count

    def b_wait(unit):
        slot = unit % 3
        pltpu.make_async_copy(ins[4].at[:, pl.ds(0, width)], b_buf.at[slot], b_sem.at[slot]).wait()

    def a_index(unit):
        layer = unit // per_layer
        j = unit % per_layer
        kind = 0
        bound = 0
        for count in sources[:-1]:
            bound = bound + count
            kind = kind + jnp.where(j >= bound, 1, 0)
        return layer * 4 + kind

    def product(unit, side, tile):
        start = pl.multiple_of(side * half + tile * TILE, TILE)
        left = a_buf[a_index(unit), :, pl.ds(start, TILE)]
        return lax.dot_general(
            left, b_buf[unit % 3], (((0,), (0,)), ((), ())), preferred_element_type=jnp.float32
        )

    def core_copy(unit):
        return remote(
            core_out.at[unit % 2],
            core_in.at[unit % 4],
            core_sems,
            (0, unit % 2),
            (1, unit % 4),
            to_core,
        )

    def first_copies(unit):
        here = sum_core.at[unit % 3]
        return (
            remote(
                here.at[pl.ds(pl.multiple_of((1 - x) * quarter, quarter), quarter), pl.ds(0, half)],
                first_in.at[unit % 4, 0],
                first_sems,
                (0, 0, unit % 3),
                (1, 0, unit % 4),
                to_x,
            ),
            *(
                remote(
                    here.at[
                        pl.ds(pl.multiple_of(i * quarter + (1 - y) * eighth, eighth), eighth),
                        pl.ds(half, half),
                    ],
                    first_in.at[unit % 4, 1, pl.ds(i * eighth, eighth)],
                    first_sems,
                    (0, 1 + i, unit % 3),
                    (1, 1 + i, unit % 4),
                    to_y,
                )
                for i in range(2)
            ),
        )

    def second_copies(unit):
        here = sum_first.at[unit % 3]
        return (
            remote(
                here.at[0, pl.ds(pl.multiple_of((1 - y) * eighth, eighth), eighth)],
                second_in.at[unit % 4, 0],
                second_sems,
                (0, 0, unit % 3),
                (1, 0, unit % 4),
                to_y,
            ),
            remote(
                here.at[1, pl.ds(pl.multiple_of((1 - x) * eighth, eighth), eighth)],
                second_in.at[unit % 4, 1],
                second_sems,
                (0, 1, unit % 3),
                (1, 1, unit % 4),
                to_x,
            ),
        )

    def z_copies(unit):
        return [
            remote(
                sum_second.at[unit % 3, pl.ds(pl.multiple_of(((z + k) % 4) * piece, piece), piece)],
                z_in.at[unit % 4, k - 1],
                z_sems,
                (0, k - 1, unit % 3),
                (1, k - 1, unit % 4),
                to_z[k - 1],
            )
            for k in (1, 2, 3)
        ]

    small_peers = (to_core, to_x, to_y, to_z1, to_z2)

    def small_copy(stage):
        return remote(
            small_sum.at[stage],
            small_got.at[stage],
            small_sems,
            (0, stage),
            (1, stage),
            small_peers[stage],
        )

    b_copy(jnp.int32(0))
    small_sum[0] = small_in[...]
    for load in loads:
        load.wait()
    pl.semaphore_wait(barrier, 6)
    small_copy(0).start()

    def step(s, carry):
        @pl.when(s < units)
        def _():
            b_wait(s)

            @pl.when(s + 1 < units)
            def _():
                b_copy(s + 1)

            @pl.when(s >= 2)
            def _():
                core_copy(s - 2).wait_send()

            def one(tile, carry):
                rows = pl.ds(pl.multiple_of(tile * TILE, TILE), TILE)
                core_out[s % 2, rows, :] = product(s, 1 - c, tile).astype(jnp.bfloat16)
                return carry

            lax.fori_loop(0, half // TILE, one, 0)
            core_copy(s).start()

        last = s - 3 * LAG - 1

        @pl.when((last >= 0) & (last < units))
        def _():
            for copy in z_copies(last):
                copy.wait()
            total = sum_second[last % 3, pl.ds(pl.multiple_of(z * piece, piece), piece), :].astype(
                jnp.float32
            )
            for k in range(3):
                total = total + z_in[last % 4, k].astype(jnp.float32)
            out_ref[last] = total.astype(out_ref.dtype)

        third = s - 2 * LAG - 1

        @pl.when((third >= 0) & (third < units))
        def _():
            for copy in second_copies(third):
                copy.wait()
            for part, side in ((0, y), (1, x)):
                mine = sum_first[
                    third % 3, part, pl.ds(pl.multiple_of(side * eighth, eighth), eighth), :
                ]
                total = mine.astype(jnp.float32) + second_in[third % 4, part].astype(jnp.float32)
                sum_second[third % 3, :, part * half : (part + 1) * half] = total.astype(
                    jnp.bfloat16
                )
            for copy in z_copies(third):
                copy.start()

        second = s - LAG - 1

        @pl.when((second >= 0) & (second < units))
        def _():
            for copy in first_copies(second):
                copy.wait()
            mine = sum_core[
                second % 3, pl.ds(pl.multiple_of(x * quarter, quarter), quarter), 0:half
            ]
            total = mine.astype(jnp.float32) + first_in[second % 4, 0].astype(jnp.float32)
            sum_first[second % 3, 0] = total.astype(jnp.bfloat16)
            for i in range(2):
                mine = sum_core[
                    second % 3,
                    pl.ds(pl.multiple_of(i * quarter + y * eighth, eighth), eighth),
                    half : 2 * half,
                ]
                rows = pl.ds(i * eighth, eighth)
                total = mine.astype(jnp.float32) + first_in[second % 4, 1, rows, :].astype(
                    jnp.float32
                )
                sum_first[second % 3, 1, rows, :] = total.astype(jnp.bfloat16)
            for copy in second_copies(second):
                copy.start()

        first = s - 1

        @pl.when((first >= 0) & (first < units))
        def _():
            core_copy(first).wait_recv()

            def one(tile, carry):
                rows = pl.ds(pl.multiple_of(tile * TILE, TILE), TILE)
                total = product(first, c, tile) + core_in[first % 4, rows, :].astype(jnp.float32)
                sum_core[first % 3, rows, :] = total.astype(jnp.bfloat16)
                return carry

            lax.fori_loop(0, half // TILE, one, 0)
            for copy in first_copies(first):
                copy.start()

        for stage in range(5):

            @pl.when(s == 2 * (stage + 1))
            def _(stage=stage):
                small_copy(stage).wait()
                total = small_sum[stage] + small_got[stage]
                if stage < 4:
                    small_sum[stage + 1] = total
                    small_copy(stage + 1).start()
                else:
                    small_out[...] = total

        return carry

    lax.fori_loop(0, units + 3 * LAG + 1, step, 0)
    for unit in (units - 2, units - 1):
        core_copy(unit).wait_send()


def reduce_pieces(operands, small, units, sources, piece, width):
    rows = operands[0].shape[0]
    half = width // 2
    low = jnp.bfloat16
    any_spec = pl.BlockSpec(memory_space=pl.ANY)
    vmem_spec = pl.BlockSpec(memory_space=pltpu.VMEM)
    dma = pltpu.SemaphoreType.DMA
    return pl.pallas_call(
        functools.partial(reduce_kernel, units, sources),
        out_shape=(
            jax.ShapeDtypeStruct((units, piece, width), low),
            jax.ShapeDtypeStruct(small.shape, jnp.float32),
        ),
        in_specs=[any_spec] * len(operands) + [vmem_spec],
        out_specs=(vmem_spec, vmem_spec),
        scratch_shapes=[
            pltpu.VMEM((4 * LAYERS, rows, width), low),
            pltpu.VMEM((3, rows, width), low),
            pltpu.VMEM((2, half, width), low),
            pltpu.VMEM((4, half, width), low),
            pltpu.VMEM((3, half, width), low),
            pltpu.VMEM((4, 2, half // 2, half), low),
            pltpu.VMEM((3, 2, half // 2, half), low),
            pltpu.VMEM((4, 2, half // 4, half), low),
            pltpu.VMEM((3, half // 4, width), low),
            pltpu.VMEM((4, 3, piece, width), low),
            pltpu.VMEM((5,) + small.shape, jnp.float32),
            pltpu.VMEM((5,) + small.shape, jnp.float32),
            dma((4 * LAYERS,)),
            dma((3,)),
            dma((2, 4)),
            dma((2, 3, 4)),
            dma((2, 2, 4)),
            dma((2, 3, 4)),
            dma((2, 5)),
        ],
        compiler_params=pltpu.CompilerParams(
            collective_id=1, has_side_effects=True, vmem_limit_bytes=60 * 1024 * 1024
        ),
        name="weight_gradients",
    )(*operands, small)


def local(
    hidden_in,
    doc_ids,
    unit_slot,
    masters,
    first_moment,
    second_moment,
    column_state,
    row_state,
    out_grad,
):
    slot_count, width, col_width = masters.shape
    units = unit_slot.shape[0]
    per_layer = units // LAYERS
    blocks = (per_layer - 4) // 2
    dp_size = lax.axis_size("dp")
    tensor_size = lax.axis_size("tensor")
    devices = dp_size * tensor_size
    slots = slot_count * dp_size
    rows = hidden_in.shape[0]
    seq_len = doc_ids.shape[1]
    heads = width // HEAD_DIM
    piece = width // devices
    share = seq_len // rows
    tensor_index = lax.axis_index("tensor")
    groups = [list(range(i, i + share)) for i in range(0, tensor_size, share)]
    score_scale = HEAD_DIM ** (-0.5)
    kernels = dp_size == 8 and tensor_size == 4 and share == 1

    sent = masters.astype(jnp.bfloat16).reshape(slot_count, devices, piece, col_width)
    spread = lax.all_to_all(sent.transpose(1, 0, 2, 3), BOTH, 0, 0)
    spread = spread.reshape(dp_size, tensor_size, slot_count, piece, col_width)
    spread = spread.transpose(0, 2, 3, 1, 4).reshape(slots, piece, width)
    mine = spread[unit_slot]
    layer_mats = []
    for layer in range(LAYERS):
        own = mine[layer * per_layer : (layer + 1) * per_layer].transpose(1, 0, 2)
        full = lax.all_gather(own.reshape(piece, per_layer * width), BOTH, axis=0, tiled=True)
        layer_mats.append(
            (
                full[:, : 3 * width],
                full[:, 3 * width : 4 * width],
                full[:, 4 * width : (4 + blocks) * width],
                full[:, (4 + blocks) * width :],
            )
        )

    row_docs = lax.dynamic_slice_in_dim(doc_ids, tensor_index // share, 1, axis=0)[0]
    my_docs = lax.dynamic_slice_in_dim(row_docs, (tensor_index % share) * rows, rows)
    same_doc = (my_docs[:, None] == row_docs[None, :])[None]

    def whole_row(value):
        if share == 1:
            return value
        return lax.all_gather(value, "tensor", axis=0, tiled=True, axis_index_groups=groups)

    def own_rows(value):
        if share == 1:
            return value
        return lax.psum_scatter(
            value, "tensor", scatter_dimension=0, tiled=True, axis_index_groups=groups
        )

    col_full = lax.all_gather(column_state[0], "tensor", axis=2, tiled=True)
    hidden = hidden_in.astype(jnp.float32)
    saved_layers = []
    for layer in range(LAYERS):
        w_qkv, w_proj, w_in, w_out = layer_mats[layer]
        row_now = row_state[0, layer]
        col_now = col_full[layer]
        hidden_bf = hidden.astype(jnp.bfloat16)
        mixed = dot(hidden_bf, w_qkv, ((1,), (0,)))
        query = (mixed[:, :width] + col_now[0]).astype(jnp.bfloat16)
        key = whole_row(mixed[:, width : 2 * width].astype(jnp.bfloat16))
        value = whole_row((mixed[:, 2 * width :] + col_now[1]).astype(jnp.bfloat16))
        query = query.reshape(rows, heads, HEAD_DIM)
        key = key.reshape(seq_len, heads, HEAD_DIM)
        value = value.reshape(seq_len, heads, HEAD_DIM)
        scores = (
            jnp.einsum("qhd,khd->hqk", query, key, preferred_element_type=jnp.float32) * score_scale
        )
        scores = jnp.where(same_doc, scores, -1e30)
        row_top = jnp.max(scores, axis=-1, keepdims=True)
        log_total = row_top + jnp.log(jnp.sum(jnp.exp(scores - row_top), axis=-1, keepdims=True))
        soft_bf = jnp.exp(scores - log_total).astype(jnp.bfloat16)
        context = jnp.einsum("hqk,khd->qhd", soft_bf, value, preferred_element_type=jnp.float32)
        context = context.reshape(rows, width).astype(jnp.bfloat16)
        attended = dot(context, w_proj, ((1,), (1,)))
        normed, scaled_one, inverse_one = norm_forward(
            hidden + attended + row_now[0], row_now[2], row_now[3]
        )
        normed_bf = normed.astype(jnp.bfloat16)
        pre_act = dot(normed_bf, w_in, ((1,), (0,))) + col_now[2:].reshape(-1)
        activated, slope = gelu_pair(pre_act)
        activated = activated.astype(jnp.bfloat16)
        slope = slope.astype(jnp.bfloat16)
        mlp_out = dot(activated, w_out, ((1,), (1,)))
        output, scaled_two, inverse_two = norm_forward(
            normed + mlp_out + row_now[1], row_now[4], row_now[5]
        )
        saved_layers.append(
            (hidden_bf, query, key, value, log_total, context, scaled_one, inverse_one, normed_bf)
            + (slope, activated, scaled_two, inverse_two)
        )
        hidden = output
    upstream = out_grad.astype(jnp.float32)
    operands = [None] * LAYERS
    col_parts = [None] * LAYERS
    row_parts = [None] * LAYERS
    for layer in reversed(range(LAYERS)):
        w_qkv, w_proj, w_in, w_out = layer_mats[layer]
        row_now = row_state[0, layer]
        (
            hidden_bf,
            query,
            key,
            value,
            log_total,
            context,
            scaled_one,
            inverse_one,
            normed_bf,
            slope,
            activated,
            scaled_two,
            inverse_two,
        ) = saved_layers[layer]
        d_two, gain_two, shift_two = norm_backward(upstream, scaled_two, inverse_two, row_now[4])
        grad_bias_two = jnp.sum(d_two, axis=0)
        d_two_bf = d_two.astype(jnp.bfloat16)
        d_pre = (dot(d_two_bf, w_out, ((1,), (0,))) * slope).astype(jnp.bfloat16)
        grad_bias_in = jnp.sum(d_pre, axis=0, dtype=jnp.float32)
        d_normed = d_two + dot(d_pre, w_in, ((1,), (1,)))
        d_one, gain_one, shift_one = norm_backward(d_normed, scaled_one, inverse_one, row_now[2])
        grad_bias_proj = jnp.sum(d_one, axis=0)
        d_one_bf = d_one.astype(jnp.bfloat16)
        d_context = (
            dot(d_one_bf, w_proj, ((1,), (0,))).astype(jnp.bfloat16).reshape(rows, heads, HEAD_DIM)
        )
        scores = (
            jnp.einsum("qhd,khd->hqk", query, key, preferred_element_type=jnp.float32) * score_scale
        )
        scores = jnp.where(same_doc, scores, -1e30)
        soft = jnp.exp(scores - log_total)
        d_values = jnp.einsum(
            "hqk,qhd->khd", soft.astype(jnp.bfloat16), d_context, preferred_element_type=jnp.float32
        )
        d_probs = jnp.einsum("qhd,khd->hqk", d_context, value, preferred_element_type=jnp.float32)
        d_scores = (
            soft * (d_probs - jnp.sum(soft * d_probs, axis=-1, keepdims=True))
        ).astype(jnp.bfloat16)
        d_queries = (
            jnp.einsum("hqk,khd->qhd", d_scores, key, preferred_element_type=jnp.float32)
            * score_scale
        )
        d_keys = (
            jnp.einsum("hqk,qhd->khd", d_scores, query, preferred_element_type=jnp.float32)
            * score_scale
        )
        d_qkv = jnp.concatenate(
            [
                d_queries.reshape(rows, width),
                own_rows(d_keys.reshape(seq_len, width)),
                own_rows(d_values.reshape(seq_len, width)),
            ],
            axis=1,
        ).astype(jnp.bfloat16)
        grad_bias_qkv = jnp.sum(d_qkv, axis=0, dtype=jnp.float32)
        upstream = d_one + dot(d_qkv, w_qkv, ((1,), (1,)))
        operands[layer] = (hidden_bf, d_one_bf, normed_bf, d_two_bf)
        operands[layer] += (d_qkv, context, d_pre, activated)
        col_parts[layer] = jnp.concatenate(
            [
                grad_bias_qkv[:width][None],
                grad_bias_qkv[2 * width :][None],
                grad_bias_in.reshape(blocks, width),
            ],
            axis=0,
        )
        row_parts[layer] = jnp.stack(
            [grad_bias_proj, grad_bias_two, gain_one, shift_one, gain_two, shift_two]
        )
    small = jnp.stack([jnp.stack(col_parts), jnp.stack(row_parts)])
    if kernels:
        flat = [array for layer in operands for array in layer]
        summed, total = reduce_pieces(
            flat, small.reshape(-1, width), units, (3, 1, blocks, blocks), piece, width
        )
        small = total.reshape(small.shape)
    else:
        summed = []
        for layer in operands:
            whole = jnp.concatenate(
                [dot(layer[i], layer[4 + i], ((0,), (0,))) for i in range(4)], axis=1
            )
            part = lax.psum_scatter(
                whole.astype(jnp.bfloat16), BOTH, scatter_dimension=0, tiled=True
            )
            summed.append(part.reshape(piece, per_layer, width).transpose(1, 0, 2))
        summed = jnp.concatenate(summed, axis=0)
        small = lax.psum(small, BOTH)
    row_total = small[1]
    col_total = lax.dynamic_slice_in_dim(small[0], tensor_index * col_width, col_width, axis=2)

    slot_ids = jnp.arange(slots, dtype=jnp.int32)
    named = unit_slot[None, :] == slot_ids[:, None]
    holds = jnp.any(named, axis=1)
    unit_of = jnp.argmax(named, axis=1)
    back = jnp.where(holds[:, None, None], summed[unit_of], jnp.zeros((), jnp.bfloat16))
    back = back.reshape(dp_size, slot_count, piece, tensor_size, col_width)
    back = back.transpose(0, 3, 1, 2, 4).reshape(devices, slot_count, piece, col_width)
    owned = lax.all_to_all(back, BOTH, 0, 0)
    if kernels:
        owned = owned.reshape(4, 2, 2, 2, slot_count, piece, col_width)
        owned = owned.transpose(4, 3, 2, 1, 0, 5, 6)
    else:
        owned = owned.transpose(1, 0, 2, 3)
    owned = owned.reshape(slot_count, width, col_width).astype(jnp.float32)
    occupied = lax.dynamic_slice_in_dim(holds, lax.axis_index("dp") * slot_count, slot_count)
    occupied = occupied.astype(jnp.float32)[:, None, None]
    new_master, new_first, new_second = adamw_update(
        masters, owned, first_moment, second_moment, RATE_UNITS
    )
    unit_master = new_master * occupied
    unit_state = jnp.stack([new_first * occupied, new_second * occupied])
    new_col, col_first, col_second = adamw_update(
        column_state[0], col_total, column_state[1], column_state[2], RATE_SMALL
    )
    column_out = jnp.stack([col_total, new_col, col_first, col_second])
    new_row, row_first, row_second = adamw_update(
        row_state[0], row_total, row_state[1], row_state[2], RATE_SMALL
    )
    row_out = jnp.stack([row_total, new_row, row_first, row_second])
    return (hidden, upstream, unit_master, unit_state, column_out, row_out)


def solution(mesh):
    return jax.shard_map(
        local,
        mesh=mesh,
        in_specs=(
            P(("dp", "tensor"), None),
            P("dp", None),
            P(),
            P("dp", None, "tensor"),
            P("dp", None, "tensor"),
            P("dp", None, "tensor"),
            P(None, None, None, "tensor"),
            P(),
            P(("dp", "tensor"), None),
        ),
        out_specs=(
            P(("dp", "tensor"), None),
            P(("dp", "tensor"), None),
            P("dp", None, "tensor"),
            P(None, "dp", None, "tensor"),
            P(None, None, None, "tensor"),
            P(),
        ),
        check_vma=False,
    )
```

```python
import functools
import math

import jax
import jax.numpy as jnp
from jax import lax
from jax.experimental import pallas as pl
from jax.experimental.pallas import tpu as pltpu
from jax.sharding import PartitionSpec as P

HEAD_DIM = 64
LAYERS = 2
STEP = 3

EPS_NORM = 1e-06
RATE_UNITS = 0.05
RATE_SMALL = 0.2
WEIGHT_DECAY = 0.01
ADAM_EPS = 1e-08
BETA_MOMENT = 0.5
BOTH = ("dp", "tensor")


def norm_forward(summed, gain, shift):
    row_mean = jnp.mean(summed, axis=1, keepdims=True)
    centred = summed - row_mean
    inverse = lax.rsqrt(jnp.mean(centred * centred, axis=1, keepdims=True) + EPS_NORM)
    scaled = centred * inverse
    return (scaled * gain + shift, scaled, inverse)


def norm_backward(upstream, scaled, inverse, gain):
    d_scaled = upstream * gain
    mean_one = jnp.mean(d_scaled, axis=1, keepdims=True)
    mean_two = jnp.mean(d_scaled * scaled, axis=1, keepdims=True)
    grad_input = inverse * (d_scaled - mean_one - scaled * mean_two)
    return (grad_input, jnp.sum(upstream * scaled, axis=0), jnp.sum(upstream, axis=0))


def gelu_pair(v):
    z = jnp.abs(v) * (2.0**-0.5)
    t = 1.0 / (1.0 + 0.5 * z)
    poly = 0.17087277
    for coefficient in (
        -0.82215223,
        1.48851587,
        -1.13520398,
        0.27886807,
        -0.18628806,
        0.09678418,
        0.37409196,
        1.00002368,
        -1.26551223,
    ):
        poly = poly * t + coefficient
    bell = jnp.exp(-0.5 * v * v)
    tail = 0.5 * t * jnp.exp(poly) * bell
    cdf = jnp.where(v >= 0.0, 1.0 - tail, tail)
    return (v * cdf, cdf + v * bell * (2.0 * math.pi) ** (-0.5))


def adamw_update(old_value, gradient, first_old, second_old, learn_rate):
    first_new = BETA_MOMENT * first_old + (1.0 - BETA_MOMENT) * gradient
    second_new = BETA_MOMENT * second_old + (1.0 - BETA_MOMENT) * gradient * gradient
    correct = 1.0 - BETA_MOMENT**STEP
    step_size = first_new / correct / (jnp.sqrt(second_new / correct) + ADAM_EPS)
    return (old_value - learn_rate * (step_size + WEIGHT_DECAY * old_value), first_new, second_new)


def dot(left, right, dims):
    return lax.dot_general(left, right, (dims, ((), ())), preferred_element_type=jnp.float32)


TILE = 256
LAG = 2


def reduce_kernel(units, sources, *refs):
    n_in = 8 * LAYERS + 1
    ins, small_in = refs[: n_in - 1], refs[n_in - 1]
    out_ref, small_out = refs[n_in : n_in + 2]
    (
        a_buf,
        b_buf,
        core_out,
        core_in,
        sum_core,
        first_in,
        sum_first,
        second_in,
        sum_second,
        z_in,
        small_sum,
        small_got,
        a_sem,
        b_sem,
        core_sems,
        first_sems,
        second_sems,
        z_sems,
        small_sems,
    ) = refs[n_in + 2 :]
    dp, tensor = lax.axis_index("dp"), lax.axis_index("tensor")
    z, y, x, c = dp // 2, dp % 2, tensor // 2, tensor % 2
    width = out_ref.shape[2]
    half = width // 2
    per_layer = units // LAYERS
    quarter, eighth, piece = half // 2, half // 4, out_ref.shape[1]
    to_core = (dp, x * 2 + 1 - c)
    to_x = (dp, (1 - x) * 2 + c)
    to_y = (z * 2 + 1 - y, tensor)
    to_z = [(((z + k) % 4) * 2 + y, tensor) for k in (1, 2, 3)]
    to_z1 = ((z + 1 - 2 * (z % 2)) * 2 + y, tensor)
    to_z2 = (((z + 2) % 4) * 2 + y, tensor)
    mesh_id = pl.DeviceIdType.MESH

    barrier = pltpu.get_barrier_semaphore()
    for peer in (to_core, to_x, to_y, *to_z):
        pl.semaphore_signal(barrier, inc=1, device_id=peer, device_id_type=mesh_id)

    def remote(src, dst, sems, send, recv, peer):
        return pltpu.make_async_remote_copy(
            src_ref=src,
            dst_ref=dst,
            send_sem=sems.at[send],
            recv_sem=sems.at[recv],
            device_id=peer,
            device_id_type=mesh_id,
        )

    loads = []
    for layer in range(LAYERS):
        for kind in range(4):
            loads.append(
                pltpu.make_async_copy(
                    ins[layer * 8 + kind], a_buf.at[layer * 4 + kind], a_sem.at[layer * 4 + kind]
                )
            )
    for load in loads:
        load.start()

    def b_copy(unit):
        slot = unit % 3
        for layer in range(LAYERS):
            start = layer * per_layer
            for kind, count in enumerate(sources):
                ref = ins[layer * 8 + 4 + kind]

                @pl.when((unit >= start) & (unit < start + count))
                def _(ref=ref, start=start):
                    pltpu.make_async_copy(
                        ref.at[unit - start], b_buf.at[slot], b_sem.at[slot]
                    ).start()

                start = start + count

    def b_wait(unit):
        slot = unit % 3
        pltpu.make_async_copy(ins[4].at[0], b_buf.at[slot], b_sem.at[slot]).wait()

    def a_index(unit):
        layer = unit // per_layer
        j = unit % per_layer
        kind = 0
        bound = 0
        for count in sources[:-1]:
            bound = bound + count
            kind = kind + jnp.where(j >= bound, 1, 0)
        return layer * 4 + kind

    def product(unit, side, tile):
        start = pl.multiple_of(side * half + tile * TILE, TILE)
        left = a_buf[a_index(unit), :, pl.ds(start, TILE)]
        return lax.dot_general(
            left, b_buf[unit % 3], (((0,), (0,)), ((), ())), preferred_element_type=jnp.float32
        )

    def core_copy(unit):
        return remote(
            core_out.at[unit % 2],
            core_in.at[unit % 4],
            core_sems,
            (0, unit % 2),
            (1, unit % 4),
            to_core,
        )

    def first_copies(unit):
        here = sum_core.at[unit % 3]
        return (
            remote(
                here.at[pl.ds(pl.multiple_of((1 - x) * quarter, quarter), quarter), pl.ds(0, half)],
                first_in.at[unit % 4, 0],
                first_sems,
                (0, 0, unit % 3),
                (1, 0, unit % 4),
                to_x,
            ),
            *(
                remote(
                    here.at[
                        pl.ds(pl.multiple_of(i * quarter + (1 - y) * eighth, eighth), eighth),
                        pl.ds(half, half),
                    ],
                    first_in.at[unit % 4, 1, pl.ds(i * eighth, eighth)],
                    first_sems,
                    (0, 1 + i, unit % 3),
                    (1, 1 + i, unit % 4),
                    to_y,
                )
                for i in range(2)
            ),
        )

    def second_copies(unit):
        here = sum_first.at[unit % 3]
        return (
            remote(
                here.at[0, pl.ds(pl.multiple_of((1 - y) * eighth, eighth), eighth)],
                second_in.at[unit % 4, 0],
                second_sems,
                (0, 0, unit % 3),
                (1, 0, unit % 4),
                to_y,
            ),
            remote(
                here.at[1, pl.ds(pl.multiple_of((1 - x) * eighth, eighth), eighth)],
                second_in.at[unit % 4, 1],
                second_sems,
                (0, 1, unit % 3),
                (1, 1, unit % 4),
                to_x,
            ),
        )

    def z_copies(unit):
        return [
            remote(
                sum_second.at[unit % 3, pl.ds(pl.multiple_of(((z + k) % 4) * piece, piece), piece)],
                z_in.at[unit % 4, k - 1],
                z_sems,
                (0, k - 1, unit % 3),
                (1, k - 1, unit % 4),
                to_z[k - 1],
            )
            for k in (1, 2, 3)
        ]

    small_peers = (to_core, to_x, to_y, to_z1, to_z2)

    def small_copy(stage):
        return remote(
            small_sum.at[stage],
            small_got.at[stage],
            small_sems,
            (0, stage),
            (1, stage),
            small_peers[stage],
        )

    b_copy(jnp.int32(0))
    small_sum[0] = small_in[...]
    for load in loads:
        load.wait()
    pl.semaphore_wait(barrier, 6)
    small_copy(0).start()

    def step(s, carry):
        @pl.when(s < units)
        def _():
            b_wait(s)

            @pl.when(s + 1 < units)
            def _():
                b_copy(s + 1)

            @pl.when(s >= 2)
            def _():
                core_copy(s - 2).wait_send()

            def one(tile, carry):
                rows = pl.ds(pl.multiple_of(tile * TILE, TILE), TILE)
                core_out[s % 2, rows, :] = product(s, 1 - c, tile).astype(jnp.bfloat16)
                return carry

            lax.fori_loop(0, half // TILE, one, 0)
            core_copy(s).start()

        last = s - 3 * LAG - 1

        @pl.when((last >= 0) & (last < units))
        def _():
            for copy in z_copies(last):
                copy.wait()
            total = sum_second[last % 3, pl.ds(pl.multiple_of(z * piece, piece), piece), :].astype(
                jnp.float32
            )
            for k in range(3):
                total = total + z_in[last % 4, k].astype(jnp.float32)
            out_ref[last] = total.astype(out_ref.dtype)

        third = s - 2 * LAG - 1

        @pl.when((third >= 0) & (third < units))
        def _():
            for copy in second_copies(third):
                copy.wait()
            for part, side in ((0, y), (1, x)):
                mine = sum_first[
                    third % 3, part, pl.ds(pl.multiple_of(side * eighth, eighth), eighth), :
                ]
                total = mine.astype(jnp.float32) + second_in[third % 4, part].astype(jnp.float32)
                sum_second[third % 3, :, part * half : (part + 1) * half] = total.astype(
                    jnp.bfloat16
                )
            for copy in z_copies(third):
                copy.start()

        second = s - LAG - 1

        @pl.when((second >= 0) & (second < units))
        def _():
            for copy in first_copies(second):
                copy.wait()
            mine = sum_core[
                second % 3, pl.ds(pl.multiple_of(x * quarter, quarter), quarter), 0:half
            ]
            total = mine.astype(jnp.float32) + first_in[second % 4, 0].astype(jnp.float32)
            sum_first[second % 3, 0] = total.astype(jnp.bfloat16)
            for i in range(2):
                mine = sum_core[
                    second % 3,
                    pl.ds(pl.multiple_of(i * quarter + y * eighth, eighth), eighth),
                    half : 2 * half,
                ]
                rows = pl.ds(i * eighth, eighth)
                total = mine.astype(jnp.float32) + first_in[second % 4, 1, rows, :].astype(
                    jnp.float32
                )
                sum_first[second % 3, 1, rows, :] = total.astype(jnp.bfloat16)
            for copy in second_copies(second):
                copy.start()

        first = s - 1

        @pl.when((first >= 0) & (first < units))
        def _():
            core_copy(first).wait_recv()

            def one(tile, carry):
                rows = pl.ds(pl.multiple_of(tile * TILE, TILE), TILE)
                total = product(first, c, tile) + core_in[first % 4, rows, :].astype(jnp.float32)
                sum_core[first % 3, rows, :] = total.astype(jnp.bfloat16)
                return carry

            lax.fori_loop(0, half // TILE, one, 0)
            for copy in first_copies(first):
                copy.start()

        for stage in range(5):

            @pl.when(s == 2 * (stage + 1))
            def _(stage=stage):
                small_copy(stage).wait()
                total = small_sum[stage] + small_got[stage]
                if stage < 4:
                    small_sum[stage + 1] = total
                    small_copy(stage + 1).start()
                else:
                    small_out[...] = total

        return carry

    lax.fori_loop(0, units + 3 * LAG + 1, step, 0)
    for unit in (units - 2, units - 1):
        core_copy(unit).wait_send()


def reduce_pieces(operands, small, units, sources, piece, width):
    rows = operands[0].shape[0]
    half = width // 2
    low = jnp.bfloat16
    any_spec = pl.BlockSpec(memory_space=pl.ANY)
    vmem_spec = pl.BlockSpec(memory_space=pltpu.VMEM)
    dma = pltpu.SemaphoreType.DMA
    return pl.pallas_call(
        functools.partial(reduce_kernel, units, sources),
        out_shape=(
            jax.ShapeDtypeStruct((units, piece, width), low),
            jax.ShapeDtypeStruct(small.shape, jnp.float32),
        ),
        in_specs=[any_spec] * len(operands) + [vmem_spec],
        out_specs=(vmem_spec, vmem_spec),
        scratch_shapes=[
            pltpu.VMEM((4 * LAYERS, rows, width), low),
            pltpu.VMEM((3, rows, width), low),
            pltpu.VMEM((2, half, width), low),
            pltpu.VMEM((4, half, width), low),
            pltpu.VMEM((3, half, width), low),
            pltpu.VMEM((4, 2, half // 2, half), low),
            pltpu.VMEM((3, 2, half // 2, half), low),
            pltpu.VMEM((4, 2, half // 4, half), low),
            pltpu.VMEM((3, half // 4, width), low),
            pltpu.VMEM((4, 3, piece, width), low),
            pltpu.VMEM((5,) + small.shape, jnp.float32),
            pltpu.VMEM((5,) + small.shape, jnp.float32),
            dma((4 * LAYERS,)),
            dma((3,)),
            dma((2, 4)),
            dma((2, 3, 4)),
            dma((2, 2, 4)),
            dma((2, 3, 4)),
            dma((2, 5)),
        ],
        compiler_params=pltpu.CompilerParams(
            collective_id=1, has_side_effects=True, vmem_limit_bytes=60 * 1024 * 1024
        ),
        name="weight_gradients",
    )(*operands, small)


def gather_kernel(own_ref, out_ref, own_sem, sems):
    units, piece, width = own_ref.shape
    dp, tensor = lax.axis_index("dp"), lax.axis_index("tensor")
    z, y, x, c = dp // 2, dp % 2, tensor // 2, tensor % 2
    half = width // 2
    line, plane = 4 * piece, 8 * piece
    to_core = (dp, x * 2 + 1 - c)
    to_x = (dp, (1 - x) * 2 + c)
    to_y = (z * 2 + 1 - y, tensor)
    to_z = [(((z + k) % 4) * 2 + y, tensor) for k in (1, 2, 3)]
    mesh_id = pl.DeviceIdType.MESH

    barrier = pltpu.get_barrier_semaphore()
    for peer in (to_core, to_x, to_y, *to_z):
        pl.semaphore_signal(barrier, inc=1, device_id=peer, device_id_type=mesh_id)
    pl.semaphore_wait(barrier, 6)

    my_line = pl.multiple_of(((c * 2 + x) * 2 + y) * line, line)
    my_rows = pl.ds(pl.multiple_of(my_line + z * piece, piece), piece)
    first, second = pl.ds(0, half), pl.ds(half, half)

    def remote(src, dst, index, unit, peer):
        return pltpu.make_async_remote_copy(
            src_ref=src,
            dst_ref=dst,
            send_sem=sems.at[0, index, unit],
            recv_sem=sems.at[1, index, unit],
            device_id=peer,
            device_id_type=mesh_id,
        )

    def own_copy(unit):
        return pltpu.make_async_copy(own_ref.at[unit], out_ref.at[unit, my_rows], own_sem.at[unit])

    def stage_z(unit):
        there = out_ref.at[unit, my_rows]
        return [remote(own_ref.at[unit], there, k, unit, to_z[k]) for k in range(3)]

    def stage_one(unit):
        rows = pl.ds(my_line, line)
        one, two = out_ref.at[unit, rows, first], out_ref.at[unit, rows, second]
        return [remote(one, one, 3, unit, to_y), remote(two, two, 4, unit, to_x)]

    def stage_two(unit):
        rows = pl.ds(pl.multiple_of((c * 2 + x) * plane, plane), plane)
        one = out_ref.at[unit, rows, first]
        copies = [remote(one, one, 5, unit, to_x)]
        for i in range(2):
            rows = pl.ds(pl.multiple_of(((c * 2 + i) * 2 + y) * line, line), line)
            two = out_ref.at[unit, rows, second]
            copies.append(remote(two, two, 6 + i, unit, to_y))
        return copies

    def stage_core(unit):
        there = out_ref.at[unit, pl.ds(pl.multiple_of(c * 2 * plane, 2 * plane), 2 * plane)]
        return [remote(there, there, 8, unit, to_core)]

    stages = (stage_z, stage_one, stage_two, stage_core)

    def step(s, carry):
        for number in range(len(stages) + 1):
            unit = s - number * LAG

            @pl.when((unit >= 0) & (unit < units))
            def _(unit=unit, number=number):
                if number == 0:
                    own_copy(unit).start()
                else:
                    if number == 1:
                        own_copy(unit).wait()
                    for copy in stages[number - 1](unit):
                        copy.wait()
                if number < len(stages):
                    for copy in stages[number](unit):
                        copy.start()

        return carry

    lax.fori_loop(0, units + len(stages) * LAG, step, 0)


def gather_pieces(own):
    units, piece, width = own.shape
    any_spec = pl.BlockSpec(memory_space=pl.ANY)
    return pl.pallas_call(
        gather_kernel,
        out_shape=jax.ShapeDtypeStruct((units, width, width), own.dtype),
        in_specs=[any_spec],
        out_specs=any_spec,
        scratch_shapes=[
            pltpu.SemaphoreType.DMA((units,)),
            pltpu.SemaphoreType.DMA((2, 9, units)),
        ],
        compiler_params=pltpu.CompilerParams(collective_id=2, has_side_effects=True),
        name="gather_weights",
    )(own)


def local(
    hidden_in,
    doc_ids,
    unit_slot,
    masters,
    first_moment,
    second_moment,
    column_state,
    row_state,
    out_grad,
):
    slot_count, width, col_width = masters.shape
    units = unit_slot.shape[0]
    per_layer = units // LAYERS
    blocks = (per_layer - 4) // 2
    dp_size = lax.axis_size("dp")
    tensor_size = lax.axis_size("tensor")
    devices = dp_size * tensor_size
    slots = slot_count * dp_size
    rows = hidden_in.shape[0]
    seq_len = doc_ids.shape[1]
    heads = width // HEAD_DIM
    piece = width // devices
    share = seq_len // rows
    tensor_index = lax.axis_index("tensor")
    groups = [list(range(i, i + share)) for i in range(0, tensor_size, share)]
    score_scale = HEAD_DIM ** (-0.5)
    kernels = dp_size == 8 and tensor_size == 4 and share == 1

    sent = masters.astype(jnp.bfloat16)
    if kernels:
        sent = sent.reshape(slot_count, 2, 2, 2, 4, piece, col_width)
        sent = sent.transpose(4, 3, 2, 1, 0, 5, 6)
    else:
        sent = sent.reshape(slot_count, devices, piece, col_width).transpose(1, 0, 2, 3)
    spread = lax.all_to_all(sent.reshape(devices, slot_count, piece, col_width), BOTH, 0, 0)
    spread = spread.reshape(dp_size, tensor_size, slot_count, piece, col_width)
    spread = spread.transpose(0, 2, 3, 1, 4).reshape(slots, piece, width)
    mine = spread[unit_slot]
    if kernels:
        weights = gather_pieces(mine)
    else:
        weights = jnp.concatenate(
            [
                lax.all_gather(
                    mine[layer * per_layer : (layer + 1) * per_layer], BOTH, axis=1, tiled=True
                )
                for layer in range(LAYERS)
            ],
            axis=0,
        )

    def matrices(layer):
        unit = weights[layer * per_layer : (layer + 1) * per_layer]
        return (unit[:3], unit[3], unit[4 : 4 + blocks], unit[4 + blocks :])

    row_docs = lax.dynamic_slice_in_dim(doc_ids, tensor_index // share, 1, axis=0)[0]
    my_docs = lax.dynamic_slice_in_dim(row_docs, (tensor_index % share) * rows, rows)
    same_doc = (my_docs[:, None] == row_docs[None, :])[None]

    def whole_row(value):
        if share == 1:
            return value
        return lax.all_gather(value, "tensor", axis=0, tiled=True, axis_index_groups=groups)

    def own_rows(value):
        if share == 1:
            return value
        return lax.psum_scatter(
            value, "tensor", scatter_dimension=0, tiled=True, axis_index_groups=groups
        )

    col_full = lax.all_gather(column_state[0], "tensor", axis=2, tiled=True)
    hidden = hidden_in.astype(jnp.float32)
    saved_layers = []
    for layer in range(LAYERS):
        w_qkv, w_proj, w_in, w_out = matrices(layer)
        row_now = row_state[0, layer]
        col_now = col_full[layer]
        hidden_bf = hidden.astype(jnp.bfloat16)
        query, key, value = (dot(hidden_bf, w_qkv[i], ((1,), (0,))) for i in range(3))
        query = (query + col_now[0]).astype(jnp.bfloat16)
        key = whole_row(key.astype(jnp.bfloat16))
        value = whole_row((value + col_now[1]).astype(jnp.bfloat16))
        query = query.reshape(rows, heads, HEAD_DIM)
        key = key.reshape(seq_len, heads, HEAD_DIM)
        value = value.reshape(seq_len, heads, HEAD_DIM)
        scores = (
            jnp.einsum("qhd,khd->hqk", query, key, preferred_element_type=jnp.float32) * score_scale
        )
        scores = jnp.where(same_doc, scores, -1e30)
        row_top = jnp.max(scores, axis=-1, keepdims=True)
        log_total = row_top + jnp.log(jnp.sum(jnp.exp(scores - row_top), axis=-1, keepdims=True))
        soft_bf = jnp.exp(scores - log_total).astype(jnp.bfloat16)
        context = jnp.einsum("hqk,khd->qhd", soft_bf, value, preferred_element_type=jnp.float32)
        context = context.reshape(rows, width).astype(jnp.bfloat16)
        attended = dot(context, w_proj, ((1,), (1,)))
        normed, scaled_one, inverse_one = norm_forward(
            hidden + attended + row_now[0], row_now[2], row_now[3]
        )
        normed_bf = normed.astype(jnp.bfloat16)
        pre_act = jnp.einsum("rd,bdc->brc", normed_bf, w_in, preferred_element_type=jnp.float32)
        pre_act = pre_act + col_now[2:, None]
        activated, slope = gelu_pair(pre_act)
        activated = activated.astype(jnp.bfloat16)
        slope = slope.astype(jnp.bfloat16)
        mlp_out = jnp.einsum("brc,bdc->rd", activated, w_out, preferred_element_type=jnp.float32)
        output, scaled_two, inverse_two = norm_forward(
            normed + mlp_out + row_now[1], row_now[4], row_now[5]
        )
        saved_layers.append(
            (hidden_bf, query, key, value, log_total, context, scaled_one, inverse_one, normed_bf)
            + (slope, activated, scaled_two, inverse_two)
        )
        hidden = output
    upstream = out_grad.astype(jnp.float32)
    operands = [None] * LAYERS
    col_parts = [None] * LAYERS
    row_parts = [None] * LAYERS
    for layer in reversed(range(LAYERS)):
        w_qkv, w_proj, w_in, w_out = matrices(layer)
        row_now = row_state[0, layer]
        (
            hidden_bf,
            query,
            key,
            value,
            log_total,
            context,
            scaled_one,
            inverse_one,
            normed_bf,
            slope,
            activated,
            scaled_two,
            inverse_two,
        ) = saved_layers[layer]
        d_two, gain_two, shift_two = norm_backward(upstream, scaled_two, inverse_two, row_now[4])
        grad_bias_two = jnp.sum(d_two, axis=0)
        d_two_bf = d_two.astype(jnp.bfloat16)
        d_act = jnp.einsum("rd,bdc->brc", d_two_bf, w_out, preferred_element_type=jnp.float32)
        d_pre = (d_act * slope).astype(jnp.bfloat16)
        grad_bias_in = jnp.sum(d_pre, axis=1, dtype=jnp.float32)
        d_normed = d_two + jnp.einsum(
            "brc,bdc->rd", d_pre, w_in, preferred_element_type=jnp.float32
        )
        d_one, gain_one, shift_one = norm_backward(d_normed, scaled_one, inverse_one, row_now[2])
        grad_bias_proj = jnp.sum(d_one, axis=0)
        d_one_bf = d_one.astype(jnp.bfloat16)
        d_context = (
            dot(d_one_bf, w_proj, ((1,), (0,))).astype(jnp.bfloat16).reshape(rows, heads, HEAD_DIM)
        )
        scores = (
            jnp.einsum("qhd,khd->hqk", query, key, preferred_element_type=jnp.float32) * score_scale
        )
        scores = jnp.where(same_doc, scores, -1e30)
        soft = jnp.exp(scores - log_total)
        d_values = jnp.einsum(
            "hqk,qhd->khd", soft.astype(jnp.bfloat16), d_context, preferred_element_type=jnp.float32
        )
        d_probs = jnp.einsum("qhd,khd->hqk", d_context, value, preferred_element_type=jnp.float32)
        d_scores = (
            soft * (d_probs - jnp.sum(soft * d_probs, axis=-1, keepdims=True))
        ).astype(jnp.bfloat16)
        d_queries = (
            jnp.einsum("hqk,khd->qhd", d_scores, key, preferred_element_type=jnp.float32)
            * score_scale
        )
        d_keys = (
            jnp.einsum("hqk,qhd->khd", d_scores, query, preferred_element_type=jnp.float32)
            * score_scale
        )
        d_qkv = jnp.stack(
            [
                d_queries.reshape(rows, width),
                own_rows(d_keys.reshape(seq_len, width)),
                own_rows(d_values.reshape(seq_len, width)),
            ]
        ).astype(jnp.bfloat16)
        grad_bias_qkv = jnp.sum(d_qkv, axis=1, dtype=jnp.float32)
        upstream = d_one + jnp.einsum(
            "brc,bdc->rd", d_qkv, w_qkv, preferred_element_type=jnp.float32
        )
        operands[layer] = (hidden_bf, d_one_bf, normed_bf, d_two_bf)
        operands[layer] += (d_qkv, context[None], d_pre, activated)
        col_parts[layer] = jnp.concatenate(
            [
                grad_bias_qkv[0:1],
                grad_bias_qkv[2:3],
                grad_bias_in,
            ],
            axis=0,
        )
        row_parts[layer] = jnp.stack(
            [grad_bias_proj, grad_bias_two, gain_one, shift_one, gain_two, shift_two]
        )
    small = jnp.stack([jnp.stack(col_parts), jnp.stack(row_parts)])
    if kernels:
        flat = [array for layer in operands for array in layer]
        summed, total = reduce_pieces(
            flat, small.reshape(-1, width), units, (3, 1, blocks, blocks), piece, width
        )
        small = total.reshape(small.shape)
    else:
        summed = []
        for layer in operands:
            whole = jnp.concatenate(
                [
                    jnp.einsum(
                        "rd,brc->bdc", layer[i], layer[4 + i], preferred_element_type=jnp.float32
                    )
                    for i in range(4)
                ],
                axis=0,
            )
            summed.append(
                lax.psum_scatter(
                    whole.astype(jnp.bfloat16), BOTH, scatter_dimension=1, tiled=True
                )
            )
        summed = jnp.concatenate(summed, axis=0)
        small = lax.psum(small, BOTH)
    row_total = small[1]
    col_total = lax.dynamic_slice_in_dim(small[0], tensor_index * col_width, col_width, axis=2)

    slot_ids = jnp.arange(slots, dtype=jnp.int32)
    named = unit_slot[None, :] == slot_ids[:, None]
    holds = jnp.any(named, axis=1)
    unit_of = jnp.argmax(named, axis=1)
    back = jnp.where(holds[:, None, None], summed[unit_of], jnp.zeros((), jnp.bfloat16))
    back = back.reshape(dp_size, slot_count, piece, tensor_size, col_width)
    back = back.transpose(0, 3, 1, 2, 4).reshape(devices, slot_count, piece, col_width)
    owned = lax.all_to_all(back, BOTH, 0, 0)
    if kernels:
        owned = owned.reshape(4, 2, 2, 2, slot_count, piece, col_width)
        owned = owned.transpose(4, 3, 2, 1, 0, 5, 6)
    else:
        owned = owned.transpose(1, 0, 2, 3)
    owned = owned.reshape(slot_count, width, col_width).astype(jnp.float32)
    occupied = lax.dynamic_slice_in_dim(holds, lax.axis_index("dp") * slot_count, slot_count)
    occupied = occupied.astype(jnp.float32)[:, None, None]
    new_master, new_first, new_second = adamw_update(
        masters, owned, first_moment, second_moment, RATE_UNITS
    )
    unit_master = new_master * occupied
    unit_state = jnp.stack([new_first * occupied, new_second * occupied])
    new_col, col_first, col_second = adamw_update(
        column_state[0], col_total, column_state[1], column_state[2], RATE_SMALL
    )
    column_out = jnp.stack([col_total, new_col, col_first, col_second])
    new_row, row_first, row_second = adamw_update(
        row_state[0], row_total, row_state[1], row_state[2], RATE_SMALL
    )
    row_out = jnp.stack([row_total, new_row, row_first, row_second])
    return (hidden, upstream, unit_master, unit_state, column_out, row_out)


def solution(mesh):
    return jax.shard_map(
        local,
        mesh=mesh,
        in_specs=(
            P(("dp", "tensor"), None),
            P("dp", None),
            P(),
            P("dp", None, "tensor"),
            P("dp", None, "tensor"),
            P("dp", None, "tensor"),
            P(None, None, None, "tensor"),
            P(),
            P(("dp", "tensor"), None),
        ),
        out_specs=(
            P(("dp", "tensor"), None),
            P(("dp", "tensor"), None),
            P("dp", None, "tensor"),
            P(None, "dp", None, "tensor"),
            P(None, None, None, "tensor"),
            P(),
        ),
        check_vma=False,
    )
```

```python
import functools
import math

import jax
import jax.numpy as jnp
from jax import lax
from jax.experimental import pallas as pl
from jax.experimental.pallas import tpu as pltpu
from jax.sharding import PartitionSpec as P

HEAD_DIM = 64
LAYERS = 2
STEP = 3

EPS_NORM = 1e-06
RATE_UNITS = 0.05
RATE_SMALL = 0.2
WEIGHT_DECAY = 0.01
ADAM_EPS = 1e-08
BETA_MOMENT = 0.5
BOTH = ("dp", "tensor")


def norm_forward(summed, gain, shift):
    row_mean = jnp.mean(summed, axis=1, keepdims=True)
    centred = summed - row_mean
    inverse = lax.rsqrt(jnp.mean(centred * centred, axis=1, keepdims=True) + EPS_NORM)
    scaled = centred * inverse
    return (scaled * gain + shift, scaled, inverse)


def norm_backward(upstream, scaled, inverse, gain):
    d_scaled = upstream * gain
    mean_one = jnp.mean(d_scaled, axis=1, keepdims=True)
    mean_two = jnp.mean(d_scaled * scaled, axis=1, keepdims=True)
    grad_input = inverse * (d_scaled - mean_one - scaled * mean_two)
    return (grad_input, jnp.sum(upstream * scaled, axis=0), jnp.sum(upstream, axis=0))


def gelu_pair(v):
    cdf = 0.5 * (1.0 + lax.erf(v * 2.0 ** (-0.5)))
    bell = jnp.exp(-0.5 * v * v) * (2.0 * math.pi) ** (-0.5)
    return (v * cdf, cdf + v * bell)


def adamw_update(old_value, gradient, first_old, second_old, learn_rate):
    first_new = BETA_MOMENT * first_old + (1.0 - BETA_MOMENT) * gradient
    second_new = BETA_MOMENT * second_old + (1.0 - BETA_MOMENT) * gradient * gradient
    correct = 1.0 - BETA_MOMENT**STEP
    step_size = first_new / correct / (jnp.sqrt(second_new / correct) + ADAM_EPS)
    return (old_value - learn_rate * (step_size + WEIGHT_DECAY * old_value), first_new, second_new)


def dot(left, right, dims):
    return lax.dot_general(left, right, (dims, ((), ())), preferred_element_type=jnp.float32)


LANES = 2 * HEAD_DIM


def head_lanes(value, head):
    lane = lax.broadcasted_iota(jnp.int32, value.shape, 1)
    keep = lane < HEAD_DIM if head == 0 else lane >= HEAD_DIM
    return jnp.where(keep, value, jnp.zeros_like(value))


def pair_lanes(first, second):
    lane = lax.broadcasted_iota(jnp.int32, first.shape, 1)
    return jnp.where(lane < HEAD_DIM, first, second)


def attend_pair(pair, q_ref, k_ref, v_ref, mask_ref, ctx_ref, lse_ref):
    lanes = pl.ds(pl.multiple_of(pair * LANES, LANES), LANES)
    query, key, value = q_ref[:, lanes], k_ref[:, lanes], v_ref[:, lanes]
    value_t = value.T
    parts = []
    for head in range(2):
        scores = dot(head_lanes(key, head), query, ((1,), (1,))) + mask_ref[...]
        top = jnp.max(scores, axis=0, keepdims=True)
        weight = jnp.exp(scores - top)
        total = jnp.sum(weight, axis=0, keepdims=True)
        lse_ref[pair * 2 + head] = top + jnp.log(total)
        mine = value_t[head * HEAD_DIM : (head + 1) * HEAD_DIM]
        mixed = dot(mine, weight.astype(jnp.bfloat16), ((1,), (0,)))
        parts.append(mixed * (1.0 / total))
    ctx_ref[:, lanes] = jnp.concatenate(parts, axis=0).T.astype(ctx_ref.dtype)


def attend_back_pair(pair, q_ref, k_ref, v_ref, d_ref, mask_ref, lse_ref, dq_ref, dk_ref, dv_ref):
    lanes = pl.ds(pl.multiple_of(pair * LANES, LANES), LANES)
    query, key, value = q_ref[:, lanes], k_ref[:, lanes], v_ref[:, lanes]
    grad = d_ref[:, lanes]
    key_t = key.T
    parts, d_keys, d_values = [], [], []
    for head in range(2):
        scores = dot(head_lanes(key, head), query, ((1,), (1,))) + mask_ref[...]
        soft = jnp.exp(scores - lse_ref[pair * 2 + head])
        d_values.append(dot(soft.astype(jnp.bfloat16), grad, ((1,), (0,))))
        d_soft = dot(head_lanes(value, head), grad, ((1,), (1,)))
        both = soft * d_soft
        mean = jnp.sum(both, axis=0, keepdims=True)
        d_scores = (both - soft * mean).astype(jnp.bfloat16)
        d_keys.append(dot(d_scores, query, ((1,), (0,))))
        mine = key_t[head * HEAD_DIM : (head + 1) * HEAD_DIM]
        parts.append(dot(mine, d_scores, ((1,), (0,))))
    scale = HEAD_DIM ** (-0.5)
    dq_ref[:, lanes] = (jnp.concatenate(parts, axis=0).T * scale).astype(dq_ref.dtype)
    dk_ref[:, lanes] = pair_lanes(*d_keys).astype(dk_ref.dtype)
    dv_ref[:, lanes] = pair_lanes(*d_values).astype(dv_ref.dtype)


def fill_mask(mask_ref, docs_col_ref, docs_row_ref):
    same = docs_col_ref[...] == docs_row_ref[...]
    mask_ref[...] = jnp.where(same, 0.0, -1e30).astype(jnp.float32)


def attend_kernel(q_ref, k_ref, v_ref, col_ref, row_ref, ctx_ref, lse_ref, mask_ref):
    fill_mask(mask_ref, col_ref, row_ref)

    def two(step, carry):
        for pair in (2 * step, 2 * step + 1):
            attend_pair(pair, q_ref, k_ref, v_ref, mask_ref, ctx_ref, lse_ref)
        return carry

    lax.fori_loop(0, q_ref.shape[1] // (2 * LANES), two, 0)


def attend_back_kernel(
    q_ref, k_ref, v_ref, d_ref, lse_ref, col_ref, row_ref, out_ref, mask_ref
):
    fill_mask(mask_ref, col_ref, row_ref)

    grads = [out_ref.at[i] for i in range(3)]

    def two(step, carry):
        for pair in (2 * step, 2 * step + 1):
            attend_back_pair(pair, q_ref, k_ref, v_ref, d_ref, mask_ref, lse_ref, *grads)
        return carry

    lax.fori_loop(0, q_ref.shape[1] // (2 * LANES), two, 0)


def attend(query, key, value, docs):
    rows, width = query.shape
    return pl.pallas_call(
        attend_kernel,
        out_shape=(
            jax.ShapeDtypeStruct((rows, width), jnp.bfloat16),
            jax.ShapeDtypeStruct((width // HEAD_DIM, 1, rows), jnp.float32),
        ),
        scratch_shapes=[pltpu.VMEM((rows, rows), jnp.float32)],
        compiler_params=pltpu.CompilerParams(vmem_limit_bytes=40 * 1024 * 1024),
        name="attention",
    )(query, key, value, docs[:, None], docs[None, :])


def attend_back(query, key, value, grad, lse, docs):
    rows, width = query.shape
    return pl.pallas_call(
        attend_back_kernel,
        out_shape=jax.ShapeDtypeStruct((3, rows, width), jnp.bfloat16),
        scratch_shapes=[pltpu.VMEM((rows, rows), jnp.float32)],
        compiler_params=pltpu.CompilerParams(vmem_limit_bytes=40 * 1024 * 1024),
        name="attention_backward",
    )(query, key, value, grad, lse, docs[:, None], docs[None, :])


ROWS = 512


def mlp_kernel(x_ref, in_ref, out_w_ref, bias_ref, act_ref, slope_ref, out_ref, total_ref):
    block = pl.program_id(0)

    def one(tile, carry):
        rows = pl.ds(pl.multiple_of(tile * ROWS, ROWS), ROWS)
        pre_act = dot(x_ref[rows, :], in_ref[0], ((1,), (0,))) + bias_ref[0]
        act, slope = gelu_pair(pre_act)
        act = act.astype(act_ref.dtype)
        act_ref[0, rows, :] = act
        slope_ref[0, rows, :] = slope.astype(slope_ref.dtype)
        part = dot(act, out_w_ref[0], ((1,), (1,)))

        @pl.when(block == 0)
        def _():
            total_ref[rows, :] = part

        @pl.when(block > 0)
        def _():
            total_ref[rows, :] += part

        return carry

    lax.fori_loop(0, x_ref.shape[0] // ROWS, one, 0)

    @pl.when(block == pl.num_programs(0) - 1)
    def _():
        out_ref[...] = total_ref[...]


def mlp(normed, weights, first, blocks, bias):
    rows, width = normed.shape
    whole = pl.BlockSpec((rows, width), lambda b: (0, 0))
    tile = pl.BlockSpec((1, rows, width), lambda b: (b, 0, 0))
    low = jax.ShapeDtypeStruct((blocks, rows, width), jnp.bfloat16)
    return pl.pallas_call(
        mlp_kernel,
        grid=(blocks,),
        in_specs=[
            whole,
            pl.BlockSpec((1, width, width), lambda b: (first + b, 0, 0)),
            pl.BlockSpec((1, width, width), lambda b: (first + blocks + b, 0, 0)),
            pl.BlockSpec((1, 1, width), lambda b: (b, 0, 0)),
        ],
        out_specs=(tile, tile, whole),
        out_shape=(low, low, jax.ShapeDtypeStruct((rows, width), jnp.float32)),
        scratch_shapes=[pltpu.VMEM((rows, width), jnp.float32)],
        compiler_params=pltpu.CompilerParams(vmem_limit_bytes=48 * 1024 * 1024),
        name="feed_forward",
    )(normed, weights, weights, bias[:, None])


def mlp_back_kernel(d_ref, in_ref, out_w_ref, slope_ref, d_pre_ref, bias_ref, out_ref, total_ref):
    block = pl.program_id(0)

    def one(tile, carry):
        rows = pl.ds(pl.multiple_of(tile * ROWS, ROWS), ROWS)
        d_act = dot(d_ref[rows, :], out_w_ref[0], ((1,), (0,)))
        d_pre = (d_act * slope_ref[0, rows, :].astype(jnp.float32)).astype(jnp.bfloat16)
        d_pre_ref[0, rows, :] = d_pre
        sums = jnp.sum(d_pre.astype(jnp.float32), axis=0, keepdims=True)
        part = dot(d_pre, in_ref[0], ((1,), (1,)))

        @pl.when(block == 0)
        def _():
            total_ref[rows, :] = part

        @pl.when(block > 0)
        def _():
            total_ref[rows, :] += part

        return carry + sums

    width = d_ref.shape[1]
    bias_ref[0] = lax.fori_loop(
        0, d_ref.shape[0] // ROWS, one, jnp.zeros((1, width), jnp.float32)
    )

    @pl.when(block == pl.num_programs(0) - 1)
    def _():
        out_ref[...] = total_ref[...]


def mlp_back(grad, weights, first, blocks, slope):
    rows, width = grad.shape
    whole = pl.BlockSpec((rows, width), lambda b: (0, 0))
    tile = pl.BlockSpec((1, rows, width), lambda b: (b, 0, 0))
    d_pre, d_bias, out = pl.pallas_call(
        mlp_back_kernel,
        grid=(blocks,),
        in_specs=[
            whole,
            pl.BlockSpec((1, width, width), lambda b: (first + b, 0, 0)),
            pl.BlockSpec((1, width, width), lambda b: (first + blocks + b, 0, 0)),
            tile,
        ],
        out_specs=(tile, pl.BlockSpec((1, 1, width), lambda b: (b, 0, 0)), whole),
        out_shape=(
            jax.ShapeDtypeStruct((blocks, rows, width), jnp.bfloat16),
            jax.ShapeDtypeStruct((blocks, 1, width), jnp.float32),
            jax.ShapeDtypeStruct((rows, width), jnp.float32),
        ),
        scratch_shapes=[pltpu.VMEM((rows, width), jnp.float32)],
        compiler_params=pltpu.CompilerParams(vmem_limit_bytes=48 * 1024 * 1024),
        name="feed_forward_backward",
    )(grad, weights, weights, slope)
    return (d_pre, d_bias[:, 0], out)


TILE = 256
LAG = 2


def reduce_kernel(units, sources, *refs):
    n_in = 8 * LAYERS + 1
    ins, small_in = refs[: n_in - 1], refs[n_in - 1]
    out_ref, small_out = refs[n_in : n_in + 2]
    (
        a_buf,
        b_buf,
        core_out,
        core_in,
        sum_core,
        first_in,
        sum_first,
        second_in,
        sum_second,
        z_in,
        small_sum,
        small_got,
        a_sem,
        b_sem,
        core_sems,
        first_sems,
        second_sems,
        z_sems,
        small_sems,
    ) = refs[n_in + 2 :]
    dp, tensor = lax.axis_index("dp"), lax.axis_index("tensor")
    z, y, x, c = dp // 2, dp % 2, tensor // 2, tensor % 2
    width = out_ref.shape[2]
    half = width // 2
    per_layer = units // LAYERS
    quarter, eighth, piece = half // 2, half // 4, out_ref.shape[1]
    to_core = (dp, x * 2 + 1 - c)
    to_x = (dp, (1 - x) * 2 + c)
    to_y = (z * 2 + 1 - y, tensor)
    to_z = [(((z + k) % 4) * 2 + y, tensor) for k in (1, 2, 3)]
    to_z1 = ((z + 1 - 2 * (z % 2)) * 2 + y, tensor)
    to_z2 = (((z + 2) % 4) * 2 + y, tensor)
    mesh_id = pl.DeviceIdType.MESH

    barrier = pltpu.get_barrier_semaphore()
    for peer in (to_core, to_x, to_y, *to_z):
        pl.semaphore_signal(barrier, inc=1, device_id=peer, device_id_type=mesh_id)

    def remote(src, dst, sems, send, recv, peer):
        return pltpu.make_async_remote_copy(
            src_ref=src,
            dst_ref=dst,
            send_sem=sems.at[send],
            recv_sem=sems.at[recv],
            device_id=peer,
            device_id_type=mesh_id,
        )

    loads = []
    for layer in range(LAYERS):
        for kind in range(4):
            loads.append(
                pltpu.make_async_copy(
                    ins[layer * 8 + kind], a_buf.at[layer * 4 + kind], a_sem.at[layer * 4 + kind]
                )
            )
    for load in loads:
        load.start()

    def b_copy(unit):
        slot = unit % 3
        for layer in range(LAYERS):
            start = layer * per_layer
            for kind, count in enumerate(sources):
                ref = ins[layer * 8 + 4 + kind]

                @pl.when((unit >= start) & (unit < start + count))
                def _(ref=ref, start=start):
                    pltpu.make_async_copy(
                        ref.at[unit - start], b_buf.at[slot], b_sem.at[slot]
                    ).start()

                start = start + count

    def b_wait(unit):
        slot = unit % 3
        pltpu.make_async_copy(ins[4].at[0], b_buf.at[slot], b_sem.at[slot]).wait()

    def a_index(unit):
        layer = unit // per_layer
        j = unit % per_layer
        kind = 0
        bound = 0
        for count in sources[:-1]:
            bound = bound + count
            kind = kind + jnp.where(j >= bound, 1, 0)
        return layer * 4 + kind

    def product(unit, side, tile):
        start = pl.multiple_of(side * half + tile * TILE, TILE)
        left = a_buf[a_index(unit), :, pl.ds(start, TILE)]
        return lax.dot_general(
            left, b_buf[unit % 3], (((0,), (0,)), ((), ())), preferred_element_type=jnp.float32
        )

    def core_copy(unit):
        return remote(
            core_out.at[unit % 2],
            core_in.at[unit % 4],
            core_sems,
            (0, unit % 2),
            (1, unit % 4),
            to_core,
        )

    def first_copies(unit):
        here = sum_core.at[unit % 3]
        return (
            remote(
                here.at[pl.ds(pl.multiple_of((1 - x) * quarter, quarter), quarter), pl.ds(0, half)],
                first_in.at[unit % 4, 0],
                first_sems,
                (0, 0, unit % 3),
                (1, 0, unit % 4),
                to_x,
            ),
            *(
                remote(
                    here.at[
                        pl.ds(pl.multiple_of(i * quarter + (1 - y) * eighth, eighth), eighth),
                        pl.ds(half, half),
                    ],
                    first_in.at[unit % 4, 1, pl.ds(i * eighth, eighth)],
                    first_sems,
                    (0, 1 + i, unit % 3),
                    (1, 1 + i, unit % 4),
                    to_y,
                )
                for i in range(2)
            ),
        )

    def second_copies(unit):
        here = sum_first.at[unit % 3]
        return (
            remote(
                here.at[0, pl.ds(pl.multiple_of((1 - y) * eighth, eighth), eighth)],
                second_in.at[unit % 4, 0],
                second_sems,
                (0, 0, unit % 3),
                (1, 0, unit % 4),
                to_y,
            ),
            remote(
                here.at[1, pl.ds(pl.multiple_of((1 - x) * eighth, eighth), eighth)],
                second_in.at[unit % 4, 1],
                second_sems,
                (0, 1, unit % 3),
                (1, 1, unit % 4),
                to_x,
            ),
        )

    def z_copies(unit):
        return [
            remote(
                sum_second.at[unit % 3, pl.ds(pl.multiple_of(((z + k) % 4) * piece, piece), piece)],
                z_in.at[unit % 4, k - 1],
                z_sems,
                (0, k - 1, unit % 3),
                (1, k - 1, unit % 4),
                to_z[k - 1],
            )
            for k in (1, 2, 3)
        ]

    small_peers = (to_core, to_x, to_y, to_z1, to_z2)

    def small_copy(stage):
        return remote(
            small_sum.at[stage],
            small_got.at[stage],
            small_sems,
            (0, stage),
            (1, stage),
            small_peers[stage],
        )

    b_copy(jnp.int32(0))
    small_sum[0] = small_in[...]
    for load in loads:
        load.wait()
    pl.semaphore_wait(barrier, 6)
    small_copy(0).start()

    def step(s, carry):
        @pl.when(s < units)
        def _():
            b_wait(s)

            @pl.when(s + 1 < units)
            def _():
                b_copy(s + 1)

            @pl.when(s >= 2)
            def _():
                core_copy(s - 2).wait_send()

            def one(tile, carry):
                rows = pl.ds(pl.multiple_of(tile * TILE, TILE), TILE)
                core_out[s % 2, rows, :] = product(s, 1 - c, tile).astype(jnp.bfloat16)
                return carry

            lax.fori_loop(0, half // TILE, one, 0)
            core_copy(s).start()

        last = s - 3 * LAG - 1

        @pl.when((last >= 0) & (last < units))
        def _():
            for copy in z_copies(last):
                copy.wait()
            total = sum_second[last % 3, pl.ds(pl.multiple_of(z * piece, piece), piece), :].astype(
                jnp.float32
            )
            for k in range(3):
                total = total + z_in[last % 4, k].astype(jnp.float32)
            out_ref[last] = total.astype(out_ref.dtype)

        third = s - 2 * LAG - 1

        @pl.when((third >= 0) & (third < units))
        def _():
            for copy in second_copies(third):
                copy.wait()
            for part, side in ((0, y), (1, x)):
                mine = sum_first[
                    third % 3, part, pl.ds(pl.multiple_of(side * eighth, eighth), eighth), :
                ]
                total = mine.astype(jnp.float32) + second_in[third % 4, part].astype(jnp.float32)
                sum_second[third % 3, :, part * half : (part + 1) * half] = total.astype(
                    jnp.bfloat16
                )
            for copy in z_copies(third):
                copy.start()

        second = s - LAG - 1

        @pl.when((second >= 0) & (second < units))
        def _():
            for copy in first_copies(second):
                copy.wait()
            mine = sum_core[
                second % 3, pl.ds(pl.multiple_of(x * quarter, quarter), quarter), 0:half
            ]
            total = mine.astype(jnp.float32) + first_in[second % 4, 0].astype(jnp.float32)
            sum_first[second % 3, 0] = total.astype(jnp.bfloat16)
            for i in range(2):
                mine = sum_core[
                    second % 3,
                    pl.ds(pl.multiple_of(i * quarter + y * eighth, eighth), eighth),
                    half : 2 * half,
                ]
                rows = pl.ds(i * eighth, eighth)
                total = mine.astype(jnp.float32) + first_in[second % 4, 1, rows, :].astype(
                    jnp.float32
                )
                sum_first[second % 3, 1, rows, :] = total.astype(jnp.bfloat16)
            for copy in second_copies(second):
                copy.start()

        first = s - 1

        @pl.when((first >= 0) & (first < units))
        def _():
            core_copy(first).wait_recv()

            def one(tile, carry):
                rows = pl.ds(pl.multiple_of(tile * TILE, TILE), TILE)
                total = product(first, c, tile) + core_in[first % 4, rows, :].astype(jnp.float32)
                sum_core[first % 3, rows, :] = total.astype(jnp.bfloat16)
                return carry

            lax.fori_loop(0, half // TILE, one, 0)
            for copy in first_copies(first):
                copy.start()

        for stage in range(5):

            @pl.when(s == 2 * (stage + 1))
            def _(stage=stage):
                small_copy(stage).wait()
                total = small_sum[stage] + small_got[stage]
                if stage < 4:
                    small_sum[stage + 1] = total
                    small_copy(stage + 1).start()
                else:
                    small_out[...] = total

        return carry

    lax.fori_loop(0, units + 3 * LAG + 1, step, 0)
    for unit in (units - 2, units - 1):
        core_copy(unit).wait_send()


def reduce_pieces(operands, small, units, sources, piece, width):
    rows = operands[0].shape[0]
    half = width // 2
    low = jnp.bfloat16
    any_spec = pl.BlockSpec(memory_space=pl.ANY)
    vmem_spec = pl.BlockSpec(memory_space=pltpu.VMEM)
    dma = pltpu.SemaphoreType.DMA
    return pl.pallas_call(
        functools.partial(reduce_kernel, units, sources),
        out_shape=(
            jax.ShapeDtypeStruct((units, piece, width), low),
            jax.ShapeDtypeStruct(small.shape, jnp.float32),
        ),
        in_specs=[any_spec] * len(operands) + [vmem_spec],
        out_specs=(vmem_spec, vmem_spec),
        scratch_shapes=[
            pltpu.VMEM((4 * LAYERS, rows, width), low),
            pltpu.VMEM((3, rows, width), low),
            pltpu.VMEM((2, half, width), low),
            pltpu.VMEM((4, half, width), low),
            pltpu.VMEM((3, half, width), low),
            pltpu.VMEM((4, 2, half // 2, half), low),
            pltpu.VMEM((3, 2, half // 2, half), low),
            pltpu.VMEM((4, 2, half // 4, half), low),
            pltpu.VMEM((3, half // 4, width), low),
            pltpu.VMEM((4, 3, piece, width), low),
            pltpu.VMEM((5,) + small.shape, jnp.float32),
            pltpu.VMEM((5,) + small.shape, jnp.float32),
            dma((4 * LAYERS,)),
            dma((3,)),
            dma((2, 4)),
            dma((2, 3, 4)),
            dma((2, 2, 4)),
            dma((2, 3, 4)),
            dma((2, 5)),
        ],
        compiler_params=pltpu.CompilerParams(
            collective_id=1, has_side_effects=True, vmem_limit_bytes=60 * 1024 * 1024
        ),
        name="weight_gradients",
    )(*operands, small)


def gather_kernel(own_ref, out_ref, own_sem, sems):
    units, piece, width = own_ref.shape
    dp, tensor = lax.axis_index("dp"), lax.axis_index("tensor")
    z, y, x, c = dp // 2, dp % 2, tensor // 2, tensor % 2
    half = width // 2
    line, plane = 4 * piece, 8 * piece
    to_core = (dp, x * 2 + 1 - c)
    to_x = (dp, (1 - x) * 2 + c)
    to_y = (z * 2 + 1 - y, tensor)
    to_z = [(((z + k) % 4) * 2 + y, tensor) for k in (1, 2, 3)]
    mesh_id = pl.DeviceIdType.MESH

    barrier = pltpu.get_barrier_semaphore()
    for peer in (to_core, to_x, to_y, *to_z):
        pl.semaphore_signal(barrier, inc=1, device_id=peer, device_id_type=mesh_id)
    pl.semaphore_wait(barrier, 6)

    my_line = pl.multiple_of(((c * 2 + x) * 2 + y) * line, line)
    my_rows = pl.ds(pl.multiple_of(my_line + z * piece, piece), piece)
    first, second = pl.ds(0, half), pl.ds(half, half)

    def remote(src, dst, index, unit, peer):
        return pltpu.make_async_remote_copy(
            src_ref=src,
            dst_ref=dst,
            send_sem=sems.at[0, index, unit],
            recv_sem=sems.at[1, index, unit],
            device_id=peer,
            device_id_type=mesh_id,
        )

    def own_copy(unit):
        return pltpu.make_async_copy(own_ref.at[unit], out_ref.at[unit, my_rows], own_sem.at[unit])

    def stage_z(unit):
        there = out_ref.at[unit, my_rows]
        return [remote(own_ref.at[unit], there, k, unit, to_z[k]) for k in range(3)]

    def stage_one(unit):
        rows = pl.ds(my_line, line)
        one, two = out_ref.at[unit, rows, first], out_ref.at[unit, rows, second]
        return [remote(one, one, 3, unit, to_y), remote(two, two, 4, unit, to_x)]

    def stage_two(unit):
        rows = pl.ds(pl.multiple_of((c * 2 + x) * plane, plane), plane)
        one = out_ref.at[unit, rows, first]
        copies = [remote(one, one, 5, unit, to_x)]
        for i in range(2):
            rows = pl.ds(pl.multiple_of(((c * 2 + i) * 2 + y) * line, line), line)
            two = out_ref.at[unit, rows, second]
            copies.append(remote(two, two, 6 + i, unit, to_y))
        return copies

    def stage_core(unit):
        there = out_ref.at[unit, pl.ds(pl.multiple_of(c * 2 * plane, 2 * plane), 2 * plane)]
        return [remote(there, there, 8, unit, to_core)]

    stages = (stage_z, stage_one, stage_two, stage_core)

    def step(s, carry):
        for number in range(len(stages) + 1):
            unit = s - number * LAG

            @pl.when((unit >= 0) & (unit < units))
            def _(unit=unit, number=number):
                if number == 0:
                    own_copy(unit).start()
                else:
                    if number == 1:
                        own_copy(unit).wait()
                    for copy in stages[number - 1](unit):
                        copy.wait()
                if number < len(stages):
                    for copy in stages[number](unit):
                        copy.start()

        return carry

    lax.fori_loop(0, units + len(stages) * LAG, step, 0)


def gather_pieces(own):
    units, piece, width = own.shape
    any_spec = pl.BlockSpec(memory_space=pl.ANY)
    return pl.pallas_call(
        gather_kernel,
        out_shape=jax.ShapeDtypeStruct((units, width, width), own.dtype),
        in_specs=[any_spec],
        out_specs=any_spec,
        scratch_shapes=[
            pltpu.SemaphoreType.DMA((units,)),
            pltpu.SemaphoreType.DMA((2, 9, units)),
        ],
        compiler_params=pltpu.CompilerParams(collective_id=2, has_side_effects=True),
        name="gather_weights",
    )(own)


def local(
    hidden_in,
    doc_ids,
    unit_slot,
    masters,
    first_moment,
    second_moment,
    column_state,
    row_state,
    out_grad,
):
    slot_count, width, col_width = masters.shape
    units = unit_slot.shape[0]
    per_layer = units // LAYERS
    blocks = (per_layer - 4) // 2
    dp_size = lax.axis_size("dp")
    tensor_size = lax.axis_size("tensor")
    devices = dp_size * tensor_size
    slots = slot_count * dp_size
    rows = hidden_in.shape[0]
    seq_len = doc_ids.shape[1]
    heads = width // HEAD_DIM
    piece = width // devices
    share = seq_len // rows
    tensor_index = lax.axis_index("tensor")
    groups = [list(range(i, i + share)) for i in range(0, tensor_size, share)]
    score_scale = HEAD_DIM ** (-0.5)
    kernels = dp_size == 8 and tensor_size == 4 and share == 1

    sent = masters.astype(jnp.bfloat16)
    if kernels:
        sent = sent.reshape(slot_count, 2, 2, 2, 4, piece, col_width)
        sent = sent.transpose(4, 3, 2, 1, 0, 5, 6)
    else:
        sent = sent.reshape(slot_count, devices, piece, col_width).transpose(1, 0, 2, 3)
    spread = lax.all_to_all(sent.reshape(devices, slot_count, piece, col_width), BOTH, 0, 0)
    spread = spread.reshape(dp_size, tensor_size, slot_count, piece, col_width)
    spread = spread.transpose(0, 2, 3, 1, 4).reshape(slots, piece, width)
    mine = spread[unit_slot]
    if kernels:
        weights = gather_pieces(mine)
    else:
        weights = jnp.concatenate(
            [
                lax.all_gather(
                    mine[layer * per_layer : (layer + 1) * per_layer], BOTH, axis=1, tiled=True
                )
                for layer in range(LAYERS)
            ],
            axis=0,
        )

    def matrices(layer):
        unit = weights[layer * per_layer : (layer + 1) * per_layer]
        return (unit[:3], unit[3], unit[4 : 4 + blocks], unit[4 + blocks :])

    row_docs = lax.dynamic_slice_in_dim(doc_ids, tensor_index // share, 1, axis=0)[0]
    my_docs = lax.dynamic_slice_in_dim(row_docs, (tensor_index % share) * rows, rows)
    same_doc = (my_docs[:, None] == row_docs[None, :])[None]

    def whole_row(value):
        if share == 1:
            return value
        return lax.all_gather(value, "tensor", axis=0, tiled=True, axis_index_groups=groups)

    def own_rows(value):
        if share == 1:
            return value
        return lax.psum_scatter(
            value, "tensor", scatter_dimension=0, tiled=True, axis_index_groups=groups
        )

    col_full = lax.all_gather(column_state[0], "tensor", axis=2, tiled=True)
    hidden = hidden_in.astype(jnp.float32)
    saved_layers = []
    for layer in range(LAYERS):
        w_qkv, w_proj, w_in, w_out = matrices(layer)
        row_now = row_state[0, layer]
        col_now = col_full[layer]
        hidden_bf = hidden.astype(jnp.bfloat16)
        query, key, value = (dot(hidden_bf, w_qkv[i], ((1,), (0,))) for i in range(3))
        query = ((query + col_now[0]) * score_scale).astype(jnp.bfloat16)
        key = key.astype(jnp.bfloat16)
        value = (value + col_now[1]).astype(jnp.bfloat16)
        if kernels:
            context, log_total = attend(query, key, value, row_docs)
        else:
            query = query.reshape(rows, heads, HEAD_DIM)
            key = whole_row(key).reshape(seq_len, heads, HEAD_DIM)
            value = whole_row(value).reshape(seq_len, heads, HEAD_DIM)
            scores = jnp.einsum("qhd,khd->hqk", query, key, preferred_element_type=jnp.float32)
            scores = jnp.where(same_doc, scores, -1e30)
            row_top = jnp.max(scores, axis=-1, keepdims=True)
            log_total = row_top + jnp.log(
                jnp.sum(jnp.exp(scores - row_top), axis=-1, keepdims=True)
            )
            soft_bf = jnp.exp(scores - log_total).astype(jnp.bfloat16)
            context = jnp.einsum("hqk,khd->qhd", soft_bf, value, preferred_element_type=jnp.float32)
            context = context.reshape(rows, width).astype(jnp.bfloat16)
        attended = dot(context, w_proj, ((1,), (1,)))
        normed, scaled_one, inverse_one = norm_forward(
            hidden + attended + row_now[0], row_now[2], row_now[3]
        )
        normed_bf = normed.astype(jnp.bfloat16)
        if kernels:
            activated, slope, mlp_out = mlp(
                normed_bf, weights, layer * per_layer + 4, blocks, col_now[2:]
            )
        else:
            pre_act = jnp.einsum("rd,bdc->brc", normed_bf, w_in, preferred_element_type=jnp.float32)
            activated, slope = gelu_pair(pre_act + col_now[2:, None])
            activated = activated.astype(jnp.bfloat16)
            slope = slope.astype(jnp.bfloat16)
            mlp_out = jnp.einsum(
                "brc,bdc->rd", activated, w_out, preferred_element_type=jnp.float32
            )
        output, scaled_two, inverse_two = norm_forward(
            normed + mlp_out + row_now[1], row_now[4], row_now[5]
        )
        saved_layers.append(
            (hidden_bf, query, key, value, log_total, context, scaled_one, inverse_one, normed_bf)
            + (slope, activated, scaled_two, inverse_two)
        )
        hidden = output
    upstream = out_grad.astype(jnp.float32)
    operands = [None] * LAYERS
    col_parts = [None] * LAYERS
    row_parts = [None] * LAYERS
    for layer in reversed(range(LAYERS)):
        w_qkv, w_proj, w_in, w_out = matrices(layer)
        row_now = row_state[0, layer]
        (
            hidden_bf,
            query,
            key,
            value,
            log_total,
            context,
            scaled_one,
            inverse_one,
            normed_bf,
            slope,
            activated,
            scaled_two,
            inverse_two,
        ) = saved_layers[layer]
        d_two, gain_two, shift_two = norm_backward(upstream, scaled_two, inverse_two, row_now[4])
        grad_bias_two = jnp.sum(d_two, axis=0)
        d_two_bf = d_two.astype(jnp.bfloat16)
        if kernels:
            d_pre, grad_bias_in, d_normed = mlp_back(
                d_two_bf, weights, layer * per_layer + 4, blocks, slope
            )
        else:
            d_act = jnp.einsum("rd,bdc->brc", d_two_bf, w_out, preferred_element_type=jnp.float32)
            d_pre = (d_act * slope).astype(jnp.bfloat16)
            grad_bias_in = jnp.sum(d_pre, axis=1, dtype=jnp.float32)
            d_normed = jnp.einsum("brc,bdc->rd", d_pre, w_in, preferred_element_type=jnp.float32)
        d_normed = d_two + d_normed
        d_one, gain_one, shift_one = norm_backward(d_normed, scaled_one, inverse_one, row_now[2])
        grad_bias_proj = jnp.sum(d_one, axis=0)
        d_one_bf = d_one.astype(jnp.bfloat16)
        d_context = dot(d_one_bf, w_proj, ((1,), (0,))).astype(jnp.bfloat16)
        if kernels:
            d_qkv = attend_back(query, key, value, d_context, log_total, row_docs)
        else:
            d_context = d_context.reshape(rows, heads, HEAD_DIM)
            scores = jnp.einsum("qhd,khd->hqk", query, key, preferred_element_type=jnp.float32)
            scores = jnp.where(same_doc, scores, -1e30)
            soft = jnp.exp(scores - log_total)
            d_values = jnp.einsum(
                "hqk,qhd->khd",
                soft.astype(jnp.bfloat16),
                d_context,
                preferred_element_type=jnp.float32,
            )
            d_probs = jnp.einsum(
                "qhd,khd->hqk", d_context, value, preferred_element_type=jnp.float32
            )
            d_scores = (
                soft * (d_probs - jnp.sum(soft * d_probs, axis=-1, keepdims=True))
            ).astype(jnp.bfloat16)
            d_queries = (
                jnp.einsum("hqk,khd->qhd", d_scores, key, preferred_element_type=jnp.float32)
                * score_scale
            )
            d_keys = jnp.einsum("hqk,qhd->khd", d_scores, query, preferred_element_type=jnp.float32)
            d_qkv = jnp.stack(
                [
                    d_queries.reshape(rows, width),
                    own_rows(d_keys.reshape(seq_len, width)),
                    own_rows(d_values.reshape(seq_len, width)),
                ]
            ).astype(jnp.bfloat16)
        grad_bias_qkv = jnp.sum(d_qkv, axis=1, dtype=jnp.float32)
        upstream = d_one + jnp.einsum(
            "brc,bdc->rd", d_qkv, w_qkv, preferred_element_type=jnp.float32
        )
        operands[layer] = (hidden_bf, d_one_bf, normed_bf, d_two_bf)
        operands[layer] += (d_qkv, context[None], d_pre, activated)
        col_parts[layer] = jnp.concatenate(
            [
                grad_bias_qkv[0:1],
                grad_bias_qkv[2:3],
                grad_bias_in,
            ],
            axis=0,
        )
        row_parts[layer] = jnp.stack(
            [grad_bias_proj, grad_bias_two, gain_one, shift_one, gain_two, shift_two]
        )
    small = jnp.stack([jnp.stack(col_parts), jnp.stack(row_parts)])
    if kernels:
        flat = [array for layer in operands for array in layer]
        summed, total = reduce_pieces(
            flat, small.reshape(-1, width), units, (3, 1, blocks, blocks), piece, width
        )
        small = total.reshape(small.shape)
    else:
        summed = []
        for layer in operands:
            whole = jnp.concatenate(
                [
                    jnp.einsum(
                        "rd,brc->bdc", layer[i], layer[4 + i], preferred_element_type=jnp.float32
                    )
                    for i in range(4)
                ],
                axis=0,
            )
            summed.append(
                lax.psum_scatter(
                    whole.astype(jnp.bfloat16), BOTH, scatter_dimension=1, tiled=True
                )
            )
        summed = jnp.concatenate(summed, axis=0)
        small = lax.psum(small, BOTH)
    row_total = small[1]
    col_total = lax.dynamic_slice_in_dim(small[0], tensor_index * col_width, col_width, axis=2)

    slot_ids = jnp.arange(slots, dtype=jnp.int32)
    named = unit_slot[None, :] == slot_ids[:, None]
    holds = jnp.any(named, axis=1)
    unit_of = jnp.argmax(named, axis=1)
    back = jnp.where(holds[:, None, None], summed[unit_of], jnp.zeros((), jnp.bfloat16))
    back = back.reshape(dp_size, slot_count, piece, tensor_size, col_width)
    back = back.transpose(0, 3, 1, 2, 4).reshape(devices, slot_count, piece, col_width)
    owned = lax.all_to_all(back, BOTH, 0, 0)
    if kernels:
        owned = owned.reshape(4, 2, 2, 2, slot_count, piece, col_width)
        owned = owned.transpose(4, 3, 2, 1, 0, 5, 6)
    else:
        owned = owned.transpose(1, 0, 2, 3)
    owned = owned.reshape(slot_count, width, col_width).astype(jnp.float32)
    occupied = lax.dynamic_slice_in_dim(holds, lax.axis_index("dp") * slot_count, slot_count)
    occupied = occupied.astype(jnp.float32)[:, None, None]
    new_master, new_first, new_second = adamw_update(
        masters, owned, first_moment, second_moment, RATE_UNITS
    )
    unit_master = new_master * occupied
    unit_state = jnp.stack([new_first * occupied, new_second * occupied])
    new_col, col_first, col_second = adamw_update(
        column_state[0], col_total, column_state[1], column_state[2], RATE_SMALL
    )
    column_out = jnp.stack([col_total, new_col, col_first, col_second])
    new_row, row_first, row_second = adamw_update(
        row_state[0], row_total, row_state[1], row_state[2], RATE_SMALL
    )
    row_out = jnp.stack([row_total, new_row, row_first, row_second])
    return (hidden, upstream, unit_master, unit_state, column_out, row_out)


def solution(mesh):
    return jax.shard_map(
        local,
        mesh=mesh,
        in_specs=(
            P(("dp", "tensor"), None),
            P("dp", None),
            P(),
            P("dp", None, "tensor"),
            P("dp", None, "tensor"),
            P("dp", None, "tensor"),
            P(None, None, None, "tensor"),
            P(),
            P(("dp", "tensor"), None),
        ),
        out_specs=(
            P(("dp", "tensor"), None),
            P(("dp", "tensor"), None),
            P("dp", None, "tensor"),
            P(None, "dp", None, "tensor"),
            P(None, None, None, "tensor"),
            P(),
        ),
        check_vma=False,
    )
```

```python
import functools
import math

import jax
import jax.numpy as jnp
from jax import lax
from jax.experimental import pallas as pl
from jax.experimental.pallas import tpu as pltpu
from jax.sharding import PartitionSpec as P

HEAD_DIM = 64
LAYERS = 2
STEP = 3

EPS_NORM = 1e-06
RATE_UNITS = 0.05
RATE_SMALL = 0.2
WEIGHT_DECAY = 0.01
ADAM_EPS = 1e-08
BETA_MOMENT = 0.5
BOTH = ("dp", "tensor")


def norm_forward(summed, gain, shift):
    row_mean = jnp.mean(summed, axis=1, keepdims=True)
    centred = summed - row_mean
    inverse = lax.rsqrt(jnp.mean(centred * centred, axis=1, keepdims=True) + EPS_NORM)
    scaled = centred * inverse
    return (scaled * gain + shift, scaled, inverse)


def norm_backward(upstream, scaled, inverse, gain):
    d_scaled = upstream * gain
    mean_one = jnp.mean(d_scaled, axis=1, keepdims=True)
    mean_two = jnp.mean(d_scaled * scaled, axis=1, keepdims=True)
    grad_input = inverse * (d_scaled - mean_one - scaled * mean_two)
    return (grad_input, jnp.sum(upstream * scaled, axis=0), jnp.sum(upstream, axis=0))


def gelu_pair(v):
    cdf = 0.5 * (1.0 + lax.erf(v * 2.0 ** (-0.5)))
    bell = jnp.exp(-0.5 * v * v) * (2.0 * math.pi) ** (-0.5)
    return (v * cdf, cdf + v * bell)


def adamw_update(old_value, gradient, first_old, second_old, learn_rate):
    first_new = BETA_MOMENT * first_old + (1.0 - BETA_MOMENT) * gradient
    second_new = BETA_MOMENT * second_old + (1.0 - BETA_MOMENT) * gradient * gradient
    correct = 1.0 - BETA_MOMENT**STEP
    step_size = first_new / correct / (jnp.sqrt(second_new / correct) + ADAM_EPS)
    return (old_value - learn_rate * (step_size + WEIGHT_DECAY * old_value), first_new, second_new)


def dot(left, right, dims):
    return lax.dot_general(left, right, (dims, ((), ())), preferred_element_type=jnp.float32)


LANES = 2 * HEAD_DIM


def head_lanes(value, head):
    lane = lax.broadcasted_iota(jnp.int32, value.shape, 1)
    keep = lane < HEAD_DIM if head == 0 else lane >= HEAD_DIM
    return jnp.where(keep, value, jnp.zeros_like(value))


def pair_lanes(first, second):
    lane = lax.broadcasted_iota(jnp.int32, first.shape, 1)
    return jnp.where(lane < HEAD_DIM, first, second)


def attend_pair(pair, q_ref, k_ref, v_ref, mask_ref, ctx_ref, lse_ref):
    lanes = pl.ds(pl.multiple_of(pair * LANES, LANES), LANES)
    query, key, value = q_ref[:, lanes], k_ref[:, lanes], v_ref[:, lanes]
    value_t = value.T
    parts = []
    for head in range(2):
        scores = dot(head_lanes(key, head), query, ((1,), (1,))) + mask_ref[...]
        top = jnp.max(scores, axis=0, keepdims=True)
        weight = jnp.exp(scores - top)
        total = jnp.sum(weight, axis=0, keepdims=True)
        lse_ref[pair * 2 + head] = top + jnp.log(total)
        mine = value_t[head * HEAD_DIM : (head + 1) * HEAD_DIM]
        mixed = dot(mine, weight.astype(jnp.bfloat16), ((1,), (0,)))
        parts.append(mixed * (1.0 / total))
    ctx_ref[:, lanes] = jnp.concatenate(parts, axis=0).T.astype(ctx_ref.dtype)


def attend_back_pair(pair, q_ref, k_ref, v_ref, d_ref, mask_ref, lse_ref, dq_ref, dk_ref, dv_ref):
    lanes = pl.ds(pl.multiple_of(pair * LANES, LANES), LANES)
    query, key, value = q_ref[:, lanes], k_ref[:, lanes], v_ref[:, lanes]
    grad = d_ref[:, lanes]
    key_t = key.T
    parts, d_keys, d_values = [], [], []
    for head in range(2):
        scores = dot(head_lanes(key, head), query, ((1,), (1,))) + mask_ref[...]
        soft = jnp.exp(scores - lse_ref[pair * 2 + head])
        d_values.append(dot(soft.astype(jnp.bfloat16), grad, ((1,), (0,))))
        d_soft = dot(head_lanes(value, head), grad, ((1,), (1,)))
        both = soft * d_soft
        mean = jnp.sum(both, axis=0, keepdims=True)
        d_scores = (both - soft * mean).astype(jnp.bfloat16)
        d_keys.append(dot(d_scores, query, ((1,), (0,))))
        mine = key_t[head * HEAD_DIM : (head + 1) * HEAD_DIM]
        parts.append(dot(mine, d_scores, ((1,), (0,))))
    scale = HEAD_DIM ** (-0.5)
    dq_ref[:, lanes] = (jnp.concatenate(parts, axis=0).T * scale).astype(dq_ref.dtype)
    dk_ref[:, lanes] = pair_lanes(*d_keys).astype(dk_ref.dtype)
    dv_ref[:, lanes] = pair_lanes(*d_values).astype(dv_ref.dtype)


def fill_mask(mask_ref, docs_col_ref, docs_row_ref):
    same = docs_col_ref[...] == docs_row_ref[...]
    mask_ref[...] = jnp.where(same, 0.0, -1e30).astype(jnp.float32)


def attend_back_kernel(mixed_ref, d_ref, lse_ref, col_ref, row_ref, out_ref, mask_ref):
    fill_mask(mask_ref, col_ref, row_ref)
    inputs = [mixed_ref.at[0, i] for i in range(3)]
    grads = [out_ref.at[i] for i in range(3)]

    def two(step, carry):
        for pair in (2 * step, 2 * step + 1):
            attend_back_pair(pair, *inputs, d_ref, mask_ref, lse_ref.at[0], *grads)
        return carry

    lax.fori_loop(0, d_ref.shape[1] // (2 * LANES), two, 0)


def attend_back(mixed, layer, grad, lse, docs):
    rows, width = grad.shape
    return pl.pallas_call(
        attend_back_kernel,
        grid=(1,),
        in_specs=[
            pl.BlockSpec((1, 3, rows, width), lambda i: (layer, 0, 0, 0)),
            pl.BlockSpec((rows, width), lambda i: (0, 0)),
            pl.BlockSpec((1,) + lse.shape[1:], lambda i: (layer, 0, 0, 0)),
            pl.BlockSpec((rows, 1), lambda i: (0, 0)),
            pl.BlockSpec((1, rows), lambda i: (0, 0)),
        ],
        out_specs=pl.BlockSpec((3, rows, width), lambda i: (0, 0, 0)),
        out_shape=jax.ShapeDtypeStruct((3, rows, width), jnp.bfloat16),
        scratch_shapes=[pltpu.VMEM((rows, rows), jnp.float32)],
        compiler_params=pltpu.CompilerParams(vmem_limit_bytes=40 * 1024 * 1024),
        name="attention_backward",
    )(mixed, grad, lse, docs[:, None], docs[None, :])


ROWS = 512


def mlp_back_kernel(d_ref, in_ref, out_w_ref, slope_ref, d_pre_ref, bias_ref, out_ref, total_ref):
    block = pl.program_id(0)

    def one(tile, carry):
        rows = pl.ds(pl.multiple_of(tile * ROWS, ROWS), ROWS)
        d_act = dot(d_ref[rows, :], out_w_ref[0], ((1,), (0,)))
        d_pre = (d_act * slope_ref[0, 0, rows, :].astype(jnp.float32)).astype(jnp.bfloat16)
        d_pre_ref[0, rows, :] = d_pre
        sums = jnp.sum(d_pre.astype(jnp.float32), axis=0, keepdims=True)
        part = dot(d_pre, in_ref[0], ((1,), (1,)))

        @pl.when(block == 0)
        def _():
            total_ref[rows, :] = part

        @pl.when(block > 0)
        def _():
            total_ref[rows, :] += part

        return carry + sums

    width = d_ref.shape[1]
    bias_ref[0] = lax.fori_loop(
        0, d_ref.shape[0] // ROWS, one, jnp.zeros((1, width), jnp.float32)
    )

    @pl.when(block == pl.num_programs(0) - 1)
    def _():
        out_ref[...] = total_ref[...]


def mlp_back(grad, weights, layer, first, blocks, slope):
    rows, width = grad.shape
    whole = pl.BlockSpec((rows, width), lambda b: (0, 0))
    tile = pl.BlockSpec((1, rows, width), lambda b: (b, 0, 0))
    d_pre, d_bias, out = pl.pallas_call(
        mlp_back_kernel,
        grid=(blocks,),
        in_specs=[
            whole,
            pl.BlockSpec((1, width, width), lambda b: (first + b, 0, 0)),
            pl.BlockSpec((1, width, width), lambda b: (first + blocks + b, 0, 0)),
            pl.BlockSpec((1, 1, rows, width), lambda b: (layer, b, 0, 0)),
        ],
        out_specs=(tile, pl.BlockSpec((1, 1, width), lambda b: (b, 0, 0)), whole),
        out_shape=(
            jax.ShapeDtypeStruct((blocks, rows, width), jnp.bfloat16),
            jax.ShapeDtypeStruct((blocks, 1, width), jnp.float32),
            jax.ShapeDtypeStruct((rows, width), jnp.float32),
        ),
        scratch_shapes=[pltpu.VMEM((rows, width), jnp.float32)],
        compiler_params=pltpu.CompilerParams(vmem_limit_bytes=48 * 1024 * 1024),
        name="feed_forward_backward",
    )(grad, weights, weights, slope)
    return (d_pre, d_bias[:, 0], out)


TILE = 256
LAG = 2


def reduce_kernel(units, sources, *refs):
    n_in = 4 + 4 * LAYERS + 1
    ins, small_in = refs[: n_in - 1], refs[n_in - 1]
    out_ref, small_out = refs[n_in : n_in + 2]
    (
        a_buf,
        b_buf,
        core_out,
        core_in,
        sum_core,
        first_in,
        sum_first,
        second_in,
        sum_second,
        z_in,
        small_sum,
        small_got,
        a_sem,
        b_sem,
        core_sems,
        first_sems,
        second_sems,
        z_sems,
        small_sems,
    ) = refs[n_in + 2 :]
    dp, tensor = lax.axis_index("dp"), lax.axis_index("tensor")
    z, y, x, c = dp // 2, dp % 2, tensor // 2, tensor % 2
    width = out_ref.shape[2]
    half = width // 2
    per_layer = units // LAYERS
    quarter, eighth, piece = half // 2, half // 4, out_ref.shape[1]
    to_core = (dp, x * 2 + 1 - c)
    to_x = (dp, (1 - x) * 2 + c)
    to_y = (z * 2 + 1 - y, tensor)
    to_z = [(((z + k) % 4) * 2 + y, tensor) for k in (1, 2, 3)]
    to_z1 = ((z + 1 - 2 * (z % 2)) * 2 + y, tensor)
    to_z2 = (((z + 2) % 4) * 2 + y, tensor)
    mesh_id = pl.DeviceIdType.MESH

    barrier = pltpu.get_barrier_semaphore()
    for peer in (to_core, to_x, to_y, *to_z):
        pl.semaphore_signal(barrier, inc=1, device_id=peer, device_id_type=mesh_id)

    def remote(src, dst, sems, send, recv, peer):
        return pltpu.make_async_remote_copy(
            src_ref=src,
            dst_ref=dst,
            send_sem=sems.at[send],
            recv_sem=sems.at[recv],
            device_id=peer,
            device_id_type=mesh_id,
        )

    loads = []
    for layer in range(LAYERS):
        d_one, d_two = ins[4 + 4 * layer : 6 + 4 * layer]
        for kind, ref in enumerate((ins[0].at[layer], d_one, ins[1].at[layer], d_two)):
            loads.append(
                pltpu.make_async_copy(ref, a_buf.at[layer * 4 + kind], a_sem.at[layer * 4 + kind])
            )
    for load in loads:
        load.start()

    def b_copy(unit):
        slot = unit % 3
        for layer in range(LAYERS):
            start = layer * per_layer
            d_mixed, d_pre = ins[6 + 4 * layer : 8 + 4 * layer]
            rights = (d_mixed, ins[2].at[pl.ds(layer, 1)], d_pre, ins[3].at[layer])
            for ref, count in zip(rights, sources):

                @pl.when((unit >= start) & (unit < start + count))
                def _(ref=ref, start=start):
                    pltpu.make_async_copy(
                        ref.at[unit - start], b_buf.at[slot], b_sem.at[slot]
                    ).start()

                start = start + count

    def b_wait(unit):
        slot = unit % 3
        pltpu.make_async_copy(ins[2].at[0], b_buf.at[slot], b_sem.at[slot]).wait()

    def a_index(unit):
        layer = unit // per_layer
        j = unit % per_layer
        kind = 0
        bound = 0
        for count in sources[:-1]:
            bound = bound + count
            kind = kind + jnp.where(j >= bound, 1, 0)
        return layer * 4 + kind

    def product(unit, side, tile):
        start = pl.multiple_of(side * half + tile * TILE, TILE)
        left = a_buf[a_index(unit), :, pl.ds(start, TILE)]
        return lax.dot_general(
            left, b_buf[unit % 3], (((0,), (0,)), ((), ())), preferred_element_type=jnp.float32
        )

    def core_copy(unit):
        return remote(
            core_out.at[unit % 2],
            core_in.at[unit % 4],
            core_sems,
            (0, unit % 2),
            (1, unit % 4),
            to_core,
        )

    def first_copies(unit):
        here = sum_core.at[unit % 3]
        return (
            remote(
                here.at[pl.ds(pl.multiple_of((1 - x) * quarter, quarter), quarter), pl.ds(0, half)],
                first_in.at[unit % 4, 0],
                first_sems,
                (0, 0, unit % 3),
                (1, 0, unit % 4),
                to_x,
            ),
            *(
                remote(
                    here.at[
                        pl.ds(pl.multiple_of(i * quarter + (1 - y) * eighth, eighth), eighth),
                        pl.ds(half, half),
                    ],
                    first_in.at[unit % 4, 1, pl.ds(i * eighth, eighth)],
                    first_sems,
                    (0, 1 + i, unit % 3),
                    (1, 1 + i, unit % 4),
                    to_y,
                )
                for i in range(2)
            ),
        )

    def second_copies(unit):
        here = sum_first.at[unit % 3]
        return (
            remote(
                here.at[0, pl.ds(pl.multiple_of((1 - y) * eighth, eighth), eighth)],
                second_in.at[unit % 4, 0],
                second_sems,
                (0, 0, unit % 3),
                (1, 0, unit % 4),
                to_y,
            ),
            remote(
                here.at[1, pl.ds(pl.multiple_of((1 - x) * eighth, eighth), eighth)],
                second_in.at[unit % 4, 1],
                second_sems,
                (0, 1, unit % 3),
                (1, 1, unit % 4),
                to_x,
            ),
        )

    def z_copies(unit):
        return [
            remote(
                sum_second.at[unit % 3, pl.ds(pl.multiple_of(((z + k) % 4) * piece, piece), piece)],
                z_in.at[unit % 4, k - 1],
                z_sems,
                (0, k - 1, unit % 3),
                (1, k - 1, unit % 4),
                to_z[k - 1],
            )
            for k in (1, 2, 3)
        ]

    small_peers = (to_core, to_x, to_y, to_z1, to_z2)

    def small_copy(stage):
        return remote(
            small_sum.at[stage],
            small_got.at[stage],
            small_sems,
            (0, stage),
            (1, stage),
            small_peers[stage],
        )

    b_copy(jnp.int32(0))
    small_sum[0] = small_in[...]
    for load in loads:
        load.wait()
    pl.semaphore_wait(barrier, 6)
    small_copy(0).start()

    def step(s, carry):
        @pl.when(s < units)
        def _():
            b_wait(s)

            @pl.when(s + 1 < units)
            def _():
                b_copy(s + 1)

            @pl.when(s >= 2)
            def _():
                core_copy(s - 2).wait_send()

            def one(tile, carry):
                rows = pl.ds(pl.multiple_of(tile * TILE, TILE), TILE)
                core_out[s % 2, rows, :] = product(s, 1 - c, tile).astype(jnp.bfloat16)
                return carry

            lax.fori_loop(0, half // TILE, one, 0)
            core_copy(s).start()

        last = s - 3 * LAG - 1

        @pl.when((last >= 0) & (last < units))
        def _():
            for copy in z_copies(last):
                copy.wait()
            total = sum_second[last % 3, pl.ds(pl.multiple_of(z * piece, piece), piece), :].astype(
                jnp.float32
            )
            for k in range(3):
                total = total + z_in[last % 4, k].astype(jnp.float32)
            out_ref[last] = total.astype(out_ref.dtype)

        third = s - 2 * LAG - 1

        @pl.when((third >= 0) & (third < units))
        def _():
            for copy in second_copies(third):
                copy.wait()
            for part, side in ((0, y), (1, x)):
                mine = sum_first[
                    third % 3, part, pl.ds(pl.multiple_of(side * eighth, eighth), eighth), :
                ]
                total = mine.astype(jnp.float32) + second_in[third % 4, part].astype(jnp.float32)
                sum_second[third % 3, :, part * half : (part + 1) * half] = total.astype(
                    jnp.bfloat16
                )
            for copy in z_copies(third):
                copy.start()

        second = s - LAG - 1

        @pl.when((second >= 0) & (second < units))
        def _():
            for copy in first_copies(second):
                copy.wait()
            mine = sum_core[
                second % 3, pl.ds(pl.multiple_of(x * quarter, quarter), quarter), 0:half
            ]
            total = mine.astype(jnp.float32) + first_in[second % 4, 0].astype(jnp.float32)
            sum_first[second % 3, 0] = total.astype(jnp.bfloat16)
            for i in range(2):
                mine = sum_core[
                    second % 3,
                    pl.ds(pl.multiple_of(i * quarter + y * eighth, eighth), eighth),
                    half : 2 * half,
                ]
                rows = pl.ds(i * eighth, eighth)
                total = mine.astype(jnp.float32) + first_in[second % 4, 1, rows, :].astype(
                    jnp.float32
                )
                sum_first[second % 3, 1, rows, :] = total.astype(jnp.bfloat16)
            for copy in second_copies(second):
                copy.start()

        first = s - 1

        @pl.when((first >= 0) & (first < units))
        def _():
            core_copy(first).wait_recv()

            def one(tile, carry):
                rows = pl.ds(pl.multiple_of(tile * TILE, TILE), TILE)
                total = product(first, c, tile) + core_in[first % 4, rows, :].astype(jnp.float32)
                sum_core[first % 3, rows, :] = total.astype(jnp.bfloat16)
                return carry

            lax.fori_loop(0, half // TILE, one, 0)
            for copy in first_copies(first):
                copy.start()

        for stage in range(5):

            @pl.when(s == 2 * (stage + 1))
            def _(stage=stage):
                small_copy(stage).wait()
                total = small_sum[stage] + small_got[stage]
                if stage < 4:
                    small_sum[stage + 1] = total
                    small_copy(stage + 1).start()
                else:
                    small_out[...] = total

        return carry

    lax.fori_loop(0, units + 3 * LAG + 1, step, 0)
    for unit in (units - 2, units - 1):
        core_copy(unit).wait_send()


def reduce_pieces(operands, small, units, sources, piece, width):
    rows = operands[0].shape[1]
    half = width // 2
    low = jnp.bfloat16
    any_spec = pl.BlockSpec(memory_space=pl.ANY)
    vmem_spec = pl.BlockSpec(memory_space=pltpu.VMEM)
    dma = pltpu.SemaphoreType.DMA
    return pl.pallas_call(
        functools.partial(reduce_kernel, units, sources),
        out_shape=(
            jax.ShapeDtypeStruct((units, piece, width), low),
            jax.ShapeDtypeStruct(small.shape, jnp.float32),
        ),
        in_specs=[any_spec] * len(operands) + [vmem_spec],
        out_specs=(vmem_spec, vmem_spec),
        scratch_shapes=[
            pltpu.VMEM((4 * LAYERS, rows, width), low),
            pltpu.VMEM((3, rows, width), low),
            pltpu.VMEM((2, half, width), low),
            pltpu.VMEM((4, half, width), low),
            pltpu.VMEM((3, half, width), low),
            pltpu.VMEM((4, 2, half // 2, half), low),
            pltpu.VMEM((3, 2, half // 2, half), low),
            pltpu.VMEM((4, 2, half // 4, half), low),
            pltpu.VMEM((3, half // 4, width), low),
            pltpu.VMEM((4, 3, piece, width), low),
            pltpu.VMEM((5,) + small.shape, jnp.float32),
            pltpu.VMEM((5,) + small.shape, jnp.float32),
            dma((4 * LAYERS,)),
            dma((3,)),
            dma((2, 4)),
            dma((2, 3, 4)),
            dma((2, 2, 4)),
            dma((2, 3, 4)),
            dma((2, 5)),
        ],
        compiler_params=pltpu.CompilerParams(
            collective_id=1, has_side_effects=True, vmem_limit_bytes=60 * 1024 * 1024
        ),
        name="weight_gradients",
    )(*operands, small)


def norm_rows(value, gain, shift):
    centred = value - jnp.mean(value, axis=1, keepdims=True)
    inverse = lax.rsqrt(jnp.mean(centred * centred, axis=1, keepdims=True) + EPS_NORM)
    scaled = centred * inverse
    return (scaled * gain + shift, scaled, inverse)


NORM_ROWS = 128


def forward_kernel(
    own_ref,
    hidden_ref,
    docs_col_ref,
    docs_row_ref,
    bias_ref,
    row_ref,
    out_ref,
    final_ref,
    *refs,
):
    saved, bufs = refs[:11], refs[11:22]
    (x_buf, normed_buf, total_buf, mask_buf, unit_buf, own_sem, sems, unit_sem, save_sem) = refs[22:]
    (low_buf, mixed_buf, ctx_buf, lse_buf, one_buf, inv_one_buf, nb_buf) = bufs[:7]
    (act_buf, slope_buf, two_buf, inv_two_buf) = bufs[7:]
    units, piece, width = own_ref.shape
    rows = hidden_ref.shape[0]
    per_layer = units // LAYERS
    blocks = (per_layer - 4) // 2
    dp, tensor = lax.axis_index("dp"), lax.axis_index("tensor")
    z, y, x, c = dp // 2, dp % 2, tensor // 2, tensor % 2
    half = width // 2
    line, plane = 4 * piece, 8 * piece
    to_core = (dp, x * 2 + 1 - c)
    to_x = (dp, (1 - x) * 2 + c)
    to_y = (z * 2 + 1 - y, tensor)
    to_z = [(((z + k) % 4) * 2 + y, tensor) for k in (1, 2, 3)]
    mesh_id = pl.DeviceIdType.MESH

    barrier = pltpu.get_barrier_semaphore()
    for peer in (to_core, to_x, to_y, *to_z):
        pl.semaphore_signal(barrier, inc=1, device_id=peer, device_id_type=mesh_id)
    pl.semaphore_wait(barrier, 6)

    my_line = pl.multiple_of(((c * 2 + x) * 2 + y) * line, line)
    my_rows = pl.ds(pl.multiple_of(my_line + z * piece, piece), piece)
    first, second = pl.ds(0, half), pl.ds(half, half)

    def remote(src, dst, index, unit, peer):
        return pltpu.make_async_remote_copy(
            src_ref=src,
            dst_ref=dst,
            send_sem=sems.at[0, index, unit],
            recv_sem=sems.at[1, index, unit],
            device_id=peer,
            device_id_type=mesh_id,
        )

    def own_copy(unit):
        return pltpu.make_async_copy(own_ref.at[unit], out_ref.at[unit, my_rows], own_sem.at[unit])

    def stage_z(unit):
        there = out_ref.at[unit, my_rows]
        return [remote(own_ref.at[unit], there, k, unit, to_z[k]) for k in range(3)]

    def stage_one(unit):
        rows = pl.ds(my_line, line)
        one, two = out_ref.at[unit, rows, first], out_ref.at[unit, rows, second]
        return [remote(one, one, 3, unit, to_y), remote(two, two, 4, unit, to_x)]

    def stage_two(unit):
        rows = pl.ds(pl.multiple_of((c * 2 + x) * plane, plane), plane)
        one = out_ref.at[unit, rows, first]
        copies = [remote(one, one, 5, unit, to_x)]
        for i in range(2):
            rows = pl.ds(pl.multiple_of(((c * 2 + i) * 2 + y) * line, line), line)
            two = out_ref.at[unit, rows, second]
            copies.append(remote(two, two, 6 + i, unit, to_y))
        return copies

    def stage_core(unit):
        there = out_ref.at[unit, pl.ds(pl.multiple_of(c * 2 * plane, 2 * plane), 2 * plane)]
        return [remote(there, there, 8, unit, to_core)]

    stages = (stage_z, stage_one, stage_two, stage_core)

    def unit_copy(unit):
        slot = unit % 2
        return pltpu.make_async_copy(out_ref.at[unit], unit_buf.at[slot], unit_sem.at[slot])

    def save(number, layer, block=None):
        src, dst, sem = bufs[number], saved[number].at[layer], save_sem.at[number, 0]
        if block is not None:
            src, dst, sem = src.at[block], dst.at[block], save_sem.at[number, block]
        return pltpu.make_async_copy(src, dst, sem)

    def free(numbers, layer, block=None):
        @pl.when(layer > 0)
        def _():
            for number in numbers:
                save(number, layer - 1, block).wait()

    def heads(start, stop):
        def one(pair, carry):
            attend_pair(
                pair, mixed_buf.at[0], mixed_buf.at[1], mixed_buf.at[2], mask_buf, ctx_buf, lse_buf
            )
            return carry

        lax.fori_loop(start, stop, one, 0)

    def over_rows(body):
        def one(tile, carry):
            body(pl.ds(pl.multiple_of(tile * NORM_ROWS, NORM_ROWS), NORM_ROWS))
            return carry

        lax.fori_loop(0, rows // NORM_ROWS, one, 0)

    pairs = width // LANES

    def compute(unit):
        layer, j = unit // per_layer, unit % per_layer
        matrix = unit_buf.at[unit % 2]

        def small(i):
            return row_ref[layer * 6 + i]

        @pl.when(j == 0)
        def _():
            free((0, 1), layer)

            @pl.when(layer == 0)
            def _():
                x_buf[...] = hidden_ref[...].astype(jnp.float32)

            low_buf[...] = x_buf[...].astype(jnp.bfloat16)
            save(0, layer).start()

        @pl.when(j < 3)
        def _():
            value = dot(low_buf[...], matrix[...], ((1,), (0,)))
            value = value + bias_ref[layer * (3 + blocks) + j]
            scale = jnp.where(j == 0, HEAD_DIM ** (-0.5), 1.0)
            mixed_buf[j] = (value * scale).astype(jnp.bfloat16)

        @pl.when(j == 2)
        def _():
            save(1, layer).start()
            free((2, 3), layer)
            heads(0, pairs // 2)

        @pl.when(j == 3)
        def _():
            heads(pairs // 2, pairs)
            save(2, layer).start()
            save(3, layer).start()
            total_buf[...] = dot(ctx_buf[...], matrix[...], ((1,), (1,)))
            free((4, 5, 6), layer)

            def body(part):
                value = x_buf[part, :] + total_buf[part, :] + small(0)
                normed, scaled, inverse = norm_rows(value, small(2), small(3))
                normed_buf[part, :] = normed
                nb_buf[part, :] = normed.astype(jnp.bfloat16)
                one_buf[part, :] = scaled
                inv_one_buf[part, :] = jnp.broadcast_to(inverse, (NORM_ROWS, 128))

            over_rows(body)
            for number in (4, 5, 6):
                save(number, layer).start()

        @pl.when((j >= 4) & (j < 4 + blocks))
        def _():
            block = j - 4
            free((7, 8), layer, block)
            value = dot(nb_buf[...], matrix[...], ((1,), (0,)))
            act, slope = gelu_pair(value + bias_ref[layer * (3 + blocks) + 3 + block])
            act_buf[block] = act.astype(jnp.bfloat16)
            slope_buf[block] = slope.astype(jnp.bfloat16)
            save(7, layer, block).start()
            save(8, layer, block).start()

        @pl.when(j >= 4 + blocks)
        def _():
            block = j - 4 - blocks
            part = dot(act_buf[block], matrix[...], ((1,), (1,)))

            @pl.when(block == 0)
            def _():
                total_buf[...] = part

            @pl.when(block > 0)
            def _():
                total_buf[...] += part

        @pl.when(j == per_layer - 1)
        def _():
            free((9, 10), layer)

            def body(part):
                value = normed_buf[part, :] + total_buf[part, :] + small(1)
                output, scaled, inverse = norm_rows(value, small(4), small(5))
                x_buf[part, :] = output
                two_buf[part, :] = scaled
                inv_two_buf[part, :] = jnp.broadcast_to(inverse, (NORM_ROWS, 128))

            over_rows(body)
            save(9, layer).start()
            save(10, layer).start()

    def step(s, carry):
        for number in range(len(stages) + 1):
            unit = s - number * LAG

            @pl.when((unit >= 0) & (unit < units))
            def _(unit=unit, number=number):
                if number == 0:
                    own_copy(unit).start()
                else:
                    if number == 1:
                        own_copy(unit).wait()
                    for copy in stages[number - 1](unit):
                        copy.wait()
                if number < len(stages):
                    for copy in stages[number](unit):
                        copy.start()
                else:
                    unit_copy(unit).start()

        done = s - len(stages) * LAG - 1

        @pl.when(done >= 0)
        def _():
            unit_copy(done).wait()
            compute(done)

        return carry

    fill_mask(mask_buf, docs_col_ref, docs_row_ref)
    lax.fori_loop(0, units + len(stages) * LAG + 1, step, 0)
    final_ref[...] = x_buf[...]
    last = LAYERS - 1
    for number in (0, 1, 2, 3, 4, 5, 6, 9, 10):
        save(number, last).wait()
    for block in range(blocks):
        save(7, last, block).wait()
        save(8, last, block).wait()


def forward(own, hidden_in, docs, bias, row_now):
    units, piece, width = own.shape
    rows = hidden_in.shape[0]
    blocks = (units // LAYERS - 4) // 2
    low, full = jnp.bfloat16, jnp.float32
    kept = [
        ((rows, width), low),
        ((3, rows, width), low),
        ((rows, width), low),
        ((width // HEAD_DIM, 1, rows), full),
        ((rows, width), full),
        ((rows, 128), full),
        ((rows, width), low),
        ((blocks, rows, width), low),
        ((blocks, rows, width), low),
        ((rows, width), full),
        ((rows, 128), full),
    ]
    any_spec = pl.BlockSpec(memory_space=pl.ANY)
    vmem_spec = pl.BlockSpec(memory_space=pltpu.VMEM)
    dma = pltpu.SemaphoreType.DMA
    return pl.pallas_call(
        forward_kernel,
        out_shape=[
            jax.ShapeDtypeStruct((units, width, width), low),
            jax.ShapeDtypeStruct((rows, width), full),
        ]
        + [jax.ShapeDtypeStruct((LAYERS,) + shape, dtype) for shape, dtype in kept],
        in_specs=[any_spec] + [vmem_spec] * 5,
        out_specs=[any_spec, vmem_spec] + [any_spec] * len(kept),
        scratch_shapes=[pltpu.VMEM(shape, dtype) for shape, dtype in kept]
        + [
            pltpu.VMEM((rows, width), full),
            pltpu.VMEM((rows, width), full),
            pltpu.VMEM((rows, width), full),
            pltpu.VMEM((rows, rows), full),
            pltpu.VMEM((2, width, width), low),
            dma((units,)),
            dma((2, 9, units)),
            dma((2,)),
            dma((len(kept), blocks)),
        ],
        compiler_params=pltpu.CompilerParams(
            collective_id=2, has_side_effects=True, vmem_limit_bytes=60 * 1024 * 1024
        ),
        name="gather_forward",
    )(
        own,
        hidden_in,
        docs[:, None],
        docs[None, :],
        bias.reshape(-1, 1, width),
        row_now.reshape(-1, 1, width),
    )


def run_general(mine, hidden_in, doc_ids, column_state, row_state, out_grad):
    units, piece, width = mine.shape
    per_layer = units // LAYERS
    blocks = (per_layer - 4) // 2
    tensor_size = lax.axis_size("tensor")
    rows = hidden_in.shape[0]
    seq_len = doc_ids.shape[1]
    heads = width // HEAD_DIM
    share = seq_len // rows
    tensor_index = lax.axis_index("tensor")
    groups = [list(range(i, i + share)) for i in range(0, tensor_size, share)]
    score_scale = HEAD_DIM ** (-0.5)
    weights = jnp.concatenate(
        [
            lax.all_gather(
                mine[layer * per_layer : (layer + 1) * per_layer], BOTH, axis=1, tiled=True
            )
            for layer in range(LAYERS)
        ],
        axis=0,
    )

    def matrices(layer):
        unit = weights[layer * per_layer : (layer + 1) * per_layer]
        return (unit[:3], unit[3], unit[4 : 4 + blocks], unit[4 + blocks :])

    row_docs = lax.dynamic_slice_in_dim(doc_ids, tensor_index // share, 1, axis=0)[0]
    my_docs = lax.dynamic_slice_in_dim(row_docs, (tensor_index % share) * rows, rows)
    same_doc = (my_docs[:, None] == row_docs[None, :])[None]

    def whole_row(value):
        if share == 1:
            return value
        return lax.all_gather(value, "tensor", axis=0, tiled=True, axis_index_groups=groups)

    def own_rows(value):
        if share == 1:
            return value
        return lax.psum_scatter(
            value, "tensor", scatter_dimension=0, tiled=True, axis_index_groups=groups
        )

    col_full = lax.all_gather(column_state[0], "tensor", axis=2, tiled=True)
    hidden = hidden_in.astype(jnp.float32)
    saved_layers = []
    for layer in range(LAYERS):
        w_qkv, w_proj, w_in, w_out = matrices(layer)
        row_now = row_state[0, layer]
        col_now = col_full[layer]
        hidden_bf = hidden.astype(jnp.bfloat16)
        query, key, value = (dot(hidden_bf, w_qkv[i], ((1,), (0,))) for i in range(3))
        query = ((query + col_now[0]) * score_scale).astype(jnp.bfloat16)
        key = key.astype(jnp.bfloat16)
        value = (value + col_now[1]).astype(jnp.bfloat16)
        query = query.reshape(rows, heads, HEAD_DIM)
        key = whole_row(key).reshape(seq_len, heads, HEAD_DIM)
        value = whole_row(value).reshape(seq_len, heads, HEAD_DIM)
        scores = jnp.einsum("qhd,khd->hqk", query, key, preferred_element_type=jnp.float32)
        scores = jnp.where(same_doc, scores, -1e30)
        row_top = jnp.max(scores, axis=-1, keepdims=True)
        log_total = row_top + jnp.log(
            jnp.sum(jnp.exp(scores - row_top), axis=-1, keepdims=True)
        )
        soft_bf = jnp.exp(scores - log_total).astype(jnp.bfloat16)
        context = jnp.einsum("hqk,khd->qhd", soft_bf, value, preferred_element_type=jnp.float32)
        context = context.reshape(rows, width).astype(jnp.bfloat16)
        attended = dot(context, w_proj, ((1,), (1,)))
        normed, scaled_one, inverse_one = norm_forward(
            hidden + attended + row_now[0], row_now[2], row_now[3]
        )
        normed_bf = normed.astype(jnp.bfloat16)
        pre_act = jnp.einsum("rd,bdc->brc", normed_bf, w_in, preferred_element_type=jnp.float32)
        activated, slope = gelu_pair(pre_act + col_now[2:, None])
        activated = activated.astype(jnp.bfloat16)
        slope = slope.astype(jnp.bfloat16)
        mlp_out = jnp.einsum(
            "brc,bdc->rd", activated, w_out, preferred_element_type=jnp.float32
        )
        output, scaled_two, inverse_two = norm_forward(
            normed + mlp_out + row_now[1], row_now[4], row_now[5]
        )
        saved_layers.append(
            (hidden_bf, query, key, value, log_total, context, scaled_one, inverse_one, normed_bf)
            + (slope, activated, scaled_two, inverse_two)
        )
        hidden = output
    upstream = out_grad.astype(jnp.float32)
    operands = [None] * LAYERS
    col_parts = [None] * LAYERS
    row_parts = [None] * LAYERS
    for layer in reversed(range(LAYERS)):
        w_qkv, w_proj, w_in, w_out = matrices(layer)
        row_now = row_state[0, layer]
        (
            hidden_bf,
            query,
            key,
            value,
            log_total,
            context,
            scaled_one,
            inverse_one,
            normed_bf,
            slope,
            activated,
            scaled_two,
            inverse_two,
        ) = saved_layers[layer]
        d_two, gain_two, shift_two = norm_backward(upstream, scaled_two, inverse_two, row_now[4])
        grad_bias_two = jnp.sum(d_two, axis=0)
        d_two_bf = d_two.astype(jnp.bfloat16)
        d_act = jnp.einsum("rd,bdc->brc", d_two_bf, w_out, preferred_element_type=jnp.float32)
        d_pre = (d_act * slope).astype(jnp.bfloat16)
        grad_bias_in = jnp.sum(d_pre, axis=1, dtype=jnp.float32)
        d_normed = jnp.einsum("brc,bdc->rd", d_pre, w_in, preferred_element_type=jnp.float32)
        d_normed = d_two + d_normed
        d_one, gain_one, shift_one = norm_backward(d_normed, scaled_one, inverse_one, row_now[2])
        grad_bias_proj = jnp.sum(d_one, axis=0)
        d_one_bf = d_one.astype(jnp.bfloat16)
        d_context = dot(d_one_bf, w_proj, ((1,), (0,))).astype(jnp.bfloat16)
        d_context = d_context.reshape(rows, heads, HEAD_DIM)
        scores = jnp.einsum("qhd,khd->hqk", query, key, preferred_element_type=jnp.float32)
        scores = jnp.where(same_doc, scores, -1e30)
        soft = jnp.exp(scores - log_total)
        d_values = jnp.einsum(
            "hqk,qhd->khd",
            soft.astype(jnp.bfloat16),
            d_context,
            preferred_element_type=jnp.float32,
        )
        d_probs = jnp.einsum(
            "qhd,khd->hqk", d_context, value, preferred_element_type=jnp.float32
        )
        d_scores = (
            soft * (d_probs - jnp.sum(soft * d_probs, axis=-1, keepdims=True))
        ).astype(jnp.bfloat16)
        d_queries = (
            jnp.einsum("hqk,khd->qhd", d_scores, key, preferred_element_type=jnp.float32)
            * score_scale
        )
        d_keys = jnp.einsum("hqk,qhd->khd", d_scores, query, preferred_element_type=jnp.float32)
        d_qkv = jnp.stack(
            [
                d_queries.reshape(rows, width),
                own_rows(d_keys.reshape(seq_len, width)),
                own_rows(d_values.reshape(seq_len, width)),
            ]
        ).astype(jnp.bfloat16)
        grad_bias_qkv = jnp.sum(d_qkv, axis=1, dtype=jnp.float32)
        upstream = d_one + jnp.einsum(
            "brc,bdc->rd", d_qkv, w_qkv, preferred_element_type=jnp.float32
        )
        operands[layer] = (hidden_bf, d_one_bf, normed_bf, d_two_bf)
        operands[layer] += (d_qkv, context[None], d_pre, activated)
        col_parts[layer] = jnp.concatenate(
            [
                grad_bias_qkv[0:1],
                grad_bias_qkv[2:3],
                grad_bias_in,
            ],
            axis=0,
        )
        row_parts[layer] = jnp.stack(
            [grad_bias_proj, grad_bias_two, gain_one, shift_one, gain_two, shift_two]
        )
    small = jnp.stack([jnp.stack(col_parts), jnp.stack(row_parts)])
    summed = []
    for layer in operands:
        whole = jnp.concatenate(
            [
                jnp.einsum(
                    "rd,brc->bdc", layer[i], layer[4 + i], preferred_element_type=jnp.float32
                )
                for i in range(4)
            ],
            axis=0,
        )
        summed.append(
            lax.psum_scatter(whole.astype(jnp.bfloat16), BOTH, scatter_dimension=1, tiled=True)
        )
    return (hidden, upstream, jnp.concatenate(summed, axis=0), lax.psum(small, BOTH))


def run_kernels(mine, hidden_in, doc_ids, column_state, row_state, out_grad):
    units, piece, width = mine.shape
    per_layer = units // LAYERS
    blocks = (per_layer - 4) // 2
    docs = lax.dynamic_index_in_dim(doc_ids, lax.axis_index("tensor"), 0, keepdims=False)
    col_full = lax.all_gather(column_state[0], "tensor", axis=2, tiled=True)
    none = jnp.zeros_like(col_full[:, :1])
    bias = jnp.concatenate([col_full[:, :1], none, col_full[:, 1:]], axis=1)
    weights, hidden, *saved = forward(mine, hidden_in, docs, bias, row_state[0])
    low_all, mixed, context, lse, one_all, inv_one, normed_all = saved[:7]
    act_all, slope_all, two_all, inv_two = saved[7:]
    upstream = out_grad.astype(jnp.float32)
    grads = [None] * LAYERS
    col_parts = [None] * LAYERS
    row_parts = [None] * LAYERS
    for layer in reversed(range(LAYERS)):
        row_now = row_state[0, layer]
        first = layer * per_layer
        d_two, gain_two, shift_two = norm_backward(
            upstream, two_all[layer], inv_two[layer, :, :1], row_now[4]
        )
        d_two_bf = d_two.astype(jnp.bfloat16)
        d_pre, grad_bias_in, d_normed = mlp_back(
            d_two_bf, weights, layer, first + 4, blocks, slope_all
        )
        d_one, gain_one, shift_one = norm_backward(
            d_two + d_normed, one_all[layer], inv_one[layer, :, :1], row_now[2]
        )
        d_one_bf = d_one.astype(jnp.bfloat16)
        d_context = dot(d_one_bf, weights[first + 3], ((1,), (0,))).astype(jnp.bfloat16)
        d_mixed = attend_back(mixed, layer, d_context, lse, docs)
        grad_bias_mixed = jnp.sum(d_mixed, axis=1, dtype=jnp.float32)
        upstream = d_one + jnp.einsum(
            "brc,bdc->rd", d_mixed, weights[first : first + 3], preferred_element_type=jnp.float32
        )
        grads[layer] = (d_one_bf, d_two_bf, d_mixed, d_pre)
        col_parts[layer] = jnp.concatenate(
            [grad_bias_mixed[0:1], grad_bias_mixed[2:3], grad_bias_in], axis=0
        )
        row_parts[layer] = jnp.stack(
            [jnp.sum(d_one, axis=0), jnp.sum(d_two, axis=0)]
            + [gain_one, shift_one, gain_two, shift_two]
        )
    small = jnp.stack([jnp.stack(col_parts), jnp.stack(row_parts)])
    operands = [low_all, normed_all, context, act_all]
    operands += [array for layer in grads for array in layer]
    summed, total = reduce_pieces(
        operands, small.reshape(-1, width), units, (3, 1, blocks, blocks), piece, width
    )
    return (hidden, upstream, summed, total.reshape(small.shape))


def local(
    hidden_in,
    doc_ids,
    unit_slot,
    masters,
    first_moment,
    second_moment,
    column_state,
    row_state,
    out_grad,
):
    slot_count, width, col_width = masters.shape
    dp_size = lax.axis_size("dp")
    tensor_size = lax.axis_size("tensor")
    devices = dp_size * tensor_size
    slots = slot_count * dp_size
    piece = width // devices
    tensor_index = lax.axis_index("tensor")
    kernels = dp_size == 8 and tensor_size == 4 and hidden_in.shape[0] == doc_ids.shape[1]

    sent = masters.astype(jnp.bfloat16)
    if kernels:
        sent = sent.reshape(slot_count, 2, 2, 2, 4, piece, col_width)
        sent = sent.transpose(4, 3, 2, 1, 0, 5, 6)
    else:
        sent = sent.reshape(slot_count, devices, piece, col_width).transpose(1, 0, 2, 3)
    spread = lax.all_to_all(sent.reshape(devices, slot_count, piece, col_width), BOTH, 0, 0)
    spread = spread.reshape(dp_size, tensor_size, slot_count, piece, col_width)
    spread = spread.transpose(0, 2, 3, 1, 4).reshape(slots, piece, width)
    mine = spread[unit_slot]
    run = run_kernels if kernels else run_general
    hidden, upstream, summed, small = run(
        mine, hidden_in, doc_ids, column_state, row_state, out_grad
    )
    row_total = small[1]
    col_total = lax.dynamic_slice_in_dim(small[0], tensor_index * col_width, col_width, axis=2)

    slot_ids = jnp.arange(slots, dtype=jnp.int32)
    named = unit_slot[None, :] == slot_ids[:, None]
    holds = jnp.any(named, axis=1)
    unit_of = jnp.argmax(named, axis=1)
    back = jnp.where(holds[:, None, None], summed[unit_of], jnp.zeros((), jnp.bfloat16))
    back = back.reshape(dp_size, slot_count, piece, tensor_size, col_width)
    back = back.transpose(0, 3, 1, 2, 4).reshape(devices, slot_count, piece, col_width)
    owned = lax.all_to_all(back, BOTH, 0, 0)
    if kernels:
        owned = owned.reshape(4, 2, 2, 2, slot_count, piece, col_width)
        owned = owned.transpose(4, 3, 2, 1, 0, 5, 6)
    else:
        owned = owned.transpose(1, 0, 2, 3)
    owned = owned.reshape(slot_count, width, col_width).astype(jnp.float32)
    occupied = lax.dynamic_slice_in_dim(holds, lax.axis_index("dp") * slot_count, slot_count)
    occupied = occupied.astype(jnp.float32)[:, None, None]
    new_master, new_first, new_second = adamw_update(
        masters, owned, first_moment, second_moment, RATE_UNITS
    )
    unit_master = new_master * occupied
    unit_state = jnp.stack([new_first * occupied, new_second * occupied])
    new_col, col_first, col_second = adamw_update(
        column_state[0], col_total, column_state[1], column_state[2], RATE_SMALL
    )
    column_out = jnp.stack([col_total, new_col, col_first, col_second])
    new_row, row_first, row_second = adamw_update(
        row_state[0], row_total, row_state[1], row_state[2], RATE_SMALL
    )
    row_out = jnp.stack([row_total, new_row, row_first, row_second])
    return (hidden, upstream, unit_master, unit_state, column_out, row_out)


def solution(mesh):
    return jax.shard_map(
        local,
        mesh=mesh,
        in_specs=(
            P(("dp", "tensor"), None),
            P("dp", None),
            P(),
            P("dp", None, "tensor"),
            P("dp", None, "tensor"),
            P("dp", None, "tensor"),
            P(None, None, None, "tensor"),
            P(),
            P(("dp", "tensor"), None),
        ),
        out_specs=(
            P(("dp", "tensor"), None),
            P(("dp", "tensor"), None),
            P("dp", None, "tensor"),
            P(None, "dp", None, "tensor"),
            P(None, None, None, "tensor"),
            P(),
        ),
        check_vma=False,
    )
```

```python
import functools
import math

import jax
import jax.numpy as jnp
from jax import lax
from jax.experimental import pallas as pl
from jax.experimental.pallas import tpu as pltpu
from jax.sharding import PartitionSpec as P

HEAD_DIM = 64
LAYERS = 2
STEP = 3

EPS_NORM = 1e-06
RATE_UNITS = 0.05
RATE_SMALL = 0.2
WEIGHT_DECAY = 0.01
ADAM_EPS = 1e-08
BETA_MOMENT = 0.5
BOTH = ("dp", "tensor")


def norm_forward(summed, gain, shift):
    row_mean = jnp.mean(summed, axis=1, keepdims=True)
    centred = summed - row_mean
    inverse = lax.rsqrt(jnp.mean(centred * centred, axis=1, keepdims=True) + EPS_NORM)
    scaled = centred * inverse
    return (scaled * gain + shift, scaled, inverse)


def norm_backward(upstream, scaled, inverse, gain):
    d_scaled = upstream * gain
    mean_one = jnp.mean(d_scaled, axis=1, keepdims=True)
    mean_two = jnp.mean(d_scaled * scaled, axis=1, keepdims=True)
    grad_input = inverse * (d_scaled - mean_one - scaled * mean_two)
    return (grad_input, jnp.sum(upstream * scaled, axis=0), jnp.sum(upstream, axis=0))


def gelu_pair(v):
    cdf = 0.5 * (1.0 + lax.erf(v * 2.0 ** (-0.5)))
    bell = jnp.exp(-0.5 * v * v) * (2.0 * math.pi) ** (-0.5)
    return (v * cdf, cdf + v * bell)


def adamw_update(old_value, gradient, first_old, second_old, learn_rate):
    first_new = BETA_MOMENT * first_old + (1.0 - BETA_MOMENT) * gradient
    second_new = BETA_MOMENT * second_old + (1.0 - BETA_MOMENT) * gradient * gradient
    correct = 1.0 - BETA_MOMENT**STEP
    step_size = first_new / correct / (jnp.sqrt(second_new / correct) + ADAM_EPS)
    return (old_value - learn_rate * (step_size + WEIGHT_DECAY * old_value), first_new, second_new)


def dot(left, right, dims):
    return lax.dot_general(left, right, (dims, ((), ())), preferred_element_type=jnp.float32)


LANES = 2 * HEAD_DIM


def head_lanes(value, head):
    lane = lax.broadcasted_iota(jnp.int32, value.shape, 1)
    keep = lane < HEAD_DIM if head == 0 else lane >= HEAD_DIM
    return jnp.where(keep, value, jnp.zeros_like(value))


def pair_lanes(first, second):
    lane = lax.broadcasted_iota(jnp.int32, first.shape, 1)
    return jnp.where(lane < HEAD_DIM, first, second)


def attend_pair(pair, q_ref, k_ref, v_ref, mask_ref, ctx_ref, lse_ref):
    lanes = pl.ds(pl.multiple_of(pair * LANES, LANES), LANES)
    query, key, value = q_ref[:, lanes], k_ref[:, lanes], v_ref[:, lanes]
    value_t = value.T
    parts = []
    for head in range(2):
        scores = dot(head_lanes(key, head), query, ((1,), (1,))) + mask_ref[...]
        top = jnp.max(scores, axis=0, keepdims=True)
        weight = jnp.exp(scores - top)
        total = jnp.sum(weight, axis=0, keepdims=True)
        lse_ref[pair * 2 + head] = top + jnp.log(total)
        mine = value_t[head * HEAD_DIM : (head + 1) * HEAD_DIM]
        mixed = dot(mine, weight.astype(jnp.bfloat16), ((1,), (0,)))
        parts.append(mixed * (1.0 / total))
    ctx_ref[:, lanes] = jnp.concatenate(parts, axis=0).T.astype(ctx_ref.dtype)


def attend_back_pair(pair, q_ref, k_ref, v_ref, d_ref, mask_ref, lse_ref, dq_ref, dk_ref, dv_ref):
    lanes = pl.ds(pl.multiple_of(pair * LANES, LANES), LANES)
    query, key, value = q_ref[:, lanes], k_ref[:, lanes], v_ref[:, lanes]
    grad = d_ref[:, lanes]
    key_t = key.T
    parts, d_keys, d_values = [], [], []
    for head in range(2):
        scores = dot(head_lanes(key, head), query, ((1,), (1,))) + mask_ref[...]
        soft = jnp.exp(scores - lse_ref[pair * 2 + head])
        d_values.append(dot(soft.astype(jnp.bfloat16), grad, ((1,), (0,))))
        d_soft = dot(head_lanes(value, head), grad, ((1,), (1,)))
        both = soft * d_soft
        mean = jnp.sum(both, axis=0, keepdims=True)
        d_scores = (both - soft * mean).astype(jnp.bfloat16)
        d_keys.append(dot(d_scores, query, ((1,), (0,))))
        mine = key_t[head * HEAD_DIM : (head + 1) * HEAD_DIM]
        parts.append(dot(mine, d_scores, ((1,), (0,))))
    scale = HEAD_DIM ** (-0.5)
    dq_ref[:, lanes] = (jnp.concatenate(parts, axis=0).T * scale).astype(dq_ref.dtype)
    dk_ref[:, lanes] = pair_lanes(*d_keys).astype(dk_ref.dtype)
    dv_ref[:, lanes] = pair_lanes(*d_values).astype(dv_ref.dtype)


def fill_mask(mask_ref, docs_col_ref, docs_row_ref):
    same = docs_col_ref[...] == docs_row_ref[...]
    mask_ref[...] = jnp.where(same, 0.0, -1e30).astype(jnp.float32)


LAG = 2


TILE = 256


def norm_back_rows(upstream, scaled, inverse, gain):
    d_scaled = upstream * gain
    mean_one = jnp.mean(d_scaled, axis=1, keepdims=True)
    mean_two = jnp.mean(d_scaled * scaled, axis=1, keepdims=True)
    return inverse * (d_scaled - mean_one - scaled * mean_two)


def backward_kernel(
    out_grad_ref,
    docs_col_ref,
    docs_row_ref,
    row_ref,
    weights_ref,
    low_ref,
    mixed_ref,
    ctx_ref,
    lse_ref,
    one_ref,
    inv_one_ref,
    normed_ref,
    act_ref,
    slope_ref,
    two_ref,
    inv_two_ref,
    out_ref,
    total_ref,
    small_out,
    left_buf,
    right_buf,
    unit_buf,
    scaled_buf,
    inv_buf,
    slope_buf,
    mixed_buf,
    lse_buf,
    mask_buf,
    d_ctx_buf,
    core_out,
    core_in,
    sum_core,
    first_in,
    sum_first,
    second_in,
    sum_second,
    z_in,
    small_sum,
    small_got,
    load_sem,
    core_sems,
    first_sems,
    second_sems,
    z_sems,
    small_sems,
):
    units, piece, width = out_ref.shape
    rows = total_ref.shape[0]
    per_layer = units // LAYERS
    blocks = (per_layer - 4) // 2
    at_out, at_query = 2 * blocks, 2 * blocks + 1
    dp, tensor = lax.axis_index("dp"), lax.axis_index("tensor")
    z, y, x, c = dp // 2, dp % 2, tensor // 2, tensor % 2
    half = width // 2
    quarter, eighth = half // 2, half // 4
    to_core = (dp, x * 2 + 1 - c)
    to_x = (dp, (1 - x) * 2 + c)
    to_y = (z * 2 + 1 - y, tensor)
    to_z = [(((z + k) % 4) * 2 + y, tensor) for k in (1, 2, 3)]
    to_z1 = ((z + 1 - 2 * (z % 2)) * 2 + y, tensor)
    to_z2 = (((z + 2) % 4) * 2 + y, tensor)
    mesh_id = pl.DeviceIdType.MESH

    barrier = pltpu.get_barrier_semaphore()
    for peer in (to_core, to_x, to_y, *to_z):
        pl.semaphore_signal(barrier, inc=1, device_id=peer, device_id_type=mesh_id)

    def remote(src, dst, sems, send, recv, peer):
        return pltpu.make_async_remote_copy(
            src_ref=src,
            dst_ref=dst,
            send_sem=sems.at[send],
            recv_sem=sems.at[recv],
            device_id=peer,
            device_id_type=mesh_id,
        )

    def place(s):
        return LAYERS - 1 - s // per_layer, s % per_layer

    def unit_of(s):
        layer, j = place(s)
        feed = jnp.where(j % 2 == 0, 4 + blocks + j // 2, 4 + j // 2)
        return layer * per_layer + jnp.where(
            j < at_out, feed, jnp.where(j == at_out, 3, j - at_query)
        )

    def left_of(s):
        j = s % per_layer
        feed = jnp.where(j % 2 == 0, 3, 2)
        return jnp.where(j < at_out, feed, jnp.where(j == at_out, 1, 0))

    def loaded_slot(s):
        return ((s // per_layer) * (blocks + 1) + (s % per_layer) // 2) % 2

    def right_of(s):
        j = s % per_layer
        feed = jnp.where(j % 2 == 0, loaded_slot(s), 2 + (j // 2) % 2)
        return jnp.where(
            j < at_out, feed, jnp.where(j == at_out, loaded_slot(s), 4 + j - at_query)
        )

    local = pltpu.make_async_copy

    def unit_load(s):
        return local(weights_ref.at[unit_of(s)], unit_buf.at[s % 2], load_sem.at[0, s % 2])

    def act_load(layer, block, slot):
        return local(act_ref.at[layer, block], right_buf.at[slot], load_sem.at[1, slot])

    def ctx_load(layer, slot):
        return local(ctx_ref.at[layer], right_buf.at[slot], load_sem.at[1, slot])

    def slope_load(layer, block):
        return local(slope_ref.at[layer, block], slope_buf, load_sem.at[2, 0])

    def norm_loads(layer, which):
        scaled, inv = ((one_ref, inv_one_ref), (two_ref, inv_two_ref))[which]
        return [
            local(scaled.at[layer], scaled_buf, load_sem.at[3, 0]),
            local(inv.at[layer], inv_buf, load_sem.at[3, 1]),
        ]

    def mixed_loads(layer):
        return [
            local(mixed_ref.at[layer], mixed_buf, load_sem.at[4, 0]),
            local(lse_ref.at[layer], lse_buf, load_sem.at[4, 1]),
        ]

    def normed_load(layer):
        return local(normed_ref.at[layer], left_buf.at[2], load_sem.at[2, 1])

    def low_load(layer):
        return local(low_ref.at[layer], left_buf.at[0], load_sem.at[5, 0])

    def begin(*copies):
        for copy in copies:
            copy.start()

    def finish(*copies):
        for copy in copies:
            copy.wait()

    def note(row, value):
        small_sum[0, pl.ds(row, 1), :] = value

    def column(layer, i):
        return layer * (2 + blocks) + i

    def row(layer, i):
        return LAYERS * (2 + blocks) + layer * 6 + i

    def norm_back(layer, gain_row, bias_row, low_slot):
        gain = row_ref[layer * 6 + gain_row]
        size = 128

        def one(tile, carry):
            part = pl.ds(pl.multiple_of(tile * size, size), size)
            upstream = total_ref[part, :]
            scaled = scaled_buf[part, :]
            inside = norm_back_rows(upstream, scaled, inv_buf[part, 0:1], gain)
            total_ref[part, :] = inside
            left_buf[low_slot, part, :] = inside.astype(jnp.bfloat16)
            sums = (upstream * scaled, upstream, inside)
            return tuple(a + jnp.sum(b, axis=0, keepdims=True) for a, b in zip(carry, sums))

        zero = jnp.zeros((1, width), jnp.float32)
        gains, shifts, biases = lax.fori_loop(0, rows // size, one, (zero, zero, zero))
        note(row(layer, gain_row), gains)
        note(row(layer, gain_row + 1), shifts)
        note(row(layer, bias_row), biases)

    def heads(start, stop):
        inputs = [mixed_buf.at[i] for i in range(3)]
        grads = [right_buf.at[4 + i] for i in range(3)]

        def one(pair, carry):
            attend_back_pair(pair, *inputs, d_ctx_buf, mask_buf, lse_buf, *grads)
            return carry

        lax.fori_loop(start, stop, one, 0)

    pairs = width // LANES

    def data_gradient(s):
        layer, j = place(s)
        matrix = unit_buf.at[s % 2]
        slot = loaded_slot(s)

        @pl.when(j == 0)
        def _():
            finish(*norm_loads(layer, 1))

            @pl.when(s == 0)
            def _():
                total_ref[...] = out_grad_ref[...].astype(jnp.float32)

            norm_back(layer, 4, 1, 3)
            begin(*norm_loads(layer, 0), *mixed_loads(layer))

        @pl.when(j == 1)
        def _():
            finish(normed_load(layer))
            begin(low_load(layer))

        @pl.when((j < at_out) & (j % 2 == 0))
        def _():
            block = j // 2
            finish(slope_load(layer, block), act_load(layer, block, slot))

            @pl.when(block < blocks - 1)
            def _():
                act_load(layer, block + 1, 1 - slot).start()

            @pl.when(block == blocks - 1)
            def _():
                ctx_load(layer, 1 - slot).start()

            d_act = dot(left_buf[3], matrix[...], ((1,), (0,)))
            d_pre = (d_act * slope_buf[...].astype(jnp.float32)).astype(jnp.bfloat16)
            right_buf[2 + block % 2] = d_pre
            sums = jnp.sum(d_pre.astype(jnp.float32), axis=0, keepdims=True)
            note(column(layer, 2 + block), sums)

            @pl.when(block < blocks - 1)
            def _():
                slope_load(layer, block + 1).start()

        @pl.when((j < at_out) & (j % 2 == 1))
        def _():
            total_ref[...] += dot(right_buf[2 + (j // 2) % 2], matrix[...], ((1,), (1,)))

        @pl.when(j == at_out)
        def _():
            finish(*norm_loads(layer, 0), *mixed_loads(layer), ctx_load(layer, slot))
            norm_back(layer, 2, 0, 1)

            @pl.when(layer > 0)
            def _():
                act_load(layer - 1, 0, 1 - slot).start()
                begin(*norm_loads(layer - 1, 1))
                slope_load(layer - 1, 0).start()

            d_ctx_buf[...] = dot(left_buf[1], matrix[...], ((1,), (0,))).astype(jnp.bfloat16)
            heads(0, pairs // 2)

        @pl.when(j == at_query)
        def _():
            finish(low_load(layer))

            @pl.when(layer > 0)
            def _():
                normed_load(layer - 1).start()

            heads(pairs // 2, pairs)
            for i, number in ((0, 0), (2, 1)):
                sums = jnp.sum(right_buf[4 + i].astype(jnp.float32), axis=0, keepdims=True)
                note(column(layer, number), sums)

        @pl.when(j >= at_query)
        def _():
            total_ref[...] += dot(right_buf[4 + j - at_query], matrix[...], ((1,), (1,)))

    def product(s, side, tile):
        start = pl.multiple_of(side * half + tile * TILE, TILE)
        left = left_buf[left_of(s), :, pl.ds(start, TILE)]
        return lax.dot_general(
            left, right_buf[right_of(s)], (((0,), (0,)), ((), ())), preferred_element_type=jnp.float32
        )

    def core_copy(s):
        return remote(
            core_out.at[s % 2], core_in.at[s % 4], core_sems, (0, s % 2), (1, s % 4), to_core
        )

    def first_copies(s):
        here = sum_core.at[s % 3]
        return (
            remote(
                here.at[pl.ds(pl.multiple_of((1 - x) * quarter, quarter), quarter), pl.ds(0, half)],
                first_in.at[s % 4, 0],
                first_sems,
                (0, 0, s % 3),
                (1, 0, s % 4),
                to_x,
            ),
            *(
                remote(
                    here.at[
                        pl.ds(pl.multiple_of(i * quarter + (1 - y) * eighth, eighth), eighth),
                        pl.ds(half, half),
                    ],
                    first_in.at[s % 4, 1, pl.ds(i * eighth, eighth)],
                    first_sems,
                    (0, 1 + i, s % 3),
                    (1, 1 + i, s % 4),
                    to_y,
                )
                for i in range(2)
            ),
        )

    def second_copies(s):
        here = sum_first.at[s % 3]
        return (
            remote(
                here.at[0, pl.ds(pl.multiple_of((1 - y) * eighth, eighth), eighth)],
                second_in.at[s % 4, 0],
                second_sems,
                (0, 0, s % 3),
                (1, 0, s % 4),
                to_y,
            ),
            remote(
                here.at[1, pl.ds(pl.multiple_of((1 - x) * eighth, eighth), eighth)],
                second_in.at[s % 4, 1],
                second_sems,
                (0, 1, s % 3),
                (1, 1, s % 4),
                to_x,
            ),
        )

    def z_copies(s):
        return [
            remote(
                sum_second.at[s % 3, pl.ds(pl.multiple_of(((z + k) % 4) * piece, piece), piece)],
                z_in.at[s % 4, k - 1],
                z_sems,
                (0, k - 1, s % 3),
                (1, k - 1, s % 4),
                to_z[k - 1],
            )
            for k in (1, 2, 3)
        ]

    small_peers = (to_core, to_x, to_y, to_z1, to_z2)

    def small_copy(stage):
        return remote(
            small_sum.at[stage],
            small_got.at[stage],
            small_sems,
            (0, stage),
            (1, stage),
            small_peers[stage],
        )

    top = LAYERS - 1
    begin(
        *norm_loads(top, 1),
        unit_load(jnp.int32(0)),
        slope_load(top, 0),
        act_load(top, 0, 0),
        normed_load(top),
    )
    fill_mask(mask_buf, docs_col_ref, docs_row_ref)
    pl.semaphore_wait(barrier, 6)

    def step(s, carry):
        last = s - 3 * LAG - 1

        @pl.when((last >= 0) & (last < units))
        def _():
            for copy in z_copies(last):
                copy.wait()
            total = sum_second[last % 3, pl.ds(pl.multiple_of(z * piece, piece), piece), :].astype(
                jnp.float32
            )
            for k in range(3):
                total = total + z_in[last % 4, k].astype(jnp.float32)
            out_ref[unit_of(last)] = total.astype(out_ref.dtype)

        third = s - 2 * LAG - 1

        @pl.when((third >= 0) & (third < units))
        def _():
            for copy in second_copies(third):
                copy.wait()
            for part, side in ((0, y), (1, x)):
                mine = sum_first[
                    third % 3, part, pl.ds(pl.multiple_of(side * eighth, eighth), eighth), :
                ]
                total = mine.astype(jnp.float32) + second_in[third % 4, part].astype(jnp.float32)
                sum_second[third % 3, :, part * half : (part + 1) * half] = total.astype(
                    jnp.bfloat16
                )
            for copy in z_copies(third):
                copy.start()

        second = s - LAG - 1

        @pl.when((second >= 0) & (second < units))
        def _():
            for copy in first_copies(second):
                copy.wait()
            mine = sum_core[
                second % 3, pl.ds(pl.multiple_of(x * quarter, quarter), quarter), 0:half
            ]
            total = mine.astype(jnp.float32) + first_in[second % 4, 0].astype(jnp.float32)
            sum_first[second % 3, 0] = total.astype(jnp.bfloat16)
            for i in range(2):
                mine = sum_core[
                    second % 3,
                    pl.ds(pl.multiple_of(i * quarter + y * eighth, eighth), eighth),
                    half : 2 * half,
                ]
                part = pl.ds(i * eighth, eighth)
                total = mine.astype(jnp.float32) + first_in[second % 4, 1, part, :].astype(
                    jnp.float32
                )
                sum_first[second % 3, 1, part, :] = total.astype(jnp.bfloat16)
            for copy in second_copies(second):
                copy.start()

        @pl.when(s < units)
        def _():
            unit_load(s).wait()

            @pl.when(s + 1 < units)
            def _():
                unit_load(s + 1).start()

            data_gradient(s)

            @pl.when(s >= 2)
            def _():
                core_copy(s - 2).wait_send()

            def one(tile, carry):
                part = pl.ds(pl.multiple_of(tile * TILE, TILE), TILE)
                core_out[s % 2, part, :] = product(s, 1 - c, tile).astype(jnp.bfloat16)
                return carry

            lax.fori_loop(0, half // TILE, one, 0)
            core_copy(s).start()

        first = s - 1

        @pl.when((first >= 0) & (first < units))
        def _():
            core_copy(first).wait_recv()

            def one(tile, carry):
                part = pl.ds(pl.multiple_of(tile * TILE, TILE), TILE)
                total = product(first, c, tile) + core_in[first % 4, part, :].astype(jnp.float32)
                sum_core[first % 3, part, :] = total.astype(jnp.bfloat16)
                return carry

            lax.fori_loop(0, half // TILE, one, 0)
            for copy in first_copies(first):
                copy.start()

        for stage in range(6):

            @pl.when(s == units + stage)
            def _(stage=stage):
                if stage > 0:
                    small_copy(stage - 1).wait()
                    total = small_sum[stage - 1] + small_got[stage - 1]
                    if stage < 5:
                        small_sum[stage] = total
                    else:
                        small_out[...] = total
                if stage < 5:
                    small_copy(stage).start()

        return carry

    lax.fori_loop(0, units + 3 * LAG + 1, step, 0)
    for s in (units - 2, units - 1):
        core_copy(s).wait_send()


def backward(out_grad, docs, row_now, weights, saved, piece):
    units, width, _ = weights.shape
    rows = out_grad.shape[0]
    blocks = (units // LAYERS - 4) // 2
    half = width // 2
    low, full = jnp.bfloat16, jnp.float32
    small = (LAYERS * (8 + blocks), width)
    any_spec = pl.BlockSpec(memory_space=pl.ANY)
    vmem_spec = pl.BlockSpec(memory_space=pltpu.VMEM)
    dma = pltpu.SemaphoreType.DMA
    summed, total, small = pl.pallas_call(
        backward_kernel,
        out_shape=(
            jax.ShapeDtypeStruct((units, piece, width), low),
            jax.ShapeDtypeStruct((rows, width), full),
            jax.ShapeDtypeStruct(small, full),
        ),
        in_specs=[vmem_spec] * 4 + [any_spec] * (1 + len(saved)),
        out_specs=(vmem_spec, vmem_spec, vmem_spec),
        scratch_shapes=[
            pltpu.VMEM((4, rows, width), low),
            pltpu.VMEM((7, rows, width), low),
            pltpu.VMEM((2, width, width), low),
            pltpu.VMEM((rows, width), full),
            pltpu.VMEM((rows, 128), full),
            pltpu.VMEM((rows, width), low),
            pltpu.VMEM((3, rows, width), low),
            pltpu.VMEM((width // HEAD_DIM, 1, rows), full),
            pltpu.VMEM((rows, rows), full),
            pltpu.VMEM((rows, width), low),
            pltpu.VMEM((2, half, width), low),
            pltpu.VMEM((4, half, width), low),
            pltpu.VMEM((3, half, width), low),
            pltpu.VMEM((4, 2, half // 2, half), low),
            pltpu.VMEM((3, 2, half // 2, half), low),
            pltpu.VMEM((4, 2, half // 4, half), low),
            pltpu.VMEM((3, half // 4, width), low),
            pltpu.VMEM((4, 3, piece, width), low),
            pltpu.VMEM((5,) + small, full),
            pltpu.VMEM((5,) + small, full),
            dma((6, 2)),
            dma((2, 4)),
            dma((2, 3, 4)),
            dma((2, 2, 4)),
            dma((2, 3, 4)),
            dma((2, 5)),
        ],
        compiler_params=pltpu.CompilerParams(
            collective_id=1, has_side_effects=True, vmem_limit_bytes=63 * 1024 * 1024
        ),
        name="backward_reduce",
    )(out_grad, docs[:, None], docs[None, :], row_now.reshape(-1, 1, width), weights, *saved)
    return (total, summed, small)


def norm_rows(value, gain, shift):
    centred = value - jnp.mean(value, axis=1, keepdims=True)
    inverse = lax.rsqrt(jnp.mean(centred * centred, axis=1, keepdims=True) + EPS_NORM)
    scaled = centred * inverse
    return (scaled * gain + shift, scaled, inverse)


NORM_ROWS = 128


def forward_kernel(
    own_ref,
    hidden_ref,
    docs_col_ref,
    docs_row_ref,
    bias_ref,
    row_ref,
    out_ref,
    final_ref,
    *refs,
):
    saved, bufs = refs[:11], refs[11:22]
    (x_buf, normed_buf, total_buf, mask_buf, unit_buf, own_sem, sems, unit_sem, save_sem) = refs[22:]
    (low_buf, mixed_buf, ctx_buf, lse_buf, one_buf, inv_one_buf, nb_buf) = bufs[:7]
    (act_buf, slope_buf, two_buf, inv_two_buf) = bufs[7:]
    units, piece, width = own_ref.shape
    rows = hidden_ref.shape[0]
    per_layer = units // LAYERS
    blocks = (per_layer - 4) // 2
    dp, tensor = lax.axis_index("dp"), lax.axis_index("tensor")
    z, y, x, c = dp // 2, dp % 2, tensor // 2, tensor % 2
    half = width // 2
    line, plane = 4 * piece, 8 * piece
    to_core = (dp, x * 2 + 1 - c)
    to_x = (dp, (1 - x) * 2 + c)
    to_y = (z * 2 + 1 - y, tensor)
    to_z = [(((z + k) % 4) * 2 + y, tensor) for k in (1, 2, 3)]
    mesh_id = pl.DeviceIdType.MESH

    barrier = pltpu.get_barrier_semaphore()
    for peer in (to_core, to_x, to_y, *to_z):
        pl.semaphore_signal(barrier, inc=1, device_id=peer, device_id_type=mesh_id)
    pl.semaphore_wait(barrier, 6)

    my_line = pl.multiple_of(((c * 2 + x) * 2 + y) * line, line)
    my_rows = pl.ds(pl.multiple_of(my_line + z * piece, piece), piece)
    first, second = pl.ds(0, half), pl.ds(half, half)

    def remote(src, dst, index, unit, peer):
        return pltpu.make_async_remote_copy(
            src_ref=src,
            dst_ref=dst,
            send_sem=sems.at[0, index, unit],
            recv_sem=sems.at[1, index, unit],
            device_id=peer,
            device_id_type=mesh_id,
        )

    def own_copy(unit):
        return pltpu.make_async_copy(own_ref.at[unit], out_ref.at[unit, my_rows], own_sem.at[unit])

    def stage_z(unit):
        there = out_ref.at[unit, my_rows]
        return [remote(own_ref.at[unit], there, k, unit, to_z[k]) for k in range(3)]

    def stage_one(unit):
        rows = pl.ds(my_line, line)
        one, two = out_ref.at[unit, rows, first], out_ref.at[unit, rows, second]
        return [remote(one, one, 3, unit, to_y), remote(two, two, 4, unit, to_x)]

    def stage_two(unit):
        rows = pl.ds(pl.multiple_of((c * 2 + x) * plane, plane), plane)
        one = out_ref.at[unit, rows, first]
        copies = [remote(one, one, 5, unit, to_x)]
        for i in range(2):
            rows = pl.ds(pl.multiple_of(((c * 2 + i) * 2 + y) * line, line), line)
            two = out_ref.at[unit, rows, second]
            copies.append(remote(two, two, 6 + i, unit, to_y))
        return copies

    def stage_core(unit):
        there = out_ref.at[unit, pl.ds(pl.multiple_of(c * 2 * plane, 2 * plane), 2 * plane)]
        return [remote(there, there, 8, unit, to_core)]

    stages = (stage_z, stage_one, stage_two, stage_core)

    def unit_copy(unit):
        slot = unit % 2
        return pltpu.make_async_copy(out_ref.at[unit], unit_buf.at[slot], unit_sem.at[slot])

    def save(number, layer, block=None):
        src, dst, sem = bufs[number], saved[number].at[layer], save_sem.at[number, 0]
        if block is not None:
            src, dst, sem = src.at[block], dst.at[block], save_sem.at[number, block]
        return pltpu.make_async_copy(src, dst, sem)

    def free(numbers, layer, block=None):
        @pl.when(layer > 0)
        def _():
            for number in numbers:
                save(number, layer - 1, block).wait()

    def heads(start, stop):
        def one(pair, carry):
            attend_pair(
                pair, mixed_buf.at[0], mixed_buf.at[1], mixed_buf.at[2], mask_buf, ctx_buf, lse_buf
            )
            return carry

        lax.fori_loop(start, stop, one, 0)

    def over_rows(body):
        def one(tile, carry):
            body(pl.ds(pl.multiple_of(tile * NORM_ROWS, NORM_ROWS), NORM_ROWS))
            return carry

        lax.fori_loop(0, rows // NORM_ROWS, one, 0)

    pairs = width // LANES

    def compute(unit):
        layer, j = unit // per_layer, unit % per_layer
        matrix = unit_buf.at[unit % 2]

        def small(i):
            return row_ref[layer * 6 + i]

        @pl.when(j == 0)
        def _():
            free((0, 1), layer)

            @pl.when(layer == 0)
            def _():
                x_buf[...] = hidden_ref[...].astype(jnp.float32)

            low_buf[...] = x_buf[...].astype(jnp.bfloat16)
            save(0, layer).start()

        @pl.when(j < 3)
        def _():
            value = dot(low_buf[...], matrix[...], ((1,), (0,)))
            value = value + bias_ref[layer * (3 + blocks) + j]
            scale = jnp.where(j == 0, HEAD_DIM ** (-0.5), 1.0)
            mixed_buf[j] = (value * scale).astype(jnp.bfloat16)

        @pl.when(j == 2)
        def _():
            save(1, layer).start()
            free((2, 3), layer)
            heads(0, pairs // 2)

        @pl.when(j == 3)
        def _():
            heads(pairs // 2, pairs)
            save(2, layer).start()
            save(3, layer).start()
            total_buf[...] = dot(ctx_buf[...], matrix[...], ((1,), (1,)))
            free((4, 5, 6), layer)

            def body(part):
                value = x_buf[part, :] + total_buf[part, :] + small(0)
                normed, scaled, inverse = norm_rows(value, small(2), small(3))
                normed_buf[part, :] = normed
                nb_buf[part, :] = normed.astype(jnp.bfloat16)
                one_buf[part, :] = scaled
                inv_one_buf[part, :] = jnp.broadcast_to(inverse, (NORM_ROWS, 128))

            over_rows(body)
            for number in (4, 5, 6):
                save(number, layer).start()

        @pl.when((j >= 4) & (j < 4 + blocks))
        def _():
            block = j - 4
            free((7, 8), layer, block)
            value = dot(nb_buf[...], matrix[...], ((1,), (0,)))
            act, slope = gelu_pair(value + bias_ref[layer * (3 + blocks) + 3 + block])
            act_buf[block] = act.astype(jnp.bfloat16)
            slope_buf[block] = slope.astype(jnp.bfloat16)
            save(7, layer, block).start()
            save(8, layer, block).start()

        @pl.when(j >= 4 + blocks)
        def _():
            block = j - 4 - blocks
            part = dot(act_buf[block], matrix[...], ((1,), (1,)))

            @pl.when(block == 0)
            def _():
                total_buf[...] = part

            @pl.when(block > 0)
            def _():
                total_buf[...] += part

        @pl.when(j == per_layer - 1)
        def _():
            free((9, 10), layer)

            def body(part):
                value = normed_buf[part, :] + total_buf[part, :] + small(1)
                output, scaled, inverse = norm_rows(value, small(4), small(5))
                x_buf[part, :] = output
                two_buf[part, :] = scaled
                inv_two_buf[part, :] = jnp.broadcast_to(inverse, (NORM_ROWS, 128))

            over_rows(body)
            save(9, layer).start()
            save(10, layer).start()

    def step(s, carry):
        for number in range(len(stages) + 1):
            unit = s - number * LAG

            @pl.when((unit >= 0) & (unit < units))
            def _(unit=unit, number=number):
                if number == 0:
                    own_copy(unit).start()
                else:
                    if number == 1:
                        own_copy(unit).wait()
                    for copy in stages[number - 1](unit):
                        copy.wait()
                if number < len(stages):
                    for copy in stages[number](unit):
                        copy.start()
                else:
                    unit_copy(unit).start()

        done = s - len(stages) * LAG - 1

        @pl.when(done >= 0)
        def _():
            unit_copy(done).wait()
            compute(done)

        return carry

    fill_mask(mask_buf, docs_col_ref, docs_row_ref)
    lax.fori_loop(0, units + len(stages) * LAG + 1, step, 0)
    final_ref[...] = x_buf[...]
    last = LAYERS - 1
    for number in (0, 1, 2, 3, 4, 5, 6, 9, 10):
        save(number, last).wait()
    for block in range(blocks):
        save(7, last, block).wait()
        save(8, last, block).wait()


def forward(own, hidden_in, docs, bias, row_now):
    units, piece, width = own.shape
    rows = hidden_in.shape[0]
    blocks = (units // LAYERS - 4) // 2
    low, full = jnp.bfloat16, jnp.float32
    kept = [
        ((rows, width), low),
        ((3, rows, width), low),
        ((rows, width), low),
        ((width // HEAD_DIM, 1, rows), full),
        ((rows, width), full),
        ((rows, 128), full),
        ((rows, width), low),
        ((blocks, rows, width), low),
        ((blocks, rows, width), low),
        ((rows, width), full),
        ((rows, 128), full),
    ]
    any_spec = pl.BlockSpec(memory_space=pl.ANY)
    vmem_spec = pl.BlockSpec(memory_space=pltpu.VMEM)
    dma = pltpu.SemaphoreType.DMA
    return pl.pallas_call(
        forward_kernel,
        out_shape=[
            jax.ShapeDtypeStruct((units, width, width), low),
            jax.ShapeDtypeStruct((rows, width), full),
        ]
        + [jax.ShapeDtypeStruct((LAYERS,) + shape, dtype) for shape, dtype in kept],
        in_specs=[any_spec] + [vmem_spec] * 5,
        out_specs=[any_spec, vmem_spec] + [any_spec] * len(kept),
        scratch_shapes=[pltpu.VMEM(shape, dtype) for shape, dtype in kept]
        + [
            pltpu.VMEM((rows, width), full),
            pltpu.VMEM((rows, width), full),
            pltpu.VMEM((rows, width), full),
            pltpu.VMEM((rows, rows), full),
            pltpu.VMEM((2, width, width), low),
            dma((units,)),
            dma((2, 9, units)),
            dma((2,)),
            dma((len(kept), blocks)),
        ],
        compiler_params=pltpu.CompilerParams(
            collective_id=2, has_side_effects=True, vmem_limit_bytes=60 * 1024 * 1024
        ),
        name="gather_forward",
    )(
        own,
        hidden_in,
        docs[:, None],
        docs[None, :],
        bias.reshape(-1, 1, width),
        row_now.reshape(-1, 1, width),
    )


def run_general(mine, hidden_in, doc_ids, column_state, row_state, out_grad):
    units, piece, width = mine.shape
    per_layer = units // LAYERS
    blocks = (per_layer - 4) // 2
    tensor_size = lax.axis_size("tensor")
    rows = hidden_in.shape[0]
    seq_len = doc_ids.shape[1]
    heads = width // HEAD_DIM
    share = seq_len // rows
    tensor_index = lax.axis_index("tensor")
    groups = [list(range(i, i + share)) for i in range(0, tensor_size, share)]
    score_scale = HEAD_DIM ** (-0.5)
    weights = jnp.concatenate(
        [
            lax.all_gather(
                mine[layer * per_layer : (layer + 1) * per_layer], BOTH, axis=1, tiled=True
            )
            for layer in range(LAYERS)
        ],
        axis=0,
    )

    def matrices(layer):
        unit = weights[layer * per_layer : (layer + 1) * per_layer]
        return (unit[:3], unit[3], unit[4 : 4 + blocks], unit[4 + blocks :])

    row_docs = lax.dynamic_slice_in_dim(doc_ids, tensor_index // share, 1, axis=0)[0]
    my_docs = lax.dynamic_slice_in_dim(row_docs, (tensor_index % share) * rows, rows)
    same_doc = (my_docs[:, None] == row_docs[None, :])[None]

    def whole_row(value):
        if share == 1:
            return value
        return lax.all_gather(value, "tensor", axis=0, tiled=True, axis_index_groups=groups)

    def own_rows(value):
        if share == 1:
            return value
        return lax.psum_scatter(
            value, "tensor", scatter_dimension=0, tiled=True, axis_index_groups=groups
        )

    col_full = lax.all_gather(column_state[0], "tensor", axis=2, tiled=True)
    hidden = hidden_in.astype(jnp.float32)
    saved_layers = []
    for layer in range(LAYERS):
        w_qkv, w_proj, w_in, w_out = matrices(layer)
        row_now = row_state[0, layer]
        col_now = col_full[layer]
        hidden_bf = hidden.astype(jnp.bfloat16)
        query, key, value = (dot(hidden_bf, w_qkv[i], ((1,), (0,))) for i in range(3))
        query = ((query + col_now[0]) * score_scale).astype(jnp.bfloat16)
        key = key.astype(jnp.bfloat16)
        value = (value + col_now[1]).astype(jnp.bfloat16)
        query = query.reshape(rows, heads, HEAD_DIM)
        key = whole_row(key).reshape(seq_len, heads, HEAD_DIM)
        value = whole_row(value).reshape(seq_len, heads, HEAD_DIM)
        scores = jnp.einsum("qhd,khd->hqk", query, key, preferred_element_type=jnp.float32)
        scores = jnp.where(same_doc, scores, -1e30)
        row_top = jnp.max(scores, axis=-1, keepdims=True)
        log_total = row_top + jnp.log(
            jnp.sum(jnp.exp(scores - row_top), axis=-1, keepdims=True)
        )
        soft_bf = jnp.exp(scores - log_total).astype(jnp.bfloat16)
        context = jnp.einsum("hqk,khd->qhd", soft_bf, value, preferred_element_type=jnp.float32)
        context = context.reshape(rows, width).astype(jnp.bfloat16)
        attended = dot(context, w_proj, ((1,), (1,)))
        normed, scaled_one, inverse_one = norm_forward(
            hidden + attended + row_now[0], row_now[2], row_now[3]
        )
        normed_bf = normed.astype(jnp.bfloat16)
        pre_act = jnp.einsum("rd,bdc->brc", normed_bf, w_in, preferred_element_type=jnp.float32)
        activated, slope = gelu_pair(pre_act + col_now[2:, None])
        activated = activated.astype(jnp.bfloat16)
        slope = slope.astype(jnp.bfloat16)
        mlp_out = jnp.einsum(
            "brc,bdc->rd", activated, w_out, preferred_element_type=jnp.float32
        )
        output, scaled_two, inverse_two = norm_forward(
            normed + mlp_out + row_now[1], row_now[4], row_now[5]
        )
        saved_layers.append(
            (hidden_bf, query, key, value, log_total, context, scaled_one, inverse_one, normed_bf)
            + (slope, activated, scaled_two, inverse_two)
        )
        hidden = output
    upstream = out_grad.astype(jnp.float32)
    operands = [None] * LAYERS
    col_parts = [None] * LAYERS
    row_parts = [None] * LAYERS
    for layer in reversed(range(LAYERS)):
        w_qkv, w_proj, w_in, w_out = matrices(layer)
        row_now = row_state[0, layer]
        (
            hidden_bf,
            query,
            key,
            value,
            log_total,
            context,
            scaled_one,
            inverse_one,
            normed_bf,
            slope,
            activated,
            scaled_two,
            inverse_two,
        ) = saved_layers[layer]
        d_two, gain_two, shift_two = norm_backward(upstream, scaled_two, inverse_two, row_now[4])
        grad_bias_two = jnp.sum(d_two, axis=0)
        d_two_bf = d_two.astype(jnp.bfloat16)
        d_act = jnp.einsum("rd,bdc->brc", d_two_bf, w_out, preferred_element_type=jnp.float32)
        d_pre = (d_act * slope).astype(jnp.bfloat16)
        grad_bias_in = jnp.sum(d_pre, axis=1, dtype=jnp.float32)
        d_normed = jnp.einsum("brc,bdc->rd", d_pre, w_in, preferred_element_type=jnp.float32)
        d_normed = d_two + d_normed
        d_one, gain_one, shift_one = norm_backward(d_normed, scaled_one, inverse_one, row_now[2])
        grad_bias_proj = jnp.sum(d_one, axis=0)
        d_one_bf = d_one.astype(jnp.bfloat16)
        d_context = dot(d_one_bf, w_proj, ((1,), (0,))).astype(jnp.bfloat16)
        d_context = d_context.reshape(rows, heads, HEAD_DIM)
        scores = jnp.einsum("qhd,khd->hqk", query, key, preferred_element_type=jnp.float32)
        scores = jnp.where(same_doc, scores, -1e30)
        soft = jnp.exp(scores - log_total)
        d_values = jnp.einsum(
            "hqk,qhd->khd",
            soft.astype(jnp.bfloat16),
            d_context,
            preferred_element_type=jnp.float32,
        )
        d_probs = jnp.einsum(
            "qhd,khd->hqk", d_context, value, preferred_element_type=jnp.float32
        )
        d_scores = (
            soft * (d_probs - jnp.sum(soft * d_probs, axis=-1, keepdims=True))
        ).astype(jnp.bfloat16)
        d_queries = (
            jnp.einsum("hqk,khd->qhd", d_scores, key, preferred_element_type=jnp.float32)
            * score_scale
        )
        d_keys = jnp.einsum("hqk,qhd->khd", d_scores, query, preferred_element_type=jnp.float32)
        d_qkv = jnp.stack(
            [
                d_queries.reshape(rows, width),
                own_rows(d_keys.reshape(seq_len, width)),
                own_rows(d_values.reshape(seq_len, width)),
            ]
        ).astype(jnp.bfloat16)
        grad_bias_qkv = jnp.sum(d_qkv, axis=1, dtype=jnp.float32)
        upstream = d_one + jnp.einsum(
            "brc,bdc->rd", d_qkv, w_qkv, preferred_element_type=jnp.float32
        )
        operands[layer] = (hidden_bf, d_one_bf, normed_bf, d_two_bf)
        operands[layer] += (d_qkv, context[None], d_pre, activated)
        col_parts[layer] = jnp.concatenate(
            [
                grad_bias_qkv[0:1],
                grad_bias_qkv[2:3],
                grad_bias_in,
            ],
            axis=0,
        )
        row_parts[layer] = jnp.stack(
            [grad_bias_proj, grad_bias_two, gain_one, shift_one, gain_two, shift_two]
        )
    small = jnp.stack([jnp.stack(col_parts), jnp.stack(row_parts)])
    summed = []
    for layer in operands:
        whole = jnp.concatenate(
            [
                jnp.einsum(
                    "rd,brc->bdc", layer[i], layer[4 + i], preferred_element_type=jnp.float32
                )
                for i in range(4)
            ],
            axis=0,
        )
        summed.append(
            lax.psum_scatter(whole.astype(jnp.bfloat16), BOTH, scatter_dimension=1, tiled=True)
        )
    return (hidden, upstream, jnp.concatenate(summed, axis=0), lax.psum(small, BOTH))


def run_kernels(mine, hidden_in, doc_ids, column_state, row_state, out_grad):
    units, piece, width = mine.shape
    per_layer = units // LAYERS
    blocks = (per_layer - 4) // 2
    docs = lax.dynamic_index_in_dim(doc_ids, lax.axis_index("tensor"), 0, keepdims=False)
    col_full = lax.all_gather(column_state[0], "tensor", axis=2, tiled=True)
    none = jnp.zeros_like(col_full[:, :1])
    bias = jnp.concatenate([col_full[:, :1], none, col_full[:, 1:]], axis=1)
    weights, hidden, *saved = forward(mine, hidden_in, docs, bias, row_state[0])
    upstream, summed, small = backward(out_grad, docs, row_state[0], weights, saved, piece)
    return (hidden, upstream, summed, small.reshape(2, LAYERS, 2 + blocks, width))


def local(
    hidden_in,
    doc_ids,
    unit_slot,
    masters,
    first_moment,
    second_moment,
    column_state,
    row_state,
    out_grad,
):
    slot_count, width, col_width = masters.shape
    dp_size = lax.axis_size("dp")
    tensor_size = lax.axis_size("tensor")
    devices = dp_size * tensor_size
    slots = slot_count * dp_size
    piece = width // devices
    tensor_index = lax.axis_index("tensor")
    kernels = dp_size == 8 and tensor_size == 4 and hidden_in.shape[0] == doc_ids.shape[1]

    sent = masters.astype(jnp.bfloat16)
    if kernels:
        sent = sent.reshape(slot_count, 2, 2, 2, 4, piece, col_width)
        sent = sent.transpose(4, 3, 2, 1, 0, 5, 6)
    else:
        sent = sent.reshape(slot_count, devices, piece, col_width).transpose(1, 0, 2, 3)
    spread = lax.all_to_all(sent.reshape(devices, slot_count, piece, col_width), BOTH, 0, 0)
    spread = spread.reshape(dp_size, tensor_size, slot_count, piece, col_width)
    spread = spread.transpose(0, 2, 3, 1, 4).reshape(slots, piece, width)
    mine = spread[unit_slot]
    run = run_kernels if kernels else run_general
    hidden, upstream, summed, small = run(
        mine, hidden_in, doc_ids, column_state, row_state, out_grad
    )
    row_total = small[1]
    col_total = lax.dynamic_slice_in_dim(small[0], tensor_index * col_width, col_width, axis=2)

    slot_ids = jnp.arange(slots, dtype=jnp.int32)
    named = unit_slot[None, :] == slot_ids[:, None]
    holds = jnp.any(named, axis=1)
    unit_of = jnp.argmax(named, axis=1)
    back = jnp.where(holds[:, None, None], summed[unit_of], jnp.zeros((), jnp.bfloat16))
    back = back.reshape(dp_size, slot_count, piece, tensor_size, col_width)
    back = back.transpose(0, 3, 1, 2, 4).reshape(devices, slot_count, piece, col_width)
    owned = lax.all_to_all(back, BOTH, 0, 0)
    if kernels:
        owned = owned.reshape(4, 2, 2, 2, slot_count, piece, col_width)
        owned = owned.transpose(4, 3, 2, 1, 0, 5, 6)
    else:
        owned = owned.transpose(1, 0, 2, 3)
    owned = owned.reshape(slot_count, width, col_width).astype(jnp.float32)
    occupied = lax.dynamic_slice_in_dim(holds, lax.axis_index("dp") * slot_count, slot_count)
    occupied = occupied.astype(jnp.float32)[:, None, None]
    new_master, new_first, new_second = adamw_update(
        masters, owned, first_moment, second_moment, RATE_UNITS
    )
    unit_master = new_master * occupied
    unit_state = jnp.stack([new_first * occupied, new_second * occupied])
    new_col, col_first, col_second = adamw_update(
        column_state[0], col_total, column_state[1], column_state[2], RATE_SMALL
    )
    column_out = jnp.stack([col_total, new_col, col_first, col_second])
    new_row, row_first, row_second = adamw_update(
        row_state[0], row_total, row_state[1], row_state[2], RATE_SMALL
    )
    row_out = jnp.stack([row_total, new_row, row_first, row_second])
    return (hidden, upstream, unit_master, unit_state, column_out, row_out)


def solution(mesh):
    return jax.shard_map(
        local,
        mesh=mesh,
        in_specs=(
            P(("dp", "tensor"), None),
            P("dp", None),
            P(),
            P("dp", None, "tensor"),
            P("dp", None, "tensor"),
            P("dp", None, "tensor"),
            P(None, None, None, "tensor"),
            P(),
            P(("dp", "tensor"), None),
        ),
        out_specs=(
            P(("dp", "tensor"), None),
            P(("dp", "tensor"), None),
            P("dp", None, "tensor"),
            P(None, "dp", None, "tensor"),
            P(None, None, None, "tensor"),
            P(),
        ),
        check_vma=False,
    )
```

```python
import math

import jax
import jax.numpy as jnp
from jax import lax
from jax.experimental import pallas as pl
from jax.experimental.pallas import tpu as pltpu
from jax.sharding import PartitionSpec as P
import numpy as np

HEAD_DIM = 64
LAYERS = 2
STEP = 3

EPS_NORM = 1e-06
RATE_UNITS = 0.05
RATE_SMALL = 0.2
WEIGHT_DECAY = 0.01
ADAM_EPS = 1e-08
BETA_MOMENT = 0.5
BOTH = ("dp", "tensor")


def norm_forward(summed, gain, shift):
    row_mean = jnp.mean(summed, axis=1, keepdims=True)
    centred = summed - row_mean
    inverse = lax.rsqrt(jnp.mean(centred * centred, axis=1, keepdims=True) + EPS_NORM)
    scaled = centred * inverse
    return (scaled * gain + shift, scaled, inverse)


def norm_backward(upstream, scaled, inverse, gain):
    d_scaled = upstream * gain
    mean_one = jnp.mean(d_scaled, axis=1, keepdims=True)
    mean_two = jnp.mean(d_scaled * scaled, axis=1, keepdims=True)
    grad_input = inverse * (d_scaled - mean_one - scaled * mean_two)
    return (grad_input, jnp.sum(upstream * scaled, axis=0), jnp.sum(upstream, axis=0))


def gelu_pair(v):
    cdf = 0.5 * (1.0 + lax.erf(v * 2.0 ** (-0.5)))
    bell = jnp.exp(-0.5 * v * v) * (2.0 * math.pi) ** (-0.5)
    return (v * cdf, cdf + v * bell)


def adamw_update(old_value, gradient, first_old, second_old, learn_rate):
    first_new = BETA_MOMENT * first_old + (1.0 - BETA_MOMENT) * gradient
    second_new = BETA_MOMENT * second_old + (1.0 - BETA_MOMENT) * gradient * gradient
    correct = 1.0 - BETA_MOMENT**STEP
    step_size = first_new / correct / (jnp.sqrt(second_new / correct) + ADAM_EPS)
    return (old_value - learn_rate * (step_size + WEIGHT_DECAY * old_value), first_new, second_new)


def dot(left, right, dims):
    return lax.dot_general(left, right, (dims, ((), ())), preferred_element_type=jnp.float32)


LANES = 2 * HEAD_DIM


def head_lanes(value, head):
    lane = lax.broadcasted_iota(jnp.int32, value.shape, 1)
    keep = lane < HEAD_DIM if head == 0 else lane >= HEAD_DIM
    return jnp.where(keep, value, jnp.zeros_like(value))


def pair_lanes(first, second):
    lane = lax.broadcasted_iota(jnp.int32, first.shape, 1)
    return jnp.where(lane < HEAD_DIM, first, second)


def attend_pair(pair, q_ref, k_ref, v_ref, mask_ref, ctx_ref, lse_ref):
    lanes = pl.ds(pl.multiple_of(pair * LANES, LANES), LANES)
    query, key, value = q_ref[:, lanes], k_ref[:, lanes], v_ref[:, lanes]
    value_t = value.T
    parts = []
    for head in range(2):
        scores = dot(head_lanes(key, head), query, ((1,), (1,))) + mask_ref[...]
        top = jnp.max(scores, axis=0, keepdims=True)
        weight = jnp.exp(scores - top)
        total = jnp.sum(weight, axis=0, keepdims=True)
        lse_ref[pair * 2 + head] = top + jnp.log(total)
        mine = value_t[head * HEAD_DIM : (head + 1) * HEAD_DIM]
        mixed = dot(mine, weight.astype(jnp.bfloat16), ((1,), (0,)))
        parts.append(mixed * (1.0 / total))
    ctx_ref[:, lanes] = jnp.concatenate(parts, axis=0).T.astype(ctx_ref.dtype)


def attend_back_pair(pair, q_ref, k_ref, v_ref, d_ref, mask_ref, lse_ref, dq_ref, dk_ref, dv_ref):
    lanes = pl.ds(pl.multiple_of(pair * LANES, LANES), LANES)
    query, key, value = q_ref[:, lanes], k_ref[:, lanes], v_ref[:, lanes]
    grad = d_ref[:, lanes]
    key_t = key.T
    parts, d_keys, d_values = [], [], []
    for head in range(2):
        scores = dot(head_lanes(key, head), query, ((1,), (1,))) + mask_ref[...]
        soft = jnp.exp(scores - lse_ref[pair * 2 + head])
        d_values.append(dot(soft.astype(jnp.bfloat16), grad, ((1,), (0,))))
        d_soft = dot(head_lanes(value, head), grad, ((1,), (1,)))
        both = soft * d_soft
        mean = jnp.sum(both, axis=0, keepdims=True)
        d_scores = (both - soft * mean).astype(jnp.bfloat16)
        d_keys.append(dot(d_scores, query, ((1,), (0,))))
        mine = key_t[head * HEAD_DIM : (head + 1) * HEAD_DIM]
        parts.append(dot(mine, d_scores, ((1,), (0,))))
    scale = HEAD_DIM ** (-0.5)
    dq_ref[:, lanes] = (jnp.concatenate(parts, axis=0).T * scale).astype(dq_ref.dtype)
    dk_ref[:, lanes] = pair_lanes(*d_keys).astype(dk_ref.dtype)
    dv_ref[:, lanes] = pair_lanes(*d_values).astype(dv_ref.dtype)


def fill_mask(mask_ref, docs_col_ref, docs_row_ref):
    same = docs_col_ref[...] == docs_row_ref[...]
    mask_ref[...] = jnp.where(same, 0.0, -1e30).astype(jnp.float32)


LAG = 2


def spread_order(z, y, x, c):
    return ((c * 2 + x) * 2 + y) * 4 + z


def every_other(z, y, x, c, body):
    for step in (2, 1, 3, 0):

        def one(i, carry, step=step):
            body((z + step) % 4, (y + i // 4) % 2, (x + (i // 2) % 2) % 2, (c + i % 2) % 2)
            return carry

        lax.fori_loop(1 if step == 0 else 0, 8, one, 0)


def greet_all(z, y, x, c):
    barrier = pltpu.get_barrier_semaphore()

    def greet(zz, yy, xx, cc):
        pl.semaphore_signal(
            barrier,
            inc=1,
            device_id=(zz * 2 + yy, xx * 2 + cc),
            device_id_type=pl.DeviceIdType.MESH,
        )

    every_other(z, y, x, c, greet)
    return barrier


TILE = 256


def norm_back_rows(upstream, scaled, inverse, gain):
    d_scaled = upstream * gain
    mean_one = jnp.mean(d_scaled, axis=1, keepdims=True)
    mean_two = jnp.mean(d_scaled * scaled, axis=1, keepdims=True)
    return inverse * (d_scaled - mean_one - scaled * mean_two)


def backward_kernel(
    pick_ref,
    out_grad_ref,
    docs_col_ref,
    docs_row_ref,
    row_ref,
    weights_ref,
    low_ref,
    mixed_ref,
    ctx_ref,
    lse_ref,
    one_ref,
    inv_one_ref,
    normed_ref,
    act_ref,
    slope_ref,
    two_ref,
    inv_two_ref,
    owned_ref,
    total_ref,
    small_out,
    out_ref,
    back_buf,
    left_buf,
    right_buf,
    unit_buf,
    scaled_buf,
    inv_buf,
    slope_buf,
    mixed_buf,
    lse_buf,
    mask_buf,
    d_ctx_buf,
    core_out,
    core_in,
    sum_core,
    first_in,
    sum_first,
    second_in,
    sum_second,
    z_in,
    small_sum,
    small_got,
    load_sem,
    core_sems,
    first_sems,
    second_sems,
    z_sems,
    small_sems,
    own_sems,
    round_sems,
):
    units, piece, width = out_ref.shape
    rows = total_ref.shape[0]
    per_layer = units // LAYERS
    blocks = (per_layer - 4) // 2
    at_out, at_query = 2 * blocks, 2 * blocks + 1
    dp, tensor = lax.axis_index("dp"), lax.axis_index("tensor")
    z, y, x, c = dp // 2, dp % 2, tensor // 2, tensor % 2
    half = width // 2
    quarter, eighth = half // 2, half // 4
    to_core = (dp, x * 2 + 1 - c)
    to_x = (dp, (1 - x) * 2 + c)
    to_y = (z * 2 + 1 - y, tensor)
    to_z = [(((z + k) % 4) * 2 + y, tensor) for k in (1, 2, 3)]
    to_z1 = ((z + 1 - 2 * (z % 2)) * 2 + y, tensor)
    to_z2 = (((z + 2) % 4) * 2 + y, tensor)
    mesh_id = pl.DeviceIdType.MESH

    barrier = greet_all(z, y, x, c)

    def remote(src, dst, sems, send, recv, peer):
        return pltpu.make_async_remote_copy(
            src_ref=src,
            dst_ref=dst,
            send_sem=sems.at[send],
            recv_sem=sems.at[recv],
            device_id=peer,
            device_id_type=mesh_id,
        )

    def place(s):
        return LAYERS - 1 - s // per_layer, s % per_layer

    def unit_of(s):
        layer, j = place(s)
        feed = jnp.where(j % 2 == 0, 4 + blocks + j // 2, 4 + j // 2)
        return layer * per_layer + jnp.where(
            j < at_out, feed, jnp.where(j == at_out, 3, j - at_query)
        )

    def left_of(s):
        j = s % per_layer
        feed = jnp.where(j % 2 == 0, 3, 2)
        return jnp.where(j < at_out, feed, jnp.where(j == at_out, 1, 0))

    def loaded_slot(s):
        return ((s // per_layer) * (blocks + 1) + (s % per_layer) // 2) % 2

    def right_of(s):
        j = s % per_layer
        feed = jnp.where(j % 2 == 0, loaded_slot(s), 2 + (j // 2) % 2)
        return jnp.where(
            j < at_out, feed, jnp.where(j == at_out, loaded_slot(s), 4 + j - at_query)
        )

    local = pltpu.make_async_copy

    def unit_load(s):
        return local(weights_ref.at[unit_of(s)], unit_buf.at[s % 2], load_sem.at[0, s % 2])

    def act_load(layer, block, slot):
        return local(act_ref.at[layer, block], right_buf.at[slot], load_sem.at[1, slot])

    def ctx_load(layer, slot):
        return local(ctx_ref.at[layer], right_buf.at[slot], load_sem.at[1, slot])

    def slope_load(layer, block):
        return local(slope_ref.at[layer, block], slope_buf, load_sem.at[2, 0])

    def norm_loads(layer, which):
        scaled, inv = ((one_ref, inv_one_ref), (two_ref, inv_two_ref))[which]
        return [
            local(scaled.at[layer], scaled_buf, load_sem.at[3, 0]),
            local(inv.at[layer], inv_buf, load_sem.at[3, 1]),
        ]

    def mixed_loads(layer):
        return [
            local(mixed_ref.at[layer], mixed_buf, load_sem.at[4, 0]),
            local(lse_ref.at[layer], lse_buf, load_sem.at[4, 1]),
        ]

    def normed_load(layer):
        return local(normed_ref.at[layer], left_buf.at[2], load_sem.at[2, 1])

    def low_load(layer):
        return local(low_ref.at[layer], left_buf.at[0], load_sem.at[5, 0])

    def begin(*copies):
        for copy in copies:
            copy.start()

    def finish(*copies):
        for copy in copies:
            copy.wait()

    def note(row, value):
        small_sum[0, pl.ds(row, 1), :] = value

    def column(layer, i):
        return layer * (2 + blocks) + i

    def row(layer, i):
        return LAYERS * (2 + blocks) + layer * 6 + i

    def norm_back(layer, gain_row, bias_row, low_slot):
        gain = row_ref[layer * 6 + gain_row]
        size = 128

        def one(tile, carry):
            part = pl.ds(pl.multiple_of(tile * size, size), size)
            upstream = total_ref[part, :]
            scaled = scaled_buf[part, :]
            inside = norm_back_rows(upstream, scaled, inv_buf[part, 0:1], gain)
            total_ref[part, :] = inside
            left_buf[low_slot, part, :] = inside.astype(jnp.bfloat16)
            sums = (upstream * scaled, upstream, inside)
            return tuple(a + jnp.sum(b, axis=0, keepdims=True) for a, b in zip(carry, sums))

        zero = jnp.zeros((1, width), jnp.float32)
        gains, shifts, biases = lax.fori_loop(0, rows // size, one, (zero, zero, zero))
        note(row(layer, gain_row), gains)
        note(row(layer, gain_row + 1), shifts)
        note(row(layer, bias_row), biases)

    def heads(start, stop):
        inputs = [mixed_buf.at[i] for i in range(3)]
        grads = [right_buf.at[4 + i] for i in range(3)]

        def one(pair, carry):
            attend_back_pair(pair, *inputs, d_ctx_buf, mask_buf, lse_buf, *grads)
            return carry

        lax.fori_loop(start, stop, one, 0)

    pairs = width // LANES

    def data_gradient(s):
        layer, j = place(s)
        matrix = unit_buf.at[s % 2]
        slot = loaded_slot(s)

        @pl.when(j == 0)
        def _():
            finish(*norm_loads(layer, 1))

            @pl.when(s == 0)
            def _():
                total_ref[...] = out_grad_ref[...].astype(jnp.float32)

            norm_back(layer, 4, 1, 3)
            begin(*norm_loads(layer, 0), *mixed_loads(layer))

        @pl.when(j == 1)
        def _():
            finish(normed_load(layer))
            begin(low_load(layer))

        @pl.when((j < at_out) & (j % 2 == 0))
        def _():
            block = j // 2
            finish(slope_load(layer, block), act_load(layer, block, slot))

            @pl.when(block < blocks - 1)
            def _():
                act_load(layer, block + 1, 1 - slot).start()

            @pl.when(block == blocks - 1)
            def _():
                ctx_load(layer, 1 - slot).start()

            d_act = dot(left_buf[3], matrix[...], ((1,), (0,)))
            d_pre = (d_act * slope_buf[...].astype(jnp.float32)).astype(jnp.bfloat16)
            right_buf[2 + block % 2] = d_pre
            sums = jnp.sum(d_pre.astype(jnp.float32), axis=0, keepdims=True)
            note(column(layer, 2 + block), sums)

            @pl.when(block < blocks - 1)
            def _():
                slope_load(layer, block + 1).start()

        @pl.when((j < at_out) & (j % 2 == 1))
        def _():
            total_ref[...] += dot(right_buf[2 + (j // 2) % 2], matrix[...], ((1,), (1,)))

        @pl.when(j == at_out)
        def _():
            finish(*norm_loads(layer, 0), *mixed_loads(layer), ctx_load(layer, slot))
            norm_back(layer, 2, 0, 1)

            @pl.when(layer > 0)
            def _():
                act_load(layer - 1, 0, 1 - slot).start()
                begin(*norm_loads(layer - 1, 1))
                slope_load(layer - 1, 0).start()

            d_ctx_buf[...] = dot(left_buf[1], matrix[...], ((1,), (0,))).astype(jnp.bfloat16)
            heads(0, pairs // 2)

        @pl.when(j == at_query)
        def _():
            finish(low_load(layer))

            @pl.when(layer > 0)
            def _():
                normed_load(layer - 1).start()

            heads(pairs // 2, pairs)
            for i, number in ((0, 0), (2, 1)):
                sums = jnp.sum(right_buf[4 + i].astype(jnp.float32), axis=0, keepdims=True)
                note(column(layer, number), sums)

        @pl.when(j >= at_query)
        def _():
            total_ref[...] += dot(right_buf[4 + j - at_query], matrix[...], ((1,), (1,)))

    def product(s, side, tile):
        start = pl.multiple_of(side * half + tile * TILE, TILE)
        left = left_buf[left_of(s), :, pl.ds(start, TILE)]
        return lax.dot_general(
            left, right_buf[right_of(s)], (((0,), (0,)), ((), ())), preferred_element_type=jnp.float32
        )

    def core_copy(s):
        return remote(
            core_out.at[s % 2], core_in.at[s % 4], core_sems, (0, s % 2), (1, s % 4), to_core
        )

    def first_copies(s):
        here = sum_core.at[s % 3]
        return (
            remote(
                here.at[pl.ds(pl.multiple_of((1 - x) * quarter, quarter), quarter), pl.ds(0, half)],
                first_in.at[s % 4, 0],
                first_sems,
                (0, 0, s % 3),
                (1, 0, s % 4),
                to_x,
            ),
            *(
                remote(
                    here.at[
                        pl.ds(pl.multiple_of(i * quarter + (1 - y) * eighth, eighth), eighth),
                        pl.ds(half, half),
                    ],
                    first_in.at[s % 4, 1, pl.ds(i * eighth, eighth)],
                    first_sems,
                    (0, 1 + i, s % 3),
                    (1, 1 + i, s % 4),
                    to_y,
                )
                for i in range(2)
            ),
        )

    def second_copies(s):
        here = sum_first.at[s % 3]
        return (
            remote(
                here.at[0, pl.ds(pl.multiple_of((1 - y) * eighth, eighth), eighth)],
                second_in.at[s % 4, 0],
                second_sems,
                (0, 0, s % 3),
                (1, 0, s % 4),
                to_y,
            ),
            remote(
                here.at[1, pl.ds(pl.multiple_of((1 - x) * eighth, eighth), eighth)],
                second_in.at[s % 4, 1],
                second_sems,
                (0, 1, s % 3),
                (1, 1, s % 4),
                to_x,
            ),
        )

    def z_copies(s):
        return [
            remote(
                sum_second.at[s % 3, pl.ds(pl.multiple_of(((z + k) % 4) * piece, piece), piece)],
                z_in.at[s % 4, k - 1],
                z_sems,
                (0, k - 1, s % 3),
                (1, k - 1, s % 4),
                to_z[k - 1],
            )
            for k in (1, 2, 3)
        ]

    small_peers = (to_core, to_x, to_y, to_z1, to_z2)

    def small_copy(stage):
        return remote(
            small_sum.at[stage],
            small_got.at[stage],
            small_sems,
            (0, stage),
            (1, stage),
            small_peers[stage],
        )

    rounds, owners = back_buf.shape[0], back_buf.shape[1]
    cols = owned_ref.shape[3]
    me = spread_order(z, y, x, c)

    def own_back(number):
        return local(
            back_buf.at[number, dp, :, pl.ds(pl.multiple_of(tensor * cols, cols), cols)],
            owned_ref.at[number, me],
            own_sems.at[number],
        )

    def send_back(number):
        def fill(owner, carry):
            back_buf[number, owner] = out_ref[pick_ref[number * owners + owner]]
            return carry

        lax.fori_loop(0, owners, fill, 0)
        own_back(number).start()

        def send(zz, yy, xx, cc):
            there = xx * 2 + cc
            remote(
                back_buf.at[
                    number, zz * 2 + yy, :, pl.ds(pl.multiple_of(there * cols, cols), cols)
                ],
                owned_ref.at[number, me],
                round_sems,
                (0, number),
                (1, number),
                (zz * 2 + yy, there),
            ).start()

        every_other(z, y, x, c, send)

    def finish_back(number):
        own_back(number).wait()
        most = owned_ref.at[number, pl.ds(0, 31)]
        remote(most, most, round_sems, (0, number), (1, number), to_core).wait()

    top = LAYERS - 1
    begin(
        *norm_loads(top, 1),
        unit_load(jnp.int32(0)),
        slope_load(top, 0),
        act_load(top, 0, 0),
        normed_load(top),
    )
    fill_mask(mask_buf, docs_col_ref, docs_row_ref)
    pl.semaphore_wait(barrier, 31)

    def step(s, carry):
        last = s - 3 * LAG - 1

        @pl.when((last >= 0) & (last < units))
        def _():
            for copy in z_copies(last):
                copy.wait()
            total = sum_second[last % 3, pl.ds(pl.multiple_of(z * piece, piece), piece), :].astype(
                jnp.float32
            )
            for k in range(3):
                total = total + z_in[last % 4, k].astype(jnp.float32)
            out_ref[unit_of(last)] = total.astype(out_ref.dtype)

            @pl.when(last >= units - rounds)
            def _():
                send_back(last - (units - rounds))

        third = s - 2 * LAG - 1

        @pl.when((third >= 0) & (third < units))
        def _():
            for copy in second_copies(third):
                copy.wait()
            for part, side in ((0, y), (1, x)):
                mine = sum_first[
                    third % 3, part, pl.ds(pl.multiple_of(side * eighth, eighth), eighth), :
                ]
                total = mine.astype(jnp.float32) + second_in[third % 4, part].astype(jnp.float32)
                sum_second[third % 3, :, part * half : (part + 1) * half] = total.astype(
                    jnp.bfloat16
                )
            for copy in z_copies(third):
                copy.start()

        second = s - LAG - 1

        @pl.when((second >= 0) & (second < units))
        def _():
            for copy in first_copies(second):
                copy.wait()
            mine = sum_core[
                second % 3, pl.ds(pl.multiple_of(x * quarter, quarter), quarter), 0:half
            ]
            total = mine.astype(jnp.float32) + first_in[second % 4, 0].astype(jnp.float32)
            sum_first[second % 3, 0] = total.astype(jnp.bfloat16)
            for i in range(2):
                mine = sum_core[
                    second % 3,
                    pl.ds(pl.multiple_of(i * quarter + y * eighth, eighth), eighth),
                    half : 2 * half,
                ]
                part = pl.ds(i * eighth, eighth)
                total = mine.astype(jnp.float32) + first_in[second % 4, 1, part, :].astype(
                    jnp.float32
                )
                sum_first[second % 3, 1, part, :] = total.astype(jnp.bfloat16)
            for copy in second_copies(second):
                copy.start()

        @pl.when(s < units)
        def _():
            unit_load(s).wait()

            @pl.when(s + 1 < units)
            def _():
                unit_load(s + 1).start()

            data_gradient(s)

            @pl.when(s >= 2)
            def _():
                core_copy(s - 2).wait_send()

            def one(tile, carry):
                part = pl.ds(pl.multiple_of(tile * TILE, TILE), TILE)
                core_out[s % 2, part, :] = product(s, 1 - c, tile).astype(jnp.bfloat16)
                return carry

            lax.fori_loop(0, half // TILE, one, 0)
            core_copy(s).start()

        first = s - 1

        @pl.when((first >= 0) & (first < units))
        def _():
            core_copy(first).wait_recv()

            def one(tile, carry):
                part = pl.ds(pl.multiple_of(tile * TILE, TILE), TILE)
                total = product(first, c, tile) + core_in[first % 4, part, :].astype(jnp.float32)
                sum_core[first % 3, part, :] = total.astype(jnp.bfloat16)
                return carry

            lax.fori_loop(0, half // TILE, one, 0)
            for copy in first_copies(first):
                copy.start()

        for stage in range(6):

            @pl.when(s == units + stage)
            def _(stage=stage):
                if stage > 0:
                    small_copy(stage - 1).wait()
                    total = small_sum[stage - 1] + small_got[stage - 1]
                    if stage < 5:
                        small_sum[stage] = total
                    else:
                        small_out[...] = total
                if stage < 5:
                    small_copy(stage).start()

        return carry

    lax.fori_loop(0, units + 3 * LAG + 1, step, 0)
    for s in (units - 2, units - 1):
        core_copy(s).wait_send()
    for number in range(rounds):
        finish_back(number)


def backward(pick, out_grad, docs, row_now, weights, saved, piece, cols):
    units, width, _ = weights.shape
    rows = out_grad.shape[0]
    blocks = (units // LAYERS - 4) // 2
    half = width // 2
    low, full = jnp.bfloat16, jnp.float32
    rounds = pick.shape[0] // 8
    small = (LAYERS * (8 + blocks), width)
    any_spec = pl.BlockSpec(memory_space=pl.ANY)
    vmem_spec = pl.BlockSpec(memory_space=pltpu.VMEM)
    dma = pltpu.SemaphoreType.DMA
    summed, total, small = pl.pallas_call(
        backward_kernel,
        out_shape=(
            jax.ShapeDtypeStruct((rounds, width // piece, piece, cols), low),
            jax.ShapeDtypeStruct((rows, width), full),
            jax.ShapeDtypeStruct(small, full),
        ),
        in_specs=[pl.BlockSpec(memory_space=pltpu.SMEM)] + [vmem_spec] * 4 + [any_spec] * (1 + len(saved)),
        out_specs=(vmem_spec, vmem_spec, vmem_spec),
        scratch_shapes=[
            pltpu.VMEM((units, piece, width), low),
            pltpu.VMEM((rounds, 8, piece, width), low),
            pltpu.VMEM((4, rows, width), low),
            pltpu.VMEM((7, rows, width), low),
            pltpu.VMEM((2, width, width), low),
            pltpu.VMEM((rows, width), full),
            pltpu.VMEM((rows, 128), full),
            pltpu.VMEM((rows, width), low),
            pltpu.VMEM((3, rows, width), low),
            pltpu.VMEM((width // HEAD_DIM, 1, rows), full),
            pltpu.VMEM((rows, rows), full),
            pltpu.VMEM((rows, width), low),
            pltpu.VMEM((2, half, width), low),
            pltpu.VMEM((4, half, width), low),
            pltpu.VMEM((3, half, width), low),
            pltpu.VMEM((4, 2, half // 2, half), low),
            pltpu.VMEM((3, 2, half // 2, half), low),
            pltpu.VMEM((4, 2, half // 4, half), low),
            pltpu.VMEM((3, half // 4, width), low),
            pltpu.VMEM((4, 3, piece, width), low),
            pltpu.VMEM((5,) + small, full),
            pltpu.VMEM((5,) + small, full),
            dma((6, 2)),
            dma((2, 4)),
            dma((2, 3, 4)),
            dma((2, 2, 4)),
            dma((2, 3, 4)),
            dma((2, 5)),
            dma((rounds,)),
            dma((2, rounds)),
        ],
        compiler_params=pltpu.CompilerParams(
            collective_id=1, has_side_effects=True, vmem_limit_bytes=63 * 1024 * 1024
        ),
        name="backward_reduce",
    )(pick, out_grad, docs[:, None], docs[None, :], row_now.reshape(-1, 1, width), weights, *saved)
    return (total, summed, small)


def norm_rows(value, gain, shift):
    centred = value - jnp.mean(value, axis=1, keepdims=True)
    inverse = lax.rsqrt(jnp.mean(centred * centred, axis=1, keepdims=True) + EPS_NORM)
    scaled = centred * inverse
    return (scaled * gain + shift, scaled, inverse)


NORM_ROWS = 128


def forward_kernel(
    rank_ref,
    owner_ref,
    sent_ref,
    hidden_ref,
    docs_col_ref,
    docs_row_ref,
    bias_ref,
    row_ref,
    out_ref,
    final_ref,
    *refs,
):
    saved, bufs = refs[:11], refs[11:22]
    rounds = sent_ref.shape[0]
    (x_buf, normed_buf, total_buf, mask_buf, unit_buf, own_ref) = refs[22:28]
    (own_sem, sems, unit_sem, save_sem, got_sem, round_sems) = refs[28:34]
    got = refs[34:]
    (low_buf, mixed_buf, ctx_buf, lse_buf, one_buf, inv_one_buf, nb_buf) = bufs[:7]
    (act_buf, slope_buf, two_buf, inv_two_buf) = bufs[7:]
    units, piece, width = own_ref.shape
    rows = hidden_ref.shape[0]
    per_layer = units // LAYERS
    blocks = (per_layer - 4) // 2
    dp, tensor = lax.axis_index("dp"), lax.axis_index("tensor")
    z, y, x, c = dp // 2, dp % 2, tensor // 2, tensor % 2
    half = width // 2
    line, plane = 4 * piece, 8 * piece
    to_core = (dp, x * 2 + 1 - c)
    to_x = (dp, (1 - x) * 2 + c)
    to_y = (z * 2 + 1 - y, tensor)
    to_z = [(((z + k) % 4) * 2 + y, tensor) for k in (1, 2, 3)]
    mesh_id = pl.DeviceIdType.MESH

    barrier = greet_all(z, y, x, c)
    pl.semaphore_wait(barrier, 31)
    cols = sent_ref.shape[2]
    me = dp * 4 + tensor

    def part_for(number, zz, yy, xx, cc):
        start = pl.multiple_of(spread_order(zz, yy, xx, cc) * piece, piece)
        return sent_ref.at[number, pl.ds(start, piece)]

    def keep(number):
        return pltpu.make_async_copy(
            part_for(number, z, y, x, c), got[number].at[me], got_sem.at[number]
        )

    def round_copy(number, src, dst, peer):
        return pltpu.make_async_remote_copy(
            src_ref=src,
            dst_ref=dst,
            send_sem=round_sems.at[0, number],
            recv_sem=round_sems.at[1, number],
            device_id=peer,
            device_id_type=mesh_id,
        )

    def start_round(number):
        keep(number).start()

        def send(zz, yy, xx, cc):
            src = part_for(number, zz, yy, xx, cc)
            round_copy(number, src, got[number].at[me], (zz * 2 + yy, xx * 2 + cc)).start()

        every_other(z, y, x, c, send)

    def finish_round(number):
        keep(number).wait()
        most = got[number].at[pl.ds(0, 31)]
        round_copy(number, most, most, to_core).wait()

    def pick(unit, there):
        rank, owner = rank_ref[unit], owner_ref[unit]
        for j in range(4):
            value = got[0][owner * 4 + j]
            for number in range(1, there):
                value = jnp.where(rank == number, got[number][owner * 4 + j], value)
            own_ref[unit, :, j * cols : (j + 1) * cols] = value

    start_round(0)
    start_round(1)

    my_line = pl.multiple_of(((c * 2 + x) * 2 + y) * line, line)
    my_rows = pl.ds(pl.multiple_of(my_line + z * piece, piece), piece)
    first, second = pl.ds(0, half), pl.ds(half, half)

    def remote(src, dst, index, unit, peer):
        return pltpu.make_async_remote_copy(
            src_ref=src,
            dst_ref=dst,
            send_sem=sems.at[0, index, unit],
            recv_sem=sems.at[1, index, unit],
            device_id=peer,
            device_id_type=mesh_id,
        )

    def own_copy(unit):
        return pltpu.make_async_copy(own_ref.at[unit], out_ref.at[unit, my_rows], own_sem.at[unit])

    def stage_z(unit):
        there = out_ref.at[unit, my_rows]
        return [remote(own_ref.at[unit], there, k, unit, to_z[k]) for k in range(3)]

    def stage_one(unit):
        rows = pl.ds(my_line, line)
        one, two = out_ref.at[unit, rows, first], out_ref.at[unit, rows, second]
        return [remote(one, one, 3, unit, to_y), remote(two, two, 4, unit, to_x)]

    def stage_two(unit):
        rows = pl.ds(pl.multiple_of((c * 2 + x) * plane, plane), plane)
        one = out_ref.at[unit, rows, first]
        copies = [remote(one, one, 5, unit, to_x)]
        for i in range(2):
            rows = pl.ds(pl.multiple_of(((c * 2 + i) * 2 + y) * line, line), line)
            two = out_ref.at[unit, rows, second]
            copies.append(remote(two, two, 6 + i, unit, to_y))
        return copies

    def stage_core(unit):
        there = out_ref.at[unit, pl.ds(pl.multiple_of(c * 2 * plane, 2 * plane), 2 * plane)]
        return [remote(there, there, 8, unit, to_core)]

    stages = (stage_z, stage_one, stage_two, stage_core)

    def unit_copy(unit):
        slot = unit % 2
        return pltpu.make_async_copy(out_ref.at[unit], unit_buf.at[slot], unit_sem.at[slot])

    def save(number, layer, block=None):
        src, dst, sem = bufs[number], saved[number].at[layer], save_sem.at[number, 0]
        if block is not None:
            src, dst, sem = src.at[block], dst.at[block], save_sem.at[number, block]
        return pltpu.make_async_copy(src, dst, sem)

    def free(numbers, layer, block=None):
        @pl.when(layer > 0)
        def _():
            for number in numbers:
                save(number, layer - 1, block).wait()

    def heads(start, stop):
        def one(pair, carry):
            attend_pair(
                pair, mixed_buf.at[0], mixed_buf.at[1], mixed_buf.at[2], mask_buf, ctx_buf, lse_buf
            )
            return carry

        lax.fori_loop(start, stop, one, 0)

    def over_rows(body):
        def one(tile, carry):
            body(pl.ds(pl.multiple_of(tile * NORM_ROWS, NORM_ROWS), NORM_ROWS))
            return carry

        lax.fori_loop(0, rows // NORM_ROWS, one, 0)

    pairs = width // LANES

    def compute(unit):
        layer, j = unit // per_layer, unit % per_layer
        matrix = unit_buf.at[unit % 2]

        def small(i):
            return row_ref[layer * 6 + i]

        @pl.when(j == 0)
        def _():
            free((0, 1), layer)

            @pl.when(layer == 0)
            def _():
                x_buf[...] = hidden_ref[...].astype(jnp.float32)

            low_buf[...] = x_buf[...].astype(jnp.bfloat16)
            save(0, layer).start()

        @pl.when(j < 3)
        def _():
            value = dot(low_buf[...], matrix[...], ((1,), (0,)))
            value = value + bias_ref[layer * (3 + blocks) + j]
            scale = jnp.where(j == 0, HEAD_DIM ** (-0.5), 1.0)
            mixed_buf[j] = (value * scale).astype(jnp.bfloat16)

        @pl.when(j == 2)
        def _():
            save(1, layer).start()
            free((2, 3), layer)
            heads(0, pairs // 2)

        @pl.when(j == 3)
        def _():
            heads(pairs // 2, pairs)
            save(2, layer).start()
            save(3, layer).start()
            total_buf[...] = dot(ctx_buf[...], matrix[...], ((1,), (1,)))
            free((4, 5, 6), layer)

            def body(part):
                value = x_buf[part, :] + total_buf[part, :] + small(0)
                normed, scaled, inverse = norm_rows(value, small(2), small(3))
                normed_buf[part, :] = normed
                nb_buf[part, :] = normed.astype(jnp.bfloat16)
                one_buf[part, :] = scaled
                inv_one_buf[part, :] = jnp.broadcast_to(inverse, (NORM_ROWS, 128))

            over_rows(body)
            for number in (4, 5, 6):
                save(number, layer).start()

        @pl.when((j >= 4) & (j < 4 + blocks))
        def _():
            block = j - 4
            free((7, 8), layer, block)
            value = dot(nb_buf[...], matrix[...], ((1,), (0,)))
            act, slope = gelu_pair(value + bias_ref[layer * (3 + blocks) + 3 + block])
            act_buf[block] = act.astype(jnp.bfloat16)
            slope_buf[block] = slope.astype(jnp.bfloat16)
            save(7, layer, block).start()
            save(8, layer, block).start()

        @pl.when(j >= 4 + blocks)
        def _():
            block = j - 4 - blocks
            part = dot(act_buf[block], matrix[...], ((1,), (1,)))

            @pl.when(block == 0)
            def _():
                total_buf[...] = part

            @pl.when(block > 0)
            def _():
                total_buf[...] += part

        @pl.when(j == per_layer - 1)
        def _():
            free((9, 10), layer)

            def body(part):
                value = normed_buf[part, :] + total_buf[part, :] + small(1)
                output, scaled, inverse = norm_rows(value, small(4), small(5))
                x_buf[part, :] = output
                two_buf[part, :] = scaled
                inv_two_buf[part, :] = jnp.broadcast_to(inverse, (NORM_ROWS, 128))

            over_rows(body)
            save(9, layer).start()
            save(10, layer).start()

    def step(s, carry):
        for number in range(len(stages), -1, -1):
            unit = s - number * LAG

            if number == 0:
                for turn in range(rounds):

                    @pl.when((s == turn) if turn < rounds - 1 else ((s >= turn) & (s < units)))
                    def _(turn=turn):
                        if turn < rounds - 1:
                            finish_round(turn)
                        else:

                            @pl.when(s == turn)
                            def _():
                                finish_round(turn)

                        if turn + 2 < rounds:
                            start_round(turn + 2)
                        pick(s, turn + 1)

            @pl.when((unit >= 0) & (unit < units))
            def _(unit=unit, number=number):
                if number == 0:
                    own_copy(unit).start()
                else:
                    if number == 1:
                        own_copy(unit).wait()
                    for copy in stages[number - 1](unit):
                        copy.wait()
                if number < len(stages):
                    for copy in stages[number](unit):
                        copy.start()
                else:
                    unit_copy(unit).start()

        done = s - len(stages) * LAG - 1

        @pl.when(done >= 0)
        def _():
            unit_copy(done).wait()
            compute(done)

        return carry

    fill_mask(mask_buf, docs_col_ref, docs_row_ref)
    lax.fori_loop(0, units + len(stages) * LAG + 1, step, 0)
    final_ref[...] = x_buf[...]
    last = LAYERS - 1
    for number in (0, 1, 2, 3, 4, 5, 6, 9, 10):
        save(number, last).wait()
    for block in range(blocks):
        save(7, last, block).wait()
        save(8, last, block).wait()


def forward(rank, owner, sent, hidden_in, docs, bias, row_now, piece):
    units, rounds, width = rank.shape[0], sent.shape[0], sent.shape[1]
    rows = hidden_in.shape[0]
    blocks = (units // LAYERS - 4) // 2
    low, full = jnp.bfloat16, jnp.float32
    kept = [
        ((rows, width), low),
        ((3, rows, width), low),
        ((rows, width), low),
        ((width // HEAD_DIM, 1, rows), full),
        ((rows, width), full),
        ((rows, 128), full),
        ((rows, width), low),
        ((blocks, rows, width), low),
        ((blocks, rows, width), low),
        ((rows, width), full),
        ((rows, 128), full),
    ]
    any_spec = pl.BlockSpec(memory_space=pl.ANY)
    vmem_spec = pl.BlockSpec(memory_space=pltpu.VMEM)
    smem_spec = pl.BlockSpec(memory_space=pltpu.SMEM)
    dma = pltpu.SemaphoreType.DMA
    return pl.pallas_call(
        forward_kernel,
        out_shape=[
            jax.ShapeDtypeStruct((units, width, width), low),
            jax.ShapeDtypeStruct((rows, width), full),
        ]
        + [jax.ShapeDtypeStruct((LAYERS,) + shape, dtype) for shape, dtype in kept],
        in_specs=[smem_spec] * 2 + [any_spec] + [vmem_spec] * 5,
        out_specs=[any_spec, vmem_spec] + [any_spec] * len(kept),
        scratch_shapes=[pltpu.VMEM(shape, dtype) for shape, dtype in kept]
        + [
            pltpu.VMEM((rows, width), full),
            pltpu.VMEM((rows, width), full),
            pltpu.VMEM((rows, width), full),
            pltpu.VMEM((rows, rows), full),
            pltpu.VMEM((2, width, width), low),
            pltpu.VMEM((units, piece, width), low),
            dma((units,)),
            dma((2, 9, units)),
            dma((2,)),
            dma((len(kept), blocks)),
            dma((rounds,)),
            dma((2, rounds)),
        ]
        + [pltpu.VMEM((width // piece, piece, sent.shape[2]), low)] * rounds,
        compiler_params=pltpu.CompilerParams(
            collective_id=2, has_side_effects=True, vmem_limit_bytes=60 * 1024 * 1024
        ),
        name="gather_forward",
    )(
        rank,
        owner,
        sent,
        hidden_in,
        docs[:, None],
        docs[None, :],
        bias.reshape(-1, 1, width),
        row_now.reshape(-1, 1, width),
    )


def run_general(unit_slot, masters, hidden_in, doc_ids, column_state, row_state, out_grad):
    slot_count, width, col_width = masters.shape
    units = unit_slot.shape[0]
    dp_size = lax.axis_size("dp")
    devices = dp_size * lax.axis_size("tensor")
    slots = slot_count * dp_size
    piece = width // devices
    per_layer = units // LAYERS
    blocks = (per_layer - 4) // 2
    tensor_size = lax.axis_size("tensor")
    rows = hidden_in.shape[0]
    seq_len = doc_ids.shape[1]
    heads = width // HEAD_DIM
    share = seq_len // rows
    tensor_index = lax.axis_index("tensor")
    groups = [list(range(i, i + share)) for i in range(0, tensor_size, share)]
    score_scale = HEAD_DIM ** (-0.5)
    sent = masters.astype(jnp.bfloat16).reshape(slot_count, devices, piece, col_width)
    spread = lax.all_to_all(sent.transpose(1, 0, 2, 3), BOTH, 0, 0)
    spread = spread.reshape(dp_size, tensor_size, slot_count, piece, col_width)
    spread = spread.transpose(0, 2, 3, 1, 4).reshape(slots, piece, width)
    mine = spread[unit_slot]
    weights = jnp.concatenate(
        [
            lax.all_gather(
                mine[layer * per_layer : (layer + 1) * per_layer], BOTH, axis=1, tiled=True
            )
            for layer in range(LAYERS)
        ],
        axis=0,
    )

    def matrices(layer):
        unit = weights[layer * per_layer : (layer + 1) * per_layer]
        return (unit[:3], unit[3], unit[4 : 4 + blocks], unit[4 + blocks :])

    row_docs = lax.dynamic_slice_in_dim(doc_ids, tensor_index // share, 1, axis=0)[0]
    my_docs = lax.dynamic_slice_in_dim(row_docs, (tensor_index % share) * rows, rows)
    same_doc = (my_docs[:, None] == row_docs[None, :])[None]

    def whole_row(value):
        if share == 1:
            return value
        return lax.all_gather(value, "tensor", axis=0, tiled=True, axis_index_groups=groups)

    def own_rows(value):
        if share == 1:
            return value
        return lax.psum_scatter(
            value, "tensor", scatter_dimension=0, tiled=True, axis_index_groups=groups
        )

    col_full = lax.all_gather(column_state[0], "tensor", axis=2, tiled=True)
    hidden = hidden_in.astype(jnp.float32)
    saved_layers = []
    for layer in range(LAYERS):
        w_qkv, w_proj, w_in, w_out = matrices(layer)
        row_now = row_state[0, layer]
        col_now = col_full[layer]
        hidden_bf = hidden.astype(jnp.bfloat16)
        query, key, value = (dot(hidden_bf, w_qkv[i], ((1,), (0,))) for i in range(3))
        query = ((query + col_now[0]) * score_scale).astype(jnp.bfloat16)
        key = key.astype(jnp.bfloat16)
        value = (value + col_now[1]).astype(jnp.bfloat16)
        query = query.reshape(rows, heads, HEAD_DIM)
        key = whole_row(key).reshape(seq_len, heads, HEAD_DIM)
        value = whole_row(value).reshape(seq_len, heads, HEAD_DIM)
        scores = jnp.einsum("qhd,khd->hqk", query, key, preferred_element_type=jnp.float32)
        scores = jnp.where(same_doc, scores, -1e30)
        row_top = jnp.max(scores, axis=-1, keepdims=True)
        log_total = row_top + jnp.log(
            jnp.sum(jnp.exp(scores - row_top), axis=-1, keepdims=True)
        )
        soft_bf = jnp.exp(scores - log_total).astype(jnp.bfloat16)
        context = jnp.einsum("hqk,khd->qhd", soft_bf, value, preferred_element_type=jnp.float32)
        context = context.reshape(rows, width).astype(jnp.bfloat16)
        attended = dot(context, w_proj, ((1,), (1,)))
        normed, scaled_one, inverse_one = norm_forward(
            hidden + attended + row_now[0], row_now[2], row_now[3]
        )
        normed_bf = normed.astype(jnp.bfloat16)
        pre_act = jnp.einsum("rd,bdc->brc", normed_bf, w_in, preferred_element_type=jnp.float32)
        activated, slope = gelu_pair(pre_act + col_now[2:, None])
        activated = activated.astype(jnp.bfloat16)
        slope = slope.astype(jnp.bfloat16)
        mlp_out = jnp.einsum(
            "brc,bdc->rd", activated, w_out, preferred_element_type=jnp.float32
        )
        output, scaled_two, inverse_two = norm_forward(
            normed + mlp_out + row_now[1], row_now[4], row_now[5]
        )
        saved_layers.append(
            (hidden_bf, query, key, value, log_total, context, scaled_one, inverse_one, normed_bf)
            + (slope, activated, scaled_two, inverse_two)
        )
        hidden = output
    upstream = out_grad.astype(jnp.float32)
    operands = [None] * LAYERS
    col_parts = [None] * LAYERS
    row_parts = [None] * LAYERS
    for layer in reversed(range(LAYERS)):
        w_qkv, w_proj, w_in, w_out = matrices(layer)
        row_now = row_state[0, layer]
        (
            hidden_bf,
            query,
            key,
            value,
            log_total,
            context,
            scaled_one,
            inverse_one,
            normed_bf,
            slope,
            activated,
            scaled_two,
            inverse_two,
        ) = saved_layers[layer]
        d_two, gain_two, shift_two = norm_backward(upstream, scaled_two, inverse_two, row_now[4])
        grad_bias_two = jnp.sum(d_two, axis=0)
        d_two_bf = d_two.astype(jnp.bfloat16)
        d_act = jnp.einsum("rd,bdc->brc", d_two_bf, w_out, preferred_element_type=jnp.float32)
        d_pre = (d_act * slope).astype(jnp.bfloat16)
        grad_bias_in = jnp.sum(d_pre, axis=1, dtype=jnp.float32)
        d_normed = jnp.einsum("brc,bdc->rd", d_pre, w_in, preferred_element_type=jnp.float32)
        d_normed = d_two + d_normed
        d_one, gain_one, shift_one = norm_backward(d_normed, scaled_one, inverse_one, row_now[2])
        grad_bias_proj = jnp.sum(d_one, axis=0)
        d_one_bf = d_one.astype(jnp.bfloat16)
        d_context = dot(d_one_bf, w_proj, ((1,), (0,))).astype(jnp.bfloat16)
        d_context = d_context.reshape(rows, heads, HEAD_DIM)
        scores = jnp.einsum("qhd,khd->hqk", query, key, preferred_element_type=jnp.float32)
        scores = jnp.where(same_doc, scores, -1e30)
        soft = jnp.exp(scores - log_total)
        d_values = jnp.einsum(
            "hqk,qhd->khd",
            soft.astype(jnp.bfloat16),
            d_context,
            preferred_element_type=jnp.float32,
        )
        d_probs = jnp.einsum(
            "qhd,khd->hqk", d_context, value, preferred_element_type=jnp.float32
        )
        d_scores = (
            soft * (d_probs - jnp.sum(soft * d_probs, axis=-1, keepdims=True))
        ).astype(jnp.bfloat16)
        d_queries = (
            jnp.einsum("hqk,khd->qhd", d_scores, key, preferred_element_type=jnp.float32)
            * score_scale
        )
        d_keys = jnp.einsum("hqk,qhd->khd", d_scores, query, preferred_element_type=jnp.float32)
        d_qkv = jnp.stack(
            [
                d_queries.reshape(rows, width),
                own_rows(d_keys.reshape(seq_len, width)),
                own_rows(d_values.reshape(seq_len, width)),
            ]
        ).astype(jnp.bfloat16)
        grad_bias_qkv = jnp.sum(d_qkv, axis=1, dtype=jnp.float32)
        upstream = d_one + jnp.einsum(
            "brc,bdc->rd", d_qkv, w_qkv, preferred_element_type=jnp.float32
        )
        operands[layer] = (hidden_bf, d_one_bf, normed_bf, d_two_bf)
        operands[layer] += (d_qkv, context[None], d_pre, activated)
        col_parts[layer] = jnp.concatenate(
            [
                grad_bias_qkv[0:1],
                grad_bias_qkv[2:3],
                grad_bias_in,
            ],
            axis=0,
        )
        row_parts[layer] = jnp.stack(
            [grad_bias_proj, grad_bias_two, gain_one, shift_one, gain_two, shift_two]
        )
    small = jnp.stack([jnp.stack(col_parts), jnp.stack(row_parts)])
    summed = []
    for layer in operands:
        whole = jnp.concatenate(
            [
                jnp.einsum(
                    "rd,brc->bdc", layer[i], layer[4 + i], preferred_element_type=jnp.float32
                )
                for i in range(4)
            ],
            axis=0,
        )
        summed.append(
            lax.psum_scatter(whole.astype(jnp.bfloat16), BOTH, scatter_dimension=1, tiled=True)
        )
    summed = jnp.concatenate(summed, axis=0)

    slot_ids = jnp.arange(slots, dtype=jnp.int32)
    named = unit_slot[None, :] == slot_ids[:, None]
    holds = jnp.any(named, axis=1)
    unit_of = jnp.argmax(named, axis=1)
    back = jnp.where(holds[:, None, None], summed[unit_of], jnp.zeros((), jnp.bfloat16))
    back = back.reshape(dp_size, slot_count, piece, tensor_size, col_width)
    back = back.transpose(0, 3, 1, 2, 4).reshape(devices, slot_count, piece, col_width)
    owned = lax.all_to_all(back, BOTH, 0, 0)
    owned = owned.transpose(1, 0, 2, 3)
    owned = owned.reshape(slot_count, width, col_width)
    return (hidden, upstream, owned, lax.psum(small, BOTH))


def run_kernels(unit_slot, masters, hidden_in, doc_ids, column_state, row_state, out_grad):
    slot_count, width, cols = masters.shape
    units = unit_slot.shape[0]
    per_layer = units // LAYERS
    blocks = (per_layer - 4) // 2
    dp_size = lax.axis_size("dp")
    piece = width // (dp_size * lax.axis_size("tensor"))
    dp = lax.axis_index("dp")
    owner = unit_slot // slot_count
    mates = owner[:, None] == owner[None, :]
    order = np.arange(units)
    rank = jnp.sum(mates & (order[:, None] > order[None, :]), axis=1, dtype=jnp.int32)
    feed = [4 + blocks, 4]
    made = [base + b for b in range(blocks) for base in feed] + [3, 0, 1, 2]
    made = [layer * per_layer + j for layer in reversed(range(LAYERS)) for j in made]
    turn = np.argsort(np.array(made))
    later = jnp.sum(mates & (turn[:, None] < turn[None, :]), axis=1, dtype=jnp.int32)
    back = slot_count - 1 - later
    spots = np.arange(slot_count * dp_size)
    asked = (back * dp_size + owner)[None, :] == spots[:, None]
    pick = jnp.max(jnp.where(asked, order[None, :], -1), axis=1)
    pick = jnp.where(pick < 0, made[0], pick).astype(jnp.int32)
    own_slots = dp * slot_count + jnp.arange(slot_count, dtype=jnp.int32)
    named = unit_slot[None, :] == own_slots[:, None]
    slot_rank = jnp.sum(jnp.where(named, rank[None, :], 0), axis=1)
    slot_back = jnp.sum(jnp.where(named, back[None, :], 0), axis=1)
    holds = jnp.any(named, axis=1)
    local_slot = jnp.arange(slot_count)
    first = [
        jnp.max(jnp.where(holds & (slot_rank == turn_now), local_slot, 0))
        for turn_now in range(slot_count)
    ]
    sent = jnp.stack(
        [lax.dynamic_index_in_dim(masters, i, 0, keepdims=False) for i in first]
    ).astype(jnp.bfloat16)

    docs = lax.dynamic_index_in_dim(doc_ids, lax.axis_index("tensor"), 0, keepdims=False)
    col_full = lax.all_gather(column_state[0], "tensor", axis=2, tiled=True)
    none = jnp.zeros_like(col_full[:, :1])
    bias = jnp.concatenate([col_full[:, :1], none, col_full[:, 1:]], axis=1)
    weights, hidden, *saved = forward(
        rank, owner, sent, hidden_in, docs, bias, row_state[0], piece
    )
    upstream, owned, small = backward(
        pick, out_grad, docs, row_state[0], weights, saved, piece, cols
    )
    owned = owned.reshape(slot_count, width, cols)
    owned = jnp.stack(
        [
            lax.dynamic_index_in_dim(owned, slot_back[i], 0, keepdims=False)
            for i in range(slot_count)
        ]
    )
    owned = jnp.where(holds[:, None, None], owned, jnp.zeros((), owned.dtype))
    return (hidden, upstream, owned, small.reshape(2, LAYERS, 2 + blocks, width))


def local(
    hidden_in,
    doc_ids,
    unit_slot,
    masters,
    first_moment,
    second_moment,
    column_state,
    row_state,
    out_grad,
):
    slot_count, width, col_width = masters.shape
    dp_size = lax.axis_size("dp")
    tensor_size = lax.axis_size("tensor")
    slots = slot_count * dp_size
    tensor_index = lax.axis_index("tensor")
    kernels = dp_size == 8 and tensor_size == 4 and hidden_in.shape[0] == doc_ids.shape[1]

    run = run_kernels if kernels else run_general
    hidden, upstream, owned, small = run(
        unit_slot, masters, hidden_in, doc_ids, column_state, row_state, out_grad
    )
    owned = owned.astype(jnp.float32)
    slot_ids = jnp.arange(slots, dtype=jnp.int32)
    holds = jnp.any(unit_slot[None, :] == slot_ids[:, None], axis=1)
    row_total = small[1]
    col_total = lax.dynamic_slice_in_dim(small[0], tensor_index * col_width, col_width, axis=2)

    occupied = lax.dynamic_slice_in_dim(holds, lax.axis_index("dp") * slot_count, slot_count)
    occupied = occupied.astype(jnp.float32)[:, None, None]
    new_master, new_first, new_second = adamw_update(
        masters, owned, first_moment, second_moment, RATE_UNITS
    )
    unit_master = new_master * occupied
    unit_state = jnp.stack([new_first * occupied, new_second * occupied])
    new_col, col_first, col_second = adamw_update(
        column_state[0], col_total, column_state[1], column_state[2], RATE_SMALL
    )
    column_out = jnp.stack([col_total, new_col, col_first, col_second])
    new_row, row_first, row_second = adamw_update(
        row_state[0], row_total, row_state[1], row_state[2], RATE_SMALL
    )
    row_out = jnp.stack([row_total, new_row, row_first, row_second])
    return (hidden, upstream, unit_master, unit_state, column_out, row_out)


def solution(mesh):
    return jax.shard_map(
        local,
        mesh=mesh,
        in_specs=(
            P(("dp", "tensor"), None),
            P("dp", None),
            P(),
            P("dp", None, "tensor"),
            P("dp", None, "tensor"),
            P("dp", None, "tensor"),
            P(None, None, None, "tensor"),
            P(),
            P(("dp", "tensor"), None),
        ),
        out_specs=(
            P(("dp", "tensor"), None),
            P(("dp", "tensor"), None),
            P("dp", None, "tensor"),
            P(None, "dp", None, "tensor"),
            P(None, None, None, "tensor"),
            P(),
        ),
        check_vma=False,
    )
```

```python
import math

import jax
import jax.numpy as jnp
from jax import lax
from jax.experimental import pallas as pl
from jax.experimental.pallas import tpu as pltpu
from jax.sharding import PartitionSpec as P
import numpy as np

HEAD_DIM = 64
LAYERS = 2
STEP = 3

EPS_NORM = 1e-06
RATE_UNITS = 0.05
RATE_SMALL = 0.2
WEIGHT_DECAY = 0.01
ADAM_EPS = 1e-08
BETA_MOMENT = 0.5
BOTH = ("dp", "tensor")


def norm_forward(summed, gain, shift):
    row_mean = jnp.mean(summed, axis=1, keepdims=True)
    centred = summed - row_mean
    inverse = lax.rsqrt(jnp.mean(centred * centred, axis=1, keepdims=True) + EPS_NORM)
    scaled = centred * inverse
    return (scaled * gain + shift, scaled, inverse)


def norm_backward(upstream, scaled, inverse, gain):
    d_scaled = upstream * gain
    mean_one = jnp.mean(d_scaled, axis=1, keepdims=True)
    mean_two = jnp.mean(d_scaled * scaled, axis=1, keepdims=True)
    grad_input = inverse * (d_scaled - mean_one - scaled * mean_two)
    return (grad_input, jnp.sum(upstream * scaled, axis=0), jnp.sum(upstream, axis=0))


def gelu_pair(v):
    cdf = 0.5 * (1.0 + lax.erf(v * 2.0 ** (-0.5)))
    bell = jnp.exp(-0.5 * v * v) * (2.0 * math.pi) ** (-0.5)
    return (v * cdf, cdf + v * bell)


def adamw_update(old_value, gradient, first_old, second_old, learn_rate):
    first_new = BETA_MOMENT * first_old + (1.0 - BETA_MOMENT) * gradient
    second_new = BETA_MOMENT * second_old + (1.0 - BETA_MOMENT) * gradient * gradient
    correct = 1.0 - BETA_MOMENT**STEP
    step_size = first_new / correct / (jnp.sqrt(second_new / correct) + ADAM_EPS)
    return (old_value - learn_rate * (step_size + WEIGHT_DECAY * old_value), first_new, second_new)


def dot(left, right, dims):
    return lax.dot_general(left, right, (dims, ((), ())), preferred_element_type=jnp.float32)


LANES = 2 * HEAD_DIM


def head_lanes(value, head):
    lane = lax.broadcasted_iota(jnp.int32, value.shape, 1)
    keep = lane < HEAD_DIM if head == 0 else lane >= HEAD_DIM
    return jnp.where(keep, value, jnp.zeros_like(value))


def pair_lanes(first, second):
    lane = lax.broadcasted_iota(jnp.int32, first.shape, 1)
    return jnp.where(lane < HEAD_DIM, first, second)


def attend_pair(pair, q_ref, k_ref, v_ref, mask_ref, ctx_ref, lse_ref):
    lanes = pl.ds(pl.multiple_of(pair * LANES, LANES), LANES)
    query, key, value = q_ref[:, lanes], k_ref[:, lanes], v_ref[:, lanes]
    value_t = value.T
    parts = []
    for head in range(2):
        scores = dot(head_lanes(key, head), query, ((1,), (1,))) + mask_ref[...]
        top = jnp.max(scores, axis=0, keepdims=True)
        weight = jnp.exp(scores - top)
        total = jnp.sum(weight, axis=0, keepdims=True)
        lse_ref[pair * 2 + head] = top + jnp.log(total)
        mine = value_t[head * HEAD_DIM : (head + 1) * HEAD_DIM]
        mixed = dot(mine, weight.astype(jnp.bfloat16), ((1,), (0,)))
        parts.append(mixed * (1.0 / total))
    ctx_ref[:, lanes] = jnp.concatenate(parts, axis=0).T.astype(ctx_ref.dtype)


def attend_back_pair(pair, q_ref, k_ref, v_ref, d_ref, mask_ref, lse_ref, dq_ref, dk_ref, dv_ref):
    lanes = pl.ds(pl.multiple_of(pair * LANES, LANES), LANES)
    query, key, value = q_ref[:, lanes], k_ref[:, lanes], v_ref[:, lanes]
    grad = d_ref[:, lanes]
    key_t = key.T
    parts, d_keys, d_values = [], [], []
    for head in range(2):
        scores = dot(head_lanes(key, head), query, ((1,), (1,))) + mask_ref[...]
        soft = jnp.exp(scores - lse_ref[pair * 2 + head])
        d_values.append(dot(soft.astype(jnp.bfloat16), grad, ((1,), (0,))))
        d_soft = dot(head_lanes(value, head), grad, ((1,), (1,)))
        both = soft * d_soft
        mean = jnp.sum(both, axis=0, keepdims=True)
        d_scores = (both - soft * mean).astype(jnp.bfloat16)
        d_keys.append(dot(d_scores, query, ((1,), (0,))))
        mine = key_t[head * HEAD_DIM : (head + 1) * HEAD_DIM]
        parts.append(dot(mine, d_scores, ((1,), (0,))))
    scale = HEAD_DIM ** (-0.5)
    dq_ref[:, lanes] = (jnp.concatenate(parts, axis=0).T * scale).astype(dq_ref.dtype)
    dk_ref[:, lanes] = pair_lanes(*d_keys).astype(dk_ref.dtype)
    dv_ref[:, lanes] = pair_lanes(*d_values).astype(dv_ref.dtype)


def fill_mask(mask_ref, docs_col_ref, docs_row_ref):
    same = docs_col_ref[...] == docs_row_ref[...]
    mask_ref[...] = jnp.where(same, 0.0, -1e30).astype(jnp.float32)


LAG = 2


def spread_order(z, y, x, c):
    return ((c * 2 + x) * 2 + y) * 4 + z


def every_other(z, y, x, c, body):
    for step in (2, 1, 3, 0):

        def one(i, carry, step=step):
            body((z + step) % 4, (y + i // 4) % 2, (x + (i // 2) % 2) % 2, (c + i % 2) % 2)
            return carry

        lax.fori_loop(1 if step == 0 else 0, 8, one, 0)


def greet_all(z, y, x, c):
    barrier = pltpu.get_barrier_semaphore()

    def greet(zz, yy, xx, cc):
        pl.semaphore_signal(
            barrier,
            inc=1,
            device_id=(zz * 2 + yy, xx * 2 + cc),
            device_id_type=pl.DeviceIdType.MESH,
        )

    every_other(z, y, x, c, greet)
    return barrier


TILE = 256


def norm_back_rows(upstream, scaled, inverse, gain):
    d_scaled = upstream * gain
    mean_one = jnp.mean(d_scaled, axis=1, keepdims=True)
    mean_two = jnp.mean(d_scaled * scaled, axis=1, keepdims=True)
    return inverse * (d_scaled - mean_one - scaled * mean_two)


def backward_kernel(
    pick_ref,
    out_grad_ref,
    docs_col_ref,
    docs_row_ref,
    row_ref,
    weights_ref,
    low_ref,
    mixed_ref,
    ctx_ref,
    lse_ref,
    one_ref,
    inv_one_ref,
    normed_ref,
    act_ref,
    slope_ref,
    two_ref,
    inv_two_ref,
    owned_ref,
    total_ref,
    small_out,
    out_ref,
    back_buf,
    left_buf,
    right_buf,
    unit_buf,
    scaled_buf,
    inv_buf,
    slope_buf,
    mixed_buf,
    lse_buf,
    mask_buf,
    d_ctx_buf,
    core_out,
    core_in,
    sum_core,
    first_in,
    sum_first,
    second_in,
    sum_second,
    z_in,
    small_sum,
    small_got,
    load_sem,
    core_sems,
    first_sems,
    second_sems,
    z_sems,
    small_sems,
    own_sems,
    round_sems,
):
    units, piece, width = out_ref.shape
    rows = total_ref.shape[0]
    per_layer = units // LAYERS
    blocks = (per_layer - 4) // 2
    at_out, at_query = 2 * blocks, 2 * blocks + 1
    dp, tensor = lax.axis_index("dp"), lax.axis_index("tensor")
    z, y, x, c = dp // 2, dp % 2, tensor // 2, tensor % 2
    half, parts = width // 2, 2
    side_cols = half // 2
    quarter, eighth = half // 2, half // 4
    to_core = (dp, x * 2 + 1 - c)
    to_x = (dp, (1 - x) * 2 + c)
    to_y = (z * 2 + 1 - y, tensor)
    to_z = [(((z + k) % 4) * 2 + y, tensor) for k in (1, 2, 3)]
    to_z1 = ((z + 1 - 2 * (z % 2)) * 2 + y, tensor)
    to_z2 = (((z + 2) % 4) * 2 + y, tensor)
    mesh_id = pl.DeviceIdType.MESH

    barrier = greet_all(z, y, x, c)

    def remote(src, dst, sems, send, recv, peer):
        return pltpu.make_async_remote_copy(
            src_ref=src,
            dst_ref=dst,
            send_sem=sems.at[send],
            recv_sem=sems.at[recv],
            device_id=peer,
            device_id_type=mesh_id,
        )

    def place(s):
        return LAYERS - 1 - s // per_layer, s % per_layer

    def unit_of(s):
        layer, j = place(s)
        feed = jnp.where(j % 2 == 0, 4 + blocks + j // 2, 4 + j // 2)
        return layer * per_layer + jnp.where(
            j < at_out, feed, jnp.where(j == at_out, 3, j - at_query)
        )

    def left_of(s):
        j = s % per_layer
        feed = jnp.where(j % 2 == 0, 3, 2)
        return jnp.where(j < at_out, feed, jnp.where(j == at_out, 1, 0))

    def loaded_slot(s):
        return ((s // per_layer) * (blocks + 1) + (s % per_layer) // 2) % 2

    def right_of(s):
        j = s % per_layer
        feed = jnp.where(j % 2 == 0, loaded_slot(s), 2 + (j // 2) % 2)
        return jnp.where(
            j < at_out, feed, jnp.where(j == at_out, loaded_slot(s), 4 + j - at_query)
        )

    local = pltpu.make_async_copy

    def unit_load(s):
        return local(weights_ref.at[unit_of(s)], unit_buf.at[s % 3], load_sem.at[0, s % 3])

    def act_load(layer, block, slot):
        return local(act_ref.at[layer, block], right_buf.at[slot], load_sem.at[1, slot])

    def ctx_load(layer, slot):
        return local(ctx_ref.at[layer], right_buf.at[slot], load_sem.at[1, slot])

    def slope_load(layer, block):
        return local(slope_ref.at[layer, block], slope_buf, load_sem.at[2, 0])

    def norm_loads(layer, which):
        scaled, inv = ((one_ref, inv_one_ref), (two_ref, inv_two_ref))[which]
        return [
            local(scaled.at[layer], scaled_buf, load_sem.at[3, 0]),
            local(inv.at[layer], inv_buf, load_sem.at[3, 1]),
        ]

    def mixed_loads(layer):
        return [
            local(mixed_ref.at[layer], mixed_buf, load_sem.at[4, 0]),
            local(lse_ref.at[layer], lse_buf, load_sem.at[4, 1]),
        ]

    def normed_load(layer):
        return local(normed_ref.at[layer], left_buf.at[2], load_sem.at[2, 1])

    def low_load(layer):
        return local(low_ref.at[layer], left_buf.at[0], load_sem.at[5, 0])

    def begin(*copies):
        for copy in copies:
            copy.start()

    def finish(*copies):
        for copy in copies:
            copy.wait()

    def note(row, value):
        small_sum[0, pl.ds(row, 1), :] = value

    def column(layer, i):
        return layer * (2 + blocks) + i

    def row(layer, i):
        return LAYERS * (2 + blocks) + layer * 6 + i

    def norm_back(layer, gain_row, bias_row, low_slot):
        gain = row_ref[layer * 6 + gain_row]
        size = 128

        def one(tile, carry):
            part = pl.ds(pl.multiple_of(tile * size, size), size)
            upstream = total_ref[part, :]
            scaled = scaled_buf[part, :]
            inside = norm_back_rows(upstream, scaled, inv_buf[part, 0:1], gain)
            total_ref[part, :] = inside
            left_buf[low_slot, part, :] = inside.astype(jnp.bfloat16)
            sums = (upstream * scaled, upstream, inside)
            return tuple(a + jnp.sum(b, axis=0, keepdims=True) for a, b in zip(carry, sums))

        zero = jnp.zeros((1, width), jnp.float32)
        gains, shifts, biases = lax.fori_loop(0, rows // size, one, (zero, zero, zero))
        note(row(layer, gain_row), gains)
        note(row(layer, gain_row + 1), shifts)
        note(row(layer, bias_row), biases)

    def heads(start, stop):
        inputs = [mixed_buf.at[i] for i in range(3)]
        grads = [right_buf.at[4 + i] for i in range(3)]

        def one(pair, carry):
            attend_back_pair(pair, *inputs, d_ctx_buf, mask_buf, lse_buf, *grads)
            return carry

        lax.fori_loop(start, stop, one, 0)

    pairs = width // LANES

    def data_gradient(s):
        layer, j = place(s)
        matrix = unit_buf.at[s % 3]
        before = unit_buf.at[(s + 2) % 3]
        slot = loaded_slot(s)

        @pl.when(j == 0)
        def _():
            finish(*norm_loads(layer, 1))

            @pl.when(s == 0)
            def _():
                total_ref[...] = out_grad_ref[...].astype(jnp.float32)

            norm_back(layer, 4, 1, 3)
            begin(*norm_loads(layer, 0), *mixed_loads(layer))

        @pl.when(j == 1)
        def _():
            finish(normed_load(layer))
            begin(low_load(layer))

        @pl.when((j < at_out) & (j % 2 == 0))
        def _():
            block = j // 2
            finish(slope_load(layer, block), act_load(layer, block, slot))

            @pl.when(block < blocks - 1)
            def _():
                act_load(layer, block + 1, 1 - slot).start()

            @pl.when(block == blocks - 1)
            def _():
                ctx_load(layer, 1 - slot).start()

            d_act = dot(left_buf[3], matrix[...], ((1,), (0,)))
            d_pre = (d_act * slope_buf[...].astype(jnp.float32)).astype(jnp.bfloat16)
            right_buf[2 + block % 2] = d_pre
            sums = jnp.sum(d_pre.astype(jnp.float32), axis=0, keepdims=True)
            note(column(layer, 2 + block), sums)

            @pl.when(block < blocks - 1)
            def _():
                slope_load(layer, block + 1).start()

        @pl.when((j < at_out) & (j % 2 == 1))
        def _():
            total_ref[...] += dot(right_buf[2 + (j // 2) % 2], matrix[...], ((1,), (1,)))

        @pl.when(j == at_out)
        def _():
            finish(*norm_loads(layer, 0), *mixed_loads(layer), ctx_load(layer, slot))
            norm_back(layer, 2, 0, 1)

            @pl.when(layer > 0)
            def _():
                act_load(layer - 1, 0, 1 - slot).start()
                begin(*norm_loads(layer - 1, 1))
                slope_load(layer - 1, 0).start()

            d_ctx_buf[...] = dot(left_buf[1], matrix[...], ((1,), (0,))).astype(jnp.bfloat16)

        @pl.when(j == at_query)
        def _():
            finish(low_load(layer))

            @pl.when(layer > 0)
            def _():
                normed_load(layer - 1).start()

            heads(3 * pairs // 8, 5 * pairs // 8)

        @pl.when(j == at_query + 1)
        def _():
            total_ref[...] += dot(right_buf[4], before[...], ((1,), (1,)))

        @pl.when(j == at_query + 2)
        def _():
            total_ref[...] += dot(right_buf[6], matrix[...], ((1,), (1,)))

    def data_gradient_rest(s):
        layer, j = place(s)

        @pl.when(j == at_out)
        def _():
            heads(0, 3 * pairs // 8)

        @pl.when(j == at_query)
        def _():
            heads(5 * pairs // 8, pairs)

        @pl.when(j == at_query + 1)
        def _():
            total_ref[...] += dot(right_buf[5], unit_buf[s % 3], ((1,), (1,)))
            for i, number in ((0, 0), (2, 1)):
                sums = jnp.sum(right_buf[4 + i].astype(jnp.float32), axis=0, keepdims=True)
                note(column(layer, number), sums)

    def product(s, side, tile):
        unit = s // parts
        start = pl.multiple_of(side * half + tile * TILE, TILE)
        left = left_buf[left_of(unit), :, pl.ds(start, TILE)]
        right = right_buf[
            right_of(unit), :, pl.ds(pl.multiple_of((s % parts) * half, half), half)
        ]
        return lax.dot_general(
            left, right, (((0,), (0,)), ((), ())), preferred_element_type=jnp.float32
        )

    def core_copy(s):
        return remote(
            core_out.at[s % 2], core_in.at[s % 4], core_sems, (0, s % 2), (1, s % 4), to_core
        )

    def first_copies(s):
        here = sum_core.at[s % 3]
        return (
            remote(
                here.at[pl.ds(pl.multiple_of((1 - x) * quarter, quarter), quarter), pl.ds(0, side_cols)],
                first_in.at[s % 4, 0],
                first_sems,
                (0, 0, s % 3),
                (1, 0, s % 4),
                to_x,
            ),
            *(
                remote(
                    here.at[
                        pl.ds(pl.multiple_of(i * quarter + (1 - y) * eighth, eighth), eighth),
                        pl.ds(side_cols, side_cols),
                    ],
                    first_in.at[s % 4, 1, pl.ds(i * eighth, eighth)],
                    first_sems,
                    (0, 1 + i, s % 3),
                    (1, 1 + i, s % 4),
                    to_y,
                )
                for i in range(2)
            ),
        )

    def second_copies(s):
        here = sum_first.at[s % 3]
        return (
            remote(
                here.at[0, pl.ds(pl.multiple_of((1 - y) * eighth, eighth), eighth)],
                second_in.at[s % 4, 0],
                second_sems,
                (0, 0, s % 3),
                (1, 0, s % 4),
                to_y,
            ),
            remote(
                here.at[1, pl.ds(pl.multiple_of((1 - x) * eighth, eighth), eighth)],
                second_in.at[s % 4, 1],
                second_sems,
                (0, 1, s % 3),
                (1, 1, s % 4),
                to_x,
            ),
        )

    def z_copies(s):
        return [
            remote(
                sum_second.at[s % 3, pl.ds(pl.multiple_of(((z + k) % 4) * piece, piece), piece)],
                z_in.at[s % 4, k - 1],
                z_sems,
                (0, k - 1, s % 3),
                (1, k - 1, s % 4),
                to_z[k - 1],
            )
            for k in (1, 2, 3)
        ]

    small_peers = (to_core, to_x, to_y, to_z1, to_z2)

    def small_copy(stage):
        return remote(
            small_sum.at[stage],
            small_got.at[stage],
            small_sems,
            (0, stage),
            (1, stage),
            small_peers[stage],
        )

    rounds, owners = back_buf.shape[0], back_buf.shape[1]
    cols = owned_ref.shape[3]
    me = spread_order(z, y, x, c)

    def own_back(number):
        return local(
            back_buf.at[number, dp, :, pl.ds(pl.multiple_of(tensor * cols, cols), cols)],
            owned_ref.at[number, me],
            own_sems.at[number],
        )

    def send_back(number):
        def fill(owner, carry):
            back_buf[number, owner] = out_ref[pick_ref[number * owners + owner]]
            return carry

        lax.fori_loop(0, owners, fill, 0)
        own_back(number).start()

        def send(zz, yy, xx, cc):
            there = xx * 2 + cc
            remote(
                back_buf.at[
                    number, zz * 2 + yy, :, pl.ds(pl.multiple_of(there * cols, cols), cols)
                ],
                owned_ref.at[number, me],
                round_sems,
                (0, number),
                (1, number),
                (zz * 2 + yy, there),
            ).start()

        every_other(z, y, x, c, send)

    def finish_back(number):
        own_back(number).wait()
        most = owned_ref.at[number, pl.ds(0, 31)]
        remote(most, most, round_sems, (0, number), (1, number), to_core).wait()

    top = LAYERS - 1
    steps = parts * units
    begin(
        *norm_loads(top, 1),
        unit_load(jnp.int32(0)),
        slope_load(top, 0),
        act_load(top, 0, 0),
        normed_load(top),
    )
    fill_mask(mask_buf, docs_col_ref, docs_row_ref)
    pl.semaphore_wait(barrier, 31)

    def step(s, carry):
        last = s - 3 * LAG - 1

        @pl.when((last >= 0) & (last < steps))
        def _():
            for copy in z_copies(last):
                copy.wait()
            total = sum_second[last % 3, pl.ds(pl.multiple_of(z * piece, piece), piece), :].astype(
                jnp.float32
            )
            for k in range(3):
                total = total + z_in[last % 4, k].astype(jnp.float32)
            cols_now = pl.ds(pl.multiple_of((last % parts) * half, half), half)
            out_ref[unit_of(last // parts), :, cols_now] = total.astype(out_ref.dtype)

            @pl.when((last // parts >= units - rounds) & (last % parts == parts - 1))
            def _():
                send_back(last // parts - (units - rounds))

        third = s - 2 * LAG - 1

        @pl.when((third >= 0) & (third < steps))
        def _():
            for copy in second_copies(third):
                copy.wait()
            for part, side in ((0, y), (1, x)):
                mine = sum_first[
                    third % 3, part, pl.ds(pl.multiple_of(side * eighth, eighth), eighth), :
                ]
                total = mine.astype(jnp.float32) + second_in[third % 4, part].astype(jnp.float32)
                sum_second[third % 3, :, part * side_cols : (part + 1) * side_cols] = total.astype(
                    jnp.bfloat16
                )
            for copy in z_copies(third):
                copy.start()

        second = s - LAG - 1

        @pl.when((second >= 0) & (second < steps))
        def _():
            for copy in first_copies(second):
                copy.wait()
            mine = sum_core[
                second % 3, pl.ds(pl.multiple_of(x * quarter, quarter), quarter), 0:side_cols
            ]
            total = mine.astype(jnp.float32) + first_in[second % 4, 0].astype(jnp.float32)
            sum_first[second % 3, 0] = total.astype(jnp.bfloat16)
            for i in range(2):
                mine = sum_core[
                    second % 3,
                    pl.ds(pl.multiple_of(i * quarter + y * eighth, eighth), eighth),
                    side_cols : 2 * side_cols,
                ]
                part = pl.ds(i * eighth, eighth)
                total = mine.astype(jnp.float32) + first_in[second % 4, 1, part, :].astype(
                    jnp.float32
                )
                sum_first[second % 3, 1, part, :] = total.astype(jnp.bfloat16)
            for copy in second_copies(second):
                copy.start()

        @pl.when(s < steps)
        def _():
            unit = s // parts

            @pl.when(s % parts == 0)
            def _():
                unit_load(unit).wait()

                @pl.when(unit + 1 < units)
                def _():
                    unit_load(unit + 1).start()

                data_gradient(unit)

            @pl.when(s % parts == 1)
            def _():
                data_gradient_rest(unit)

            @pl.when(s >= 2)
            def _():
                core_copy(s - 2).wait_send()

            def one(tile, carry):
                part = pl.ds(pl.multiple_of(tile * TILE, TILE), TILE)
                core_out[s % 2, part, :] = product(s, 1 - c, tile).astype(jnp.bfloat16)
                return carry

            lax.fori_loop(0, half // TILE, one, 0)
            core_copy(s).start()

        first = s - 1

        @pl.when((first >= 0) & (first < steps))
        def _():
            core_copy(first).wait_recv()

            def one(tile, carry):
                part = pl.ds(pl.multiple_of(tile * TILE, TILE), TILE)
                total = product(first, c, tile) + core_in[first % 4, part, :].astype(jnp.float32)
                sum_core[first % 3, part, :] = total.astype(jnp.bfloat16)
                return carry

            lax.fori_loop(0, half // TILE, one, 0)
            for copy in first_copies(first):
                copy.start()

        for stage in range(6):

            @pl.when(s == steps + stage)
            def _(stage=stage):
                if stage > 0:
                    small_copy(stage - 1).wait()
                    total = small_sum[stage - 1] + small_got[stage - 1]
                    if stage < 5:
                        small_sum[stage] = total
                    else:
                        small_out[...] = total
                if stage < 5:
                    small_copy(stage).start()

        return carry

    lax.fori_loop(0, steps + 3 * LAG + 1, step, 0)
    for s in (steps - 2, steps - 1):
        core_copy(s).wait_send()
    for number in range(rounds):
        finish_back(number)


def backward(pick, out_grad, docs, row_now, weights, saved, piece, cols):
    units, width, _ = weights.shape
    rows = out_grad.shape[0]
    blocks = (units // LAYERS - 4) // 2
    half = width // 2
    low, full = jnp.bfloat16, jnp.float32
    rounds = pick.shape[0] // 8
    small = (LAYERS * (8 + blocks), width)
    any_spec = pl.BlockSpec(memory_space=pl.ANY)
    vmem_spec = pl.BlockSpec(memory_space=pltpu.VMEM)
    dma = pltpu.SemaphoreType.DMA
    summed, total, small = pl.pallas_call(
        backward_kernel,
        out_shape=(
            jax.ShapeDtypeStruct((rounds, width // piece, piece, cols), low),
            jax.ShapeDtypeStruct((rows, width), full),
            jax.ShapeDtypeStruct(small, full),
        ),
        in_specs=[pl.BlockSpec(memory_space=pltpu.SMEM)] + [vmem_spec] * 4 + [any_spec] * (1 + len(saved)),
        out_specs=(vmem_spec, vmem_spec, vmem_spec),
        scratch_shapes=[
            pltpu.VMEM((units, piece, width), low),
            pltpu.VMEM((rounds, 8, piece, width), low),
            pltpu.VMEM((4, rows, width), low),
            pltpu.VMEM((7, rows, width), low),
            pltpu.VMEM((3, width, width), low),
            pltpu.VMEM((rows, width), full),
            pltpu.VMEM((rows, 128), full),
            pltpu.VMEM((rows, width), low),
            pltpu.VMEM((3, rows, width), low),
            pltpu.VMEM((width // HEAD_DIM, 1, rows), full),
            pltpu.VMEM((rows, rows), full),
            pltpu.VMEM((rows, width), low),
            pltpu.VMEM((2, half, half), low),
            pltpu.VMEM((4, half, half), low),
            pltpu.VMEM((3, half, half), low),
            pltpu.VMEM((4, 2, half // 2, half // 2), low),
            pltpu.VMEM((3, 2, half // 2, half // 2), low),
            pltpu.VMEM((4, 2, half // 4, half // 2), low),
            pltpu.VMEM((3, half // 4, half), low),
            pltpu.VMEM((4, 3, piece, half), low),
            pltpu.VMEM((5,) + small, full),
            pltpu.VMEM((5,) + small, full),
            dma((6, 3)),
            dma((2, 4)),
            dma((2, 3, 4)),
            dma((2, 2, 4)),
            dma((2, 3, 4)),
            dma((2, 5)),
            dma((rounds,)),
            dma((2, rounds)),
        ],
        compiler_params=pltpu.CompilerParams(
            collective_id=1, has_side_effects=True, vmem_limit_bytes=63 * 1024 * 1024
        ),
        name="backward_reduce",
    )(pick, out_grad, docs[:, None], docs[None, :], row_now.reshape(-1, 1, width), weights, *saved)
    return (total, summed, small)


def norm_rows(value, gain, shift):
    centred = value - jnp.mean(value, axis=1, keepdims=True)
    inverse = lax.rsqrt(jnp.mean(centred * centred, axis=1, keepdims=True) + EPS_NORM)
    scaled = centred * inverse
    return (scaled * gain + shift, scaled, inverse)


NORM_ROWS = 128


def forward_kernel(
    rank_ref,
    owner_ref,
    sent_ref,
    hidden_ref,
    docs_col_ref,
    docs_row_ref,
    bias_ref,
    row_ref,
    out_ref,
    final_ref,
    *refs,
):
    saved, bufs = refs[:11], refs[11:22]
    rounds = sent_ref.shape[0]
    (x_buf, normed_buf, total_buf, mask_buf, unit_buf, own_ref) = refs[22:28]
    (own_sem, sems, unit_sem, save_sem, got_sem, round_sems) = refs[28:34]
    got = refs[34:]
    (low_buf, mixed_buf, ctx_buf, lse_buf, one_buf, inv_one_buf, nb_buf) = bufs[:7]
    (act_buf, slope_buf, two_buf, inv_two_buf) = bufs[7:]
    units, piece, width = own_ref.shape
    rows = hidden_ref.shape[0]
    per_layer = units // LAYERS
    blocks = (per_layer - 4) // 2
    dp, tensor = lax.axis_index("dp"), lax.axis_index("tensor")
    z, y, x, c = dp // 2, dp % 2, tensor // 2, tensor % 2
    half = width // 2
    line, plane = 4 * piece, 8 * piece
    to_core = (dp, x * 2 + 1 - c)
    to_x = (dp, (1 - x) * 2 + c)
    to_y = (z * 2 + 1 - y, tensor)
    to_z = [(((z + k) % 4) * 2 + y, tensor) for k in (1, 2, 3)]
    mesh_id = pl.DeviceIdType.MESH

    barrier = greet_all(z, y, x, c)
    pl.semaphore_wait(barrier, 31)
    cols = sent_ref.shape[2]
    me = dp * 4 + tensor

    def part_for(number, zz, yy, xx, cc):
        start = pl.multiple_of(spread_order(zz, yy, xx, cc) * piece, piece)
        return sent_ref.at[number, pl.ds(start, piece)]

    def keep(number):
        return pltpu.make_async_copy(
            part_for(number, z, y, x, c), got[number].at[me], got_sem.at[number]
        )

    def round_copy(number, src, dst, peer):
        return pltpu.make_async_remote_copy(
            src_ref=src,
            dst_ref=dst,
            send_sem=round_sems.at[0, number],
            recv_sem=round_sems.at[1, number],
            device_id=peer,
            device_id_type=mesh_id,
        )

    def start_round(number):
        keep(number).start()

        def send(zz, yy, xx, cc):
            src = part_for(number, zz, yy, xx, cc)
            round_copy(number, src, got[number].at[me], (zz * 2 + yy, xx * 2 + cc)).start()

        every_other(z, y, x, c, send)

    def finish_round(number):
        keep(number).wait()
        most = got[number].at[pl.ds(0, 31)]
        round_copy(number, most, most, to_core).wait()

    def pick(unit, there):
        rank, owner = rank_ref[unit], owner_ref[unit]
        for j in range(4):
            value = got[0][owner * 4 + j]
            for number in range(1, there):
                value = jnp.where(rank == number, got[number][owner * 4 + j], value)
            own_ref[unit, :, j * cols : (j + 1) * cols] = value

    start_round(0)
    start_round(1)

    my_line = pl.multiple_of(((c * 2 + x) * 2 + y) * line, line)
    my_rows = pl.ds(pl.multiple_of(my_line + z * piece, piece), piece)
    parts, cycle = 2, sems.shape[2]

    def half_of(s):
        return pl.ds(pl.multiple_of((s % parts) * half, half), half)

    def first(s):
        return pl.ds(pl.multiple_of((s % parts) * half, half), half // 2)

    def second(s):
        return pl.ds(pl.multiple_of((s % parts) * half + half // 2, half // 2), half // 2)

    def remote(src, dst, index, s, peer):
        return pltpu.make_async_remote_copy(
            src_ref=src,
            dst_ref=dst,
            send_sem=sems.at[0, index, s % cycle],
            recv_sem=sems.at[1, index, s % cycle],
            device_id=peer,
            device_id_type=mesh_id,
        )

    def own_copy(s):
        unit, cols_now = s // parts, half_of(s)
        return pltpu.make_async_copy(
            own_ref.at[unit, :, cols_now],
            out_ref.at[unit, my_rows, cols_now],
            own_sem.at[s % cycle],
        )

    def stage_z(s):
        unit, cols_now = s // parts, half_of(s)
        here, there = own_ref.at[unit, :, cols_now], out_ref.at[unit, my_rows, cols_now]
        return [remote(here, there, k, s, to_z[k]) for k in range(3)]

    def stage_one(s):
        unit, rows = s // parts, pl.ds(my_line, line)
        one, two = out_ref.at[unit, rows, first(s)], out_ref.at[unit, rows, second(s)]
        return [remote(one, one, 3, s, to_y), remote(two, two, 4, s, to_x)]

    def stage_two(s):
        unit = s // parts
        rows = pl.ds(pl.multiple_of((c * 2 + x) * plane, plane), plane)
        one = out_ref.at[unit, rows, first(s)]
        copies = [remote(one, one, 5, s, to_x)]
        for i in range(2):
            rows = pl.ds(pl.multiple_of(((c * 2 + i) * 2 + y) * line, line), line)
            two = out_ref.at[unit, rows, second(s)]
            copies.append(remote(two, two, 6 + i, s, to_y))
        return copies

    def stage_core(s):
        rows = pl.ds(pl.multiple_of(c * 2 * plane, 2 * plane), 2 * plane)
        there = out_ref.at[s // parts, rows, half_of(s)]
        return [remote(there, there, 8, s, to_core)]

    stages = (stage_z, stage_one, stage_two, stage_core)

    def unit_copy(unit):
        slot = unit % 2
        return pltpu.make_async_copy(out_ref.at[unit], unit_buf.at[slot], unit_sem.at[slot])

    def save(number, layer, block=None):
        src, dst, sem = bufs[number], saved[number].at[layer], save_sem.at[number, 0]
        if block is not None:
            src, dst, sem = src.at[block], dst.at[block], save_sem.at[number, block]
        return pltpu.make_async_copy(src, dst, sem)

    def free(numbers, layer, block=None):
        @pl.when(layer > 0)
        def _():
            for number in numbers:
                save(number, layer - 1, block).wait()

    def heads(start, stop):
        def one(pair, carry):
            attend_pair(
                pair, mixed_buf.at[0], mixed_buf.at[1], mixed_buf.at[2], mask_buf, ctx_buf, lse_buf
            )
            return carry

        lax.fori_loop(start, stop, one, 0)

    tall = rows // parts
    pairs = width // LANES

    def compute(unit, turn):
        layer, j = unit // per_layer, unit % per_layer
        matrix = unit_buf.at[unit % 2]
        mine = pl.ds(pl.multiple_of(turn * tall, tall), tall)

        def small(i):
            return row_ref[layer * 6 + i]

        def over_rows(body):
            def one(tile, carry):
                body(pl.ds(pl.multiple_of(turn * tall + tile * NORM_ROWS, NORM_ROWS), NORM_ROWS))
                return carry

            lax.fori_loop(0, tall // NORM_ROWS, one, 0)

        @pl.when((j == 0) & (turn == 0))
        def _():
            free((0, 1), layer)

            @pl.when(layer == 0)
            def _():
                x_buf[...] = hidden_ref[...].astype(jnp.float32)

            low_buf[...] = x_buf[...].astype(jnp.bfloat16)
            save(0, layer).start()

        @pl.when(j < 3)
        def _():
            value = dot(low_buf[mine, :], matrix[...], ((1,), (0,)))
            value = value + bias_ref[layer * (3 + blocks) + j]
            scale = jnp.where(j == 0, HEAD_DIM ** (-0.5), 1.0)
            mixed_buf[j, mine, :] = (value * scale).astype(jnp.bfloat16)

        @pl.when((j == 2) & (turn == 1))
        def _():
            save(1, layer).start()
            free((2, 3), layer)
            heads(0, pairs // 4)

        @pl.when((j == 3) & (turn == 0))
        def _():
            heads(pairs // 4, 3 * pairs // 4)

        @pl.when((j == 3) & (turn == 1))
        def _():
            heads(3 * pairs // 4, pairs)
            save(2, layer).start()
            save(3, layer).start()
            total_buf[...] = dot(ctx_buf[...], matrix[...], ((1,), (1,)))
            free((4, 5, 6), layer)

            def body(tile, carry):
                part = pl.ds(pl.multiple_of(tile * NORM_ROWS, NORM_ROWS), NORM_ROWS)
                value = x_buf[part, :] + total_buf[part, :] + small(0)
                normed, scaled, inverse = norm_rows(value, small(2), small(3))
                normed_buf[part, :] = normed
                nb_buf[part, :] = normed.astype(jnp.bfloat16)
                one_buf[part, :] = scaled
                inv_one_buf[part, :] = jnp.broadcast_to(inverse, (NORM_ROWS, 128))
                return carry

            lax.fori_loop(0, rows // NORM_ROWS, body, 0)
            for number in (4, 5, 6):
                save(number, layer).start()

        @pl.when((j >= 4) & (j < 4 + blocks))
        def _():
            block = j - 4

            @pl.when(turn == 0)
            def _():
                free((7, 8), layer, block)

            value = dot(nb_buf[mine, :], matrix[...], ((1,), (0,)))
            act, slope = gelu_pair(value + bias_ref[layer * (3 + blocks) + 3 + block])
            act_buf[block, mine, :] = act.astype(jnp.bfloat16)
            slope_buf[block, mine, :] = slope.astype(jnp.bfloat16)

            @pl.when(turn == 1)
            def _():
                save(7, layer, block).start()
                save(8, layer, block).start()

        @pl.when(j >= 4 + blocks)
        def _():
            block = j - 4 - blocks
            part = dot(act_buf[block, mine, :], matrix[...], ((1,), (1,)))

            @pl.when(block == 0)
            def _():
                total_buf[mine, :] = part

            @pl.when(block > 0)
            def _():
                total_buf[mine, :] += part

        @pl.when(j == per_layer - 1)
        def _():
            @pl.when(turn == 0)
            def _():
                free((9, 10), layer)

            def body(part):
                value = normed_buf[part, :] + total_buf[part, :] + small(1)
                output, scaled, inverse = norm_rows(value, small(4), small(5))
                x_buf[part, :] = output
                two_buf[part, :] = scaled
                inv_two_buf[part, :] = jnp.broadcast_to(inverse, (NORM_ROWS, 128))

            over_rows(body)

            @pl.when(turn == 1)
            def _():
                save(9, layer).start()
                save(10, layer).start()

    steps = parts * units

    def step(s, carry):
        for number in range(len(stages), -1, -1):
            now = s - number * LAG

            if number == 0:
                for turn in range(rounds):
                    last = turn == rounds - 1
                    due = (s == parts * turn) | (last & (s > parts * turn) & (s % parts == 0))

                    @pl.when(due & (s < steps))
                    def _(turn=turn):
                        @pl.when(s == parts * turn)
                        def _():
                            finish_round(turn)

                        if turn + 2 < rounds:
                            start_round(turn + 2)
                        pick(s // parts, turn + 1)

            @pl.when((now >= 0) & (now < steps))
            def _(now=now, number=number):
                if number == 0:
                    own_copy(now).start()
                else:
                    if number == 1:
                        own_copy(now).wait()
                    for copy in stages[number - 1](now):
                        copy.wait()
                if number < len(stages):
                    for copy in stages[number](now):
                        copy.start()
                else:

                    @pl.when(now % parts == parts - 1)
                    def _():
                        unit_copy(now // parts).start()

        done = s - len(stages) * LAG - parts

        @pl.when(done >= 0)
        def _():
            @pl.when(done % parts == 0)
            def _():
                unit_copy(done // parts).wait()

            compute(done // parts, done % parts)

        return carry

    fill_mask(mask_buf, docs_col_ref, docs_row_ref)
    lax.fori_loop(0, steps + len(stages) * LAG + parts, step, 0)
    final_ref[...] = x_buf[...]
    last = LAYERS - 1
    for number in (0, 1, 2, 3, 4, 5, 6, 9, 10):
        save(number, last).wait()
    for block in range(blocks):
        save(7, last, block).wait()
        save(8, last, block).wait()


def forward(rank, owner, sent, hidden_in, docs, bias, row_now, piece):
    units, rounds, width = rank.shape[0], sent.shape[0], sent.shape[1]
    rows = hidden_in.shape[0]
    blocks = (units // LAYERS - 4) // 2
    low, full = jnp.bfloat16, jnp.float32
    kept = [
        ((rows, width), low),
        ((3, rows, width), low),
        ((rows, width), low),
        ((width // HEAD_DIM, 1, rows), full),
        ((rows, width), full),
        ((rows, 128), full),
        ((rows, width), low),
        ((blocks, rows, width), low),
        ((blocks, rows, width), low),
        ((rows, width), full),
        ((rows, 128), full),
    ]
    any_spec = pl.BlockSpec(memory_space=pl.ANY)
    vmem_spec = pl.BlockSpec(memory_space=pltpu.VMEM)
    smem_spec = pl.BlockSpec(memory_space=pltpu.SMEM)
    dma = pltpu.SemaphoreType.DMA
    return pl.pallas_call(
        forward_kernel,
        out_shape=[
            jax.ShapeDtypeStruct((units, width, width), low),
            jax.ShapeDtypeStruct((rows, width), full),
        ]
        + [jax.ShapeDtypeStruct((LAYERS,) + shape, dtype) for shape, dtype in kept],
        in_specs=[smem_spec] * 2 + [any_spec] + [vmem_spec] * 5,
        out_specs=[any_spec, vmem_spec] + [any_spec] * len(kept),
        scratch_shapes=[pltpu.VMEM(shape, dtype) for shape, dtype in kept]
        + [
            pltpu.VMEM((rows, width), full),
            pltpu.VMEM((rows, width), full),
            pltpu.VMEM((rows, width), full),
            pltpu.VMEM((rows, rows), full),
            pltpu.VMEM((2, width, width), low),
            pltpu.VMEM((units, piece, width), low),
            dma((8,)),
            dma((2, 9, 8)),
            dma((2,)),
            dma((len(kept), blocks)),
            dma((rounds,)),
            dma((2, rounds)),
        ]
        + [pltpu.VMEM((width // piece, piece, sent.shape[2]), low)] * rounds,
        compiler_params=pltpu.CompilerParams(
            collective_id=2, has_side_effects=True, vmem_limit_bytes=60 * 1024 * 1024
        ),
        name="gather_forward",
    )(
        rank,
        owner,
        sent,
        hidden_in,
        docs[:, None],
        docs[None, :],
        bias.reshape(-1, 1, width),
        row_now.reshape(-1, 1, width),
    )


def run_general(unit_slot, masters, hidden_in, doc_ids, column_state, row_state, out_grad):
    slot_count, width, col_width = masters.shape
    units = unit_slot.shape[0]
    dp_size = lax.axis_size("dp")
    devices = dp_size * lax.axis_size("tensor")
    slots = slot_count * dp_size
    piece = width // devices
    per_layer = units // LAYERS
    blocks = (per_layer - 4) // 2
    tensor_size = lax.axis_size("tensor")
    rows = hidden_in.shape[0]
    seq_len = doc_ids.shape[1]
    heads = width // HEAD_DIM
    share = seq_len // rows
    tensor_index = lax.axis_index("tensor")
    groups = [list(range(i, i + share)) for i in range(0, tensor_size, share)]
    score_scale = HEAD_DIM ** (-0.5)
    sent = masters.astype(jnp.bfloat16).reshape(slot_count, devices, piece, col_width)
    spread = lax.all_to_all(sent.transpose(1, 0, 2, 3), BOTH, 0, 0)
    spread = spread.reshape(dp_size, tensor_size, slot_count, piece, col_width)
    spread = spread.transpose(0, 2, 3, 1, 4).reshape(slots, piece, width)
    mine = spread[unit_slot]
    weights = jnp.concatenate(
        [
            lax.all_gather(
                mine[layer * per_layer : (layer + 1) * per_layer], BOTH, axis=1, tiled=True
            )
            for layer in range(LAYERS)
        ],
        axis=0,
    )

    def matrices(layer):
        unit = weights[layer * per_layer : (layer + 1) * per_layer]
        return (unit[:3], unit[3], unit[4 : 4 + blocks], unit[4 + blocks :])

    row_docs = lax.dynamic_slice_in_dim(doc_ids, tensor_index // share, 1, axis=0)[0]
    my_docs = lax.dynamic_slice_in_dim(row_docs, (tensor_index % share) * rows, rows)
    same_doc = (my_docs[:, None] == row_docs[None, :])[None]

    def whole_row(value):
        if share == 1:
            return value
        return lax.all_gather(value, "tensor", axis=0, tiled=True, axis_index_groups=groups)

    def own_rows(value):
        if share == 1:
            return value
        return lax.psum_scatter(
            value, "tensor", scatter_dimension=0, tiled=True, axis_index_groups=groups
        )

    col_full = lax.all_gather(column_state[0], "tensor", axis=2, tiled=True)
    hidden = hidden_in.astype(jnp.float32)
    saved_layers = []
    for layer in range(LAYERS):
        w_qkv, w_proj, w_in, w_out = matrices(layer)
        row_now = row_state[0, layer]
        col_now = col_full[layer]
        hidden_bf = hidden.astype(jnp.bfloat16)
        query, key, value = (dot(hidden_bf, w_qkv[i], ((1,), (0,))) for i in range(3))
        query = ((query + col_now[0]) * score_scale).astype(jnp.bfloat16)
        key = key.astype(jnp.bfloat16)
        value = (value + col_now[1]).astype(jnp.bfloat16)
        query = query.reshape(rows, heads, HEAD_DIM)
        key = whole_row(key).reshape(seq_len, heads, HEAD_DIM)
        value = whole_row(value).reshape(seq_len, heads, HEAD_DIM)
        scores = jnp.einsum("qhd,khd->hqk", query, key, preferred_element_type=jnp.float32)
        scores = jnp.where(same_doc, scores, -1e30)
        row_top = jnp.max(scores, axis=-1, keepdims=True)
        log_total = row_top + jnp.log(
            jnp.sum(jnp.exp(scores - row_top), axis=-1, keepdims=True)
        )
        soft_bf = jnp.exp(scores - log_total).astype(jnp.bfloat16)
        context = jnp.einsum("hqk,khd->qhd", soft_bf, value, preferred_element_type=jnp.float32)
        context = context.reshape(rows, width).astype(jnp.bfloat16)
        attended = dot(context, w_proj, ((1,), (1,)))
        normed, scaled_one, inverse_one = norm_forward(
            hidden + attended + row_now[0], row_now[2], row_now[3]
        )
        normed_bf = normed.astype(jnp.bfloat16)
        pre_act = jnp.einsum("rd,bdc->brc", normed_bf, w_in, preferred_element_type=jnp.float32)
        activated, slope = gelu_pair(pre_act + col_now[2:, None])
        activated = activated.astype(jnp.bfloat16)
        slope = slope.astype(jnp.bfloat16)
        mlp_out = jnp.einsum(
            "brc,bdc->rd", activated, w_out, preferred_element_type=jnp.float32
        )
        output, scaled_two, inverse_two = norm_forward(
            normed + mlp_out + row_now[1], row_now[4], row_now[5]
        )
        saved_layers.append(
            (hidden_bf, query, key, value, log_total, context, scaled_one, inverse_one, normed_bf)
            + (slope, activated, scaled_two, inverse_two)
        )
        hidden = output
    upstream = out_grad.astype(jnp.float32)
    operands = [None] * LAYERS
    col_parts = [None] * LAYERS
    row_parts = [None] * LAYERS
    for layer in reversed(range(LAYERS)):
        w_qkv, w_proj, w_in, w_out = matrices(layer)
        row_now = row_state[0, layer]
        (
            hidden_bf,
            query,
            key,
            value,
            log_total,
            context,
            scaled_one,
            inverse_one,
            normed_bf,
            slope,
            activated,
            scaled_two,
            inverse_two,
        ) = saved_layers[layer]
        d_two, gain_two, shift_two = norm_backward(upstream, scaled_two, inverse_two, row_now[4])
        grad_bias_two = jnp.sum(d_two, axis=0)
        d_two_bf = d_two.astype(jnp.bfloat16)
        d_act = jnp.einsum("rd,bdc->brc", d_two_bf, w_out, preferred_element_type=jnp.float32)
        d_pre = (d_act * slope).astype(jnp.bfloat16)
        grad_bias_in = jnp.sum(d_pre, axis=1, dtype=jnp.float32)
        d_normed = jnp.einsum("brc,bdc->rd", d_pre, w_in, preferred_element_type=jnp.float32)
        d_normed = d_two + d_normed
        d_one, gain_one, shift_one = norm_backward(d_normed, scaled_one, inverse_one, row_now[2])
        grad_bias_proj = jnp.sum(d_one, axis=0)
        d_one_bf = d_one.astype(jnp.bfloat16)
        d_context = dot(d_one_bf, w_proj, ((1,), (0,))).astype(jnp.bfloat16)
        d_context = d_context.reshape(rows, heads, HEAD_DIM)
        scores = jnp.einsum("qhd,khd->hqk", query, key, preferred_element_type=jnp.float32)
        scores = jnp.where(same_doc, scores, -1e30)
        soft = jnp.exp(scores - log_total)
        d_values = jnp.einsum(
            "hqk,qhd->khd",
            soft.astype(jnp.bfloat16),
            d_context,
            preferred_element_type=jnp.float32,
        )
        d_probs = jnp.einsum(
            "qhd,khd->hqk", d_context, value, preferred_element_type=jnp.float32
        )
        d_scores = (
            soft * (d_probs - jnp.sum(soft * d_probs, axis=-1, keepdims=True))
        ).astype(jnp.bfloat16)
        d_queries = (
            jnp.einsum("hqk,khd->qhd", d_scores, key, preferred_element_type=jnp.float32)
            * score_scale
        )
        d_keys = jnp.einsum("hqk,qhd->khd", d_scores, query, preferred_element_type=jnp.float32)
        d_qkv = jnp.stack(
            [
                d_queries.reshape(rows, width),
                own_rows(d_keys.reshape(seq_len, width)),
                own_rows(d_values.reshape(seq_len, width)),
            ]
        ).astype(jnp.bfloat16)
        grad_bias_qkv = jnp.sum(d_qkv, axis=1, dtype=jnp.float32)
        upstream = d_one + jnp.einsum(
            "brc,bdc->rd", d_qkv, w_qkv, preferred_element_type=jnp.float32
        )
        operands[layer] = (hidden_bf, d_one_bf, normed_bf, d_two_bf)
        operands[layer] += (d_qkv, context[None], d_pre, activated)
        col_parts[layer] = jnp.concatenate(
            [
                grad_bias_qkv[0:1],
                grad_bias_qkv[2:3],
                grad_bias_in,
            ],
            axis=0,
        )
        row_parts[layer] = jnp.stack(
            [grad_bias_proj, grad_bias_two, gain_one, shift_one, gain_two, shift_two]
        )
    small = jnp.stack([jnp.stack(col_parts), jnp.stack(row_parts)])
    summed = []
    for layer in operands:
        whole = jnp.concatenate(
            [
                jnp.einsum(
                    "rd,brc->bdc", layer[i], layer[4 + i], preferred_element_type=jnp.float32
                )
                for i in range(4)
            ],
            axis=0,
        )
        summed.append(
            lax.psum_scatter(whole.astype(jnp.bfloat16), BOTH, scatter_dimension=1, tiled=True)
        )
    summed = jnp.concatenate(summed, axis=0)

    slot_ids = jnp.arange(slots, dtype=jnp.int32)
    named = unit_slot[None, :] == slot_ids[:, None]
    holds = jnp.any(named, axis=1)
    unit_of = jnp.argmax(named, axis=1)
    back = jnp.where(holds[:, None, None], summed[unit_of], jnp.zeros((), jnp.bfloat16))
    back = back.reshape(dp_size, slot_count, piece, tensor_size, col_width)
    back = back.transpose(0, 3, 1, 2, 4).reshape(devices, slot_count, piece, col_width)
    owned = lax.all_to_all(back, BOTH, 0, 0)
    owned = owned.transpose(1, 0, 2, 3)
    owned = owned.reshape(slot_count, width, col_width)
    return (hidden, upstream, owned, lax.psum(small, BOTH))


def run_kernels(unit_slot, masters, hidden_in, doc_ids, column_state, row_state, out_grad):
    slot_count, width, cols = masters.shape
    units = unit_slot.shape[0]
    per_layer = units // LAYERS
    blocks = (per_layer - 4) // 2
    dp_size = lax.axis_size("dp")
    piece = width // (dp_size * lax.axis_size("tensor"))
    dp = lax.axis_index("dp")
    owner = unit_slot // slot_count
    mates = owner[:, None] == owner[None, :]
    order = np.arange(units)
    rank = jnp.sum(mates & (order[:, None] > order[None, :]), axis=1, dtype=jnp.int32)
    feed = [4 + blocks, 4]
    made = [base + b for b in range(blocks) for base in feed] + [3, 0, 1, 2]
    made = [layer * per_layer + j for layer in reversed(range(LAYERS)) for j in made]
    turn = np.argsort(np.array(made))
    later = jnp.sum(mates & (turn[:, None] < turn[None, :]), axis=1, dtype=jnp.int32)
    back = slot_count - 1 - later
    spots = np.arange(slot_count * dp_size)
    asked = (back * dp_size + owner)[None, :] == spots[:, None]
    pick = jnp.max(jnp.where(asked, order[None, :], -1), axis=1)
    pick = jnp.where(pick < 0, made[0], pick).astype(jnp.int32)
    own_slots = dp * slot_count + jnp.arange(slot_count, dtype=jnp.int32)
    named = unit_slot[None, :] == own_slots[:, None]
    slot_rank = jnp.sum(jnp.where(named, rank[None, :], 0), axis=1)
    slot_back = jnp.sum(jnp.where(named, back[None, :], 0), axis=1)
    holds = jnp.any(named, axis=1)
    local_slot = jnp.arange(slot_count)
    first = [
        jnp.max(jnp.where(holds & (slot_rank == turn_now), local_slot, 0))
        for turn_now in range(slot_count)
    ]
    sent = jnp.stack(
        [lax.dynamic_index_in_dim(masters, i, 0, keepdims=False) for i in first]
    ).astype(jnp.bfloat16)

    docs = lax.dynamic_index_in_dim(doc_ids, lax.axis_index("tensor"), 0, keepdims=False)
    col_full = lax.all_gather(column_state[0], "tensor", axis=2, tiled=True)
    none = jnp.zeros_like(col_full[:, :1])
    bias = jnp.concatenate([col_full[:, :1], none, col_full[:, 1:]], axis=1)
    weights, hidden, *saved = forward(
        rank, owner, sent, hidden_in, docs, bias, row_state[0], piece
    )
    upstream, owned, small = backward(
        pick, out_grad, docs, row_state[0], weights, saved, piece, cols
    )
    owned = owned.reshape(slot_count, width, cols)
    owned = jnp.stack(
        [
            lax.dynamic_index_in_dim(owned, slot_back[i], 0, keepdims=False)
            for i in range(slot_count)
        ]
    )
    owned = jnp.where(holds[:, None, None], owned, jnp.zeros((), owned.dtype))
    return (hidden, upstream, owned, small.reshape(2, LAYERS, 2 + blocks, width))


def local(
    hidden_in,
    doc_ids,
    unit_slot,
    masters,
    first_moment,
    second_moment,
    column_state,
    row_state,
    out_grad,
):
    slot_count, width, col_width = masters.shape
    dp_size = lax.axis_size("dp")
    tensor_size = lax.axis_size("tensor")
    slots = slot_count * dp_size
    tensor_index = lax.axis_index("tensor")
    kernels = dp_size == 8 and tensor_size == 4 and hidden_in.shape[0] == doc_ids.shape[1]

    run = run_kernels if kernels else run_general
    hidden, upstream, owned, small = run(
        unit_slot, masters, hidden_in, doc_ids, column_state, row_state, out_grad
    )
    owned = owned.astype(jnp.float32)
    slot_ids = jnp.arange(slots, dtype=jnp.int32)
    holds = jnp.any(unit_slot[None, :] == slot_ids[:, None], axis=1)
    row_total = small[1]
    col_total = lax.dynamic_slice_in_dim(small[0], tensor_index * col_width, col_width, axis=2)

    occupied = lax.dynamic_slice_in_dim(holds, lax.axis_index("dp") * slot_count, slot_count)
    occupied = occupied.astype(jnp.float32)[:, None, None]
    new_master, new_first, new_second = adamw_update(
        masters, owned, first_moment, second_moment, RATE_UNITS
    )
    unit_master = new_master * occupied
    unit_state = jnp.stack([new_first * occupied, new_second * occupied])
    new_col, col_first, col_second = adamw_update(
        column_state[0], col_total, column_state[1], column_state[2], RATE_SMALL
    )
    column_out = jnp.stack([col_total, new_col, col_first, col_second])
    new_row, row_first, row_second = adamw_update(
        row_state[0], row_total, row_state[1], row_state[2], RATE_SMALL
    )
    row_out = jnp.stack([row_total, new_row, row_first, row_second])
    return (hidden, upstream, unit_master, unit_state, column_out, row_out)


def solution(mesh):
    return jax.shard_map(
        local,
        mesh=mesh,
        in_specs=(
            P(("dp", "tensor"), None),
            P("dp", None),
            P(),
            P("dp", None, "tensor"),
            P("dp", None, "tensor"),
            P("dp", None, "tensor"),
            P(None, None, None, "tensor"),
            P(),
            P(("dp", "tensor"), None),
        ),
        out_specs=(
            P(("dp", "tensor"), None),
            P(("dp", "tensor"), None),
            P("dp", None, "tensor"),
            P(None, "dp", None, "tensor"),
            P(None, None, None, "tensor"),
            P(),
        ),
        check_vma=False,
    )
```

```python
import math

import jax
import jax.numpy as jnp
from jax import lax
from jax.experimental import pallas as pl
from jax.experimental.pallas import tpu as pltpu
from jax.sharding import PartitionSpec as P
import numpy as np

HEAD_DIM = 64
LAYERS = 2
STEP = 3

EPS_NORM = 1e-06
RATE_UNITS = 0.05
RATE_SMALL = 0.2
WEIGHT_DECAY = 0.01
ADAM_EPS = 1e-08
BETA_MOMENT = 0.5
BOTH = ("dp", "tensor")


def norm_forward(summed, gain, shift):
    row_mean = jnp.mean(summed, axis=1, keepdims=True)
    centred = summed - row_mean
    inverse = lax.rsqrt(jnp.mean(centred * centred, axis=1, keepdims=True) + EPS_NORM)
    scaled = centred * inverse
    return (scaled * gain + shift, scaled, inverse)


def norm_backward(upstream, scaled, inverse, gain):
    d_scaled = upstream * gain
    mean_one = jnp.mean(d_scaled, axis=1, keepdims=True)
    mean_two = jnp.mean(d_scaled * scaled, axis=1, keepdims=True)
    grad_input = inverse * (d_scaled - mean_one - scaled * mean_two)
    return (grad_input, jnp.sum(upstream * scaled, axis=0), jnp.sum(upstream, axis=0))


def gelu_pair(v):
    cdf = 0.5 * (1.0 + lax.erf(v * 2.0 ** (-0.5)))
    bell = jnp.exp(-0.5 * v * v) * (2.0 * math.pi) ** (-0.5)
    return (v * cdf, cdf + v * bell)


def adamw_update(old_value, gradient, first_old, second_old, learn_rate):
    first_new = BETA_MOMENT * first_old + (1.0 - BETA_MOMENT) * gradient
    second_new = BETA_MOMENT * second_old + (1.0 - BETA_MOMENT) * gradient * gradient
    correct = 1.0 - BETA_MOMENT**STEP
    step_size = first_new / correct / (jnp.sqrt(second_new / correct) + ADAM_EPS)
    return (old_value - learn_rate * (step_size + WEIGHT_DECAY * old_value), first_new, second_new)


def dot(left, right, dims):
    return lax.dot_general(left, right, (dims, ((), ())), preferred_element_type=jnp.float32)


LANES = 2 * HEAD_DIM


def head_lanes(value, head):
    lane = lax.broadcasted_iota(jnp.int32, value.shape, 1)
    keep = lane < HEAD_DIM if head == 0 else lane >= HEAD_DIM
    return jnp.where(keep, value, jnp.zeros_like(value))


def pair_lanes(first, second):
    lane = lax.broadcasted_iota(jnp.int32, first.shape, 1)
    return jnp.where(lane < HEAD_DIM, first, second)


def attend_pair(pair, q_ref, k_ref, v_ref, mask_ref, ctx_ref, lse_ref):
    lanes = pl.ds(pl.multiple_of(pair * LANES, LANES), LANES)
    query, key, value = q_ref[:, lanes], k_ref[:, lanes], v_ref[:, lanes]
    value_t = value.T
    parts = []
    for head in range(2):
        scores = dot(head_lanes(key, head), query, ((1,), (1,))) + mask_ref[...]
        top = jnp.max(scores, axis=0, keepdims=True)
        weight = jnp.exp(scores - top)
        total = jnp.sum(weight, axis=0, keepdims=True)
        lse_ref[pair * 2 + head] = top + jnp.log(total)
        mine = value_t[head * HEAD_DIM : (head + 1) * HEAD_DIM]
        mixed = dot(mine, weight.astype(jnp.bfloat16), ((1,), (0,)))
        parts.append(mixed * (1.0 / total))
    ctx_ref[:, lanes] = jnp.concatenate(parts, axis=0).T.astype(ctx_ref.dtype)


def attend_back_pair(pair, q_ref, k_ref, v_ref, d_ref, mask_ref, lse_ref, dq_ref, dk_ref, dv_ref):
    lanes = pl.ds(pl.multiple_of(pair * LANES, LANES), LANES)
    query, key, value = q_ref[:, lanes], k_ref[:, lanes], v_ref[:, lanes]
    grad = d_ref[:, lanes]
    key_t = key.T
    parts, d_keys, d_values = [], [], []
    for head in range(2):
        scores = dot(head_lanes(key, head), query, ((1,), (1,))) + mask_ref[...]
        soft = jnp.exp(scores - lse_ref[pair * 2 + head])
        d_values.append(dot(soft.astype(jnp.bfloat16), grad, ((1,), (0,))))
        d_soft = dot(head_lanes(value, head), grad, ((1,), (1,)))
        both = soft * d_soft
        mean = jnp.sum(both, axis=0, keepdims=True)
        d_scores = (both - soft * mean).astype(jnp.bfloat16)
        d_keys.append(dot(d_scores, query, ((1,), (0,))))
        mine = key_t[head * HEAD_DIM : (head + 1) * HEAD_DIM]
        parts.append(dot(mine, d_scores, ((1,), (0,))))
    scale = HEAD_DIM ** (-0.5)
    dq_ref[:, lanes] = (jnp.concatenate(parts, axis=0).T * scale).astype(dq_ref.dtype)
    dk_ref[:, lanes] = pair_lanes(*d_keys).astype(dk_ref.dtype)
    dv_ref[:, lanes] = pair_lanes(*d_values).astype(dv_ref.dtype)


def fill_mask(mask_ref, docs_col_ref, docs_row_ref):
    same = docs_col_ref[...] == docs_row_ref[...]
    mask_ref[...] = jnp.where(same, 0.0, -1e30).astype(jnp.float32)


LAG = 2


def spread_order(z, y, x, c):
    return ((c * 2 + x) * 2 + y) * 4 + z


def every_other(z, y, x, c, body):
    for step in (2, 1, 3, 0):

        def one(i, carry, step=step):
            body((z + step) % 4, (y + i // 4) % 2, (x + (i // 2) % 2) % 2, (c + i % 2) % 2)
            return carry

        lax.fori_loop(1 if step == 0 else 0, 8, one, 0)


def greet_all(z, y, x, c):
    barrier = pltpu.get_barrier_semaphore()

    def greet(zz, yy, xx, cc):
        pl.semaphore_signal(
            barrier,
            inc=1,
            device_id=(zz * 2 + yy, xx * 2 + cc),
            device_id_type=pl.DeviceIdType.MESH,
        )

    every_other(z, y, x, c, greet)
    return barrier


TILE = 256


def norm_back_rows(upstream, scaled, inverse, gain):
    d_scaled = upstream * gain
    mean_one = jnp.mean(d_scaled, axis=1, keepdims=True)
    mean_two = jnp.mean(d_scaled * scaled, axis=1, keepdims=True)
    return inverse * (d_scaled - mean_one - scaled * mean_two)


def backward_kernel(
    pick_ref,
    out_grad_ref,
    docs_col_ref,
    docs_row_ref,
    row_ref,
    weights_ref,
    low_ref,
    mixed_ref,
    ctx_ref,
    lse_ref,
    one_ref,
    inv_one_ref,
    normed_ref,
    act_ref,
    slope_ref,
    two_ref,
    inv_two_ref,
    owned_ref,
    total_ref,
    small_out,
    out_ref,
    back_buf,
    left_buf,
    right_buf,
    unit_buf,
    scaled_buf,
    inv_buf,
    slope_buf,
    mixed_buf,
    lse_buf,
    mask_buf,
    d_ctx_buf,
    core_out,
    core_in,
    sum_core,
    first_in,
    sum_first,
    second_in,
    sum_second,
    z_in,
    small_sum,
    small_got,
    load_sem,
    core_sems,
    first_sems,
    second_sems,
    z_sems,
    small_sems,
    own_sems,
    round_sems,
):
    units, piece, width = out_ref.shape
    rows = total_ref.shape[0]
    per_layer = units // LAYERS
    blocks = (per_layer - 4) // 2
    at_out, at_query = 2 * blocks, 2 * blocks + 1
    dp, tensor = lax.axis_index("dp"), lax.axis_index("tensor")
    z, y, x, c = dp // 2, dp % 2, tensor // 2, tensor % 2
    half, parts = width // 2, 2
    side_cols = half // 2
    quarter, eighth = half // 2, half // 4
    to_core = (dp, x * 2 + 1 - c)
    to_x = (dp, (1 - x) * 2 + c)
    to_y = (z * 2 + 1 - y, tensor)
    to_z = [(((z + k) % 4) * 2 + y, tensor) for k in (1, 2, 3)]
    to_z1 = ((z + 1 - 2 * (z % 2)) * 2 + y, tensor)
    to_z2 = (((z + 2) % 4) * 2 + y, tensor)
    mesh_id = pl.DeviceIdType.MESH

    barrier = greet_all(z, y, x, c)

    def remote(src, dst, sems, send, recv, peer):
        return pltpu.make_async_remote_copy(
            src_ref=src,
            dst_ref=dst,
            send_sem=sems.at[send],
            recv_sem=sems.at[recv],
            device_id=peer,
            device_id_type=mesh_id,
        )

    def place(s):
        return LAYERS - 1 - s // per_layer, s % per_layer

    def unit_of(s):
        layer, j = place(s)
        feed = jnp.where(j % 2 == 0, 4 + blocks + j // 2, 4 + j // 2)
        return layer * per_layer + jnp.where(
            j < at_out, feed, jnp.where(j == at_out, 3, j - at_query)
        )

    def left_of(s):
        j = s % per_layer
        feed = jnp.where(j % 2 == 0, 3, 2)
        return jnp.where(j < at_out, feed, jnp.where(j == at_out, 1, 0))

    def loaded_slot(s):
        return ((s // per_layer) * (blocks + 1) + (s % per_layer) // 2) % 2

    def right_of(s):
        j = s % per_layer
        feed = jnp.where(j % 2 == 0, loaded_slot(s), 2 + (j // 2) % 2)
        return jnp.where(
            j < at_out, feed, jnp.where(j == at_out, loaded_slot(s), 4 + j - at_query)
        )

    local = pltpu.make_async_copy

    def unit_load(s):
        return local(weights_ref.at[unit_of(s)], unit_buf.at[s % 3], load_sem.at[0, s % 3])

    def act_load(layer, block, slot):
        return local(act_ref.at[layer, block], right_buf.at[slot], load_sem.at[1, slot])

    def ctx_load(layer, slot):
        return local(ctx_ref.at[layer], right_buf.at[slot], load_sem.at[1, slot])

    def slope_load(layer, block):
        return local(slope_ref.at[layer, block], slope_buf, load_sem.at[2, 0])

    def norm_loads(layer, which):
        scaled, inv = ((one_ref, inv_one_ref), (two_ref, inv_two_ref))[which]
        return [
            local(scaled.at[layer], scaled_buf, load_sem.at[3, 0]),
            local(inv.at[layer], inv_buf, load_sem.at[3, 1]),
        ]

    def mixed_loads(layer):
        return [
            local(mixed_ref.at[layer], mixed_buf, load_sem.at[4, 0]),
            local(lse_ref.at[layer], lse_buf, load_sem.at[4, 1]),
        ]

    def normed_load(layer):
        return local(normed_ref.at[layer], left_buf.at[2], load_sem.at[2, 1])

    def low_load(layer):
        return local(low_ref.at[layer], left_buf.at[0], load_sem.at[5, 0])

    def begin(*copies):
        for copy in copies:
            copy.start()

    def finish(*copies):
        for copy in copies:
            copy.wait()

    def note(row, value):
        small_sum[0, pl.ds(row, 1), :] = value

    def column(layer, i):
        return layer * (2 + blocks) + i

    def row(layer, i):
        return LAYERS * (2 + blocks) + layer * 6 + i

    def norm_back(layer, gain_row, bias_row, low_slot):
        gain = row_ref[0, layer, gain_row : gain_row + 1, :]
        size = 128

        def one(tile, carry):
            part = pl.ds(pl.multiple_of(tile * size, size), size)
            upstream = total_ref[part, :]
            scaled = scaled_buf[part, :]
            inside = norm_back_rows(upstream, scaled, inv_buf[part, 0:1], gain)
            total_ref[part, :] = inside
            left_buf[low_slot, part, :] = inside.astype(jnp.bfloat16)
            sums = (upstream * scaled, upstream, inside)
            return tuple(a + jnp.sum(b, axis=0, keepdims=True) for a, b in zip(carry, sums))

        zero = jnp.zeros((1, width), jnp.float32)
        gains, shifts, biases = lax.fori_loop(0, rows // size, one, (zero, zero, zero))
        note(row(layer, gain_row), gains)
        note(row(layer, gain_row + 1), shifts)
        note(row(layer, bias_row), biases)

    def heads(start, stop):
        inputs = [mixed_buf.at[i] for i in range(3)]
        grads = [right_buf.at[4 + i] for i in range(3)]

        def one(pair, carry):
            attend_back_pair(pair, *inputs, d_ctx_buf, mask_buf, lse_buf, *grads)
            return carry

        lax.fori_loop(start, stop, one, 0)

    pairs = width // LANES

    def data_gradient(s):
        layer, j = place(s)
        matrix = unit_buf.at[s % 3]
        before = unit_buf.at[(s + 2) % 3]
        slot = loaded_slot(s)

        @pl.when(j == 0)
        def _():
            finish(*norm_loads(layer, 1))

            @pl.when(s == 0)
            def _():
                total_ref[...] = out_grad_ref[...].astype(jnp.float32)

            norm_back(layer, 4, 1, 3)
            begin(*norm_loads(layer, 0), *mixed_loads(layer))

        @pl.when(j == 1)
        def _():
            finish(normed_load(layer))
            begin(low_load(layer))

        @pl.when((j < at_out) & (j % 2 == 0))
        def _():
            block = j // 2
            finish(slope_load(layer, block), act_load(layer, block, slot))

            @pl.when(block < blocks - 1)
            def _():
                act_load(layer, block + 1, 1 - slot).start()

            @pl.when(block == blocks - 1)
            def _():
                ctx_load(layer, 1 - slot).start()

            d_act = dot(left_buf[3], matrix[...], ((1,), (0,)))
            d_pre = (d_act * slope_buf[...].astype(jnp.float32)).astype(jnp.bfloat16)
            right_buf[2 + block % 2] = d_pre
            sums = jnp.sum(d_pre.astype(jnp.float32), axis=0, keepdims=True)
            note(column(layer, 2 + block), sums)

            @pl.when(block < blocks - 1)
            def _():
                slope_load(layer, block + 1).start()

        @pl.when((j < at_out) & (j % 2 == 1))
        def _():
            total_ref[...] += dot(right_buf[2 + (j // 2) % 2], matrix[...], ((1,), (1,)))

        @pl.when(j == at_out)
        def _():
            finish(*norm_loads(layer, 0), *mixed_loads(layer), ctx_load(layer, slot))
            norm_back(layer, 2, 0, 1)

            @pl.when(layer > 0)
            def _():
                act_load(layer - 1, 0, 1 - slot).start()
                begin(*norm_loads(layer - 1, 1))
                slope_load(layer - 1, 0).start()

            d_ctx_buf[...] = dot(left_buf[1], matrix[...], ((1,), (0,))).astype(jnp.bfloat16)

        @pl.when(j == at_query)
        def _():
            finish(low_load(layer))

            @pl.when(layer > 0)
            def _():
                normed_load(layer - 1).start()

            heads(3 * pairs // 8, 5 * pairs // 8)

        @pl.when(j == at_query + 1)
        def _():
            total_ref[...] += dot(right_buf[4], before[...], ((1,), (1,)))

        @pl.when(j == at_query + 2)
        def _():
            total_ref[...] += dot(right_buf[6], matrix[...], ((1,), (1,)))

    def data_gradient_rest(s):
        layer, j = place(s)

        @pl.when(j == at_out)
        def _():
            heads(0, 3 * pairs // 8)

        @pl.when(j == at_query)
        def _():
            heads(5 * pairs // 8, pairs)

        @pl.when(j == at_query + 1)
        def _():
            total_ref[...] += dot(right_buf[5], unit_buf[s % 3], ((1,), (1,)))
            for i, number in ((0, 0), (2, 1)):
                sums = jnp.sum(right_buf[4 + i].astype(jnp.float32), axis=0, keepdims=True)
                note(column(layer, number), sums)

    def product(s, side, tile):
        unit = s // parts
        start = pl.multiple_of(side * half + tile * TILE, TILE)
        left = left_buf[left_of(unit), :, pl.ds(start, TILE)]
        right = right_buf[
            right_of(unit), :, pl.ds(pl.multiple_of((s % parts) * half, half), half)
        ]
        return lax.dot_general(
            left, right, (((0,), (0,)), ((), ())), preferred_element_type=jnp.float32
        )

    def core_copy(s):
        return remote(
            core_out.at[s % 2], core_in.at[s % 4], core_sems, (0, s % 2), (1, s % 4), to_core
        )

    def first_copies(s):
        here = sum_core.at[s % 3]
        return (
            remote(
                here.at[pl.ds(pl.multiple_of((1 - x) * quarter, quarter), quarter), pl.ds(0, side_cols)],
                first_in.at[s % 4, 0],
                first_sems,
                (0, 0, s % 3),
                (1, 0, s % 4),
                to_x,
            ),
            *(
                remote(
                    here.at[
                        pl.ds(pl.multiple_of(i * quarter + (1 - y) * eighth, eighth), eighth),
                        pl.ds(side_cols, side_cols),
                    ],
                    first_in.at[s % 4, 1, pl.ds(i * eighth, eighth)],
                    first_sems,
                    (0, 1 + i, s % 3),
                    (1, 1 + i, s % 4),
                    to_y,
                )
                for i in range(2)
            ),
        )

    def second_copies(s):
        here = sum_first.at[s % 3]
        return (
            remote(
                here.at[0, pl.ds(pl.multiple_of((1 - y) * eighth, eighth), eighth)],
                second_in.at[s % 4, 0],
                second_sems,
                (0, 0, s % 3),
                (1, 0, s % 4),
                to_y,
            ),
            remote(
                here.at[1, pl.ds(pl.multiple_of((1 - x) * eighth, eighth), eighth)],
                second_in.at[s % 4, 1],
                second_sems,
                (0, 1, s % 3),
                (1, 1, s % 4),
                to_x,
            ),
        )

    def z_copies(s):
        return [
            remote(
                sum_second.at[s % 3, pl.ds(pl.multiple_of(((z + k) % 4) * piece, piece), piece)],
                z_in.at[s % 4, k - 1],
                z_sems,
                (0, k - 1, s % 3),
                (1, k - 1, s % 4),
                to_z[k - 1],
            )
            for k in (1, 2, 3)
        ]

    small_peers = (to_core, to_x, to_y, to_z1, to_z2)

    def small_copy(stage):
        return remote(
            small_sum.at[stage],
            small_got.at[stage],
            small_sems,
            (0, stage),
            (1, stage),
            small_peers[stage],
        )

    rounds, owners = back_buf.shape[0], back_buf.shape[1]
    cols = owned_ref.shape[3]
    me = spread_order(z, y, x, c)

    def own_back(number):
        return local(
            back_buf.at[number, dp, :, pl.ds(pl.multiple_of(tensor * cols, cols), cols)],
            owned_ref.at[number, me],
            own_sems.at[number],
        )

    def send_back(number):
        def fill(owner, carry):
            back_buf[number, owner] = out_ref[pick_ref[number * owners + owner]]
            return carry

        lax.fori_loop(0, owners, fill, 0)
        own_back(number).start()

        def send(zz, yy, xx, cc):
            there = xx * 2 + cc
            remote(
                back_buf.at[
                    number, zz * 2 + yy, :, pl.ds(pl.multiple_of(there * cols, cols), cols)
                ],
                owned_ref.at[number, me],
                round_sems,
                (0, number),
                (1, number),
                (zz * 2 + yy, there),
            ).start()

        every_other(z, y, x, c, send)

    def finish_back(number):
        own_back(number).wait()
        most = owned_ref.at[number, pl.ds(0, 31)]
        remote(most, most, round_sems, (0, number), (1, number), to_core).wait()

    top = LAYERS - 1
    steps = parts * units
    begin(
        *norm_loads(top, 1),
        unit_load(jnp.int32(0)),
        slope_load(top, 0),
        act_load(top, 0, 0),
        normed_load(top),
    )
    fill_mask(mask_buf, docs_col_ref, docs_row_ref)
    pl.semaphore_wait(barrier, 31)

    def step(s, carry):
        last = s - 3 * LAG - 1

        @pl.when((last >= 0) & (last < steps))
        def _():
            for copy in z_copies(last):
                copy.wait()
            total = sum_second[last % 3, pl.ds(pl.multiple_of(z * piece, piece), piece), :].astype(
                jnp.float32
            )
            for k in range(3):
                total = total + z_in[last % 4, k].astype(jnp.float32)
            cols_now = pl.ds(pl.multiple_of((last % parts) * half, half), half)
            out_ref[unit_of(last // parts), :, cols_now] = total.astype(out_ref.dtype)

            @pl.when((last // parts >= units - rounds) & (last % parts == parts - 1))
            def _():
                send_back(last // parts - (units - rounds))

        third = s - 2 * LAG - 1

        @pl.when((third >= 0) & (third < steps))
        def _():
            for copy in second_copies(third):
                copy.wait()
            for part, side in ((0, y), (1, x)):
                mine = sum_first[
                    third % 3, part, pl.ds(pl.multiple_of(side * eighth, eighth), eighth), :
                ]
                total = mine.astype(jnp.float32) + second_in[third % 4, part].astype(jnp.float32)
                sum_second[third % 3, :, part * side_cols : (part + 1) * side_cols] = total.astype(
                    jnp.bfloat16
                )
            for copy in z_copies(third):
                copy.start()

        second = s - LAG - 1

        @pl.when((second >= 0) & (second < steps))
        def _():
            for copy in first_copies(second):
                copy.wait()
            mine = sum_core[
                second % 3, pl.ds(pl.multiple_of(x * quarter, quarter), quarter), 0:side_cols
            ]
            total = mine.astype(jnp.float32) + first_in[second % 4, 0].astype(jnp.float32)
            sum_first[second % 3, 0] = total.astype(jnp.bfloat16)
            for i in range(2):
                mine = sum_core[
                    second % 3,
                    pl.ds(pl.multiple_of(i * quarter + y * eighth, eighth), eighth),
                    side_cols : 2 * side_cols,
                ]
                part = pl.ds(i * eighth, eighth)
                total = mine.astype(jnp.float32) + first_in[second % 4, 1, part, :].astype(
                    jnp.float32
                )
                sum_first[second % 3, 1, part, :] = total.astype(jnp.bfloat16)
            for copy in second_copies(second):
                copy.start()

        @pl.when(s < steps)
        def _():
            unit = s // parts

            @pl.when(s % parts == 0)
            def _():
                unit_load(unit).wait()

                @pl.when(unit + 1 < units)
                def _():
                    unit_load(unit + 1).start()

                data_gradient(unit)

            @pl.when(s % parts == 1)
            def _():
                data_gradient_rest(unit)

            @pl.when(s >= 2)
            def _():
                core_copy(s - 2).wait_send()

            def one(tile, carry):
                part = pl.ds(pl.multiple_of(tile * TILE, TILE), TILE)
                core_out[s % 2, part, :] = product(s, 1 - c, tile).astype(jnp.bfloat16)
                return carry

            lax.fori_loop(0, half // TILE, one, 0)
            core_copy(s).start()

        first = s - 1

        @pl.when((first >= 0) & (first < steps))
        def _():
            core_copy(first).wait_recv()

            def one(tile, carry):
                part = pl.ds(pl.multiple_of(tile * TILE, TILE), TILE)
                total = product(first, c, tile) + core_in[first % 4, part, :].astype(jnp.float32)
                sum_core[first % 3, part, :] = total.astype(jnp.bfloat16)
                return carry

            lax.fori_loop(0, half // TILE, one, 0)
            for copy in first_copies(first):
                copy.start()

        for stage in range(6):

            @pl.when(s == steps + stage)
            def _(stage=stage):
                if stage > 0:
                    small_copy(stage - 1).wait()
                    total = small_sum[stage - 1] + small_got[stage - 1]
                    if stage < 5:
                        small_sum[stage] = total
                    else:
                        small_out[...] = total
                if stage < 5:
                    small_copy(stage).start()

        return carry

    lax.fori_loop(0, steps + 3 * LAG + 1, step, 0)
    for s in (steps - 2, steps - 1):
        core_copy(s).wait_send()
    for number in range(rounds):
        finish_back(number)


def backward(pick, out_grad, docs, row_state, weights, saved, piece, cols):
    units, width, _ = weights.shape
    rows = out_grad.shape[0]
    blocks = (units // LAYERS - 4) // 2
    half = width // 2
    low, full = jnp.bfloat16, jnp.float32
    rounds = pick.shape[0] // 8
    small = (LAYERS * (8 + blocks), width)
    any_spec = pl.BlockSpec(memory_space=pl.ANY)
    vmem_spec = pl.BlockSpec(memory_space=pltpu.VMEM)
    dma = pltpu.SemaphoreType.DMA
    summed, total, small = pl.pallas_call(
        backward_kernel,
        out_shape=(
            jax.ShapeDtypeStruct((rounds, width // piece, piece, cols), low),
            jax.ShapeDtypeStruct((rows, width), full),
            jax.ShapeDtypeStruct(small, full),
        ),
        in_specs=[pl.BlockSpec(memory_space=pltpu.SMEM)] + [vmem_spec] * 4 + [any_spec] * (1 + len(saved)),
        out_specs=(vmem_spec, vmem_spec, vmem_spec),
        scratch_shapes=[
            pltpu.VMEM((units, piece, width), low),
            pltpu.VMEM((rounds, 8, piece, width), low),
            pltpu.VMEM((4, rows, width), low),
            pltpu.VMEM((7, rows, width), low),
            pltpu.VMEM((3, width, width), low),
            pltpu.VMEM((rows, width), full),
            pltpu.VMEM((rows, 128), full),
            pltpu.VMEM((rows, width), low),
            pltpu.VMEM((3, rows, width), low),
            pltpu.VMEM((width // HEAD_DIM, 1, rows), full),
            pltpu.VMEM((rows, rows), full),
            pltpu.VMEM((rows, width), low),
            pltpu.VMEM((2, half, half), low),
            pltpu.VMEM((4, half, half), low),
            pltpu.VMEM((3, half, half), low),
            pltpu.VMEM((4, 2, half // 2, half // 2), low),
            pltpu.VMEM((3, 2, half // 2, half // 2), low),
            pltpu.VMEM((4, 2, half // 4, half // 2), low),
            pltpu.VMEM((3, half // 4, half), low),
            pltpu.VMEM((4, 3, piece, half), low),
            pltpu.VMEM((5,) + small, full),
            pltpu.VMEM((5,) + small, full),
            dma((6, 3)),
            dma((2, 4)),
            dma((2, 3, 4)),
            dma((2, 2, 4)),
            dma((2, 3, 4)),
            dma((2, 5)),
            dma((rounds,)),
            dma((2, rounds)),
        ],
        compiler_params=pltpu.CompilerParams(
            collective_id=1, has_side_effects=True, vmem_limit_bytes=63 * 1024 * 1024
        ),
        name="backward_reduce",
    )(pick, out_grad, docs[:, None], docs[None, :], row_state, weights, *saved)
    return (total, summed, small)


def norm_rows(value, gain, shift):
    centred = value - jnp.mean(value, axis=1, keepdims=True)
    inverse = lax.rsqrt(jnp.mean(centred * centred, axis=1, keepdims=True) + EPS_NORM)
    scaled = centred * inverse
    return (scaled * gain + shift, scaled, inverse)


NORM_ROWS = 128


def forward_kernel(
    rank_ref,
    owner_ref,
    first_ref,
    masters_ref,
    hidden_ref,
    docs_col_ref,
    docs_row_ref,
    col_ref,
    row_ref,
    out_ref,
    final_ref,
    *refs,
):
    saved, bufs = refs[:11], refs[11:22]
    rounds = masters_ref.shape[0]
    (x_buf, normed_buf, total_buf, mask_buf, unit_buf, own_ref) = refs[22:28]
    (own_sem, sems, unit_sem, save_sem, got_sem, round_sems) = refs[28:34]
    (masters_buf, sent_ref, col_got, bias_buf, master_sem, col_sems) = refs[34:40]
    got = refs[40:]
    (low_buf, mixed_buf, ctx_buf, lse_buf, one_buf, inv_one_buf, nb_buf) = bufs[:7]
    (act_buf, slope_buf, two_buf, inv_two_buf) = bufs[7:]
    units, piece, width = own_ref.shape
    rows = hidden_ref.shape[0]
    per_layer = units // LAYERS
    blocks = (per_layer - 4) // 2
    dp, tensor = lax.axis_index("dp"), lax.axis_index("tensor")
    z, y, x, c = dp // 2, dp % 2, tensor // 2, tensor % 2
    half = width // 2
    line, plane = 4 * piece, 8 * piece
    to_core = (dp, x * 2 + 1 - c)
    to_x = (dp, (1 - x) * 2 + c)
    to_y = (z * 2 + 1 - y, tensor)
    to_z = [(((z + k) % 4) * 2 + y, tensor) for k in (1, 2, 3)]
    mesh_id = pl.DeviceIdType.MESH

    barrier = greet_all(z, y, x, c)
    masters_in = [
        pltpu.make_async_copy(masters_ref.at[i], masters_buf.at[i], master_sem.at[i])
        for i in range(rounds)
    ]
    for copy in masters_in:
        copy.start()
    cols = sent_ref.shape[2]
    me = dp * 4 + tensor

    def part_for(number, zz, yy, xx, cc):
        start = pl.multiple_of(spread_order(zz, yy, xx, cc) * piece, piece)
        return sent_ref.at[number, pl.ds(start, piece)]

    def keep(number):
        return pltpu.make_async_copy(
            part_for(number, z, y, x, c), got[number].at[me], got_sem.at[number]
        )

    def round_copy(number, src, dst, peer):
        return pltpu.make_async_remote_copy(
            src_ref=src,
            dst_ref=dst,
            send_sem=round_sems.at[0, number],
            recv_sem=round_sems.at[1, number],
            device_id=peer,
            device_id_type=mesh_id,
        )

    def start_round(number):
        keep(number).start()

        def send(zz, yy, xx, cc):
            src = part_for(number, zz, yy, xx, cc)
            round_copy(number, src, got[number].at[me], (zz * 2 + yy, xx * 2 + cc)).start()

        every_other(z, y, x, c, send)

    def finish_round(number):
        keep(number).wait()
        most = got[number].at[pl.ds(0, 31)]
        round_copy(number, most, most, to_core).wait()

    def pick(unit, there):
        rank, owner = rank_ref[unit], owner_ref[unit]
        for j in range(4):
            value = got[0][owner * 4 + j]
            for number in range(1, there):
                value = jnp.where(rank == number, got[number][owner * 4 + j], value)
            own_ref[unit, :, j * cols : (j + 1) * cols] = value

    def column_copies():
        return [
            pltpu.make_async_remote_copy(
                src_ref=col_ref,
                dst_ref=col_got.at[tensor],
                send_sem=col_sems.at[0, k],
                recv_sem=col_sems.at[1, k],
                device_id=(dp, (tensor + k + 1) % 4),
                device_id_type=mesh_id,
            )
            for k in range(3)
        ]

    for copy in masters_in:
        copy.wait()
    sent_ref[0] = masters_buf[first_ref[0]].astype(sent_ref.dtype)
    pl.semaphore_wait(barrier, 31)
    start_round(0)
    for number in range(1, rounds):
        sent_ref[number] = masters_buf[first_ref[number]].astype(sent_ref.dtype)
    start_round(1)
    col_got[tensor] = col_ref[...]
    for copy in column_copies():
        copy.start()

    my_line = pl.multiple_of(((c * 2 + x) * 2 + y) * line, line)
    my_rows = pl.ds(pl.multiple_of(my_line + z * piece, piece), piece)
    parts, cycle = 2, sems.shape[2]

    def half_of(s):
        return pl.ds(pl.multiple_of((s % parts) * half, half), half)

    def first(s):
        return pl.ds(pl.multiple_of((s % parts) * half, half), half // 2)

    def second(s):
        return pl.ds(pl.multiple_of((s % parts) * half + half // 2, half // 2), half // 2)

    def remote(src, dst, index, s, peer):
        return pltpu.make_async_remote_copy(
            src_ref=src,
            dst_ref=dst,
            send_sem=sems.at[0, index, s % cycle],
            recv_sem=sems.at[1, index, s % cycle],
            device_id=peer,
            device_id_type=mesh_id,
        )

    def own_copy(s):
        unit, cols_now = s // parts, half_of(s)
        return pltpu.make_async_copy(
            own_ref.at[unit, :, cols_now],
            out_ref.at[unit, my_rows, cols_now],
            own_sem.at[s % cycle],
        )

    def stage_z(s):
        unit, cols_now = s // parts, half_of(s)
        here, there = own_ref.at[unit, :, cols_now], out_ref.at[unit, my_rows, cols_now]
        return [remote(here, there, k, s, to_z[k]) for k in range(3)]

    def stage_one(s):
        unit, rows = s // parts, pl.ds(my_line, line)
        one, two = out_ref.at[unit, rows, first(s)], out_ref.at[unit, rows, second(s)]
        return [remote(one, one, 3, s, to_y), remote(two, two, 4, s, to_x)]

    def stage_two(s):
        unit = s // parts
        rows = pl.ds(pl.multiple_of((c * 2 + x) * plane, plane), plane)
        one = out_ref.at[unit, rows, first(s)]
        copies = [remote(one, one, 5, s, to_x)]
        for i in range(2):
            rows = pl.ds(pl.multiple_of(((c * 2 + i) * 2 + y) * line, line), line)
            two = out_ref.at[unit, rows, second(s)]
            copies.append(remote(two, two, 6 + i, s, to_y))
        return copies

    def stage_core(s):
        rows = pl.ds(pl.multiple_of(c * 2 * plane, 2 * plane), 2 * plane)
        there = out_ref.at[s // parts, rows, half_of(s)]
        return [remote(there, there, 8, s, to_core)]

    stages = (stage_z, stage_one, stage_two, stage_core)

    def unit_copy(unit):
        slot = unit % 2
        return pltpu.make_async_copy(out_ref.at[unit], unit_buf.at[slot], unit_sem.at[slot])

    def save(number, layer, block=None):
        src, dst, sem = bufs[number], saved[number].at[layer], save_sem.at[number, 0]
        if block is not None:
            src, dst, sem = src.at[block], dst.at[block], save_sem.at[number, block]
        return pltpu.make_async_copy(src, dst, sem)

    def free(numbers, layer, block=None):
        @pl.when(layer > 0)
        def _():
            for number in numbers:
                save(number, layer - 1, block).wait()

    def heads(start, stop):
        def one(pair, carry):
            attend_pair(
                pair, mixed_buf.at[0], mixed_buf.at[1], mixed_buf.at[2], mask_buf, ctx_buf, lse_buf
            )
            return carry

        lax.fori_loop(start, stop, one, 0)

    tall = rows // parts
    pairs = width // LANES

    def compute(unit, turn):
        layer, j = unit // per_layer, unit % per_layer
        matrix = unit_buf.at[unit % 2]
        mine = pl.ds(pl.multiple_of(turn * tall, tall), tall)

        def small(i):
            return row_ref[0, layer, i : i + 1, :]

        def bias(i):
            return bias_buf[pl.ds(layer * (2 + blocks) + i, 1), :]

        def over_rows(body):
            def one(tile, carry):
                body(pl.ds(pl.multiple_of(turn * tall + tile * NORM_ROWS, NORM_ROWS), NORM_ROWS))
                return carry

            lax.fori_loop(0, tall // NORM_ROWS, one, 0)

        @pl.when((j == 0) & (turn == 0))
        def _():
            free((0, 1), layer)

            @pl.when(layer == 0)
            def _():
                x_buf[...] = hidden_ref[...].astype(jnp.float32)

            low_buf[...] = x_buf[...].astype(jnp.bfloat16)
            save(0, layer).start()

        @pl.when(j < 3)
        def _():
            value = dot(low_buf[mine, :], matrix[...], ((1,), (0,)))
            value = value + jnp.where(j == 1, 0.0, bias(j // 2))
            scale = jnp.where(j == 0, HEAD_DIM ** (-0.5), 1.0)
            mixed_buf[j, mine, :] = (value * scale).astype(jnp.bfloat16)

        @pl.when((j == 2) & (turn == 1))
        def _():
            save(1, layer).start()
            free((2, 3), layer)
            heads(0, pairs // 4)

        @pl.when((j == 3) & (turn == 0))
        def _():
            heads(pairs // 4, 3 * pairs // 4)

        @pl.when((j == 3) & (turn == 1))
        def _():
            heads(3 * pairs // 4, pairs)
            save(2, layer).start()
            save(3, layer).start()
            total_buf[...] = dot(ctx_buf[...], matrix[...], ((1,), (1,)))
            free((4, 5, 6), layer)

            def body(tile, carry):
                part = pl.ds(pl.multiple_of(tile * NORM_ROWS, NORM_ROWS), NORM_ROWS)
                value = x_buf[part, :] + total_buf[part, :] + small(0)
                normed, scaled, inverse = norm_rows(value, small(2), small(3))
                normed_buf[part, :] = normed
                nb_buf[part, :] = normed.astype(jnp.bfloat16)
                one_buf[part, :] = scaled
                inv_one_buf[part, :] = jnp.broadcast_to(inverse, (NORM_ROWS, 128))
                return carry

            lax.fori_loop(0, rows // NORM_ROWS, body, 0)
            for number in (4, 5, 6):
                save(number, layer).start()

        @pl.when((j >= 4) & (j < 4 + blocks))
        def _():
            block = j - 4

            @pl.when(turn == 0)
            def _():
                free((7, 8), layer, block)

            value = dot(nb_buf[mine, :], matrix[...], ((1,), (0,)))
            act, slope = gelu_pair(value + bias(2 + block))
            act_buf[block, mine, :] = act.astype(jnp.bfloat16)
            slope_buf[block, mine, :] = slope.astype(jnp.bfloat16)

            @pl.when(turn == 1)
            def _():
                save(7, layer, block).start()
                save(8, layer, block).start()

        @pl.when(j >= 4 + blocks)
        def _():
            block = j - 4 - blocks
            part = dot(act_buf[block, mine, :], matrix[...], ((1,), (1,)))

            @pl.when(block == 0)
            def _():
                total_buf[mine, :] = part

            @pl.when(block > 0)
            def _():
                total_buf[mine, :] += part

        @pl.when(j == per_layer - 1)
        def _():
            @pl.when(turn == 0)
            def _():
                free((9, 10), layer)

            def body(part):
                value = normed_buf[part, :] + total_buf[part, :] + small(1)
                output, scaled, inverse = norm_rows(value, small(4), small(5))
                x_buf[part, :] = output
                two_buf[part, :] = scaled
                inv_two_buf[part, :] = jnp.broadcast_to(inverse, (NORM_ROWS, 128))

            over_rows(body)

            @pl.when(turn == 1)
            def _():
                save(9, layer).start()
                save(10, layer).start()

    steps = parts * units

    def step(s, carry):
        for number in range(len(stages), -1, -1):
            now = s - number * LAG

            if number == 0:
                for turn in range(rounds):
                    last = turn == rounds - 1
                    due = (s == parts * turn) | (last & (s > parts * turn) & (s % parts == 0))

                    @pl.when(due & (s < steps))
                    def _(turn=turn):
                        @pl.when(s == parts * turn)
                        def _():
                            finish_round(turn)

                        if turn + 2 < rounds:
                            start_round(turn + 2)
                        pick(s // parts, turn + 1)

            @pl.when((now >= 0) & (now < steps))
            def _(now=now, number=number):
                if number == 0:
                    own_copy(now).start()
                else:
                    if number == 1:
                        own_copy(now).wait()
                    for copy in stages[number - 1](now):
                        copy.wait()
                if number < len(stages):
                    for copy in stages[number](now):
                        copy.start()
                else:

                    @pl.when(now % parts == parts - 1)
                    def _():
                        unit_copy(now // parts).start()

        @pl.when(s == len(stages) * LAG)
        def _():
            for copy in column_copies():
                copy.wait()
            for j in range(4):
                bias_buf[:, j * cols : (j + 1) * cols] = col_got[j]

        done = s - len(stages) * LAG - parts

        @pl.when(done >= 0)
        def _():
            @pl.when(done % parts == 0)
            def _():
                unit_copy(done // parts).wait()

            compute(done // parts, done % parts)

        return carry

    fill_mask(mask_buf, docs_col_ref, docs_row_ref)
    lax.fori_loop(0, steps + len(stages) * LAG + parts, step, 0)
    final_ref[...] = x_buf[...]
    last = LAYERS - 1
    for number in (0, 1, 2, 3, 4, 5, 6, 9, 10):
        save(number, last).wait()
    for block in range(blocks):
        save(7, last, block).wait()
        save(8, last, block).wait()


def forward(rank, owner, first, masters, hidden_in, docs, col_now, row_state, piece):
    units = rank.shape[0]
    rounds, width, cols = masters.shape
    rows = hidden_in.shape[0]
    blocks = (units // LAYERS - 4) // 2
    low, full = jnp.bfloat16, jnp.float32
    kept = [
        ((rows, width), low),
        ((3, rows, width), low),
        ((rows, width), low),
        ((width // HEAD_DIM, 1, rows), full),
        ((rows, width), full),
        ((rows, 128), full),
        ((rows, width), low),
        ((blocks, rows, width), low),
        ((blocks, rows, width), low),
        ((rows, width), full),
        ((rows, 128), full),
    ]
    any_spec = pl.BlockSpec(memory_space=pl.ANY)
    vmem_spec = pl.BlockSpec(memory_space=pltpu.VMEM)
    smem_spec = pl.BlockSpec(memory_space=pltpu.SMEM)
    dma = pltpu.SemaphoreType.DMA
    return pl.pallas_call(
        forward_kernel,
        out_shape=[
            jax.ShapeDtypeStruct((units, width, width), low),
            jax.ShapeDtypeStruct((rows, width), full),
        ]
        + [jax.ShapeDtypeStruct((LAYERS,) + shape, dtype) for shape, dtype in kept],
        in_specs=[smem_spec] * 3 + [any_spec] + [vmem_spec] * 5,
        out_specs=[any_spec, vmem_spec] + [any_spec] * len(kept),
        scratch_shapes=[pltpu.VMEM(shape, dtype) for shape, dtype in kept]
        + [
            pltpu.VMEM((rows, width), full),
            pltpu.VMEM((rows, width), full),
            pltpu.VMEM((rows, width), full),
            pltpu.VMEM((rows, rows), full),
            pltpu.VMEM((2, width, width), low),
            pltpu.VMEM((units, piece, width), low),
            dma((8,)),
            dma((2, 9, 8)),
            dma((2,)),
            dma((len(kept), blocks)),
            dma((rounds,)),
            dma((2, rounds)),
            pltpu.VMEM((rounds, width, cols), full),
            pltpu.VMEM((rounds, width, cols), low),
            pltpu.VMEM((4,) + col_now.shape, full),
            pltpu.VMEM((col_now.shape[0], width), full),
            dma((rounds,)),
            dma((2, 3)),
        ]
        + [pltpu.VMEM((width // piece, piece, cols), low)] * rounds,
        compiler_params=pltpu.CompilerParams(
            collective_id=2, has_side_effects=True, vmem_limit_bytes=60 * 1024 * 1024
        ),
        name="gather_forward",
    )(
        rank,
        owner,
        first,
        masters,
        hidden_in,
        docs[:, None],
        docs[None, :],
        col_now,
        row_state,
    )


def run_general(unit_slot, masters, hidden_in, doc_ids, column_state, row_state, out_grad):
    slot_count, width, col_width = masters.shape
    units = unit_slot.shape[0]
    dp_size = lax.axis_size("dp")
    devices = dp_size * lax.axis_size("tensor")
    slots = slot_count * dp_size
    piece = width // devices
    per_layer = units // LAYERS
    blocks = (per_layer - 4) // 2
    tensor_size = lax.axis_size("tensor")
    rows = hidden_in.shape[0]
    seq_len = doc_ids.shape[1]
    heads = width // HEAD_DIM
    share = seq_len // rows
    tensor_index = lax.axis_index("tensor")
    groups = [list(range(i, i + share)) for i in range(0, tensor_size, share)]
    score_scale = HEAD_DIM ** (-0.5)
    sent = masters.astype(jnp.bfloat16).reshape(slot_count, devices, piece, col_width)
    spread = lax.all_to_all(sent.transpose(1, 0, 2, 3), BOTH, 0, 0)
    spread = spread.reshape(dp_size, tensor_size, slot_count, piece, col_width)
    spread = spread.transpose(0, 2, 3, 1, 4).reshape(slots, piece, width)
    mine = spread[unit_slot]
    weights = jnp.concatenate(
        [
            lax.all_gather(
                mine[layer * per_layer : (layer + 1) * per_layer], BOTH, axis=1, tiled=True
            )
            for layer in range(LAYERS)
        ],
        axis=0,
    )

    def matrices(layer):
        unit = weights[layer * per_layer : (layer + 1) * per_layer]
        return (unit[:3], unit[3], unit[4 : 4 + blocks], unit[4 + blocks :])

    row_docs = lax.dynamic_slice_in_dim(doc_ids, tensor_index // share, 1, axis=0)[0]
    my_docs = lax.dynamic_slice_in_dim(row_docs, (tensor_index % share) * rows, rows)
    same_doc = (my_docs[:, None] == row_docs[None, :])[None]

    def whole_row(value):
        if share == 1:
            return value
        return lax.all_gather(value, "tensor", axis=0, tiled=True, axis_index_groups=groups)

    def own_rows(value):
        if share == 1:
            return value
        return lax.psum_scatter(
            value, "tensor", scatter_dimension=0, tiled=True, axis_index_groups=groups
        )

    col_full = lax.all_gather(column_state[0], "tensor", axis=2, tiled=True)
    hidden = hidden_in.astype(jnp.float32)
    saved_layers = []
    for layer in range(LAYERS):
        w_qkv, w_proj, w_in, w_out = matrices(layer)
        row_now = row_state[0, layer]
        col_now = col_full[layer]
        hidden_bf = hidden.astype(jnp.bfloat16)
        query, key, value = (dot(hidden_bf, w_qkv[i], ((1,), (0,))) for i in range(3))
        query = ((query + col_now[0]) * score_scale).astype(jnp.bfloat16)
        key = key.astype(jnp.bfloat16)
        value = (value + col_now[1]).astype(jnp.bfloat16)
        query = query.reshape(rows, heads, HEAD_DIM)
        key = whole_row(key).reshape(seq_len, heads, HEAD_DIM)
        value = whole_row(value).reshape(seq_len, heads, HEAD_DIM)
        scores = jnp.einsum("qhd,khd->hqk", query, key, preferred_element_type=jnp.float32)
        scores = jnp.where(same_doc, scores, -1e30)
        row_top = jnp.max(scores, axis=-1, keepdims=True)
        log_total = row_top + jnp.log(
            jnp.sum(jnp.exp(scores - row_top), axis=-1, keepdims=True)
        )
        soft_bf = jnp.exp(scores - log_total).astype(jnp.bfloat16)
        context = jnp.einsum("hqk,khd->qhd", soft_bf, value, preferred_element_type=jnp.float32)
        context = context.reshape(rows, width).astype(jnp.bfloat16)
        attended = dot(context, w_proj, ((1,), (1,)))
        normed, scaled_one, inverse_one = norm_forward(
            hidden + attended + row_now[0], row_now[2], row_now[3]
        )
        normed_bf = normed.astype(jnp.bfloat16)
        pre_act = jnp.einsum("rd,bdc->brc", normed_bf, w_in, preferred_element_type=jnp.float32)
        activated, slope = gelu_pair(pre_act + col_now[2:, None])
        activated = activated.astype(jnp.bfloat16)
        slope = slope.astype(jnp.bfloat16)
        mlp_out = jnp.einsum(
            "brc,bdc->rd", activated, w_out, preferred_element_type=jnp.float32
        )
        output, scaled_two, inverse_two = norm_forward(
            normed + mlp_out + row_now[1], row_now[4], row_now[5]
        )
        saved_layers.append(
            (hidden_bf, query, key, value, log_total, context, scaled_one, inverse_one, normed_bf)
            + (slope, activated, scaled_two, inverse_two)
        )
        hidden = output
    upstream = out_grad.astype(jnp.float32)
    operands = [None] * LAYERS
    col_parts = [None] * LAYERS
    row_parts = [None] * LAYERS
    for layer in reversed(range(LAYERS)):
        w_qkv, w_proj, w_in, w_out = matrices(layer)
        row_now = row_state[0, layer]
        (
            hidden_bf,
            query,
            key,
            value,
            log_total,
            context,
            scaled_one,
            inverse_one,
            normed_bf,
            slope,
            activated,
            scaled_two,
            inverse_two,
        ) = saved_layers[layer]
        d_two, gain_two, shift_two = norm_backward(upstream, scaled_two, inverse_two, row_now[4])
        grad_bias_two = jnp.sum(d_two, axis=0)
        d_two_bf = d_two.astype(jnp.bfloat16)
        d_act = jnp.einsum("rd,bdc->brc", d_two_bf, w_out, preferred_element_type=jnp.float32)
        d_pre = (d_act * slope).astype(jnp.bfloat16)
        grad_bias_in = jnp.sum(d_pre, axis=1, dtype=jnp.float32)
        d_normed = jnp.einsum("brc,bdc->rd", d_pre, w_in, preferred_element_type=jnp.float32)
        d_normed = d_two + d_normed
        d_one, gain_one, shift_one = norm_backward(d_normed, scaled_one, inverse_one, row_now[2])
        grad_bias_proj = jnp.sum(d_one, axis=0)
        d_one_bf = d_one.astype(jnp.bfloat16)
        d_context = dot(d_one_bf, w_proj, ((1,), (0,))).astype(jnp.bfloat16)
        d_context = d_context.reshape(rows, heads, HEAD_DIM)
        scores = jnp.einsum("qhd,khd->hqk", query, key, preferred_element_type=jnp.float32)
        scores = jnp.where(same_doc, scores, -1e30)
        soft = jnp.exp(scores - log_total)
        d_values = jnp.einsum(
            "hqk,qhd->khd",
            soft.astype(jnp.bfloat16),
            d_context,
            preferred_element_type=jnp.float32,
        )
        d_probs = jnp.einsum(
            "qhd,khd->hqk", d_context, value, preferred_element_type=jnp.float32
        )
        d_scores = (
            soft * (d_probs - jnp.sum(soft * d_probs, axis=-1, keepdims=True))
        ).astype(jnp.bfloat16)
        d_queries = (
            jnp.einsum("hqk,khd->qhd", d_scores, key, preferred_element_type=jnp.float32)
            * score_scale
        )
        d_keys = jnp.einsum("hqk,qhd->khd", d_scores, query, preferred_element_type=jnp.float32)
        d_qkv = jnp.stack(
            [
                d_queries.reshape(rows, width),
                own_rows(d_keys.reshape(seq_len, width)),
                own_rows(d_values.reshape(seq_len, width)),
            ]
        ).astype(jnp.bfloat16)
        grad_bias_qkv = jnp.sum(d_qkv, axis=1, dtype=jnp.float32)
        upstream = d_one + jnp.einsum(
            "brc,bdc->rd", d_qkv, w_qkv, preferred_element_type=jnp.float32
        )
        operands[layer] = (hidden_bf, d_one_bf, normed_bf, d_two_bf)
        operands[layer] += (d_qkv, context[None], d_pre, activated)
        col_parts[layer] = jnp.concatenate(
            [
                grad_bias_qkv[0:1],
                grad_bias_qkv[2:3],
                grad_bias_in,
            ],
            axis=0,
        )
        row_parts[layer] = jnp.stack(
            [grad_bias_proj, grad_bias_two, gain_one, shift_one, gain_two, shift_two]
        )
    small = jnp.stack([jnp.stack(col_parts), jnp.stack(row_parts)])
    summed = []
    for layer in operands:
        whole = jnp.concatenate(
            [
                jnp.einsum(
                    "rd,brc->bdc", layer[i], layer[4 + i], preferred_element_type=jnp.float32
                )
                for i in range(4)
            ],
            axis=0,
        )
        summed.append(
            lax.psum_scatter(whole.astype(jnp.bfloat16), BOTH, scatter_dimension=1, tiled=True)
        )
    summed = jnp.concatenate(summed, axis=0)

    slot_ids = jnp.arange(slots, dtype=jnp.int32)
    named = unit_slot[None, :] == slot_ids[:, None]
    holds = jnp.any(named, axis=1)
    unit_of = jnp.argmax(named, axis=1)
    back = jnp.where(holds[:, None, None], summed[unit_of], jnp.zeros((), jnp.bfloat16))
    back = back.reshape(dp_size, slot_count, piece, tensor_size, col_width)
    back = back.transpose(0, 3, 1, 2, 4).reshape(devices, slot_count, piece, col_width)
    owned = lax.all_to_all(back, BOTH, 0, 0)
    owned = owned.transpose(1, 0, 2, 3)
    owned = owned.reshape(slot_count, width, col_width)
    return (hidden, upstream, owned, lax.psum(small, BOTH))


def run_kernels(unit_slot, masters, hidden_in, doc_ids, column_state, row_state, out_grad):
    slot_count, width, cols = masters.shape
    units = unit_slot.shape[0]
    per_layer = units // LAYERS
    blocks = (per_layer - 4) // 2
    dp_size = lax.axis_size("dp")
    piece = width // (dp_size * lax.axis_size("tensor"))
    dp = lax.axis_index("dp")
    owner = unit_slot // slot_count
    mates = owner[:, None] == owner[None, :]
    order = np.arange(units)
    rank = jnp.sum(mates & (order[:, None] > order[None, :]), axis=1, dtype=jnp.int32)
    feed = [4 + blocks, 4]
    made = [base + b for b in range(blocks) for base in feed] + [3, 0, 1, 2]
    made = [layer * per_layer + j for layer in reversed(range(LAYERS)) for j in made]
    turn = np.argsort(np.array(made))
    later = jnp.sum(mates & (turn[:, None] < turn[None, :]), axis=1, dtype=jnp.int32)
    back = slot_count - 1 - later
    spots = np.arange(slot_count * dp_size)
    asked = (back * dp_size + owner)[None, :] == spots[:, None]
    pick = jnp.max(jnp.where(asked, order[None, :], -1), axis=1)
    pick = jnp.where(pick < 0, made[0], pick).astype(jnp.int32)
    own_slots = dp * slot_count + jnp.arange(slot_count, dtype=jnp.int32)
    named = unit_slot[None, :] == own_slots[:, None]
    slot_rank = jnp.sum(jnp.where(named, rank[None, :], 0), axis=1)
    slot_back = jnp.sum(jnp.where(named, back[None, :], 0), axis=1)
    holds = jnp.any(named, axis=1)
    local_slot = jnp.arange(slot_count)
    first = [
        jnp.max(jnp.where(holds & (slot_rank == turn_now), local_slot, 0))
        for turn_now in range(slot_count)
    ]
    first = jnp.stack(first).astype(jnp.int32)

    docs = lax.dynamic_index_in_dim(doc_ids, lax.axis_index("tensor"), 0, keepdims=False)
    weights, hidden, *saved = forward(
        rank,
        owner,
        first,
        masters,
        hidden_in,
        docs,
        column_state[0].reshape(-1, cols),
        row_state,
        piece,
    )
    upstream, owned, small = backward(pick, out_grad, docs, row_state, weights, saved, piece, cols)
    owned = owned.reshape(slot_count, width, cols)
    mine = jnp.zeros((), owned.dtype)
    for number in range(slot_count):
        here = (holds & (slot_back == number))[:, None, None]
        mine = jnp.where(here, owned[number][None], mine)
    owned = mine
    return (hidden, upstream, owned, small.reshape(2, LAYERS, 2 + blocks, width))


def local(
    hidden_in,
    doc_ids,
    unit_slot,
    masters,
    first_moment,
    second_moment,
    column_state,
    row_state,
    out_grad,
):
    slot_count, width, col_width = masters.shape
    dp_size = lax.axis_size("dp")
    tensor_size = lax.axis_size("tensor")
    slots = slot_count * dp_size
    tensor_index = lax.axis_index("tensor")
    kernels = dp_size == 8 and tensor_size == 4 and hidden_in.shape[0] == doc_ids.shape[1]

    run = run_kernels if kernels else run_general
    hidden, upstream, owned, small = run(
        unit_slot, masters, hidden_in, doc_ids, column_state, row_state, out_grad
    )
    owned = owned.astype(jnp.float32)
    slot_ids = jnp.arange(slots, dtype=jnp.int32)
    holds = jnp.any(unit_slot[None, :] == slot_ids[:, None], axis=1)
    row_total = small[1]
    col_total = lax.dynamic_slice_in_dim(small[0], tensor_index * col_width, col_width, axis=2)

    occupied = lax.dynamic_slice_in_dim(holds, lax.axis_index("dp") * slot_count, slot_count)
    occupied = occupied.astype(jnp.float32)[:, None, None]
    new_master, new_first, new_second = adamw_update(
        masters, owned, first_moment, second_moment, RATE_UNITS
    )
    unit_master = new_master * occupied
    unit_state = jnp.stack([new_first * occupied, new_second * occupied])
    new_col, col_first, col_second = adamw_update(
        column_state[0], col_total, column_state[1], column_state[2], RATE_SMALL
    )
    column_out = jnp.stack([col_total, new_col, col_first, col_second])
    new_row, row_first, row_second = adamw_update(
        row_state[0], row_total, row_state[1], row_state[2], RATE_SMALL
    )
    row_out = jnp.stack([row_total, new_row, row_first, row_second])
    return (hidden, upstream, unit_master, unit_state, column_out, row_out)


def solution(mesh):
    return jax.shard_map(
        local,
        mesh=mesh,
        in_specs=(
            P(("dp", "tensor"), None),
            P("dp", None),
            P(),
            P("dp", None, "tensor"),
            P("dp", None, "tensor"),
            P("dp", None, "tensor"),
            P(None, None, None, "tensor"),
            P(),
            P(("dp", "tensor"), None),
        ),
        out_specs=(
            P(("dp", "tensor"), None),
            P(("dp", "tensor"), None),
            P("dp", None, "tensor"),
            P(None, "dp", None, "tensor"),
            P(None, None, None, "tensor"),
            P(),
        ),
        check_vma=False,
    )
```

```python
import math

import jax
import jax.numpy as jnp
from jax import lax
from jax.experimental import pallas as pl
from jax.experimental.pallas import tpu as pltpu
from jax.sharding import PartitionSpec as P

HEAD_DIM = 64
LAYERS = 2
STEP = 3

EPS_NORM = 1e-06
RATE_UNITS = 0.05
RATE_SMALL = 0.2
WEIGHT_DECAY = 0.01
ADAM_EPS = 1e-08
BETA_MOMENT = 0.5
BOTH = ("dp", "tensor")


def norm_forward(summed, gain, shift):
    row_mean = jnp.mean(summed, axis=1, keepdims=True)
    centred = summed - row_mean
    inverse = lax.rsqrt(jnp.mean(centred * centred, axis=1, keepdims=True) + EPS_NORM)
    scaled = centred * inverse
    return (scaled * gain + shift, scaled, inverse)


def norm_backward(upstream, scaled, inverse, gain):
    d_scaled = upstream * gain
    mean_one = jnp.mean(d_scaled, axis=1, keepdims=True)
    mean_two = jnp.mean(d_scaled * scaled, axis=1, keepdims=True)
    grad_input = inverse * (d_scaled - mean_one - scaled * mean_two)
    return (grad_input, jnp.sum(upstream * scaled, axis=0), jnp.sum(upstream, axis=0))


def gelu_pair(v):
    cdf = 0.5 * (1.0 + lax.erf(v * 2.0 ** (-0.5)))
    bell = jnp.exp(-0.5 * v * v) * (2.0 * math.pi) ** (-0.5)
    return (v * cdf, cdf + v * bell)


def adamw_update(old_value, gradient, first_old, second_old, learn_rate):
    first_new = BETA_MOMENT * first_old + (1.0 - BETA_MOMENT) * gradient
    second_new = BETA_MOMENT * second_old + (1.0 - BETA_MOMENT) * gradient * gradient
    correct = 1.0 - BETA_MOMENT**STEP
    step_size = first_new / correct / (jnp.sqrt(second_new / correct) + ADAM_EPS)
    return (old_value - learn_rate * (step_size + WEIGHT_DECAY * old_value), first_new, second_new)


def dot(left, right, dims):
    return lax.dot_general(left, right, (dims, ((), ())), preferred_element_type=jnp.float32)


LANES = 2 * HEAD_DIM


def head_lanes(value, head):
    lane = lax.broadcasted_iota(jnp.int32, value.shape, 1)
    keep = lane < HEAD_DIM if head == 0 else lane >= HEAD_DIM
    return jnp.where(keep, value, jnp.zeros_like(value))


def pair_lanes(first, second):
    lane = lax.broadcasted_iota(jnp.int32, first.shape, 1)
    return jnp.where(lane < HEAD_DIM, first, second)


def attend_pair(pair, q_ref, k_ref, v_ref, mask_ref, ctx_ref, lse_ref):
    lanes = pl.ds(pl.multiple_of(pair * LANES, LANES), LANES)
    query, key, value = q_ref[:, lanes], k_ref[:, lanes], v_ref[:, lanes]
    value_t = value.T
    parts = []
    for head in range(2):
        scores = dot(head_lanes(key, head), query, ((1,), (1,))) + mask_ref[...]
        top = jnp.max(scores, axis=0, keepdims=True)
        weight = jnp.exp(scores - top)
        total = jnp.sum(weight, axis=0, keepdims=True)
        lse_ref[pair * 2 + head] = top + jnp.log(total)
        mine = value_t[head * HEAD_DIM : (head + 1) * HEAD_DIM]
        mixed = dot(mine, weight.astype(jnp.bfloat16), ((1,), (0,)))
        parts.append(mixed * (1.0 / total))
    ctx_ref[:, lanes] = jnp.concatenate(parts, axis=0).T.astype(ctx_ref.dtype)


def attend_back_pair(pair, q_ref, k_ref, v_ref, d_ref, mask_ref, lse_ref, dq_ref, dk_ref, dv_ref):
    lanes = pl.ds(pl.multiple_of(pair * LANES, LANES), LANES)
    query, key, value = q_ref[:, lanes], k_ref[:, lanes], v_ref[:, lanes]
    grad = d_ref[:, lanes]
    key_t = key.T
    parts, d_keys, d_values = [], [], []
    for head in range(2):
        scores = dot(head_lanes(key, head), query, ((1,), (1,))) + mask_ref[...]
        soft = jnp.exp(scores - lse_ref[pair * 2 + head])
        d_values.append(dot(soft.astype(jnp.bfloat16), grad, ((1,), (0,))))
        d_soft = dot(head_lanes(value, head), grad, ((1,), (1,)))
        both = soft * d_soft
        mean = jnp.sum(both, axis=0, keepdims=True)
        d_scores = (both - soft * mean).astype(jnp.bfloat16)
        d_keys.append(dot(d_scores, query, ((1,), (0,))))
        mine = key_t[head * HEAD_DIM : (head + 1) * HEAD_DIM]
        parts.append(dot(mine, d_scores, ((1,), (0,))))
    scale = HEAD_DIM ** (-0.5)
    dq_ref[:, lanes] = (jnp.concatenate(parts, axis=0).T * scale).astype(dq_ref.dtype)
    dk_ref[:, lanes] = pair_lanes(*d_keys).astype(dk_ref.dtype)
    dv_ref[:, lanes] = pair_lanes(*d_values).astype(dv_ref.dtype)


def fill_mask(mask_ref, docs_col_ref, docs_row_ref):
    same = docs_col_ref[...] == docs_row_ref[...]
    mask_ref[...] = jnp.where(same, 0.0, -1e30).astype(jnp.float32)


LAG = 2


def spread_order(z, y, x, c):
    return ((c * 2 + x) * 2 + y) * 4 + z


def every_other(z, y, x, c, body):
    for step in (2, 1, 3, 0):

        def one(i, carry, step=step):
            body((z + step) % 4, (y + i // 4) % 2, (x + (i // 2) % 2) % 2, (c + i % 2) % 2)
            return carry

        lax.fori_loop(1 if step == 0 else 0, 8, one, 0)


def greet_all(z, y, x, c):
    barrier = pltpu.get_barrier_semaphore()

    def greet(zz, yy, xx, cc):
        pl.semaphore_signal(
            barrier,
            inc=1,
            device_id=(zz * 2 + yy, xx * 2 + cc),
            device_id_type=pl.DeviceIdType.MESH,
        )

    every_other(z, y, x, c, greet)
    return barrier


TILE = 256


def norm_back_rows(upstream, scaled, inverse, gain):
    d_scaled = upstream * gain
    mean_one = jnp.mean(d_scaled, axis=1, keepdims=True)
    mean_two = jnp.mean(d_scaled * scaled, axis=1, keepdims=True)
    return inverse * (d_scaled - mean_one - scaled * mean_two)


def backward_kernel(
    pick_ref,
    out_grad_ref,
    docs_col_ref,
    docs_row_ref,
    row_ref,
    weights_ref,
    low_ref,
    mixed_ref,
    ctx_ref,
    lse_ref,
    one_ref,
    inv_one_ref,
    normed_ref,
    act_ref,
    slope_ref,
    two_ref,
    inv_two_ref,
    owned_ref,
    total_ref,
    small_out,
    out_ref,
    back_buf,
    left_buf,
    right_buf,
    unit_buf,
    scaled_buf,
    inv_buf,
    slope_buf,
    mixed_buf,
    lse_buf,
    mask_buf,
    d_ctx_buf,
    core_out,
    core_in,
    sum_core,
    first_in,
    sum_first,
    second_in,
    sum_second,
    z_in,
    small_sum,
    small_got,
    load_sem,
    core_sems,
    first_sems,
    second_sems,
    z_sems,
    small_sems,
    own_sems,
    round_sems,
):
    units, piece, width = out_ref.shape
    rows = total_ref.shape[0]
    per_layer = units // LAYERS
    blocks = (per_layer - 4) // 2
    at_out, at_query = 2 * blocks, 2 * blocks + 1
    dp, tensor = lax.axis_index("dp"), lax.axis_index("tensor")
    z, y, x, c = dp // 2, dp % 2, tensor // 2, tensor % 2
    half, parts = width // 2, 2
    side_cols = half // 2
    quarter, eighth = half // 2, half // 4
    to_core = (dp, x * 2 + 1 - c)
    to_x = (dp, (1 - x) * 2 + c)
    to_y = (z * 2 + 1 - y, tensor)
    to_z = [(((z + k) % 4) * 2 + y, tensor) for k in (1, 2, 3)]
    to_z1 = ((z + 1 - 2 * (z % 2)) * 2 + y, tensor)
    to_z2 = (((z + 2) % 4) * 2 + y, tensor)
    mesh_id = pl.DeviceIdType.MESH

    barrier = greet_all(z, y, x, c)

    def remote(src, dst, sems, send, recv, peer):
        return pltpu.make_async_remote_copy(
            src_ref=src,
            dst_ref=dst,
            send_sem=sems.at[send],
            recv_sem=sems.at[recv],
            device_id=peer,
            device_id_type=mesh_id,
        )

    def place(s):
        return LAYERS - 1 - s // per_layer, s % per_layer

    def unit_of(s):
        layer, j = place(s)
        feed = jnp.where(j % 2 == 0, 4 + blocks + j // 2, 4 + j // 2)
        return layer * per_layer + jnp.where(
            j < at_out, feed, jnp.where(j == at_out, 3, j - at_query)
        )

    def left_of(s):
        j = s % per_layer
        feed = jnp.where(j % 2 == 0, 3, 2)
        return jnp.where(j < at_out, feed, jnp.where(j == at_out, 1, 0))

    def loaded_slot(s):
        return ((s // per_layer) * (blocks + 1) + (s % per_layer) // 2) % 2

    def right_of(s):
        j = s % per_layer
        feed = jnp.where(j % 2 == 0, loaded_slot(s), 2 + (j // 2) % 2)
        return jnp.where(
            j < at_out, feed, jnp.where(j == at_out, loaded_slot(s), 4 + j - at_query)
        )

    local = pltpu.make_async_copy

    def unit_load(s):
        return local(weights_ref.at[unit_of(s)], unit_buf.at[s % 3], load_sem.at[0, s % 3])

    def act_load(layer, block, slot):
        return local(act_ref.at[layer, block], right_buf.at[slot], load_sem.at[1, slot])

    def ctx_load(layer, slot):
        return local(ctx_ref.at[layer], right_buf.at[slot], load_sem.at[1, slot])

    def slope_load(layer, block):
        return local(slope_ref.at[layer, block], slope_buf, load_sem.at[2, 0])

    def norm_loads(layer, which):
        scaled, inv = ((one_ref, inv_one_ref), (two_ref, inv_two_ref))[which]
        return [
            local(scaled.at[layer], scaled_buf, load_sem.at[3, 0]),
            local(inv.at[layer], inv_buf, load_sem.at[3, 1]),
        ]

    def mixed_loads(layer):
        return [
            local(mixed_ref.at[layer], mixed_buf, load_sem.at[4, 0]),
            local(lse_ref.at[layer], lse_buf, load_sem.at[4, 1]),
        ]

    def normed_load(layer):
        return local(normed_ref.at[layer], left_buf.at[2], load_sem.at[2, 1])

    def low_load(layer):
        return local(low_ref.at[layer], left_buf.at[0], load_sem.at[5, 0])

    def begin(*copies):
        for copy in copies:
            copy.start()

    def finish(*copies):
        for copy in copies:
            copy.wait()

    def note(row, value):
        small_sum[0, pl.ds(row, 1), :] = value

    def column(layer, i):
        return layer * (2 + blocks) + i

    def row(layer, i):
        return LAYERS * (2 + blocks) + layer * 6 + i

    def norm_back(layer, gain_row, bias_row, low_slot):
        gain = row_ref[layer, gain_row : gain_row + 1, :]
        size = 128

        def one(tile, carry):
            part = pl.ds(pl.multiple_of(tile * size, size), size)
            upstream = total_ref[part, :]
            scaled = scaled_buf[part, :]
            inside = norm_back_rows(upstream, scaled, inv_buf[part, 0:1], gain)
            total_ref[part, :] = inside
            left_buf[low_slot, part, :] = inside.astype(jnp.bfloat16)
            sums = (upstream * scaled, upstream, inside)
            return tuple(a + jnp.sum(b, axis=0, keepdims=True) for a, b in zip(carry, sums))

        zero = jnp.zeros((1, width), jnp.float32)
        gains, shifts, biases = lax.fori_loop(0, rows // size, one, (zero, zero, zero))
        note(row(layer, gain_row), gains)
        note(row(layer, gain_row + 1), shifts)
        note(row(layer, bias_row), biases)

    def heads(start, stop):
        inputs = [mixed_buf.at[i] for i in range(3)]
        grads = [right_buf.at[4 + i] for i in range(3)]

        def one(pair, carry):
            attend_back_pair(pair, *inputs, d_ctx_buf, mask_buf, lse_buf, *grads)
            return carry

        lax.fori_loop(start, stop, one, 0)

    pairs = width // LANES

    def data_gradient(s):
        layer, j = place(s)
        matrix = unit_buf.at[s % 3]
        before = unit_buf.at[(s + 2) % 3]
        slot = loaded_slot(s)

        @pl.when(j == 0)
        def _():
            finish(*norm_loads(layer, 1))

            @pl.when(s == 0)
            def _():
                total_ref[...] = out_grad_ref[...].astype(jnp.float32)

            norm_back(layer, 4, 1, 3)
            begin(*norm_loads(layer, 0), *mixed_loads(layer))

        @pl.when(j == 1)
        def _():
            finish(normed_load(layer))
            begin(low_load(layer))

        @pl.when((j < at_out) & (j % 2 == 0))
        def _():
            block = j // 2
            finish(slope_load(layer, block), act_load(layer, block, slot))

            @pl.when(block < blocks - 1)
            def _():
                act_load(layer, block + 1, 1 - slot).start()

            @pl.when(block == blocks - 1)
            def _():
                ctx_load(layer, 1 - slot).start()

            d_act = dot(left_buf[3], matrix[...], ((1,), (0,)))
            d_pre = (d_act * slope_buf[...].astype(jnp.float32)).astype(jnp.bfloat16)
            right_buf[2 + block % 2] = d_pre
            sums = jnp.sum(d_pre.astype(jnp.float32), axis=0, keepdims=True)
            note(column(layer, 2 + block), sums)

            @pl.when(block < blocks - 1)
            def _():
                slope_load(layer, block + 1).start()

        @pl.when((j < at_out) & (j % 2 == 1))
        def _():
            total_ref[...] += dot(right_buf[2 + (j // 2) % 2], matrix[...], ((1,), (1,)))

        @pl.when(j == at_out)
        def _():
            finish(*norm_loads(layer, 0), *mixed_loads(layer), ctx_load(layer, slot))
            norm_back(layer, 2, 0, 1)

            @pl.when(layer > 0)
            def _():
                act_load(layer - 1, 0, 1 - slot).start()
                begin(*norm_loads(layer - 1, 1))
                slope_load(layer - 1, 0).start()

            d_ctx_buf[...] = dot(left_buf[1], matrix[...], ((1,), (0,))).astype(jnp.bfloat16)

        @pl.when(j == at_query)
        def _():
            finish(low_load(layer))

            @pl.when(layer > 0)
            def _():
                normed_load(layer - 1).start()

            heads(3 * pairs // 8, 5 * pairs // 8)

        @pl.when(j == at_query + 1)
        def _():
            total_ref[...] += dot(right_buf[4], before[...], ((1,), (1,)))

        @pl.when(j == at_query + 2)
        def _():
            total_ref[...] += dot(right_buf[6], matrix[...], ((1,), (1,)))

    def data_gradient_rest(s):
        layer, j = place(s)

        @pl.when(j == at_out)
        def _():
            heads(0, 3 * pairs // 8)

        @pl.when(j == at_query)
        def _():
            heads(5 * pairs // 8, pairs)

        @pl.when(j == at_query + 1)
        def _():
            total_ref[...] += dot(right_buf[5], unit_buf[s % 3], ((1,), (1,)))
            for i, number in ((0, 0), (2, 1)):
                sums = jnp.sum(right_buf[4 + i].astype(jnp.float32), axis=0, keepdims=True)
                note(column(layer, number), sums)

    def product(s, side, tile):
        unit = s // parts
        start = pl.multiple_of(side * half + tile * TILE, TILE)
        left = left_buf[left_of(unit), :, pl.ds(start, TILE)]
        right = right_buf[
            right_of(unit), :, pl.ds(pl.multiple_of((s % parts) * half, half), half)
        ]
        return lax.dot_general(
            left, right, (((0,), (0,)), ((), ())), preferred_element_type=jnp.float32
        )

    def core_copy(s):
        return remote(
            core_out.at[s % 2], core_in.at[s % 4], core_sems, (0, s % 2), (1, s % 4), to_core
        )

    def first_copies(s):
        here = sum_core.at[s % 3]
        return (
            remote(
                here.at[pl.ds(pl.multiple_of((1 - x) * quarter, quarter), quarter), pl.ds(0, side_cols)],
                first_in.at[s % 4, 0],
                first_sems,
                (0, 0, s % 3),
                (1, 0, s % 4),
                to_x,
            ),
            *(
                remote(
                    here.at[
                        pl.ds(pl.multiple_of(i * quarter + (1 - y) * eighth, eighth), eighth),
                        pl.ds(side_cols, side_cols),
                    ],
                    first_in.at[s % 4, 1, pl.ds(i * eighth, eighth)],
                    first_sems,
                    (0, 1 + i, s % 3),
                    (1, 1 + i, s % 4),
                    to_y,
                )
                for i in range(2)
            ),
        )

    def second_copies(s):
        here = sum_first.at[s % 3]
        return (
            remote(
                here.at[0, pl.ds(pl.multiple_of((1 - y) * eighth, eighth), eighth)],
                second_in.at[s % 4, 0],
                second_sems,
                (0, 0, s % 3),
                (1, 0, s % 4),
                to_y,
            ),
            remote(
                here.at[1, pl.ds(pl.multiple_of((1 - x) * eighth, eighth), eighth)],
                second_in.at[s % 4, 1],
                second_sems,
                (0, 1, s % 3),
                (1, 1, s % 4),
                to_x,
            ),
        )

    def z_copies(s):
        return [
            remote(
                sum_second.at[s % 3, pl.ds(pl.multiple_of(((z + k) % 4) * piece, piece), piece)],
                z_in.at[s % 4, k - 1],
                z_sems,
                (0, k - 1, s % 3),
                (1, k - 1, s % 4),
                to_z[k - 1],
            )
            for k in (1, 2, 3)
        ]

    small_peers = (to_core, to_x, to_y, to_z1, to_z2)

    def small_copy(stage):
        return remote(
            small_sum.at[stage],
            small_got.at[stage],
            small_sems,
            (0, stage),
            (1, stage),
            small_peers[stage],
        )

    rounds, owners = back_buf.shape[0], back_buf.shape[1]
    cols = owned_ref.shape[3]
    me = spread_order(z, y, x, c)

    def own_back(number):
        return local(
            back_buf.at[number, dp, :, pl.ds(pl.multiple_of(tensor * cols, cols), cols)],
            owned_ref.at[number, me],
            own_sems.at[number],
        )

    def send_back(number):
        def fill(owner, carry):
            back_buf[number, owner] = out_ref[pick_ref[number * owners + owner]]
            return carry

        lax.fori_loop(0, owners, fill, 0)
        own_back(number).start()

        def send(zz, yy, xx, cc):
            there = xx * 2 + cc
            remote(
                back_buf.at[
                    number, zz * 2 + yy, :, pl.ds(pl.multiple_of(there * cols, cols), cols)
                ],
                owned_ref.at[number, me],
                round_sems,
                (0, number),
                (1, number),
                (zz * 2 + yy, there),
            ).start()

        every_other(z, y, x, c, send)

    def finish_back(number):
        own_back(number).wait()
        most = owned_ref.at[number, pl.ds(0, 31)]
        remote(most, most, round_sems, (0, number), (1, number), to_core).wait()

    top = LAYERS - 1
    steps = parts * units
    begin(
        *norm_loads(top, 1),
        unit_load(jnp.int32(0)),
        slope_load(top, 0),
        act_load(top, 0, 0),
        normed_load(top),
    )
    fill_mask(mask_buf, docs_col_ref, docs_row_ref)
    pl.semaphore_wait(barrier, 31)

    def step(s, carry):
        last = s - 3 * LAG - 1

        @pl.when((last >= 0) & (last < steps))
        def _():
            for copy in z_copies(last):
                copy.wait()
            total = sum_second[last % 3, pl.ds(pl.multiple_of(z * piece, piece), piece), :].astype(
                jnp.float32
            )
            for k in range(3):
                total = total + z_in[last % 4, k].astype(jnp.float32)
            cols_now = pl.ds(pl.multiple_of((last % parts) * half, half), half)
            out_ref[unit_of(last // parts), :, cols_now] = total.astype(out_ref.dtype)

            @pl.when((last // parts >= units - rounds) & (last % parts == parts - 1))
            def _():
                send_back(last // parts - (units - rounds))

        third = s - 2 * LAG - 1

        @pl.when((third >= 0) & (third < steps))
        def _():
            for copy in second_copies(third):
                copy.wait()
            for part, side in ((0, y), (1, x)):
                mine = sum_first[
                    third % 3, part, pl.ds(pl.multiple_of(side * eighth, eighth), eighth), :
                ]
                total = mine.astype(jnp.float32) + second_in[third % 4, part].astype(jnp.float32)
                sum_second[third % 3, :, part * side_cols : (part + 1) * side_cols] = total.astype(
                    jnp.bfloat16
                )
            for copy in z_copies(third):
                copy.start()

        second = s - LAG - 1

        @pl.when((second >= 0) & (second < steps))
        def _():
            for copy in first_copies(second):
                copy.wait()
            mine = sum_core[
                second % 3, pl.ds(pl.multiple_of(x * quarter, quarter), quarter), 0:side_cols
            ]
            total = mine.astype(jnp.float32) + first_in[second % 4, 0].astype(jnp.float32)
            sum_first[second % 3, 0] = total.astype(jnp.bfloat16)
            for i in range(2):
                mine = sum_core[
                    second % 3,
                    pl.ds(pl.multiple_of(i * quarter + y * eighth, eighth), eighth),
                    side_cols : 2 * side_cols,
                ]
                part = pl.ds(i * eighth, eighth)
                total = mine.astype(jnp.float32) + first_in[second % 4, 1, part, :].astype(
                    jnp.float32
                )
                sum_first[second % 3, 1, part, :] = total.astype(jnp.bfloat16)
            for copy in second_copies(second):
                copy.start()

        @pl.when(s < steps)
        def _():
            unit = s // parts

            @pl.when(s % parts == 0)
            def _():
                unit_load(unit).wait()

                @pl.when(unit + 1 < units)
                def _():
                    unit_load(unit + 1).start()

                data_gradient(unit)

            @pl.when(s % parts == 1)
            def _():
                data_gradient_rest(unit)

            @pl.when(s >= 2)
            def _():
                core_copy(s - 2).wait_send()

            def one(tile, carry):
                part = pl.ds(pl.multiple_of(tile * TILE, TILE), TILE)
                core_out[s % 2, part, :] = product(s, 1 - c, tile).astype(jnp.bfloat16)
                return carry

            lax.fori_loop(0, half // TILE, one, 0)
            core_copy(s).start()

        first = s - 1

        @pl.when((first >= 0) & (first < steps))
        def _():
            core_copy(first).wait_recv()

            def one(tile, carry):
                part = pl.ds(pl.multiple_of(tile * TILE, TILE), TILE)
                total = product(first, c, tile) + core_in[first % 4, part, :].astype(jnp.float32)
                sum_core[first % 3, part, :] = total.astype(jnp.bfloat16)
                return carry

            lax.fori_loop(0, half // TILE, one, 0)
            for copy in first_copies(first):
                copy.start()

        for stage in range(6):

            @pl.when(s == steps + stage)
            def _(stage=stage):
                if stage > 0:
                    small_copy(stage - 1).wait()
                    total = small_sum[stage - 1] + small_got[stage - 1]
                    if stage < 5:
                        small_sum[stage] = total
                    else:
                        small_out[...] = total
                if stage < 5:
                    small_copy(stage).start()

        return carry

    lax.fori_loop(0, steps + 3 * LAG + 1, step, 0)
    for s in (steps - 2, steps - 1):
        core_copy(s).wait_send()
    for number in range(rounds):
        finish_back(number)


def backward(pick, out_grad, docs, row_now, weights, saved, piece, cols):
    units, width, _ = weights.shape
    rows = out_grad.shape[0]
    blocks = (units // LAYERS - 4) // 2
    half = width // 2
    low, full = jnp.bfloat16, jnp.float32
    rounds = pick.shape[0] // 10
    small = (LAYERS * (8 + blocks), width)
    any_spec = pl.BlockSpec(memory_space=pl.ANY)
    vmem_spec = pl.BlockSpec(memory_space=pltpu.VMEM)
    dma = pltpu.SemaphoreType.DMA
    summed, total, small = pl.pallas_call(
        backward_kernel,
        out_shape=(
            jax.ShapeDtypeStruct((rounds, width // piece, piece, cols), low),
            jax.ShapeDtypeStruct((rows, width), full),
            jax.ShapeDtypeStruct(small, full),
        ),
        in_specs=[pl.BlockSpec(memory_space=pltpu.SMEM)] + [vmem_spec] * 4 + [any_spec] * (1 + len(saved)),
        out_specs=(vmem_spec, vmem_spec, vmem_spec),
        scratch_shapes=[
            pltpu.VMEM((units, piece, width), low),
            pltpu.VMEM((rounds, 8, piece, width), low),
            pltpu.VMEM((4, rows, width), low),
            pltpu.VMEM((7, rows, width), low),
            pltpu.VMEM((3, width, width), low),
            pltpu.VMEM((rows, width), full),
            pltpu.VMEM((rows, 128), full),
            pltpu.VMEM((rows, width), low),
            pltpu.VMEM((3, rows, width), low),
            pltpu.VMEM((width // HEAD_DIM, 1, rows), full),
            pltpu.VMEM((rows, rows), full),
            pltpu.VMEM((rows, width), low),
            pltpu.VMEM((2, half, half), low),
            pltpu.VMEM((4, half, half), low),
            pltpu.VMEM((3, half, half), low),
            pltpu.VMEM((4, 2, half // 2, half // 2), low),
            pltpu.VMEM((3, 2, half // 2, half // 2), low),
            pltpu.VMEM((4, 2, half // 4, half // 2), low),
            pltpu.VMEM((3, half // 4, half), low),
            pltpu.VMEM((4, 3, piece, half), low),
            pltpu.VMEM((5,) + small, full),
            pltpu.VMEM((5,) + small, full),
            dma((6, 3)),
            dma((2, 4)),
            dma((2, 3, 4)),
            dma((2, 2, 4)),
            dma((2, 3, 4)),
            dma((2, 5)),
            dma((rounds,)),
            dma((2, rounds)),
        ],
        compiler_params=pltpu.CompilerParams(
            collective_id=1, has_side_effects=True, vmem_limit_bytes=63 * 1024 * 1024
        ),
        name="backward_reduce",
    )(pick, out_grad, docs[:, None], docs[None, :], row_now, weights, *saved)
    return (total, summed, small)


def norm_rows(value, gain, shift):
    centred = value - jnp.mean(value, axis=1, keepdims=True)
    inverse = lax.rsqrt(jnp.mean(centred * centred, axis=1, keepdims=True) + EPS_NORM)
    scaled = centred * inverse
    return (scaled * gain + shift, scaled, inverse)


NORM_ROWS = 128


def forward_kernel(
    slot_ref,
    masters_ref,
    hidden_ref,
    docs_col_ref,
    docs_row_ref,
    col_ref,
    row_ref,
    out_ref,
    final_ref,
    table_ref,
    *refs,
):
    saved, bufs = refs[:11], refs[11:22]
    rounds = masters_ref.shape[0]
    (x_buf, normed_buf, total_buf, mask_buf, unit_buf, own_ref) = refs[22:28]
    (own_sem, sems, unit_sem, save_sem, got_sem, round_sems) = refs[28:34]
    (masters_buf, sent_ref, col_got, bias_buf, master_sem, col_sems) = refs[34:40]
    rank_ref, back_ref = refs[40:42]
    got = refs[42:]
    (low_buf, mixed_buf, ctx_buf, lse_buf, one_buf, inv_one_buf, nb_buf) = bufs[:7]
    (act_buf, slope_buf, two_buf, inv_two_buf) = bufs[7:]
    units, piece, width = own_ref.shape
    rows = hidden_ref.shape[0]
    per_layer = units // LAYERS
    blocks = (per_layer - 4) // 2
    dp, tensor = lax.axis_index("dp"), lax.axis_index("tensor")
    z, y, x, c = dp // 2, dp % 2, tensor // 2, tensor % 2
    half = width // 2
    line, plane = 4 * piece, 8 * piece
    to_core = (dp, x * 2 + 1 - c)
    to_x = (dp, (1 - x) * 2 + c)
    to_y = (z * 2 + 1 - y, tensor)
    to_z = [(((z + k) % 4) * 2 + y, tensor) for k in (1, 2, 3)]
    mesh_id = pl.DeviceIdType.MESH

    barrier = greet_all(z, y, x, c)
    masters_in = [
        pltpu.make_async_copy(masters_ref.at[i], masters_buf.at[i], master_sem.at[i])
        for i in range(rounds)
    ]
    for copy in masters_in:
        copy.start()
    cols = sent_ref.shape[2]
    owners = table_ref.shape[0] // rounds - 2

    def turn_of(unit):
        layer, j = unit // per_layer, unit % per_layer
        feed = jnp.where(j < 4 + blocks, 2 * (j - 4) + 1, 2 * (j - 4 - blocks))
        place = jnp.where(j < 3, 2 * blocks + 1 + j, jnp.where(j == 3, 2 * blocks, feed))
        return (LAYERS - 1 - layer) * per_layer + place

    def rank_one(unit, carry):
        mine, turn = slot_ref[unit] // rounds, turn_of(unit)
        before, after = 0, 0
        for other in range(units):
            same = jnp.where(slot_ref[other] // rounds == mine, 1, 0)
            before = before + jnp.where(other < unit, same, 0)
            after = after + jnp.where(turn_of(other) > turn, same, 0)
        rank_ref[unit] = before
        back_ref[unit] = rounds - 1 - after
        return carry

    lax.fori_loop(0, units, rank_one, 0)

    def first_of(number):
        found = 0
        for unit in range(units):
            slot = slot_ref[unit]
            here = (slot // rounds == dp) & (rank_ref[unit] == number)
            found = found + jnp.where(here, slot % rounds, 0)
        return found

    def fill_table():
        def spot_one(spot, carry):
            found = (LAYERS - 1) * per_layer + 4 + blocks
            for unit in range(units):
                at = back_ref[unit] * owners + slot_ref[unit] // rounds
                found = jnp.where(at == spot, unit, found)
            table_ref[spot] = found
            return carry

        lax.fori_loop(0, rounds * owners, spot_one, 0)
        for i in range(rounds):
            turn, taken = 0, 0
            for unit in range(units):
                here = slot_ref[unit] == dp * rounds + i
                turn = turn + jnp.where(here, back_ref[unit], 0)
                taken = taken + jnp.where(here, 1, 0)
            table_ref[rounds * owners + i] = turn
            table_ref[rounds * (owners + 1) + i] = taken
    me = dp * 4 + tensor

    def part_for(number, zz, yy, xx, cc):
        start = pl.multiple_of(spread_order(zz, yy, xx, cc) * piece, piece)
        return sent_ref.at[number, pl.ds(start, piece)]

    def keep(number):
        return pltpu.make_async_copy(
            part_for(number, z, y, x, c), got[number].at[me], got_sem.at[number]
        )

    def round_copy(number, src, dst, peer):
        return pltpu.make_async_remote_copy(
            src_ref=src,
            dst_ref=dst,
            send_sem=round_sems.at[0, number],
            recv_sem=round_sems.at[1, number],
            device_id=peer,
            device_id_type=mesh_id,
        )

    def start_round(number):
        keep(number).start()

        def send(zz, yy, xx, cc):
            src = part_for(number, zz, yy, xx, cc)
            round_copy(number, src, got[number].at[me], (zz * 2 + yy, xx * 2 + cc)).start()

        every_other(z, y, x, c, send)

    def finish_round(number):
        keep(number).wait()
        most = got[number].at[pl.ds(0, 31)]
        round_copy(number, most, most, to_core).wait()

    def pick(unit, there):
        rank, owner = rank_ref[unit], slot_ref[unit] // rounds
        for j in range(4):
            value = got[0][owner * 4 + j]
            for number in range(1, there):
                value = jnp.where(rank == number, got[number][owner * 4 + j], value)
            own_ref[unit, :, j * cols : (j + 1) * cols] = value

    def column_copies():
        return [
            pltpu.make_async_remote_copy(
                src_ref=col_ref,
                dst_ref=col_got.at[tensor],
                send_sem=col_sems.at[0, k],
                recv_sem=col_sems.at[1, k],
                device_id=(dp, (tensor + k + 1) % 4),
                device_id_type=mesh_id,
            )
            for k in range(3)
        ]

    for copy in masters_in:
        copy.wait()
    sent_ref[0] = masters_buf[first_of(0)].astype(sent_ref.dtype)
    pl.semaphore_wait(barrier, 31)
    start_round(0)
    for number in range(1, rounds):
        sent_ref[number] = masters_buf[first_of(number)].astype(sent_ref.dtype)
    start_round(1)
    col_got[tensor] = col_ref[...]
    for copy in column_copies():
        copy.start()
    fill_table()

    my_line = pl.multiple_of(((c * 2 + x) * 2 + y) * line, line)
    my_rows = pl.ds(pl.multiple_of(my_line + z * piece, piece), piece)
    parts, cycle = 2, sems.shape[2]

    def half_of(s):
        return pl.ds(pl.multiple_of((s % parts) * half, half), half)

    def first(s):
        return pl.ds(pl.multiple_of((s % parts) * half, half), half // 2)

    def second(s):
        return pl.ds(pl.multiple_of((s % parts) * half + half // 2, half // 2), half // 2)

    def remote(src, dst, index, s, peer):
        return pltpu.make_async_remote_copy(
            src_ref=src,
            dst_ref=dst,
            send_sem=sems.at[0, index, s % cycle],
            recv_sem=sems.at[1, index, s % cycle],
            device_id=peer,
            device_id_type=mesh_id,
        )

    def own_copy(s):
        unit, cols_now = s // parts, half_of(s)
        return pltpu.make_async_copy(
            own_ref.at[unit, :, cols_now],
            out_ref.at[unit, my_rows, cols_now],
            own_sem.at[s % cycle],
        )

    def stage_z(s):
        unit, cols_now = s // parts, half_of(s)
        here, there = own_ref.at[unit, :, cols_now], out_ref.at[unit, my_rows, cols_now]
        return [remote(here, there, k, s, to_z[k]) for k in range(3)]

    def stage_one(s):
        unit, rows = s // parts, pl.ds(my_line, line)
        one, two = out_ref.at[unit, rows, first(s)], out_ref.at[unit, rows, second(s)]
        return [remote(one, one, 3, s, to_y), remote(two, two, 4, s, to_x)]

    def stage_two(s):
        unit = s // parts
        rows = pl.ds(pl.multiple_of((c * 2 + x) * plane, plane), plane)
        one = out_ref.at[unit, rows, first(s)]
        copies = [remote(one, one, 5, s, to_x)]
        for i in range(2):
            rows = pl.ds(pl.multiple_of(((c * 2 + i) * 2 + y) * line, line), line)
            two = out_ref.at[unit, rows, second(s)]
            copies.append(remote(two, two, 6 + i, s, to_y))
        return copies

    def stage_core(s):
        rows = pl.ds(pl.multiple_of(c * 2 * plane, 2 * plane), 2 * plane)
        there = out_ref.at[s // parts, rows, half_of(s)]
        return [remote(there, there, 8, s, to_core)]

    stages = (stage_z, stage_one, stage_two, stage_core)

    def unit_copy(unit):
        slot = unit % 2
        return pltpu.make_async_copy(out_ref.at[unit], unit_buf.at[slot], unit_sem.at[slot])

    def save(number, layer, block=None):
        src, dst, sem = bufs[number], saved[number].at[layer], save_sem.at[number, 0]
        if block is not None:
            src, dst, sem = src.at[block], dst.at[block], save_sem.at[number, block]
        return pltpu.make_async_copy(src, dst, sem)

    def free(numbers, layer, block=None):
        @pl.when(layer > 0)
        def _():
            for number in numbers:
                save(number, layer - 1, block).wait()

    def heads(start, stop):
        def one(pair, carry):
            attend_pair(
                pair, mixed_buf.at[0], mixed_buf.at[1], mixed_buf.at[2], mask_buf, ctx_buf, lse_buf
            )
            return carry

        lax.fori_loop(start, stop, one, 0)

    tall = rows // parts
    pairs = width // LANES

    def compute(unit, turn):
        layer, j = unit // per_layer, unit % per_layer
        matrix = unit_buf.at[unit % 2]
        mine = pl.ds(pl.multiple_of(turn * tall, tall), tall)

        def small(i):
            return row_ref[layer, i : i + 1, :]

        def bias(i):
            return bias_buf[pl.ds(layer * (2 + blocks) + i, 1), :]

        def over_rows(body):
            def one(tile, carry):
                body(pl.ds(pl.multiple_of(turn * tall + tile * NORM_ROWS, NORM_ROWS), NORM_ROWS))
                return carry

            lax.fori_loop(0, tall // NORM_ROWS, one, 0)

        @pl.when((j == 0) & (turn == 0))
        def _():
            free((0, 1), layer)

            @pl.when(layer == 0)
            def _():
                x_buf[...] = hidden_ref[...].astype(jnp.float32)

            low_buf[...] = x_buf[...].astype(jnp.bfloat16)
            save(0, layer).start()

        @pl.when(j < 3)
        def _():
            value = dot(low_buf[mine, :], matrix[...], ((1,), (0,)))
            value = value + jnp.where(j == 1, 0.0, bias(j // 2))
            scale = jnp.where(j == 0, HEAD_DIM ** (-0.5), 1.0)
            mixed_buf[j, mine, :] = (value * scale).astype(jnp.bfloat16)

        @pl.when((j == 2) & (turn == 1))
        def _():
            save(1, layer).start()
            free((2, 3), layer)
            heads(0, pairs // 4)

        @pl.when((j == 3) & (turn == 0))
        def _():
            heads(pairs // 4, 3 * pairs // 4)

        @pl.when((j == 3) & (turn == 1))
        def _():
            heads(3 * pairs // 4, pairs)
            save(2, layer).start()
            save(3, layer).start()
            total_buf[...] = dot(ctx_buf[...], matrix[...], ((1,), (1,)))
            free((4, 5, 6), layer)

            def body(tile, carry):
                part = pl.ds(pl.multiple_of(tile * NORM_ROWS, NORM_ROWS), NORM_ROWS)
                value = x_buf[part, :] + total_buf[part, :] + small(0)
                normed, scaled, inverse = norm_rows(value, small(2), small(3))
                normed_buf[part, :] = normed
                nb_buf[part, :] = normed.astype(jnp.bfloat16)
                one_buf[part, :] = scaled
                inv_one_buf[part, :] = jnp.broadcast_to(inverse, (NORM_ROWS, 128))
                return carry

            lax.fori_loop(0, rows // NORM_ROWS, body, 0)
            for number in (4, 5, 6):
                save(number, layer).start()

        @pl.when((j >= 4) & (j < 4 + blocks))
        def _():
            block = j - 4

            @pl.when(turn == 0)
            def _():
                free((7, 8), layer, block)

            value = dot(nb_buf[mine, :], matrix[...], ((1,), (0,)))
            act, slope = gelu_pair(value + bias(2 + block))
            act_buf[block, mine, :] = act.astype(jnp.bfloat16)
            slope_buf[block, mine, :] = slope.astype(jnp.bfloat16)

            @pl.when(turn == 1)
            def _():
                save(7, layer, block).start()
                save(8, layer, block).start()

        @pl.when(j >= 4 + blocks)
        def _():
            block = j - 4 - blocks
            part = dot(act_buf[block, mine, :], matrix[...], ((1,), (1,)))

            @pl.when(block == 0)
            def _():
                total_buf[mine, :] = part

            @pl.when(block > 0)
            def _():
                total_buf[mine, :] += part

        @pl.when(j == per_layer - 1)
        def _():
            @pl.when(turn == 0)
            def _():
                free((9, 10), layer)

            def body(part):
                value = normed_buf[part, :] + total_buf[part, :] + small(1)
                output, scaled, inverse = norm_rows(value, small(4), small(5))
                x_buf[part, :] = output
                two_buf[part, :] = scaled
                inv_two_buf[part, :] = jnp.broadcast_to(inverse, (NORM_ROWS, 128))

            over_rows(body)

            @pl.when(turn == 1)
            def _():
                save(9, layer).start()
                save(10, layer).start()

    steps = parts * units

    def step(s, carry):
        for number in range(len(stages), -1, -1):
            now = s - number * LAG

            if number == 0:
                for turn in range(rounds):
                    last = turn == rounds - 1
                    due = (s == parts * turn) | (last & (s > parts * turn) & (s % parts == 0))

                    @pl.when(due & (s < steps))
                    def _(turn=turn):
                        @pl.when(s == parts * turn)
                        def _():
                            finish_round(turn)

                        if turn + 2 < rounds:
                            start_round(turn + 2)
                        pick(s // parts, turn + 1)

            @pl.when((now >= 0) & (now < steps))
            def _(now=now, number=number):
                if number == 0:
                    own_copy(now).start()
                else:
                    if number == 1:
                        own_copy(now).wait()
                    for copy in stages[number - 1](now):
                        copy.wait()
                if number < len(stages):
                    for copy in stages[number](now):
                        copy.start()
                else:

                    @pl.when(now % parts == parts - 1)
                    def _():
                        unit_copy(now // parts).start()

        @pl.when(s == len(stages) * LAG)
        def _():
            for copy in column_copies():
                copy.wait()
            for j in range(4):
                bias_buf[:, j * cols : (j + 1) * cols] = col_got[j]

        done = s - len(stages) * LAG - parts

        @pl.when(done >= 0)
        def _():
            @pl.when(done % parts == 0)
            def _():
                unit_copy(done // parts).wait()

            compute(done // parts, done % parts)

        return carry

    fill_mask(mask_buf, docs_col_ref, docs_row_ref)
    lax.fori_loop(0, steps + len(stages) * LAG + parts, step, 0)
    final_ref[...] = x_buf[...]
    last = LAYERS - 1
    for number in (0, 1, 2, 3, 4, 5, 6, 9, 10):
        save(number, last).wait()
    for block in range(blocks):
        save(7, last, block).wait()
        save(8, last, block).wait()


def forward(unit_slot, masters, hidden_in, docs, col_now, row_now, piece, owners):
    units = unit_slot.shape[0]
    rounds, width, cols = masters.shape
    rows = hidden_in.shape[0]
    blocks = (units // LAYERS - 4) // 2
    low, full = jnp.bfloat16, jnp.float32
    kept = [
        ((rows, width), low),
        ((3, rows, width), low),
        ((rows, width), low),
        ((width // HEAD_DIM, 1, rows), full),
        ((rows, width), full),
        ((rows, 128), full),
        ((rows, width), low),
        ((blocks, rows, width), low),
        ((blocks, rows, width), low),
        ((rows, width), full),
        ((rows, 128), full),
    ]
    any_spec = pl.BlockSpec(memory_space=pl.ANY)
    vmem_spec = pl.BlockSpec(memory_space=pltpu.VMEM)
    smem_spec = pl.BlockSpec(memory_space=pltpu.SMEM)
    dma = pltpu.SemaphoreType.DMA
    return pl.pallas_call(
        forward_kernel,
        out_shape=[
            jax.ShapeDtypeStruct((units, width, width), low),
            jax.ShapeDtypeStruct((rows, width), full),
            jax.ShapeDtypeStruct((rounds * (owners + 2),), jnp.int32),
        ]
        + [jax.ShapeDtypeStruct((LAYERS,) + shape, dtype) for shape, dtype in kept],
        in_specs=[smem_spec] + [any_spec] + [vmem_spec] * 5,
        out_specs=[any_spec, vmem_spec, smem_spec] + [any_spec] * len(kept),
        scratch_shapes=[pltpu.VMEM(shape, dtype) for shape, dtype in kept]
        + [
            pltpu.VMEM((rows, width), full),
            pltpu.VMEM((rows, width), full),
            pltpu.VMEM((rows, width), full),
            pltpu.VMEM((rows, rows), full),
            pltpu.VMEM((2, width, width), low),
            pltpu.VMEM((units, piece, width), low),
            dma((8,)),
            dma((2, 9, 8)),
            dma((2,)),
            dma((len(kept), blocks)),
            dma((rounds,)),
            dma((2, rounds)),
            pltpu.VMEM((rounds, width, cols), full),
            pltpu.VMEM((rounds, width, cols), low),
            pltpu.VMEM((4,) + col_now.shape, full),
            pltpu.VMEM((col_now.shape[0], width), full),
            dma((rounds,)),
            dma((2, 3)),
            pltpu.SMEM((units,), jnp.int32),
            pltpu.SMEM((units,), jnp.int32),
        ]
        + [pltpu.VMEM((width // piece, piece, cols), low)] * rounds,
        compiler_params=pltpu.CompilerParams(
            collective_id=2, has_side_effects=True, vmem_limit_bytes=60 * 1024 * 1024
        ),
        name="gather_forward",
    )(
        unit_slot,
        masters,
        hidden_in,
        docs[:, None],
        docs[None, :],
        col_now,
        row_now,
    )


def run_general(
    unit_slot,
    masters,
    first_moment,
    second_moment,
    hidden_in,
    doc_ids,
    column_state,
    row_state,
    out_grad,
):
    slot_count, width, col_width = masters.shape
    units = unit_slot.shape[0]
    dp_size = lax.axis_size("dp")
    devices = dp_size * lax.axis_size("tensor")
    slots = slot_count * dp_size
    piece = width // devices
    per_layer = units // LAYERS
    blocks = (per_layer - 4) // 2
    tensor_size = lax.axis_size("tensor")
    rows = hidden_in.shape[0]
    seq_len = doc_ids.shape[1]
    heads = width // HEAD_DIM
    share = seq_len // rows
    tensor_index = lax.axis_index("tensor")
    groups = [list(range(i, i + share)) for i in range(0, tensor_size, share)]
    score_scale = HEAD_DIM ** (-0.5)
    sent = masters.astype(jnp.bfloat16).reshape(slot_count, devices, piece, col_width)
    spread = lax.all_to_all(sent.transpose(1, 0, 2, 3), BOTH, 0, 0)
    spread = spread.reshape(dp_size, tensor_size, slot_count, piece, col_width)
    spread = spread.transpose(0, 2, 3, 1, 4).reshape(slots, piece, width)
    mine = spread[unit_slot]
    weights = jnp.concatenate(
        [
            lax.all_gather(
                mine[layer * per_layer : (layer + 1) * per_layer], BOTH, axis=1, tiled=True
            )
            for layer in range(LAYERS)
        ],
        axis=0,
    )

    def matrices(layer):
        unit = weights[layer * per_layer : (layer + 1) * per_layer]
        return (unit[:3], unit[3], unit[4 : 4 + blocks], unit[4 + blocks :])

    row_docs = lax.dynamic_slice_in_dim(doc_ids, tensor_index // share, 1, axis=0)[0]
    my_docs = lax.dynamic_slice_in_dim(row_docs, (tensor_index % share) * rows, rows)
    same_doc = (my_docs[:, None] == row_docs[None, :])[None]

    def whole_row(value):
        if share == 1:
            return value
        return lax.all_gather(value, "tensor", axis=0, tiled=True, axis_index_groups=groups)

    def own_rows(value):
        if share == 1:
            return value
        return lax.psum_scatter(
            value, "tensor", scatter_dimension=0, tiled=True, axis_index_groups=groups
        )

    col_full = lax.all_gather(column_state[0], "tensor", axis=2, tiled=True)
    hidden = hidden_in.astype(jnp.float32)
    saved_layers = []
    for layer in range(LAYERS):
        w_qkv, w_proj, w_in, w_out = matrices(layer)
        row_now = row_state[0, layer]
        col_now = col_full[layer]
        hidden_bf = hidden.astype(jnp.bfloat16)
        query, key, value = (dot(hidden_bf, w_qkv[i], ((1,), (0,))) for i in range(3))
        query = ((query + col_now[0]) * score_scale).astype(jnp.bfloat16)
        key = key.astype(jnp.bfloat16)
        value = (value + col_now[1]).astype(jnp.bfloat16)
        query = query.reshape(rows, heads, HEAD_DIM)
        key = whole_row(key).reshape(seq_len, heads, HEAD_DIM)
        value = whole_row(value).reshape(seq_len, heads, HEAD_DIM)
        scores = jnp.einsum("qhd,khd->hqk", query, key, preferred_element_type=jnp.float32)
        scores = jnp.where(same_doc, scores, -1e30)
        row_top = jnp.max(scores, axis=-1, keepdims=True)
        log_total = row_top + jnp.log(
            jnp.sum(jnp.exp(scores - row_top), axis=-1, keepdims=True)
        )
        soft_bf = jnp.exp(scores - log_total).astype(jnp.bfloat16)
        context = jnp.einsum("hqk,khd->qhd", soft_bf, value, preferred_element_type=jnp.float32)
        context = context.reshape(rows, width).astype(jnp.bfloat16)
        attended = dot(context, w_proj, ((1,), (1,)))
        normed, scaled_one, inverse_one = norm_forward(
            hidden + attended + row_now[0], row_now[2], row_now[3]
        )
        normed_bf = normed.astype(jnp.bfloat16)
        pre_act = jnp.einsum("rd,bdc->brc", normed_bf, w_in, preferred_element_type=jnp.float32)
        activated, slope = gelu_pair(pre_act + col_now[2:, None])
        activated = activated.astype(jnp.bfloat16)
        slope = slope.astype(jnp.bfloat16)
        mlp_out = jnp.einsum(
            "brc,bdc->rd", activated, w_out, preferred_element_type=jnp.float32
        )
        output, scaled_two, inverse_two = norm_forward(
            normed + mlp_out + row_now[1], row_now[4], row_now[5]
        )
        saved_layers.append(
            (hidden_bf, query, key, value, log_total, context, scaled_one, inverse_one, normed_bf)
            + (slope, activated, scaled_two, inverse_two)
        )
        hidden = output
    upstream = out_grad.astype(jnp.float32)
    operands = [None] * LAYERS
    col_parts = [None] * LAYERS
    row_parts = [None] * LAYERS
    for layer in reversed(range(LAYERS)):
        w_qkv, w_proj, w_in, w_out = matrices(layer)
        row_now = row_state[0, layer]
        (
            hidden_bf,
            query,
            key,
            value,
            log_total,
            context,
            scaled_one,
            inverse_one,
            normed_bf,
            slope,
            activated,
            scaled_two,
            inverse_two,
        ) = saved_layers[layer]
        d_two, gain_two, shift_two = norm_backward(upstream, scaled_two, inverse_two, row_now[4])
        grad_bias_two = jnp.sum(d_two, axis=0)
        d_two_bf = d_two.astype(jnp.bfloat16)
        d_act = jnp.einsum("rd,bdc->brc", d_two_bf, w_out, preferred_element_type=jnp.float32)
        d_pre = (d_act * slope).astype(jnp.bfloat16)
        grad_bias_in = jnp.sum(d_pre, axis=1, dtype=jnp.float32)
        d_normed = jnp.einsum("brc,bdc->rd", d_pre, w_in, preferred_element_type=jnp.float32)
        d_normed = d_two + d_normed
        d_one, gain_one, shift_one = norm_backward(d_normed, scaled_one, inverse_one, row_now[2])
        grad_bias_proj = jnp.sum(d_one, axis=0)
        d_one_bf = d_one.astype(jnp.bfloat16)
        d_context = dot(d_one_bf, w_proj, ((1,), (0,))).astype(jnp.bfloat16)
        d_context = d_context.reshape(rows, heads, HEAD_DIM)
        scores = jnp.einsum("qhd,khd->hqk", query, key, preferred_element_type=jnp.float32)
        scores = jnp.where(same_doc, scores, -1e30)
        soft = jnp.exp(scores - log_total)
        d_values = jnp.einsum(
            "hqk,qhd->khd",
            soft.astype(jnp.bfloat16),
            d_context,
            preferred_element_type=jnp.float32,
        )
        d_probs = jnp.einsum(
            "qhd,khd->hqk", d_context, value, preferred_element_type=jnp.float32
        )
        d_scores = (
            soft * (d_probs - jnp.sum(soft * d_probs, axis=-1, keepdims=True))
        ).astype(jnp.bfloat16)
        d_queries = (
            jnp.einsum("hqk,khd->qhd", d_scores, key, preferred_element_type=jnp.float32)
            * score_scale
        )
        d_keys = jnp.einsum("hqk,qhd->khd", d_scores, query, preferred_element_type=jnp.float32)
        d_qkv = jnp.stack(
            [
                d_queries.reshape(rows, width),
                own_rows(d_keys.reshape(seq_len, width)),
                own_rows(d_values.reshape(seq_len, width)),
            ]
        ).astype(jnp.bfloat16)
        grad_bias_qkv = jnp.sum(d_qkv, axis=1, dtype=jnp.float32)
        upstream = d_one + jnp.einsum(
            "brc,bdc->rd", d_qkv, w_qkv, preferred_element_type=jnp.float32
        )
        operands[layer] = (hidden_bf, d_one_bf, normed_bf, d_two_bf)
        operands[layer] += (d_qkv, context[None], d_pre, activated)
        col_parts[layer] = jnp.concatenate(
            [
                grad_bias_qkv[0:1],
                grad_bias_qkv[2:3],
                grad_bias_in,
            ],
            axis=0,
        )
        row_parts[layer] = jnp.stack(
            [grad_bias_proj, grad_bias_two, gain_one, shift_one, gain_two, shift_two]
        )
    small = jnp.stack([jnp.stack(col_parts), jnp.stack(row_parts)])
    summed = []
    for layer in operands:
        whole = jnp.concatenate(
            [
                jnp.einsum(
                    "rd,brc->bdc", layer[i], layer[4 + i], preferred_element_type=jnp.float32
                )
                for i in range(4)
            ],
            axis=0,
        )
        summed.append(
            lax.psum_scatter(whole.astype(jnp.bfloat16), BOTH, scatter_dimension=1, tiled=True)
        )
    summed = jnp.concatenate(summed, axis=0)

    slot_ids = jnp.arange(slots, dtype=jnp.int32)
    named = unit_slot[None, :] == slot_ids[:, None]
    holds = jnp.any(named, axis=1)
    unit_of = jnp.argmax(named, axis=1)
    back = jnp.where(holds[:, None, None], summed[unit_of], jnp.zeros((), jnp.bfloat16))
    back = back.reshape(dp_size, slot_count, piece, tensor_size, col_width)
    back = back.transpose(0, 3, 1, 2, 4).reshape(devices, slot_count, piece, col_width)
    owned = lax.all_to_all(back, BOTH, 0, 0)
    owned = owned.transpose(1, 0, 2, 3)
    owned = owned.reshape(slot_count, width, col_width)
    occupied = lax.dynamic_slice_in_dim(holds, lax.axis_index("dp") * slot_count, slot_count)
    occupied = occupied.astype(jnp.float32)[:, None, None]
    new_master, new_first, new_second = adamw_update(
        masters, owned.astype(jnp.float32), first_moment, second_moment, RATE_UNITS
    )
    updated = (
        new_master * occupied,
        jnp.stack([new_first * occupied, new_second * occupied]),
    )
    return (hidden, upstream, updated, lax.psum(small, BOTH))


def adamw_kernel(table_ref, owned_ref, value_ref, first_ref, second_ref, value_out, state_out):
    taken = table_ref[table_ref.shape[0] - pl.num_programs(0) + pl.program_id(0)] > 0
    gradient = jnp.where(taken, owned_ref[0].astype(jnp.float32), 0.0)
    value, first, second = adamw_update(
        value_ref[0], gradient, first_ref[0], second_ref[0], RATE_UNITS
    )
    value_out[0] = jnp.where(taken, value, 0.0)
    state_out[0, 0] = jnp.where(taken, first, 0.0)
    state_out[1, 0] = jnp.where(taken, second, 0.0)


def adamw_slots(table, owned, masters, first_moment, second_moment):
    count, width, cols = masters.shape
    tall = width // 2
    at = table.shape[0] - 2 * count
    tile = pl.BlockSpec((1, tall, cols), lambda i, j, table: (i, j, 0))
    return pl.pallas_call(
        adamw_kernel,
        grid_spec=pltpu.PrefetchScalarGridSpec(
            num_scalar_prefetch=1,
            grid=(count, width // tall),
            in_specs=[
                pl.BlockSpec((1, tall, cols), lambda i, j, table: (table[at + i], j, 0)),
                tile,
                tile,
                tile,
            ],
            out_specs=(tile, pl.BlockSpec((2, 1, tall, cols), lambda i, j, table: (0, i, j, 0))),
        ),
        out_shape=(
            jax.ShapeDtypeStruct(masters.shape, jnp.float32),
            jax.ShapeDtypeStruct((2,) + masters.shape, jnp.float32),
        ),
        name="adamw",
    )(table, owned, masters, first_moment, second_moment)


def run_kernels(
    unit_slot,
    masters,
    first_moment,
    second_moment,
    hidden_in,
    doc_ids,
    column_state,
    row_state,
    out_grad,
):
    slot_count, width, cols = masters.shape
    blocks = (unit_slot.shape[0] // LAYERS - 4) // 2
    dp_size = lax.axis_size("dp")
    piece = width // (dp_size * lax.axis_size("tensor"))
    docs = lax.dynamic_index_in_dim(doc_ids, lax.axis_index("tensor"), 0, keepdims=False)
    row_now = row_state[0]
    weights, hidden, table, *saved = forward(
        unit_slot,
        masters,
        hidden_in,
        docs,
        column_state[0].reshape(-1, cols),
        row_now,
        piece,
        dp_size,
    )
    upstream, owned, small = backward(table, out_grad, docs, row_now, weights, saved, piece, cols)
    slots = adamw_slots(
        table, owned.reshape(masters.shape), masters, first_moment, second_moment
    )
    return (hidden, upstream, slots, small.reshape(2, LAYERS, 2 + blocks, width))


def local(
    hidden_in,
    doc_ids,
    unit_slot,
    masters,
    first_moment,
    second_moment,
    column_state,
    row_state,
    out_grad,
):
    col_width = masters.shape[2]
    tensor_index = lax.axis_index("tensor")
    kernels = (lax.axis_size("dp"), lax.axis_size("tensor")) == (8, 4)
    kernels = kernels and hidden_in.shape[0] == doc_ids.shape[1]
    run = run_kernels if kernels else run_general
    hidden, upstream, (unit_master, unit_state), small = run(
        unit_slot,
        masters,
        first_moment,
        second_moment,
        hidden_in,
        doc_ids,
        column_state,
        row_state,
        out_grad,
    )
    row_total = small[1]
    col_total = lax.dynamic_slice_in_dim(small[0], tensor_index * col_width, col_width, axis=2)
    new_col, col_first, col_second = adamw_update(
        column_state[0], col_total, column_state[1], column_state[2], RATE_SMALL
    )
    column_out = jnp.stack([col_total, new_col, col_first, col_second])
    new_row, row_first, row_second = adamw_update(
        row_state[0], row_total, row_state[1], row_state[2], RATE_SMALL
    )
    row_out = jnp.stack([row_total, new_row, row_first, row_second])
    return (hidden, upstream, unit_master, unit_state, column_out, row_out)


def solution(mesh):
    return jax.shard_map(
        local,
        mesh=mesh,
        in_specs=(
            P(("dp", "tensor"), None),
            P("dp", None),
            P(),
            P("dp", None, "tensor"),
            P("dp", None, "tensor"),
            P("dp", None, "tensor"),
            P(None, None, None, "tensor"),
            P(),
            P(("dp", "tensor"), None),
        ),
        out_specs=(
            P(("dp", "tensor"), None),
            P(("dp", "tensor"), None),
            P("dp", None, "tensor"),
            P(None, "dp", None, "tensor"),
            P(None, None, None, "tensor"),
            P(),
        ),
        check_vma=False,
    )
```

```python
import math

import jax
import jax.numpy as jnp
from jax import lax
from jax.experimental import pallas as pl
from jax.experimental.pallas import tpu as pltpu
from jax.sharding import PartitionSpec as P

HEAD_DIM = 64
LAYERS = 2
STEP = 3

EPS_NORM = 1e-06
RATE_UNITS = 0.05
RATE_SMALL = 0.2
WEIGHT_DECAY = 0.01
ADAM_EPS = 1e-08
BETA_MOMENT = 0.5
BOTH = ("dp", "tensor")


def norm_forward(summed, gain, shift):
    row_mean = jnp.mean(summed, axis=1, keepdims=True)
    centred = summed - row_mean
    inverse = lax.rsqrt(jnp.mean(centred * centred, axis=1, keepdims=True) + EPS_NORM)
    scaled = centred * inverse
    return (scaled * gain + shift, scaled, inverse)


def norm_backward(upstream, scaled, inverse, gain):
    d_scaled = upstream * gain
    mean_one = jnp.mean(d_scaled, axis=1, keepdims=True)
    mean_two = jnp.mean(d_scaled * scaled, axis=1, keepdims=True)
    grad_input = inverse * (d_scaled - mean_one - scaled * mean_two)
    return (grad_input, jnp.sum(upstream * scaled, axis=0), jnp.sum(upstream, axis=0))


def gelu_pair(v):
    cdf = 0.5 * (1.0 + lax.erf(v * 2.0 ** (-0.5)))
    bell = jnp.exp(-0.5 * v * v) * (2.0 * math.pi) ** (-0.5)
    return (v * cdf, cdf + v * bell)


def adamw_update(old_value, gradient, first_old, second_old, learn_rate):
    first_new = BETA_MOMENT * first_old + (1.0 - BETA_MOMENT) * gradient
    second_new = BETA_MOMENT * second_old + (1.0 - BETA_MOMENT) * gradient * gradient
    correct = 1.0 - BETA_MOMENT**STEP
    step_size = first_new / correct / (jnp.sqrt(second_new / correct) + ADAM_EPS)
    return (old_value - learn_rate * (step_size + WEIGHT_DECAY * old_value), first_new, second_new)


def dot(left, right, dims):
    return lax.dot_general(left, right, (dims, ((), ())), preferred_element_type=jnp.float32)


LANES = 2 * HEAD_DIM


def head_lanes(value, head):
    lane = lax.broadcasted_iota(jnp.int32, value.shape, 1)
    keep = lane < HEAD_DIM if head == 0 else lane >= HEAD_DIM
    return jnp.where(keep, value, jnp.zeros_like(value))


def pair_lanes(first, second):
    lane = lax.broadcasted_iota(jnp.int32, first.shape, 1)
    return jnp.where(lane < HEAD_DIM, first, second)


def attend_pair(pair, q_ref, k_ref, v_ref, mask_ref, ctx_ref, lse_ref):
    lanes = pl.ds(pl.multiple_of(pair * LANES, LANES), LANES)
    query, key, value = q_ref[:, lanes], k_ref[:, lanes], v_ref[:, lanes]
    value_t = value.T
    parts = []
    for head in range(2):
        scores = dot(head_lanes(key, head), query, ((1,), (1,))) + mask_ref[...]
        top = jnp.max(scores, axis=0, keepdims=True)
        weight = jnp.exp(scores - top)
        total = jnp.sum(weight, axis=0, keepdims=True)
        lse_ref[pair * 2 + head] = top + jnp.log(total)
        mine = value_t[head * HEAD_DIM : (head + 1) * HEAD_DIM]
        mixed = dot(mine, weight.astype(jnp.bfloat16), ((1,), (0,)))
        parts.append(mixed * (1.0 / total))
    ctx_ref[:, lanes] = jnp.concatenate(parts, axis=0).T.astype(ctx_ref.dtype)


def attend_back_pair(pair, q_ref, k_ref, v_ref, d_ref, mask_ref, lse_ref, dq_ref, dk_ref, dv_ref):
    lanes = pl.ds(pl.multiple_of(pair * LANES, LANES), LANES)
    query, key, value = q_ref[:, lanes], k_ref[:, lanes], v_ref[:, lanes]
    grad = d_ref[:, lanes]
    key_t = key.T
    parts, d_keys, d_values = [], [], []
    for head in range(2):
        scores = dot(head_lanes(key, head), query, ((1,), (1,))) + mask_ref[...]
        soft = jnp.exp(scores - lse_ref[pair * 2 + head])
        d_values.append(dot(soft.astype(jnp.bfloat16), grad, ((1,), (0,))))
        d_soft = dot(head_lanes(value, head), grad, ((1,), (1,)))
        both = soft * d_soft
        mean = jnp.sum(both, axis=0, keepdims=True)
        d_scores = (both - soft * mean).astype(jnp.bfloat16)
        d_keys.append(dot(d_scores, query, ((1,), (0,))))
        mine = key_t[head * HEAD_DIM : (head + 1) * HEAD_DIM]
        parts.append(dot(mine, d_scores, ((1,), (0,))))
    scale = HEAD_DIM ** (-0.5)
    dq_ref[:, lanes] = (jnp.concatenate(parts, axis=0).T * scale).astype(dq_ref.dtype)
    dk_ref[:, lanes] = pair_lanes(*d_keys).astype(dk_ref.dtype)
    dv_ref[:, lanes] = pair_lanes(*d_values).astype(dv_ref.dtype)


def fill_mask(mask_ref, docs_col_ref, docs_row_ref):
    same = docs_col_ref[...] == docs_row_ref[...]
    mask_ref[...] = jnp.where(same, 0.0, -1e30).astype(jnp.float32)


LAG = 2


def spread_order(z, y, x, c):
    return ((c * 2 + x) * 2 + y) * 4 + z


def every_other(z, y, x, c, body):
    for step in (2, 1, 3, 0):

        def one(i, carry, step=step):
            body((z + step) % 4, (y + i // 4) % 2, (x + (i // 2) % 2) % 2, (c + i % 2) % 2)
            return carry

        lax.fori_loop(1 if step == 0 else 0, 8, one, 0)


def greet_all(z, y, x, c):
    barrier = pltpu.get_barrier_semaphore()

    def greet(zz, yy, xx, cc):
        pl.semaphore_signal(
            barrier,
            inc=1,
            device_id=(zz * 2 + yy, xx * 2 + cc),
            device_id_type=pl.DeviceIdType.MESH,
        )

    every_other(z, y, x, c, greet)
    return barrier


TILE = 256


def norm_back_rows(upstream, scaled, inverse, gain):
    d_scaled = upstream * gain
    mean_one = jnp.mean(d_scaled, axis=1, keepdims=True)
    mean_two = jnp.mean(d_scaled * scaled, axis=1, keepdims=True)
    return inverse * (d_scaled - mean_one - scaled * mean_two)


def backward_kernel(
    pick_ref,
    out_grad_ref,
    docs_col_ref,
    docs_row_ref,
    row_ref,
    weights_ref,
    low_ref,
    mixed_ref,
    ctx_ref,
    lse_ref,
    one_ref,
    inv_one_ref,
    normed_ref,
    act_ref,
    slope_ref,
    two_ref,
    inv_two_ref,
    owned_ref,
    total_ref,
    small_out,
    out_ref,
    back_buf,
    left_buf,
    right_buf,
    unit_buf,
    scaled_buf,
    inv_buf,
    slope_buf,
    mixed_buf,
    lse_buf,
    mask_buf,
    d_ctx_buf,
    core_out,
    core_in,
    sum_core,
    first_in,
    sum_first,
    second_in,
    sum_second,
    z_in,
    small_sum,
    small_got,
    load_sem,
    core_sems,
    first_sems,
    second_sems,
    z_sems,
    small_sems,
    own_sems,
    round_sems,
):
    units, piece, width = out_ref.shape
    rows = total_ref.shape[0]
    per_layer = units // LAYERS
    blocks = (per_layer - 4) // 2
    at_out, at_query = 2 * blocks, 2 * blocks + 1
    dp, tensor = lax.axis_index("dp"), lax.axis_index("tensor")
    z, y, x, c = dp // 2, dp % 2, tensor // 2, tensor % 2
    half, parts = width // 2, 2
    side_cols = half // 2
    quarter, eighth = half // 2, half // 4
    to_core = (dp, x * 2 + 1 - c)
    to_x = (dp, (1 - x) * 2 + c)
    to_y = (z * 2 + 1 - y, tensor)
    to_z = [(((z + k) % 4) * 2 + y, tensor) for k in (1, 2, 3)]
    to_z1 = ((z + 1 - 2 * (z % 2)) * 2 + y, tensor)
    to_z2 = (((z + 2) % 4) * 2 + y, tensor)
    mesh_id = pl.DeviceIdType.MESH

    barrier = greet_all(z, y, x, c)

    def remote(src, dst, sems, send, recv, peer):
        return pltpu.make_async_remote_copy(
            src_ref=src,
            dst_ref=dst,
            send_sem=sems.at[send],
            recv_sem=sems.at[recv],
            device_id=peer,
            device_id_type=mesh_id,
        )

    def place(s):
        return LAYERS - 1 - s // per_layer, s % per_layer

    def unit_of(s):
        layer, j = place(s)
        feed = jnp.where(j % 2 == 0, 4 + blocks + j // 2, 4 + j // 2)
        return layer * per_layer + jnp.where(
            j < at_out, feed, jnp.where(j == at_out, 3, j - at_query)
        )

    def left_of(s):
        j = s % per_layer
        feed = jnp.where(j % 2 == 0, 3, 2)
        return jnp.where(j < at_out, feed, jnp.where(j == at_out, 1, 0))

    def loaded_slot(s):
        return ((s // per_layer) * (blocks + 1) + (s % per_layer) // 2) % 2

    def right_of(s):
        j = s % per_layer
        feed = jnp.where(j % 2 == 0, loaded_slot(s), 2 + (j // 2) % 2)
        return jnp.where(
            j < at_out, feed, jnp.where(j == at_out, loaded_slot(s), 4 + j - at_query)
        )

    local = pltpu.make_async_copy

    def unit_load(s):
        return local(weights_ref.at[unit_of(s)], unit_buf.at[s % 3], load_sem.at[0, s % 3])

    def act_load(layer, block, slot):
        return local(act_ref.at[layer, block], right_buf.at[slot], load_sem.at[1, slot])

    def ctx_load(layer, slot):
        return local(ctx_ref.at[layer], right_buf.at[slot], load_sem.at[1, slot])

    def slope_load(layer, block):
        return local(slope_ref.at[layer, block], slope_buf, load_sem.at[2, 0])

    def norm_loads(layer, which):
        scaled, inv = ((one_ref, inv_one_ref), (two_ref, inv_two_ref))[which]
        return [
            local(scaled.at[layer], scaled_buf, load_sem.at[3, 0]),
            local(inv.at[layer], inv_buf, load_sem.at[3, 1]),
        ]

    def mixed_loads(layer):
        return [
            local(mixed_ref.at[layer], mixed_buf, load_sem.at[4, 0]),
            local(lse_ref.at[layer], lse_buf, load_sem.at[4, 1]),
        ]

    def normed_load(layer):
        return local(normed_ref.at[layer], left_buf.at[2], load_sem.at[2, 1])

    def low_load(layer):
        return local(low_ref.at[layer], left_buf.at[0], load_sem.at[5, 0])

    def begin(*copies):
        for copy in copies:
            copy.start()

    def finish(*copies):
        for copy in copies:
            copy.wait()

    def note(row, value):
        small_sum[0, pl.ds(row, 1), :] = value

    def column(layer, i):
        return layer * (2 + blocks) + i

    def row(layer, i):
        return LAYERS * (2 + blocks) + layer * 6 + i

    def norm_back(layer, gain_row, bias_row, low_slot):
        gain = row_ref[layer, gain_row : gain_row + 1, :]
        size = 128

        def one(tile, carry):
            part = pl.ds(pl.multiple_of(tile * size, size), size)
            upstream = total_ref[part, :]
            scaled = scaled_buf[part, :]
            inside = norm_back_rows(upstream, scaled, inv_buf[part, 0:1], gain)
            total_ref[part, :] = inside
            left_buf[low_slot, part, :] = inside.astype(jnp.bfloat16)
            sums = (upstream * scaled, upstream, inside)
            return tuple(a + jnp.sum(b, axis=0, keepdims=True) for a, b in zip(carry, sums))

        zero = jnp.zeros((1, width), jnp.float32)
        gains, shifts, biases = lax.fori_loop(0, rows // size, one, (zero, zero, zero))
        note(row(layer, gain_row), gains)
        note(row(layer, gain_row + 1), shifts)
        note(row(layer, bias_row), biases)

    def heads(start, stop):
        inputs = [mixed_buf.at[i] for i in range(3)]
        grads = [right_buf.at[4 + i] for i in range(3)]

        def one(pair, carry):
            attend_back_pair(pair, *inputs, d_ctx_buf, mask_buf, lse_buf, *grads)
            return carry

        lax.fori_loop(start, stop, one, 0)

    pairs = width // LANES

    def data_gradient(s):
        layer, j = place(s)
        matrix = unit_buf.at[s % 3]
        before = unit_buf.at[(s + 2) % 3]
        slot = loaded_slot(s)

        @pl.when(j == 0)
        def _():
            finish(*norm_loads(layer, 1))

            @pl.when(s == 0)
            def _():
                total_ref[...] = out_grad_ref[...].astype(jnp.float32)

            norm_back(layer, 4, 1, 3)
            begin(*norm_loads(layer, 0), *mixed_loads(layer))

        @pl.when(j == 1)
        def _():
            finish(normed_load(layer))
            begin(low_load(layer))

        @pl.when((j < at_out) & (j % 2 == 0))
        def _():
            block = j // 2
            finish(slope_load(layer, block), act_load(layer, block, slot))

            @pl.when(block < blocks - 1)
            def _():
                act_load(layer, block + 1, 1 - slot).start()

            @pl.when(block == blocks - 1)
            def _():
                ctx_load(layer, 1 - slot).start()

            d_act = dot(left_buf[3], matrix[...], ((1,), (0,)))
            d_pre = (d_act * slope_buf[...].astype(jnp.float32)).astype(jnp.bfloat16)
            right_buf[2 + block % 2] = d_pre
            sums = jnp.sum(d_pre.astype(jnp.float32), axis=0, keepdims=True)
            note(column(layer, 2 + block), sums)

            @pl.when(block < blocks - 1)
            def _():
                slope_load(layer, block + 1).start()

        @pl.when((j < at_out) & (j % 2 == 1))
        def _():
            total_ref[...] += dot(right_buf[2 + (j // 2) % 2], matrix[...], ((1,), (1,)))

        @pl.when(j == at_out)
        def _():
            finish(*norm_loads(layer, 0), *mixed_loads(layer), ctx_load(layer, slot))
            norm_back(layer, 2, 0, 1)

            @pl.when(layer > 0)
            def _():
                act_load(layer - 1, 0, 1 - slot).start()
                begin(*norm_loads(layer - 1, 1))
                slope_load(layer - 1, 0).start()

            d_ctx_buf[...] = dot(left_buf[1], matrix[...], ((1,), (0,))).astype(jnp.bfloat16)

        @pl.when(j == at_query)
        def _():
            finish(low_load(layer))

            @pl.when(layer > 0)
            def _():
                normed_load(layer - 1).start()

            heads(3 * pairs // 8, 5 * pairs // 8)

        @pl.when(j == at_query + 1)
        def _():
            total_ref[...] += dot(right_buf[4], before[...], ((1,), (1,)))

        @pl.when(j == at_query + 2)
        def _():
            total_ref[...] += dot(right_buf[6], matrix[...], ((1,), (1,)))

    def data_gradient_rest(s):
        layer, j = place(s)

        @pl.when(j == at_out)
        def _():
            heads(0, 3 * pairs // 8)

        @pl.when(j == at_query)
        def _():
            heads(5 * pairs // 8, pairs)

        @pl.when(j == at_query + 1)
        def _():
            total_ref[...] += dot(right_buf[5], unit_buf[s % 3], ((1,), (1,)))
            for i, number in ((0, 0), (2, 1)):
                sums = jnp.sum(right_buf[4 + i].astype(jnp.float32), axis=0, keepdims=True)
                note(column(layer, number), sums)

    def product(s, side, tile):
        unit = s // parts
        start = pl.multiple_of(side * half + tile * TILE, TILE)
        left = left_buf[left_of(unit), :, pl.ds(start, TILE)]
        right = right_buf[
            right_of(unit), :, pl.ds(pl.multiple_of((s % parts) * half, half), half)
        ]
        return lax.dot_general(
            left, right, (((0,), (0,)), ((), ())), preferred_element_type=jnp.float32
        )

    def core_copy(s):
        return remote(
            core_out.at[s % 2], core_in.at[s % 4], core_sems, (0, s % 2), (1, s % 4), to_core
        )

    def first_copies(s):
        here = sum_core.at[s % 3]
        return (
            remote(
                here.at[pl.ds(pl.multiple_of((1 - x) * quarter, quarter), quarter), pl.ds(0, side_cols)],
                first_in.at[s % 4, 0],
                first_sems,
                (0, 0, s % 3),
                (1, 0, s % 4),
                to_x,
            ),
            *(
                remote(
                    here.at[
                        pl.ds(pl.multiple_of(i * quarter + (1 - y) * eighth, eighth), eighth),
                        pl.ds(side_cols, side_cols),
                    ],
                    first_in.at[s % 4, 1, pl.ds(i * eighth, eighth)],
                    first_sems,
                    (0, 1 + i, s % 3),
                    (1, 1 + i, s % 4),
                    to_y,
                )
                for i in range(2)
            ),
        )

    def second_copies(s):
        here = sum_first.at[s % 3]
        return (
            remote(
                here.at[0, pl.ds(pl.multiple_of((1 - y) * eighth, eighth), eighth)],
                second_in.at[s % 4, 0],
                second_sems,
                (0, 0, s % 3),
                (1, 0, s % 4),
                to_y,
            ),
            remote(
                here.at[1, pl.ds(pl.multiple_of((1 - x) * eighth, eighth), eighth)],
                second_in.at[s % 4, 1],
                second_sems,
                (0, 1, s % 3),
                (1, 1, s % 4),
                to_x,
            ),
        )

    def z_copies(s):
        return [
            remote(
                sum_second.at[s % 3, pl.ds(pl.multiple_of(((z + k) % 4) * piece, piece), piece)],
                z_in.at[s % 4, k - 1],
                z_sems,
                (0, k - 1, s % 3),
                (1, k - 1, s % 4),
                to_z[k - 1],
            )
            for k in (1, 2, 3)
        ]

    small_peers = (to_core, to_x, to_y, to_z1, to_z2)

    def small_copy(stage):
        return remote(
            small_sum.at[stage],
            small_got.at[stage],
            small_sems,
            (0, stage),
            (1, stage),
            small_peers[stage],
        )

    rounds, owners = back_buf.shape[0], back_buf.shape[1]
    cols = owned_ref.shape[3]
    me = spread_order(z, y, x, c)

    def own_back(number):
        return local(
            back_buf.at[number, dp, :, pl.ds(pl.multiple_of(tensor * cols, cols), cols)],
            owned_ref.at[number, me],
            own_sems.at[number],
        )

    def send_back(number):
        def fill(owner, carry):
            back_buf[number, owner] = out_ref[pick_ref[number * owners + owner]]
            return carry

        lax.fori_loop(0, owners, fill, 0)
        own_back(number).start()

        def send(zz, yy, xx, cc):
            there = xx * 2 + cc
            remote(
                back_buf.at[
                    number, zz * 2 + yy, :, pl.ds(pl.multiple_of(there * cols, cols), cols)
                ],
                owned_ref.at[number, me],
                round_sems,
                (0, number),
                (1, number),
                (zz * 2 + yy, there),
            ).start()

        every_other(z, y, x, c, send)

    def finish_back(number):
        own_back(number).wait()
        most = owned_ref.at[number, pl.ds(0, 31)]
        remote(most, most, round_sems, (0, number), (1, number), to_core).wait()

    top = LAYERS - 1
    steps = parts * units
    begin(
        *norm_loads(top, 1),
        unit_load(jnp.int32(0)),
        slope_load(top, 0),
        act_load(top, 0, 0),
        normed_load(top),
    )
    fill_mask(mask_buf, docs_col_ref, docs_row_ref)
    pl.semaphore_wait(barrier, 31)

    def step(s, carry):
        last = s - 3 * LAG - 1

        @pl.when((last >= 0) & (last < steps))
        def _():
            for copy in z_copies(last):
                copy.wait()
            total = sum_second[last % 3, pl.ds(pl.multiple_of(z * piece, piece), piece), :].astype(
                jnp.float32
            )
            for k in range(3):
                total = total + z_in[last % 4, k].astype(jnp.float32)
            cols_now = pl.ds(pl.multiple_of((last % parts) * half, half), half)
            out_ref[unit_of(last // parts), :, cols_now] = total.astype(out_ref.dtype)

            @pl.when((last // parts >= units - rounds) & (last % parts == parts - 1))
            def _():
                send_back(last // parts - (units - rounds))

        third = s - 2 * LAG - 1

        @pl.when((third >= 0) & (third < steps))
        def _():
            for copy in second_copies(third):
                copy.wait()
            for part, side in ((0, y), (1, x)):
                mine = sum_first[
                    third % 3, part, pl.ds(pl.multiple_of(side * eighth, eighth), eighth), :
                ]
                total = mine.astype(jnp.float32) + second_in[third % 4, part].astype(jnp.float32)
                sum_second[third % 3, :, part * side_cols : (part + 1) * side_cols] = total.astype(
                    jnp.bfloat16
                )
            for copy in z_copies(third):
                copy.start()

        second = s - LAG - 1

        @pl.when((second >= 0) & (second < steps))
        def _():
            for copy in first_copies(second):
                copy.wait()
            mine = sum_core[
                second % 3, pl.ds(pl.multiple_of(x * quarter, quarter), quarter), 0:side_cols
            ]
            total = mine.astype(jnp.float32) + first_in[second % 4, 0].astype(jnp.float32)
            sum_first[second % 3, 0] = total.astype(jnp.bfloat16)
            for i in range(2):
                mine = sum_core[
                    second % 3,
                    pl.ds(pl.multiple_of(i * quarter + y * eighth, eighth), eighth),
                    side_cols : 2 * side_cols,
                ]
                part = pl.ds(i * eighth, eighth)
                total = mine.astype(jnp.float32) + first_in[second % 4, 1, part, :].astype(
                    jnp.float32
                )
                sum_first[second % 3, 1, part, :] = total.astype(jnp.bfloat16)
            for copy in second_copies(second):
                copy.start()

        @pl.when(s < steps)
        def _():
            unit = s // parts

            @pl.when(s % parts == 0)
            def _():
                unit_load(unit).wait()

                @pl.when(unit + 1 < units)
                def _():
                    unit_load(unit + 1).start()

                data_gradient(unit)

            @pl.when(s % parts == 1)
            def _():
                data_gradient_rest(unit)

            @pl.when(s >= 2)
            def _():
                core_copy(s - 2).wait_send()

            def one(tile, carry):
                part = pl.ds(pl.multiple_of(tile * TILE, TILE), TILE)
                core_out[s % 2, part, :] = product(s, 1 - c, tile).astype(jnp.bfloat16)
                return carry

            lax.fori_loop(0, half // TILE, one, 0)
            core_copy(s).start()

        first = s - 1

        @pl.when((first >= 0) & (first < steps))
        def _():
            core_copy(first).wait_recv()

            def one(tile, carry):
                part = pl.ds(pl.multiple_of(tile * TILE, TILE), TILE)
                total = product(first, c, tile) + core_in[first % 4, part, :].astype(jnp.float32)
                sum_core[first % 3, part, :] = total.astype(jnp.bfloat16)
                return carry

            lax.fori_loop(0, half // TILE, one, 0)
            for copy in first_copies(first):
                copy.start()

        for stage in range(6):

            @pl.when(s == steps + stage)
            def _(stage=stage):
                if stage > 0:
                    small_copy(stage - 1).wait()
                    total = small_sum[stage - 1] + small_got[stage - 1]
                    if stage < 5:
                        small_sum[stage] = total
                    else:
                        small_out[...] = total
                if stage < 5:
                    small_copy(stage).start()

        return carry

    lax.fori_loop(0, steps + 3 * LAG + 1, step, 0)
    for s in (steps - 2, steps - 1):
        core_copy(s).wait_send()
    for number in range(rounds):
        finish_back(number)


def backward(pick, out_grad, docs, row_now, weights, saved, piece, cols):
    units, width, _ = weights.shape
    rows = out_grad.shape[0]
    blocks = (units // LAYERS - 4) // 2
    half = width // 2
    low, full = jnp.bfloat16, jnp.float32
    rounds = pick.shape[0] // 10
    small = (LAYERS * (8 + blocks), width)
    any_spec = pl.BlockSpec(memory_space=pl.ANY)
    vmem_spec = pl.BlockSpec(memory_space=pltpu.VMEM)
    dma = pltpu.SemaphoreType.DMA
    summed, total, small = pl.pallas_call(
        backward_kernel,
        out_shape=(
            jax.ShapeDtypeStruct((rounds, width // piece, piece, cols), low),
            jax.ShapeDtypeStruct((rows, width), full),
            jax.ShapeDtypeStruct(small, full),
        ),
        in_specs=[pl.BlockSpec(memory_space=pltpu.SMEM)] + [vmem_spec] * 4 + [any_spec] * (1 + len(saved)),
        out_specs=(vmem_spec, vmem_spec, vmem_spec),
        scratch_shapes=[
            pltpu.VMEM((units, piece, width), low),
            pltpu.VMEM((rounds, 8, piece, width), low),
            pltpu.VMEM((4, rows, width), low),
            pltpu.VMEM((7, rows, width), low),
            pltpu.VMEM((3, width, width), low),
            pltpu.VMEM((rows, width), full),
            pltpu.VMEM((rows, 128), full),
            pltpu.VMEM((rows, width), low),
            pltpu.VMEM((3, rows, width), low),
            pltpu.VMEM((width // HEAD_DIM, 1, rows), full),
            pltpu.VMEM((rows, rows), full),
            pltpu.VMEM((rows, width), low),
            pltpu.VMEM((2, half, half), low),
            pltpu.VMEM((4, half, half), low),
            pltpu.VMEM((3, half, half), low),
            pltpu.VMEM((4, 2, half // 2, half // 2), low),
            pltpu.VMEM((3, 2, half // 2, half // 2), low),
            pltpu.VMEM((4, 2, half // 4, half // 2), low),
            pltpu.VMEM((3, half // 4, half), low),
            pltpu.VMEM((4, 3, piece, half), low),
            pltpu.VMEM((5,) + small, full),
            pltpu.VMEM((5,) + small, full),
            dma((6, 3)),
            dma((2, 4)),
            dma((2, 3, 4)),
            dma((2, 2, 4)),
            dma((2, 3, 4)),
            dma((2, 5)),
            dma((rounds,)),
            dma((2, rounds)),
        ],
        compiler_params=pltpu.CompilerParams(
            collective_id=1, has_side_effects=True, vmem_limit_bytes=63 * 1024 * 1024
        ),
        name="backward_reduce",
    )(pick, out_grad, docs[:, None], docs[None, :], row_now, weights, *saved)
    return (total, summed, small)


def norm_rows(value, gain, shift):
    centred = value - jnp.mean(value, axis=1, keepdims=True)
    inverse = lax.rsqrt(jnp.mean(centred * centred, axis=1, keepdims=True) + EPS_NORM)
    scaled = centred * inverse
    return (scaled * gain + shift, scaled, inverse)


NORM_ROWS = 128


def forward_kernel(
    slot_ref,
    masters_ref,
    hidden_ref,
    docs_col_ref,
    docs_row_ref,
    col_ref,
    row_ref,
    out_ref,
    final_ref,
    table_ref,
    *refs,
):
    saved, bufs = refs[:11], refs[11:22]
    rounds = masters_ref.shape[0]
    (x_buf, normed_buf, total_buf, mask_buf, unit_buf, own_ref) = refs[22:28]
    (own_sem, sems, unit_sem, save_sem, got_sem, round_sems) = refs[28:34]
    (masters_buf, sent_ref, col_got, bias_buf, master_sem, col_sems) = refs[34:40]
    rank_ref, back_ref = refs[40:42]
    got = refs[42:]
    (low_buf, mixed_buf, ctx_buf, lse_buf, one_buf, inv_one_buf, nb_buf) = bufs[:7]
    (act_buf, slope_buf, two_buf, inv_two_buf) = bufs[7:]
    units, piece, width = own_ref.shape
    rows = hidden_ref.shape[0]
    per_layer = units // LAYERS
    blocks = (per_layer - 4) // 2
    dp, tensor = lax.axis_index("dp"), lax.axis_index("tensor")
    z, y, x, c = dp // 2, dp % 2, tensor // 2, tensor % 2
    half = width // 2
    line, plane = 4 * piece, 8 * piece
    to_core = (dp, x * 2 + 1 - c)
    to_x = (dp, (1 - x) * 2 + c)
    to_y = (z * 2 + 1 - y, tensor)
    to_z = [(((z + k) % 4) * 2 + y, tensor) for k in (1, 2, 3)]
    mesh_id = pl.DeviceIdType.MESH

    barrier = greet_all(z, y, x, c)
    masters_in = [
        pltpu.make_async_copy(masters_ref.at[i], masters_buf.at[i], master_sem.at[i])
        for i in range(rounds)
    ]
    for copy in masters_in:
        copy.start()
    cols = sent_ref.shape[2]
    owners = table_ref.shape[0] // rounds - 2

    def turn_of(unit):
        layer, j = unit // per_layer, unit % per_layer
        feed = jnp.where(j < 4 + blocks, 2 * (j - 4) + 1, 2 * (j - 4 - blocks))
        place = jnp.where(j < 3, 2 * blocks + 1 + j, jnp.where(j == 3, 2 * blocks, feed))
        return (LAYERS - 1 - layer) * per_layer + place

    def rank_one(unit, carry):
        mine, turn = slot_ref[unit] // rounds, turn_of(unit)
        before, after = 0, 0
        for other in range(units):
            same = jnp.where(slot_ref[other] // rounds == mine, 1, 0)
            before = before + jnp.where(other < unit, same, 0)
            after = after + jnp.where(turn_of(other) > turn, same, 0)
        rank_ref[unit] = before
        back_ref[unit] = rounds - 1 - after
        return carry

    lax.fori_loop(0, units, rank_one, 0)

    def first_of(number):
        found = 0
        for unit in range(units):
            slot = slot_ref[unit]
            here = (slot // rounds == dp) & (rank_ref[unit] == number)
            found = found + jnp.where(here, slot % rounds, 0)
        return found

    def fill_table():
        def spot_one(spot, carry):
            found = (LAYERS - 1) * per_layer + 4 + blocks
            for unit in range(units):
                at = back_ref[unit] * owners + slot_ref[unit] // rounds
                found = jnp.where(at == spot, unit, found)
            table_ref[spot] = found
            return carry

        lax.fori_loop(0, rounds * owners, spot_one, 0)
        for i in range(rounds):
            turn, taken = 0, 0
            for unit in range(units):
                here = slot_ref[unit] == dp * rounds + i
                turn = turn + jnp.where(here, back_ref[unit], 0)
                taken = taken + jnp.where(here, 1, 0)
            table_ref[rounds * owners + i] = turn
            table_ref[rounds * (owners + 1) + i] = taken
    me = dp * 4 + tensor

    def part_for(number, zz, yy, xx, cc):
        start = pl.multiple_of(spread_order(zz, yy, xx, cc) * piece, piece)
        return sent_ref.at[number, pl.ds(start, piece)]

    def keep(number):
        return pltpu.make_async_copy(
            part_for(number, z, y, x, c), got[number].at[me], got_sem.at[number]
        )

    def round_copy(number, src, dst, peer):
        return pltpu.make_async_remote_copy(
            src_ref=src,
            dst_ref=dst,
            send_sem=round_sems.at[0, number],
            recv_sem=round_sems.at[1, number],
            device_id=peer,
            device_id_type=mesh_id,
        )

    def start_round(number):
        keep(number).start()

        def send(zz, yy, xx, cc):
            src = part_for(number, zz, yy, xx, cc)
            round_copy(number, src, got[number].at[me], (zz * 2 + yy, xx * 2 + cc)).start()

        every_other(z, y, x, c, send)

    def finish_round(number):
        keep(number).wait()
        most = got[number].at[pl.ds(0, 31)]
        round_copy(number, most, most, to_core).wait()

    def pick(unit, there):
        rank, owner = rank_ref[unit], slot_ref[unit] // rounds
        for j in range(4):
            value = got[0][owner * 4 + j]
            for number in range(1, there):
                value = jnp.where(rank == number, got[number][owner * 4 + j], value)
            own_ref[unit, :, j * cols : (j + 1) * cols] = value

    def column_copies():
        return [
            pltpu.make_async_remote_copy(
                src_ref=col_ref,
                dst_ref=col_got.at[tensor],
                send_sem=col_sems.at[0, k],
                recv_sem=col_sems.at[1, k],
                device_id=(dp, (tensor + k + 1) % 4),
                device_id_type=mesh_id,
            )
            for k in range(3)
        ]

    for copy in masters_in:
        copy.wait()
    sent_ref[0] = masters_buf[first_of(0)].astype(sent_ref.dtype)
    pl.semaphore_wait(barrier, 31)
    start_round(0)
    for number in range(1, rounds):
        sent_ref[number] = masters_buf[first_of(number)].astype(sent_ref.dtype)
    start_round(1)
    col_got[tensor] = col_ref[...]
    for copy in column_copies():
        copy.start()
    fill_table()

    my_line = pl.multiple_of(((c * 2 + x) * 2 + y) * line, line)
    my_rows = pl.ds(pl.multiple_of(my_line + z * piece, piece), piece)
    parts, cycle = 2, sems.shape[2]

    def half_of(s):
        return pl.ds(pl.multiple_of((s % parts) * half, half), half)

    def wide(s, start, size):
        return pl.ds(pl.multiple_of((s % parts) * half + start, LANES), size)

    late_cols = LANES

    def ways(s):
        short = half // 2 - late_cols
        return (
            (s % 2 == 0, wide(s, 0, half // 2), wide(s, half // 2, half // 2), None),
            (
                s % 4 == 1,
                wide(s, 0, half // 2),
                wide(s, half // 2, short),
                wide(s, half - late_cols, late_cols),
            ),
            (
                s % 4 == 3,
                wide(s, 0, short),
                wide(s, short, half // 2),
                wide(s, half - late_cols, late_cols),
            ),
        )

    def remote(src, dst, index, s, peer):
        return pltpu.make_async_remote_copy(
            src_ref=src,
            dst_ref=dst,
            send_sem=sems.at[0, index, s % cycle],
            recv_sem=sems.at[1, index, s % cycle],
            device_id=peer,
            device_id_type=mesh_id,
        )

    def own_copy(s):
        unit, cols_now = s // parts, half_of(s)
        return pltpu.make_async_copy(
            own_ref.at[unit, :, cols_now],
            out_ref.at[unit, my_rows, cols_now],
            own_sem.at[s % cycle],
        )

    def rows_at(xx, yy, zz):
        return pl.ds(pl.multiple_of(spread_order(zz, yy, xx, c) * piece, piece), piece)

    def stage_z(s, one, two, late):
        unit, copies = s // parts, []
        size = half if late is None else half - late_cols
        early = wide(s, 0, size)
        here, there = own_ref.at[unit, :, early], out_ref.at[unit, my_rows, early]
        copies = [remote(here, there, k, s, to_z[k]) for k in range(3)]
        if late is not None:
            here, there = own_ref.at[unit, :, late], out_ref.at[unit, my_rows, late]
            copies.append(remote(here, there, 9, s, to_x))
        return copies

    def stage_one(s, one, two, late):
        unit, rows = s // parts, pl.ds(my_line, line)
        one, two = out_ref.at[unit, rows, one], out_ref.at[unit, rows, two]
        copies = [remote(one, one, 3, s, to_y), remote(two, two, 4, s, to_x)]
        if late is not None:
            for i in range(2):
                there = out_ref.at[unit, rows_at(i, y, z), late]
                copies.append(remote(there, there, 10 + i, s, to_y))
        return copies

    def stage_two(s, one, two, late):
        unit = s // parts
        rows = pl.ds(pl.multiple_of((c * 2 + x) * plane, plane), plane)
        there = out_ref.at[unit, rows, one]
        copies = [remote(there, there, 5, s, to_x)]
        for i in range(2):
            rows = pl.ds(pl.multiple_of(((c * 2 + i) * 2 + y) * line, line), line)
            there = out_ref.at[unit, rows, two]
            copies.append(remote(there, there, 6 + i, s, to_y))
        if late is not None:
            for i in range(4):
                there = out_ref.at[unit, rows_at(i // 2, i % 2, z), late]
                copies += [remote(there, there, 12 + 3 * i + k, s, to_z[k]) for k in range(3)]
        return copies

    def stage_core(s):
        rows = pl.ds(pl.multiple_of(c * 2 * plane, 2 * plane), 2 * plane)
        there = out_ref.at[s // parts, rows, half_of(s)]
        return [remote(there, there, 8, s, to_core)]

    stages = (stage_z, stage_one, stage_two, stage_core)

    def each_copy(number, s, act):
        if stages[number] is stage_core:
            for copy in stage_core(s):
                act(copy)
            return
        for kind, one, two, late in ways(s):

            @pl.when(kind)
            def _(one=one, two=two, late=late):
                for copy in stages[number](s, one, two, late):
                    act(copy)


    def unit_copy(unit):
        slot = unit % 2
        return pltpu.make_async_copy(out_ref.at[unit], unit_buf.at[slot], unit_sem.at[slot])

    def save(number, layer, block=None):
        src, dst, sem = bufs[number], saved[number].at[layer], save_sem.at[number, 0]
        if block is not None:
            src, dst, sem = src.at[block], dst.at[block], save_sem.at[number, block]
        return pltpu.make_async_copy(src, dst, sem)

    def free(numbers, layer, block=None):
        @pl.when(layer > 0)
        def _():
            for number in numbers:
                save(number, layer - 1, block).wait()

    def heads(start, stop):
        def one(pair, carry):
            attend_pair(
                pair, mixed_buf.at[0], mixed_buf.at[1], mixed_buf.at[2], mask_buf, ctx_buf, lse_buf
            )
            return carry

        lax.fori_loop(start, stop, one, 0)

    tall = rows // parts
    pairs = width // LANES

    def compute(unit, turn):
        layer, j = unit // per_layer, unit % per_layer
        matrix = unit_buf.at[unit % 2]
        mine = pl.ds(pl.multiple_of(turn * tall, tall), tall)

        def small(i):
            return row_ref[layer, i : i + 1, :]

        def bias(i):
            return bias_buf[pl.ds(layer * (2 + blocks) + i, 1), :]

        def over_rows(body):
            def one(tile, carry):
                body(pl.ds(pl.multiple_of(turn * tall + tile * NORM_ROWS, NORM_ROWS), NORM_ROWS))
                return carry

            lax.fori_loop(0, tall // NORM_ROWS, one, 0)

        @pl.when((j == 0) & (turn == 0))
        def _():
            free((0, 1), layer)

            @pl.when(layer == 0)
            def _():
                x_buf[...] = hidden_ref[...].astype(jnp.float32)

            low_buf[...] = x_buf[...].astype(jnp.bfloat16)
            save(0, layer).start()

        @pl.when(j < 3)
        def _():
            value = dot(low_buf[mine, :], matrix[...], ((1,), (0,)))
            value = value + jnp.where(j == 1, 0.0, bias(j // 2))
            scale = jnp.where(j == 0, HEAD_DIM ** (-0.5), 1.0)
            mixed_buf[j, mine, :] = (value * scale).astype(jnp.bfloat16)

        @pl.when((j == 2) & (turn == 1))
        def _():
            save(1, layer).start()
            free((2, 3), layer)
            heads(0, pairs // 4)

        @pl.when((j == 3) & (turn == 0))
        def _():
            heads(pairs // 4, 3 * pairs // 4)

        @pl.when((j == 3) & (turn == 1))
        def _():
            heads(3 * pairs // 4, pairs)
            save(2, layer).start()
            save(3, layer).start()
            total_buf[...] = dot(ctx_buf[...], matrix[...], ((1,), (1,)))
            free((4, 5, 6), layer)

            def body(tile, carry):
                part = pl.ds(pl.multiple_of(tile * NORM_ROWS, NORM_ROWS), NORM_ROWS)
                value = x_buf[part, :] + total_buf[part, :] + small(0)
                normed, scaled, inverse = norm_rows(value, small(2), small(3))
                normed_buf[part, :] = normed
                nb_buf[part, :] = normed.astype(jnp.bfloat16)
                one_buf[part, :] = scaled
                inv_one_buf[part, :] = jnp.broadcast_to(inverse, (NORM_ROWS, 128))
                return carry

            lax.fori_loop(0, rows // NORM_ROWS, body, 0)
            for number in (4, 5, 6):
                save(number, layer).start()

        @pl.when((j >= 4) & (j < 4 + blocks))
        def _():
            block = j - 4

            @pl.when(turn == 0)
            def _():
                free((7, 8), layer, block)

            value = dot(nb_buf[mine, :], matrix[...], ((1,), (0,)))
            act, slope = gelu_pair(value + bias(2 + block))
            act_buf[block, mine, :] = act.astype(jnp.bfloat16)
            slope_buf[block, mine, :] = slope.astype(jnp.bfloat16)

            @pl.when(turn == 1)
            def _():
                save(7, layer, block).start()
                save(8, layer, block).start()

        @pl.when(j >= 4 + blocks)
        def _():
            block = j - 4 - blocks
            part = dot(act_buf[block, mine, :], matrix[...], ((1,), (1,)))

            @pl.when(block == 0)
            def _():
                total_buf[mine, :] = part

            @pl.when(block > 0)
            def _():
                total_buf[mine, :] += part

        @pl.when(j == per_layer - 1)
        def _():
            @pl.when(turn == 0)
            def _():
                free((9, 10), layer)

            def body(part):
                value = normed_buf[part, :] + total_buf[part, :] + small(1)
                output, scaled, inverse = norm_rows(value, small(4), small(5))
                x_buf[part, :] = output
                two_buf[part, :] = scaled
                inv_two_buf[part, :] = jnp.broadcast_to(inverse, (NORM_ROWS, 128))

            over_rows(body)

            @pl.when(turn == 1)
            def _():
                save(9, layer).start()
                save(10, layer).start()

    steps = parts * units

    def step(s, carry):
        for number in range(len(stages), -1, -1):
            now = s - number * LAG

            if number == 0:
                for turn in range(rounds):
                    last = turn == rounds - 1
                    due = (s == parts * turn) | (last & (s > parts * turn) & (s % parts == 0))

                    @pl.when(due & (s < steps))
                    def _(turn=turn):
                        @pl.when(s == parts * turn)
                        def _():
                            finish_round(turn)

                        if turn + 2 < rounds:
                            start_round(turn + 2)
                        pick(s // parts, turn + 1)

            @pl.when((now >= 0) & (now < steps))
            def _(now=now, number=number):
                if number == 0:
                    own_copy(now).start()
                else:
                    if number == 1:
                        own_copy(now).wait()
                    each_copy(number - 1, now, lambda copy: copy.wait())
                if number < len(stages):
                    each_copy(number, now, lambda copy: copy.start())
                else:

                    @pl.when(now % parts == parts - 1)
                    def _():
                        unit_copy(now // parts).start()

        @pl.when(s == len(stages) * LAG)
        def _():
            for copy in column_copies():
                copy.wait()
            for j in range(4):
                bias_buf[:, j * cols : (j + 1) * cols] = col_got[j]

        done = s - len(stages) * LAG - parts

        @pl.when(done >= 0)
        def _():
            @pl.when(done % parts == 0)
            def _():
                unit_copy(done // parts).wait()

            compute(done // parts, done % parts)

        return carry

    fill_mask(mask_buf, docs_col_ref, docs_row_ref)
    lax.fori_loop(0, steps + len(stages) * LAG + parts, step, 0)
    final_ref[...] = x_buf[...]
    last = LAYERS - 1
    for number in (0, 1, 2, 3, 4, 5, 6, 9, 10):
        save(number, last).wait()
    for block in range(blocks):
        save(7, last, block).wait()
        save(8, last, block).wait()


def forward(unit_slot, masters, hidden_in, docs, col_now, row_now, piece, owners):
    units = unit_slot.shape[0]
    rounds, width, cols = masters.shape
    rows = hidden_in.shape[0]
    blocks = (units // LAYERS - 4) // 2
    low, full = jnp.bfloat16, jnp.float32
    kept = [
        ((rows, width), low),
        ((3, rows, width), low),
        ((rows, width), low),
        ((width // HEAD_DIM, 1, rows), full),
        ((rows, width), full),
        ((rows, 128), full),
        ((rows, width), low),
        ((blocks, rows, width), low),
        ((blocks, rows, width), low),
        ((rows, width), full),
        ((rows, 128), full),
    ]
    any_spec = pl.BlockSpec(memory_space=pl.ANY)
    vmem_spec = pl.BlockSpec(memory_space=pltpu.VMEM)
    smem_spec = pl.BlockSpec(memory_space=pltpu.SMEM)
    dma = pltpu.SemaphoreType.DMA
    return pl.pallas_call(
        forward_kernel,
        out_shape=[
            jax.ShapeDtypeStruct((units, width, width), low),
            jax.ShapeDtypeStruct((rows, width), full),
            jax.ShapeDtypeStruct((rounds * (owners + 2),), jnp.int32),
        ]
        + [jax.ShapeDtypeStruct((LAYERS,) + shape, dtype) for shape, dtype in kept],
        in_specs=[smem_spec] + [any_spec] + [vmem_spec] * 5,
        out_specs=[any_spec, vmem_spec, smem_spec] + [any_spec] * len(kept),
        scratch_shapes=[pltpu.VMEM(shape, dtype) for shape, dtype in kept]
        + [
            pltpu.VMEM((rows, width), full),
            pltpu.VMEM((rows, width), full),
            pltpu.VMEM((rows, width), full),
            pltpu.VMEM((rows, rows), full),
            pltpu.VMEM((2, width, width), low),
            pltpu.VMEM((units, piece, width), low),
            dma((8,)),
            dma((2, 24, 8)),
            dma((2,)),
            dma((len(kept), blocks)),
            dma((rounds,)),
            dma((2, rounds)),
            pltpu.VMEM((rounds, width, cols), full),
            pltpu.VMEM((rounds, width, cols), low),
            pltpu.VMEM((4,) + col_now.shape, full),
            pltpu.VMEM((col_now.shape[0], width), full),
            dma((rounds,)),
            dma((2, 3)),
            pltpu.SMEM((units,), jnp.int32),
            pltpu.SMEM((units,), jnp.int32),
        ]
        + [pltpu.VMEM((width // piece, piece, cols), low)] * rounds,
        compiler_params=pltpu.CompilerParams(
            collective_id=2, has_side_effects=True, vmem_limit_bytes=60 * 1024 * 1024
        ),
        name="gather_forward",
    )(
        unit_slot,
        masters,
        hidden_in,
        docs[:, None],
        docs[None, :],
        col_now,
        row_now,
    )


def run_general(
    unit_slot,
    masters,
    first_moment,
    second_moment,
    hidden_in,
    doc_ids,
    column_state,
    row_state,
    out_grad,
):
    slot_count, width, col_width = masters.shape
    units = unit_slot.shape[0]
    dp_size = lax.axis_size("dp")
    devices = dp_size * lax.axis_size("tensor")
    slots = slot_count * dp_size
    piece = width // devices
    per_layer = units // LAYERS
    blocks = (per_layer - 4) // 2
    tensor_size = lax.axis_size("tensor")
    rows = hidden_in.shape[0]
    seq_len = doc_ids.shape[1]
    heads = width // HEAD_DIM
    share = seq_len // rows
    tensor_index = lax.axis_index("tensor")
    groups = [list(range(i, i + share)) for i in range(0, tensor_size, share)]
    score_scale = HEAD_DIM ** (-0.5)
    sent = masters.astype(jnp.bfloat16).reshape(slot_count, devices, piece, col_width)
    spread = lax.all_to_all(sent.transpose(1, 0, 2, 3), BOTH, 0, 0)
    spread = spread.reshape(dp_size, tensor_size, slot_count, piece, col_width)
    spread = spread.transpose(0, 2, 3, 1, 4).reshape(slots, piece, width)
    mine = spread[unit_slot]
    weights = jnp.concatenate(
        [
            lax.all_gather(
                mine[layer * per_layer : (layer + 1) * per_layer], BOTH, axis=1, tiled=True
            )
            for layer in range(LAYERS)
        ],
        axis=0,
    )

    def matrices(layer):
        unit = weights[layer * per_layer : (layer + 1) * per_layer]
        return (unit[:3], unit[3], unit[4 : 4 + blocks], unit[4 + blocks :])

    row_docs = lax.dynamic_slice_in_dim(doc_ids, tensor_index // share, 1, axis=0)[0]
    my_docs = lax.dynamic_slice_in_dim(row_docs, (tensor_index % share) * rows, rows)
    same_doc = (my_docs[:, None] == row_docs[None, :])[None]

    def whole_row(value):
        if share == 1:
            return value
        return lax.all_gather(value, "tensor", axis=0, tiled=True, axis_index_groups=groups)

    def own_rows(value):
        if share == 1:
            return value
        return lax.psum_scatter(
            value, "tensor", scatter_dimension=0, tiled=True, axis_index_groups=groups
        )

    col_full = lax.all_gather(column_state[0], "tensor", axis=2, tiled=True)
    hidden = hidden_in.astype(jnp.float32)
    saved_layers = []
    for layer in range(LAYERS):
        w_qkv, w_proj, w_in, w_out = matrices(layer)
        row_now = row_state[0, layer]
        col_now = col_full[layer]
        hidden_bf = hidden.astype(jnp.bfloat16)
        query, key, value = (dot(hidden_bf, w_qkv[i], ((1,), (0,))) for i in range(3))
        query = ((query + col_now[0]) * score_scale).astype(jnp.bfloat16)
        key = key.astype(jnp.bfloat16)
        value = (value + col_now[1]).astype(jnp.bfloat16)
        query = query.reshape(rows, heads, HEAD_DIM)
        key = whole_row(key).reshape(seq_len, heads, HEAD_DIM)
        value = whole_row(value).reshape(seq_len, heads, HEAD_DIM)
        scores = jnp.einsum("qhd,khd->hqk", query, key, preferred_element_type=jnp.float32)
        scores = jnp.where(same_doc, scores, -1e30)
        row_top = jnp.max(scores, axis=-1, keepdims=True)
        log_total = row_top + jnp.log(
            jnp.sum(jnp.exp(scores - row_top), axis=-1, keepdims=True)
        )
        soft_bf = jnp.exp(scores - log_total).astype(jnp.bfloat16)
        context = jnp.einsum("hqk,khd->qhd", soft_bf, value, preferred_element_type=jnp.float32)
        context = context.reshape(rows, width).astype(jnp.bfloat16)
        attended = dot(context, w_proj, ((1,), (1,)))
        normed, scaled_one, inverse_one = norm_forward(
            hidden + attended + row_now[0], row_now[2], row_now[3]
        )
        normed_bf = normed.astype(jnp.bfloat16)
        pre_act = jnp.einsum("rd,bdc->brc", normed_bf, w_in, preferred_element_type=jnp.float32)
        activated, slope = gelu_pair(pre_act + col_now[2:, None])
        activated = activated.astype(jnp.bfloat16)
        slope = slope.astype(jnp.bfloat16)
        mlp_out = jnp.einsum(
            "brc,bdc->rd", activated, w_out, preferred_element_type=jnp.float32
        )
        output, scaled_two, inverse_two = norm_forward(
            normed + mlp_out + row_now[1], row_now[4], row_now[5]
        )
        saved_layers.append(
            (hidden_bf, query, key, value, log_total, context, scaled_one, inverse_one, normed_bf)
            + (slope, activated, scaled_two, inverse_two)
        )
        hidden = output
    upstream = out_grad.astype(jnp.float32)
    operands = [None] * LAYERS
    col_parts = [None] * LAYERS
    row_parts = [None] * LAYERS
    for layer in reversed(range(LAYERS)):
        w_qkv, w_proj, w_in, w_out = matrices(layer)
        row_now = row_state[0, layer]
        (
            hidden_bf,
            query,
            key,
            value,
            log_total,
            context,
            scaled_one,
            inverse_one,
            normed_bf,
            slope,
            activated,
            scaled_two,
            inverse_two,
        ) = saved_layers[layer]
        d_two, gain_two, shift_two = norm_backward(upstream, scaled_two, inverse_two, row_now[4])
        grad_bias_two = jnp.sum(d_two, axis=0)
        d_two_bf = d_two.astype(jnp.bfloat16)
        d_act = jnp.einsum("rd,bdc->brc", d_two_bf, w_out, preferred_element_type=jnp.float32)
        d_pre = (d_act * slope).astype(jnp.bfloat16)
        grad_bias_in = jnp.sum(d_pre, axis=1, dtype=jnp.float32)
        d_normed = jnp.einsum("brc,bdc->rd", d_pre, w_in, preferred_element_type=jnp.float32)
        d_normed = d_two + d_normed
        d_one, gain_one, shift_one = norm_backward(d_normed, scaled_one, inverse_one, row_now[2])
        grad_bias_proj = jnp.sum(d_one, axis=0)
        d_one_bf = d_one.astype(jnp.bfloat16)
        d_context = dot(d_one_bf, w_proj, ((1,), (0,))).astype(jnp.bfloat16)
        d_context = d_context.reshape(rows, heads, HEAD_DIM)
        scores = jnp.einsum("qhd,khd->hqk", query, key, preferred_element_type=jnp.float32)
        scores = jnp.where(same_doc, scores, -1e30)
        soft = jnp.exp(scores - log_total)
        d_values = jnp.einsum(
            "hqk,qhd->khd",
            soft.astype(jnp.bfloat16),
            d_context,
            preferred_element_type=jnp.float32,
        )
        d_probs = jnp.einsum(
            "qhd,khd->hqk", d_context, value, preferred_element_type=jnp.float32
        )
        d_scores = (
            soft * (d_probs - jnp.sum(soft * d_probs, axis=-1, keepdims=True))
        ).astype(jnp.bfloat16)
        d_queries = (
            jnp.einsum("hqk,khd->qhd", d_scores, key, preferred_element_type=jnp.float32)
            * score_scale
        )
        d_keys = jnp.einsum("hqk,qhd->khd", d_scores, query, preferred_element_type=jnp.float32)
        d_qkv = jnp.stack(
            [
                d_queries.reshape(rows, width),
                own_rows(d_keys.reshape(seq_len, width)),
                own_rows(d_values.reshape(seq_len, width)),
            ]
        ).astype(jnp.bfloat16)
        grad_bias_qkv = jnp.sum(d_qkv, axis=1, dtype=jnp.float32)
        upstream = d_one + jnp.einsum(
            "brc,bdc->rd", d_qkv, w_qkv, preferred_element_type=jnp.float32
        )
        operands[layer] = (hidden_bf, d_one_bf, normed_bf, d_two_bf)
        operands[layer] += (d_qkv, context[None], d_pre, activated)
        col_parts[layer] = jnp.concatenate(
            [
                grad_bias_qkv[0:1],
                grad_bias_qkv[2:3],
                grad_bias_in,
            ],
            axis=0,
        )
        row_parts[layer] = jnp.stack(
            [grad_bias_proj, grad_bias_two, gain_one, shift_one, gain_two, shift_two]
        )
    small = jnp.stack([jnp.stack(col_parts), jnp.stack(row_parts)])
    summed = []
    for layer in operands:
        whole = jnp.concatenate(
            [
                jnp.einsum(
                    "rd,brc->bdc", layer[i], layer[4 + i], preferred_element_type=jnp.float32
                )
                for i in range(4)
            ],
            axis=0,
        )
        summed.append(
            lax.psum_scatter(whole.astype(jnp.bfloat16), BOTH, scatter_dimension=1, tiled=True)
        )
    summed = jnp.concatenate(summed, axis=0)

    slot_ids = jnp.arange(slots, dtype=jnp.int32)
    named = unit_slot[None, :] == slot_ids[:, None]
    holds = jnp.any(named, axis=1)
    unit_of = jnp.argmax(named, axis=1)
    back = jnp.where(holds[:, None, None], summed[unit_of], jnp.zeros((), jnp.bfloat16))
    back = back.reshape(dp_size, slot_count, piece, tensor_size, col_width)
    back = back.transpose(0, 3, 1, 2, 4).reshape(devices, slot_count, piece, col_width)
    owned = lax.all_to_all(back, BOTH, 0, 0)
    owned = owned.transpose(1, 0, 2, 3)
    owned = owned.reshape(slot_count, width, col_width)
    occupied = lax.dynamic_slice_in_dim(holds, lax.axis_index("dp") * slot_count, slot_count)
    occupied = occupied.astype(jnp.float32)[:, None, None]
    new_master, new_first, new_second = adamw_update(
        masters, owned.astype(jnp.float32), first_moment, second_moment, RATE_UNITS
    )
    updated = (
        new_master * occupied,
        jnp.stack([new_first * occupied, new_second * occupied]),
    )
    return (hidden, upstream, updated, lax.psum(small, BOTH))


def adamw_kernel(table_ref, owned_ref, value_ref, first_ref, second_ref, value_out, state_out):
    taken = table_ref[table_ref.shape[0] - pl.num_programs(0) + pl.program_id(0)] > 0
    gradient = jnp.where(taken, owned_ref[0].astype(jnp.float32), 0.0)
    value, first, second = adamw_update(
        value_ref[0], gradient, first_ref[0], second_ref[0], RATE_UNITS
    )
    value_out[0] = jnp.where(taken, value, 0.0)
    state_out[0, 0] = jnp.where(taken, first, 0.0)
    state_out[1, 0] = jnp.where(taken, second, 0.0)


def adamw_slots(table, owned, masters, first_moment, second_moment):
    count, width, cols = masters.shape
    tall = width // 2
    at = table.shape[0] - 2 * count
    tile = pl.BlockSpec((1, tall, cols), lambda i, j, table: (i, j, 0))
    return pl.pallas_call(
        adamw_kernel,
        grid_spec=pltpu.PrefetchScalarGridSpec(
            num_scalar_prefetch=1,
            grid=(count, width // tall),
            in_specs=[
                pl.BlockSpec((1, tall, cols), lambda i, j, table: (table[at + i], j, 0)),
                tile,
                tile,
                tile,
            ],
            out_specs=(tile, pl.BlockSpec((2, 1, tall, cols), lambda i, j, table: (0, i, j, 0))),
        ),
        out_shape=(
            jax.ShapeDtypeStruct(masters.shape, jnp.float32),
            jax.ShapeDtypeStruct((2,) + masters.shape, jnp.float32),
        ),
        name="adamw",
    )(table, owned, masters, first_moment, second_moment)


def run_kernels(
    unit_slot,
    masters,
    first_moment,
    second_moment,
    hidden_in,
    doc_ids,
    column_state,
    row_state,
    out_grad,
):
    slot_count, width, cols = masters.shape
    blocks = (unit_slot.shape[0] // LAYERS - 4) // 2
    dp_size = lax.axis_size("dp")
    piece = width // (dp_size * lax.axis_size("tensor"))
    docs = lax.dynamic_index_in_dim(doc_ids, lax.axis_index("tensor"), 0, keepdims=False)
    row_now = row_state[0]
    weights, hidden, table, *saved = forward(
        unit_slot,
        masters,
        hidden_in,
        docs,
        column_state[0].reshape(-1, cols),
        row_now,
        piece,
        dp_size,
    )
    upstream, owned, small = backward(table, out_grad, docs, row_now, weights, saved, piece, cols)
    slots = adamw_slots(
        table, owned.reshape(masters.shape), masters, first_moment, second_moment
    )
    return (hidden, upstream, slots, small.reshape(2, LAYERS, 2 + blocks, width))


def local(
    hidden_in,
    doc_ids,
    unit_slot,
    masters,
    first_moment,
    second_moment,
    column_state,
    row_state,
    out_grad,
):
    col_width = masters.shape[2]
    tensor_index = lax.axis_index("tensor")
    kernels = (lax.axis_size("dp"), lax.axis_size("tensor")) == (8, 4)
    kernels = kernels and hidden_in.shape[0] == doc_ids.shape[1]
    run = run_kernels if kernels else run_general
    hidden, upstream, (unit_master, unit_state), small = run(
        unit_slot,
        masters,
        first_moment,
        second_moment,
        hidden_in,
        doc_ids,
        column_state,
        row_state,
        out_grad,
    )
    row_total = small[1]
    col_total = lax.dynamic_slice_in_dim(small[0], tensor_index * col_width, col_width, axis=2)
    new_col, col_first, col_second = adamw_update(
        column_state[0], col_total, column_state[1], column_state[2], RATE_SMALL
    )
    column_out = jnp.stack([col_total, new_col, col_first, col_second])
    new_row, row_first, row_second = adamw_update(
        row_state[0], row_total, row_state[1], row_state[2], RATE_SMALL
    )
    row_out = jnp.stack([row_total, new_row, row_first, row_second])
    return (hidden, upstream, unit_master, unit_state, column_out, row_out)


def solution(mesh):
    return jax.shard_map(
        local,
        mesh=mesh,
        in_specs=(
            P(("dp", "tensor"), None),
            P("dp", None),
            P(),
            P("dp", None, "tensor"),
            P("dp", None, "tensor"),
            P("dp", None, "tensor"),
            P(None, None, None, "tensor"),
            P(),
            P(("dp", "tensor"), None),
        ),
        out_specs=(
            P(("dp", "tensor"), None),
            P(("dp", "tensor"), None),
            P("dp", None, "tensor"),
            P(None, "dp", None, "tensor"),
            P(None, None, None, "tensor"),
            P(),
        ),
        check_vma=False,
    )
```

```python
import functools
import math

import jax
import jax.numpy as jnp
from jax import lax
from jax.experimental import pallas as pl
from jax.experimental.pallas import tpu as pltpu
from jax.sharding import PartitionSpec as P

HEAD_DIM = 64
LAYERS = 2
STEP = 3

EPS_NORM = 1e-06
RATE_UNITS = 0.05
RATE_SMALL = 0.2
WEIGHT_DECAY = 0.01
ADAM_EPS = 1e-08
BETA_MOMENT = 0.5
BOTH = ("dp", "tensor")


def norm_forward(summed, gain, shift):
    row_mean = jnp.mean(summed, axis=1, keepdims=True)
    centred = summed - row_mean
    inverse = lax.rsqrt(jnp.mean(centred * centred, axis=1, keepdims=True) + EPS_NORM)
    scaled = centred * inverse
    return (scaled * gain + shift, scaled, inverse)


def norm_backward(upstream, scaled, inverse, gain):
    d_scaled = upstream * gain
    mean_one = jnp.mean(d_scaled, axis=1, keepdims=True)
    mean_two = jnp.mean(d_scaled * scaled, axis=1, keepdims=True)
    grad_input = inverse * (d_scaled - mean_one - scaled * mean_two)
    return (grad_input, jnp.sum(upstream * scaled, axis=0), jnp.sum(upstream, axis=0))


def gelu_pair(v):
    cdf = 0.5 * (1.0 + lax.erf(v * 2.0 ** (-0.5)))
    bell = jnp.exp(-0.5 * v * v) * (2.0 * math.pi) ** (-0.5)
    return (v * cdf, cdf + v * bell)


def adamw_update(old_value, gradient, first_old, second_old, learn_rate):
    first_new = BETA_MOMENT * first_old + (1.0 - BETA_MOMENT) * gradient
    second_new = BETA_MOMENT * second_old + (1.0 - BETA_MOMENT) * gradient * gradient
    correct = 1.0 - BETA_MOMENT**STEP
    step_size = first_new / correct / (jnp.sqrt(second_new / correct) + ADAM_EPS)
    return (old_value - learn_rate * (step_size + WEIGHT_DECAY * old_value), first_new, second_new)


def dot(left, right, dims):
    return lax.dot_general(left, right, (dims, ((), ())), preferred_element_type=jnp.float32)


LANES = 2 * HEAD_DIM


def head_lanes(value, head):
    lane = lax.broadcasted_iota(jnp.int32, value.shape, 1)
    keep = lane < HEAD_DIM if head == 0 else lane >= HEAD_DIM
    return jnp.where(keep, value, jnp.zeros_like(value))


def pair_lanes(first, second):
    lane = lax.broadcasted_iota(jnp.int32, first.shape, 1)
    return jnp.where(lane < HEAD_DIM, first, second)


def attend_pair(pair, q_ref, k_ref, v_ref, mask_ref, ctx_ref, lse_ref):
    lanes = pl.ds(pl.multiple_of(pair * LANES, LANES), LANES)
    query, key, value = q_ref[:, lanes], k_ref[:, lanes], v_ref[:, lanes]
    value_t = value.T
    parts = []
    for head in range(2):
        scores = dot(head_lanes(key, head), query, ((1,), (1,))) + mask_ref[...]
        top = jnp.max(scores, axis=0, keepdims=True)
        weight = jnp.exp(scores - top)
        total = jnp.sum(weight, axis=0, keepdims=True)
        lse_ref[pair * 2 + head] = top + jnp.log(total)
        mine = value_t[head * HEAD_DIM : (head + 1) * HEAD_DIM]
        mixed = dot(mine, weight.astype(jnp.bfloat16), ((1,), (0,)))
        parts.append(mixed * (1.0 / total))
    ctx_ref[:, lanes] = jnp.concatenate(parts, axis=0).T.astype(ctx_ref.dtype)


def attend_back_pair(pair, q_ref, k_ref, v_ref, d_ref, mask_ref, lse_ref, dq_ref, dk_ref, dv_ref):
    lanes = pl.ds(pl.multiple_of(pair * LANES, LANES), LANES)
    query, key, value = q_ref[:, lanes], k_ref[:, lanes], v_ref[:, lanes]
    grad = d_ref[:, lanes]
    key_t = key.T
    parts, d_keys, d_values = [], [], []
    for head in range(2):
        scores = dot(head_lanes(key, head), query, ((1,), (1,))) + mask_ref[...]
        soft = jnp.exp(scores - lse_ref[pair * 2 + head])
        d_values.append(dot(soft.astype(jnp.bfloat16), grad, ((1,), (0,))))
        d_soft = dot(head_lanes(value, head), grad, ((1,), (1,)))
        both = soft * d_soft
        mean = jnp.sum(both, axis=0, keepdims=True)
        d_scores = (both - soft * mean).astype(jnp.bfloat16)
        d_keys.append(dot(d_scores, query, ((1,), (0,))))
        mine = key_t[head * HEAD_DIM : (head + 1) * HEAD_DIM]
        parts.append(dot(mine, d_scores, ((1,), (0,))))
    scale = HEAD_DIM ** (-0.5)
    dq_ref[:, lanes] = (jnp.concatenate(parts, axis=0).T * scale).astype(dq_ref.dtype)
    dk_ref[:, lanes] = pair_lanes(*d_keys).astype(dk_ref.dtype)
    dv_ref[:, lanes] = pair_lanes(*d_values).astype(dv_ref.dtype)


def fill_mask(mask_ref, docs_col_ref, docs_row_ref):
    same = docs_col_ref[...] == docs_row_ref[...]
    mask_ref[...] = jnp.where(same, 0.0, -1e30).astype(jnp.float32)


LAG = 2


def spread_order(z, y, x, c):
    return ((c * 2 + x) * 2 + y) * 4 + z


def every_other(z, y, x, c, body):
    for step in (2, 1, 3, 0):

        def one(i, carry, step=step):
            body((z + step) % 4, (y + i // 4) % 2, (x + (i // 2) % 2) % 2, (c + i % 2) % 2)
            return carry

        lax.fori_loop(1 if step == 0 else 0, 8, one, 0)


def greet_all(z, y, x, c):
    barrier = pltpu.get_barrier_semaphore()

    def greet(zz, yy, xx, cc):
        pl.semaphore_signal(
            barrier,
            inc=1,
            device_id=(zz * 2 + yy, xx * 2 + cc),
            device_id_type=pl.DeviceIdType.MESH,
        )

    every_other(z, y, x, c, greet)
    return barrier


TILE = 256


def norm_back_rows(upstream, scaled, inverse, gain):
    d_scaled = upstream * gain
    mean_one = jnp.mean(d_scaled, axis=1, keepdims=True)
    mean_two = jnp.mean(d_scaled * scaled, axis=1, keepdims=True)
    return inverse * (d_scaled - mean_one - scaled * mean_two)


def backward_kernel(
    pick_ref,
    out_grad_ref,
    docs_col_ref,
    docs_row_ref,
    row_ref,
    weights_ref,
    low_ref,
    mixed_ref,
    ctx_ref,
    lse_ref,
    one_ref,
    inv_one_ref,
    normed_ref,
    act_ref,
    slope_ref,
    two_ref,
    inv_two_ref,
    owned_ref,
    total_ref,
    small_out,
    out_ref,
    back_buf,
    left_buf,
    right_buf,
    unit_buf,
    scaled_buf,
    inv_buf,
    slope_buf,
    mixed_buf,
    lse_buf,
    mask_buf,
    d_ctx_buf,
    core_out,
    core_in,
    sum_core,
    first_in,
    sum_first,
    second_in,
    sum_second,
    z_in,
    late_in,
    late_sum,
    late_second_in,
    late_pair,
    late_last_in,
    small_sum,
    small_got,
    load_sem,
    core_sems,
    first_sems,
    second_sems,
    z_sems,
    small_sems,
    own_sems,
    round_sems,
):
    units, piece, width = out_ref.shape
    rows = total_ref.shape[0]
    per_layer = units // LAYERS
    blocks = (per_layer - 4) // 2
    at_out, at_query = 2 * blocks, 2 * blocks + 1
    dp, tensor = lax.axis_index("dp"), lax.axis_index("tensor")
    z, y, x, c = dp // 2, dp % 2, tensor // 2, tensor % 2
    half, parts = width // 2, 2
    side_cols = half // 2
    to_core = (dp, x * 2 + 1 - c)
    to_x = (dp, (1 - x) * 2 + c)
    to_y = (z * 2 + 1 - y, tensor)
    to_z = [(((z + k) % 4) * 2 + y, tensor) for k in (1, 2, 3)]
    to_z1 = ((z + 1 - 2 * (z % 2)) * 2 + y, tensor)
    to_z2 = (((z + 2) % 4) * 2 + y, tensor)
    mesh_id = pl.DeviceIdType.MESH

    barrier = greet_all(z, y, x, c)

    def remote(src, dst, sems, send, recv, peer):
        return pltpu.make_async_remote_copy(
            src_ref=src,
            dst_ref=dst,
            send_sem=sems.at[send],
            recv_sem=sems.at[recv],
            device_id=peer,
            device_id_type=mesh_id,
        )

    def place(s):
        return LAYERS - 1 - s // per_layer, s % per_layer

    def unit_of(s):
        layer, j = place(s)
        feed = jnp.where(j % 2 == 0, 4 + blocks + j // 2, 4 + j // 2)
        return layer * per_layer + jnp.where(
            j < at_out, feed, jnp.where(j == at_out, 3, j - at_query)
        )

    def left_of(s):
        j = s % per_layer
        feed = jnp.where(j % 2 == 0, 3, 2)
        return jnp.where(j < at_out, feed, jnp.where(j == at_out, 1, 0))

    def loaded_slot(s):
        return ((s // per_layer) * (blocks + 1) + (s % per_layer) // 2) % 2

    def right_of(s):
        j = s % per_layer
        feed = jnp.where(j % 2 == 0, loaded_slot(s), 2 + (j // 2) % 2)
        return jnp.where(
            j < at_out, feed, jnp.where(j == at_out, loaded_slot(s), 4 + j - at_query)
        )

    local = pltpu.make_async_copy

    def unit_load(s):
        return local(weights_ref.at[unit_of(s)], unit_buf.at[s % 3], load_sem.at[0, s % 3])

    def act_load(layer, block, slot):
        return local(act_ref.at[layer, block], right_buf.at[slot], load_sem.at[1, slot])

    def ctx_load(layer, slot):
        return local(ctx_ref.at[layer], right_buf.at[slot], load_sem.at[1, slot])

    def slope_load(layer, block):
        return local(slope_ref.at[layer, block], slope_buf, load_sem.at[2, 0])

    def norm_loads(layer, which):
        scaled, inv = ((one_ref, inv_one_ref), (two_ref, inv_two_ref))[which]
        return [
            local(scaled.at[layer], scaled_buf, load_sem.at[3, 0]),
            local(inv.at[layer], inv_buf, load_sem.at[3, 1]),
        ]

    def mixed_loads(layer):
        return [
            local(mixed_ref.at[layer], mixed_buf, load_sem.at[4, 0]),
            local(lse_ref.at[layer], lse_buf, load_sem.at[4, 1]),
        ]

    def normed_load(layer):
        return local(normed_ref.at[layer], left_buf.at[2], load_sem.at[2, 1])

    def low_load(layer):
        return local(low_ref.at[layer], left_buf.at[0], load_sem.at[5, 0])

    def begin(*copies):
        for copy in copies:
            copy.start()

    def finish(*copies):
        for copy in copies:
            copy.wait()

    def note(row, value):
        small_sum[0, pl.ds(row, 1), :] = value

    def column(layer, i):
        return layer * (2 + blocks) + i

    def row(layer, i):
        return LAYERS * (2 + blocks) + layer * 6 + i

    def norm_back(layer, gain_row, bias_row, low_slot):
        gain = row_ref[layer, gain_row : gain_row + 1, :]
        size = 128

        def one(tile, carry):
            part = pl.ds(pl.multiple_of(tile * size, size), size)
            upstream = total_ref[part, :]
            scaled = scaled_buf[part, :]
            inside = norm_back_rows(upstream, scaled, inv_buf[part, 0:1], gain)
            total_ref[part, :] = inside
            left_buf[low_slot, part, :] = inside.astype(jnp.bfloat16)
            sums = (upstream * scaled, upstream, inside)
            return tuple(a + jnp.sum(b, axis=0, keepdims=True) for a, b in zip(carry, sums))

        zero = jnp.zeros((1, width), jnp.float32)
        gains, shifts, biases = lax.fori_loop(0, rows // size, one, (zero, zero, zero))
        note(row(layer, gain_row), gains)
        note(row(layer, gain_row + 1), shifts)
        note(row(layer, bias_row), biases)

    def heads(start, stop):
        inputs = [mixed_buf.at[i] for i in range(3)]
        grads = [right_buf.at[4 + i] for i in range(3)]

        def one(pair, carry):
            attend_back_pair(pair, *inputs, d_ctx_buf, mask_buf, lse_buf, *grads)
            return carry

        lax.fori_loop(start, stop, one, 0)

    pairs = width // LANES

    def data_gradient(s):
        layer, j = place(s)
        matrix = unit_buf.at[s % 3]
        before = unit_buf.at[(s + 2) % 3]
        slot = loaded_slot(s)

        @pl.when(j == 0)
        def _():
            finish(*norm_loads(layer, 1))

            @pl.when(s == 0)
            def _():
                total_ref[...] = out_grad_ref[...].astype(jnp.float32)

            norm_back(layer, 4, 1, 3)
            begin(*norm_loads(layer, 0), *mixed_loads(layer))

        @pl.when(j == 1)
        def _():
            finish(normed_load(layer))
            begin(low_load(layer))

        @pl.when((j < at_out) & (j % 2 == 0))
        def _():
            block = j // 2
            finish(slope_load(layer, block), act_load(layer, block, slot))

            @pl.when(block < blocks - 1)
            def _():
                act_load(layer, block + 1, 1 - slot).start()

            @pl.when(block == blocks - 1)
            def _():
                ctx_load(layer, 1 - slot).start()

            d_act = dot(left_buf[3], matrix[...], ((1,), (0,)))
            d_pre = (d_act * slope_buf[...].astype(jnp.float32)).astype(jnp.bfloat16)
            right_buf[2 + block % 2] = d_pre
            sums = jnp.sum(d_pre.astype(jnp.float32), axis=0, keepdims=True)
            note(column(layer, 2 + block), sums)

            @pl.when(block < blocks - 1)
            def _():
                slope_load(layer, block + 1).start()

        @pl.when((j < at_out) & (j % 2 == 1))
        def _():
            total_ref[...] += dot(right_buf[2 + (j // 2) % 2], matrix[...], ((1,), (1,)))

        @pl.when(j == at_out)
        def _():
            finish(*norm_loads(layer, 0), *mixed_loads(layer), ctx_load(layer, slot))
            norm_back(layer, 2, 0, 1)

            @pl.when(layer > 0)
            def _():
                act_load(layer - 1, 0, 1 - slot).start()
                begin(*norm_loads(layer - 1, 1))
                slope_load(layer - 1, 0).start()

            d_ctx_buf[...] = dot(left_buf[1], matrix[...], ((1,), (0,))).astype(jnp.bfloat16)

        @pl.when(j == at_query)
        def _():
            finish(low_load(layer))

            @pl.when(layer > 0)
            def _():
                normed_load(layer - 1).start()

            heads(3 * pairs // 8, 5 * pairs // 8)

        @pl.when(j == at_query + 1)
        def _():
            total_ref[...] += dot(right_buf[4], before[...], ((1,), (1,)))

        @pl.when(j == at_query + 2)
        def _():
            total_ref[...] += dot(right_buf[6], matrix[...], ((1,), (1,)))

    def data_gradient_rest(s):
        layer, j = place(s)

        @pl.when(j == at_out)
        def _():
            heads(0, 3 * pairs // 8)

        @pl.when(j == at_query)
        def _():
            heads(5 * pairs // 8, pairs)

        @pl.when(j == at_query + 1)
        def _():
            total_ref[...] += dot(right_buf[5], unit_buf[s % 3], ((1,), (1,)))
            for i, number in ((0, 0), (2, 1)):
                sums = jnp.sum(right_buf[4 + i].astype(jnp.float32), axis=0, keepdims=True)
                note(column(layer, number), sums)

    def product(s, side, tile):
        unit = s // parts
        start = pl.multiple_of(side * half + tile * TILE, TILE)
        left = left_buf[left_of(unit), :, pl.ds(start, TILE)]
        right = right_buf[
            right_of(unit), :, pl.ds(pl.multiple_of((s % parts) * half, half), half)
        ]
        return lax.dot_general(
            left, right, (((0,), (0,)), ((), ())), preferred_element_type=jnp.float32
        )

    def core_copy(s):
        return remote(
            core_out.at[s % 2], core_in.at[s % 4], core_sems, (0, s % 2), (1, s % 4), to_core
        )

    def by_kind(s, body):
        short = side_cols - LANES
        late_end = parts * (units - rounds)
        kinds = (
            ((s % 2 == 0) | (s >= late_end), side_cols, side_cols, False),
            ((s % 4 == 1) & (s < late_end), side_cols, short, True),
            ((s % 4 == 3) & (s < late_end), short, side_cols, True),
        )
        for kind, one, two, late in kinds:

            @pl.when(kind)
            def _(one=one, two=two, late=late):
                body(one, two, late)

    def first_copies(s, one, two, late):
        here, there = sum_core.at[s % 3], first_in.at[s % 4]

        def send(src, dst, number, peer):
            return remote(
                src, dst, first_sems, (0, number, s % 3), (1, number, s % 4), peer
            )

        copies = [
            send(
                here.at[1 - x, :, :, :, pl.ds(0, one)],
                there.at[0, :, :, :, pl.ds(0, one)],
                0,
                to_x,
            ),
            send(
                here.at[:, 1 - y, :, :, pl.ds(one, two)],
                there.at[1, :, :, :, pl.ds(0, two)],
                1,
                to_y,
            ),
        ]
        if late:
            for k in (1, 2, 3):
                src = here.at[:, :, (z + k) % 4, :, pl.ds(one + two, LANES)]
                copies.append(send(src, late_in.at[s % 4, k - 1], 1 + k, to_z[k - 1]))
        return copies

    def second_copies(s, one, two, late):
        here, there = sum_first.at[s % 3], second_in.at[s % 4]

        def send(src, dst, number, peer):
            return remote(
                src, dst, second_sems, (0, number, s % 3), (1, number, s % 4), peer
            )

        copies = [
            send(here.at[0, 1 - y, :, :, pl.ds(0, one)], there.at[0, :, :, pl.ds(0, one)], 0, to_y),
            send(here.at[1, 1 - x, :, :, pl.ds(0, two)], there.at[1, :, :, pl.ds(0, two)], 1, to_x),
        ]
        if late:
            copies.append(send(late_sum.at[s % 3, :, 1 - y], late_second_in.at[s % 4], 2, to_y))
        return copies

    def third_copies(s, one, two, late):
        here, there = sum_second.at[s % 3], z_in.at[s % 4]

        def send(src, dst, number, peer):
            return remote(src, dst, z_sems, (0, number, s % 3), (1, number, s % 4), peer)

        cols_now = pl.ds(0, one + two)
        copies = [
            send(here.at[(z + k) % 4, :, cols_now], there.at[k - 1, :, cols_now], k - 1, to_z[k - 1])
            for k in (1, 2, 3)
        ]
        if late:
            copies.append(send(late_pair.at[s % 3, 1 - x], late_last_in.at[s % 4], 3, to_x))
        return copies

    def plus(value, *others):
        value = value.astype(jnp.float32)
        for other in others:
            value = value + other.astype(jnp.float32)
        return value.astype(jnp.bfloat16)

    def after_z(s, one, two, late):
        for copy in third_copies(s, one, two, late):
            copy.wait()
        unit, here, got = unit_of(s // parts), s % 3, s % 4
        start, size = (half if late else 0), one + two
        base = half if late else pl.multiple_of((s % 2) * half, half)
        out_ref[unit, :, pl.ds(base, size)] = plus(
            sum_second[here, z, :, 0:size], *(z_in[got, k, :, 0:size] for k in range(3))
        )
        if late:
            out_ref[unit, :, start + size : start + half] = plus(
                late_pair[here, x], late_last_in[got]
            )

    def after_second(s, one, two, late):
        for copy in second_copies(s, one, two, late):
            copy.wait()
        here, got = s % 3, s % 4
        sum_second[here, :, :, 0:one] = plus(
            sum_first[here, 0, y, :, :, 0:one], second_in[got, 0, :, :, 0:one]
        )
        sum_second[here, :, :, one : one + two] = plus(
            sum_first[here, 1, x, :, :, 0:two], second_in[got, 1, :, :, 0:two]
        )
        if late:
            late_pair[here] = plus(late_sum[here, :, y], late_second_in[got])
        for copy in third_copies(s, one, two, late):
            copy.start()

    def after_first(s, one, two, late):
        for copy in first_copies(s, one, two, late):
            copy.wait()
        here, got = s % 3, s % 4
        sum_first[here, 0, :, :, :, 0:one] = plus(
            sum_core[here, x, :, :, :, 0:one], first_in[got, 0, :, :, :, 0:one]
        )
        sum_first[here, 1, :, :, :, 0:two] = plus(
            sum_core[here, :, y, :, :, one : one + two], first_in[got, 1, :, :, :, 0:two]
        )
        if late:
            late_sum[here] = plus(
                sum_core[here, :, :, z, :, one + two : half], *(late_in[got, k] for k in range(3))
            )
        for copy in second_copies(s, one, two, late):
            copy.start()

    def start_first(s, one, two, late):
        for copy in first_copies(s, one, two, late):
            copy.start()

    small_peers = (to_core, to_x, to_y, to_z1, to_z2)

    def small_copy(stage):
        return remote(
            small_sum.at[stage],
            small_got.at[stage],
            small_sems,
            (0, stage),
            (1, stage),
            small_peers[stage],
        )

    rounds, owners = back_buf.shape[0], back_buf.shape[1]
    cols = owned_ref.shape[3]
    me = spread_order(z, y, x, c)

    def own_back(number):
        return local(
            back_buf.at[number, dp, :, pl.ds(pl.multiple_of(tensor * cols, cols), cols)],
            owned_ref.at[number, me],
            own_sems.at[number],
        )

    def send_back(number):
        def fill(owner, carry):
            back_buf[number, owner] = out_ref[pick_ref[number * owners + owner]]
            return carry

        lax.fori_loop(0, owners, fill, 0)
        own_back(number).start()

        def send(zz, yy, xx, cc):
            there = xx * 2 + cc
            remote(
                back_buf.at[
                    number, zz * 2 + yy, :, pl.ds(pl.multiple_of(there * cols, cols), cols)
                ],
                owned_ref.at[number, me],
                round_sems,
                (0, number),
                (1, number),
                (zz * 2 + yy, there),
            ).start()

        every_other(z, y, x, c, send)

    def finish_back(number):
        own_back(number).wait()
        most = owned_ref.at[number, pl.ds(0, 31)]
        remote(most, most, round_sems, (0, number), (1, number), to_core).wait()

    top = LAYERS - 1
    steps = parts * units
    begin(
        *norm_loads(top, 1),
        unit_load(jnp.int32(0)),
        slope_load(top, 0),
        act_load(top, 0, 0),
        normed_load(top),
    )
    fill_mask(mask_buf, docs_col_ref, docs_row_ref)
    pl.semaphore_wait(barrier, 31)

    def step(s, carry):
        last = s - 3 * LAG - 1

        @pl.when((last >= 0) & (last < steps))
        def _():
            by_kind(last, functools.partial(after_z, last))

            @pl.when((last // parts >= units - rounds) & (last % parts == parts - 1))
            def _():
                send_back(last // parts - (units - rounds))

        third = s - 2 * LAG - 1

        @pl.when((third >= 0) & (third < steps))
        def _():
            by_kind(third, functools.partial(after_second, third))

        second = s - LAG - 1

        @pl.when((second >= 0) & (second < steps))
        def _():
            by_kind(second, functools.partial(after_first, second))

        @pl.when(s < steps)
        def _():
            unit = s // parts

            @pl.when(s % parts == 0)
            def _():
                unit_load(unit).wait()

                @pl.when(unit + 1 < units)
                def _():
                    unit_load(unit + 1).start()

                data_gradient(unit)

            @pl.when(s % parts == 1)
            def _():
                data_gradient_rest(unit)

            @pl.when(s >= 2)
            def _():
                core_copy(s - 2).wait_send()

            def one(tile, carry):
                part = pl.ds(pl.multiple_of(tile * TILE, TILE), TILE)
                core_out[s % 2, part, :] = product(s, 1 - c, tile).astype(jnp.bfloat16)
                return carry

            lax.fori_loop(0, half // TILE, one, 0)
            core_copy(s).start()

        first = s - 1

        @pl.when((first >= 0) & (first < steps))
        def _():
            core_copy(first).wait_recv()

            def one(tile, carry):
                part = pl.ds(pl.multiple_of(tile * TILE, TILE), TILE)
                total = product(first, c, tile) + core_in[first % 4, part, :].astype(jnp.float32)
                total = total.astype(jnp.bfloat16).reshape(2, 4, piece, half)
                sum_core[first % 3, tile] = total
                return carry

            lax.fori_loop(0, half // TILE, one, 0)
            by_kind(first, functools.partial(start_first, first))

        for stage in range(6):

            @pl.when(s == steps + stage)
            def _(stage=stage):
                if stage > 0:
                    small_copy(stage - 1).wait()
                    total = small_sum[stage - 1] + small_got[stage - 1]
                    if stage < 5:
                        small_sum[stage] = total
                    else:
                        small_out[...] = total
                if stage < 5:
                    small_copy(stage).start()

        return carry

    lax.fori_loop(0, steps + 3 * LAG + 1, step, 0)
    for s in (steps - 2, steps - 1):
        core_copy(s).wait_send()
    for number in range(rounds):
        finish_back(number)


def backward(pick, out_grad, docs, row_now, weights, saved, piece, cols):
    units, width, _ = weights.shape
    rows = out_grad.shape[0]
    blocks = (units // LAYERS - 4) // 2
    half = width // 2
    low, full = jnp.bfloat16, jnp.float32
    rounds = pick.shape[0] // 10
    small = (LAYERS * (8 + blocks), width)
    any_spec = pl.BlockSpec(memory_space=pl.ANY)
    vmem_spec = pl.BlockSpec(memory_space=pltpu.VMEM)
    dma = pltpu.SemaphoreType.DMA
    summed, total, small = pl.pallas_call(
        backward_kernel,
        out_shape=(
            jax.ShapeDtypeStruct((rounds, width // piece, piece, cols), low),
            jax.ShapeDtypeStruct((rows, width), full),
            jax.ShapeDtypeStruct(small, full),
        ),
        in_specs=[pl.BlockSpec(memory_space=pltpu.SMEM)] + [vmem_spec] * 4 + [any_spec] * (1 + len(saved)),
        out_specs=(vmem_spec, vmem_spec, vmem_spec),
        scratch_shapes=[
            pltpu.VMEM((units, piece, width), low),
            pltpu.VMEM((rounds, 8, piece, width), low),
            pltpu.VMEM((4, rows, width), low),
            pltpu.VMEM((7, rows, width), low),
            pltpu.VMEM((3, width, width), low),
            pltpu.VMEM((rows, width), full),
            pltpu.VMEM((rows, 128), full),
            pltpu.VMEM((rows, width), low),
            pltpu.VMEM((3, rows, width), low),
            pltpu.VMEM((width // HEAD_DIM, 1, rows), full),
            pltpu.VMEM((rows, rows), full),
            pltpu.VMEM((rows, width), low),
            pltpu.VMEM((2, half, half), low),
            pltpu.VMEM((4, half, half), low),
            pltpu.VMEM((3, 2, 2, 4, piece, half), low),
            pltpu.VMEM((4, 2, 2, 4, piece, half // 2), low),
            pltpu.VMEM((3, 2, 2, 4, piece, half // 2), low),
            pltpu.VMEM((4, 2, 4, piece, half // 2), low),
            pltpu.VMEM((3, 4, piece, half), low),
            pltpu.VMEM((4, 3, piece, half), low),
            pltpu.VMEM((4, 3, 2, 2, piece, LANES), low),
            pltpu.VMEM((3, 2, 2, piece, LANES), low),
            pltpu.VMEM((4, 2, piece, LANES), low),
            pltpu.VMEM((3, 2, piece, LANES), low),
            pltpu.VMEM((4, piece, LANES), low),
            pltpu.VMEM((5,) + small, full),
            pltpu.VMEM((5,) + small, full),
            dma((6, 3)),
            dma((2, 4)),
            dma((2, 5, 4)),
            dma((2, 3, 4)),
            dma((2, 4, 4)),
            dma((2, 5)),
            dma((rounds,)),
            dma((2, rounds)),
        ],
        compiler_params=pltpu.CompilerParams(
            collective_id=1, has_side_effects=True, vmem_limit_bytes=63 * 1024 * 1024
        ),
        name="backward_reduce",
    )(pick, out_grad, docs[:, None], docs[None, :], row_now, weights, *saved)
    return (total, summed, small)


def norm_rows(value, gain, shift):
    centred = value - jnp.mean(value, axis=1, keepdims=True)
    inverse = lax.rsqrt(jnp.mean(centred * centred, axis=1, keepdims=True) + EPS_NORM)
    scaled = centred * inverse
    return (scaled * gain + shift, scaled, inverse)


NORM_ROWS = 128


def forward_kernel(
    slot_ref,
    masters_ref,
    hidden_ref,
    docs_col_ref,
    docs_row_ref,
    col_ref,
    row_ref,
    out_ref,
    final_ref,
    table_ref,
    *refs,
):
    saved, bufs = refs[:11], refs[11:22]
    rounds = masters_ref.shape[0]
    (x_buf, normed_buf, total_buf, mask_buf, unit_buf, own_ref) = refs[22:28]
    (own_sem, sems, unit_sem, save_sem, got_sem, round_sems) = refs[28:34]
    (masters_buf, sent_ref, col_got, bias_buf, master_sem, col_sems) = refs[34:40]
    rank_ref, back_ref = refs[40:42]
    got = refs[42:]
    (low_buf, mixed_buf, ctx_buf, lse_buf, one_buf, inv_one_buf, nb_buf) = bufs[:7]
    (act_buf, slope_buf, two_buf, inv_two_buf) = bufs[7:]
    units, piece, width = own_ref.shape
    rows = hidden_ref.shape[0]
    per_layer = units // LAYERS
    blocks = (per_layer - 4) // 2
    dp, tensor = lax.axis_index("dp"), lax.axis_index("tensor")
    z, y, x, c = dp // 2, dp % 2, tensor // 2, tensor % 2
    half = width // 2
    line, plane = 4 * piece, 8 * piece
    to_core = (dp, x * 2 + 1 - c)
    to_x = (dp, (1 - x) * 2 + c)
    to_y = (z * 2 + 1 - y, tensor)
    to_z = [(((z + k) % 4) * 2 + y, tensor) for k in (1, 2, 3)]
    mesh_id = pl.DeviceIdType.MESH

    barrier = greet_all(z, y, x, c)
    masters_in = [
        pltpu.make_async_copy(masters_ref.at[i], masters_buf.at[i], master_sem.at[i])
        for i in range(rounds)
    ]
    for copy in masters_in:
        copy.start()
    cols = sent_ref.shape[2]
    owners = table_ref.shape[0] // rounds - 2

    def turn_of(unit):
        layer, j = unit // per_layer, unit % per_layer
        feed = jnp.where(j < 4 + blocks, 2 * (j - 4) + 1, 2 * (j - 4 - blocks))
        place = jnp.where(j < 3, 2 * blocks + 1 + j, jnp.where(j == 3, 2 * blocks, feed))
        return (LAYERS - 1 - layer) * per_layer + place

    def rank_one(unit, carry):
        mine, turn = slot_ref[unit] // rounds, turn_of(unit)
        before, after = 0, 0
        for other in range(units):
            same = jnp.where(slot_ref[other] // rounds == mine, 1, 0)
            before = before + jnp.where(other < unit, same, 0)
            after = after + jnp.where(turn_of(other) > turn, same, 0)
        rank_ref[unit] = before
        back_ref[unit] = rounds - 1 - after
        return carry

    lax.fori_loop(0, units, rank_one, 0)

    def first_of(number):
        found = 0
        for unit in range(units):
            slot = slot_ref[unit]
            here = (slot // rounds == dp) & (rank_ref[unit] == number)
            found = found + jnp.where(here, slot % rounds, 0)
        return found

    def fill_table():
        def spot_one(spot, carry):
            found = (LAYERS - 1) * per_layer + 4 + blocks
            for unit in range(units):
                at = back_ref[unit] * owners + slot_ref[unit] // rounds
                found = jnp.where(at == spot, unit, found)
            table_ref[spot] = found
            return carry

        lax.fori_loop(0, rounds * owners, spot_one, 0)
        for i in range(rounds):
            turn, taken = 0, 0
            for unit in range(units):
                here = slot_ref[unit] == dp * rounds + i
                turn = turn + jnp.where(here, back_ref[unit], 0)
                taken = taken + jnp.where(here, 1, 0)
            table_ref[rounds * owners + i] = turn
            table_ref[rounds * (owners + 1) + i] = taken
    me = dp * 4 + tensor

    def part_for(number, zz, yy, xx, cc):
        start = pl.multiple_of(spread_order(zz, yy, xx, cc) * piece, piece)
        return sent_ref.at[number, pl.ds(start, piece)]

    def keep(number):
        return pltpu.make_async_copy(
            part_for(number, z, y, x, c), got[number].at[me], got_sem.at[number]
        )

    def round_copy(number, src, dst, peer):
        return pltpu.make_async_remote_copy(
            src_ref=src,
            dst_ref=dst,
            send_sem=round_sems.at[0, number],
            recv_sem=round_sems.at[1, number],
            device_id=peer,
            device_id_type=mesh_id,
        )

    def start_round(number):
        keep(number).start()

        def send(zz, yy, xx, cc):
            src = part_for(number, zz, yy, xx, cc)
            round_copy(number, src, got[number].at[me], (zz * 2 + yy, xx * 2 + cc)).start()

        every_other(z, y, x, c, send)

    def finish_round(number):
        keep(number).wait()
        most = got[number].at[pl.ds(0, 31)]
        round_copy(number, most, most, to_core).wait()

    def pick(unit, there):
        rank, owner = rank_ref[unit], slot_ref[unit] // rounds
        for j in range(4):
            value = got[0][owner * 4 + j]
            for number in range(1, there):
                value = jnp.where(rank == number, got[number][owner * 4 + j], value)
            own_ref[unit, :, j * cols : (j + 1) * cols] = value

    def column_copies():
        return [
            pltpu.make_async_remote_copy(
                src_ref=col_ref,
                dst_ref=col_got.at[tensor],
                send_sem=col_sems.at[0, k],
                recv_sem=col_sems.at[1, k],
                device_id=(dp, (tensor + k + 1) % 4),
                device_id_type=mesh_id,
            )
            for k in range(3)
        ]

    for copy in masters_in:
        copy.wait()
    sent_ref[0] = masters_buf[first_of(0)].astype(sent_ref.dtype)
    pl.semaphore_wait(barrier, 31)
    start_round(0)
    for number in range(1, rounds):
        sent_ref[number] = masters_buf[first_of(number)].astype(sent_ref.dtype)
    start_round(1)
    col_got[tensor] = col_ref[...]
    for copy in column_copies():
        copy.start()
    fill_table()

    my_line = pl.multiple_of(((c * 2 + x) * 2 + y) * line, line)
    my_rows = pl.ds(pl.multiple_of(my_line + z * piece, piece), piece)
    parts, cycle = 2, sems.shape[2]

    def half_of(s):
        return pl.ds(pl.multiple_of((s % parts) * half, half), half)

    def wide(s, start, size):
        return pl.ds(pl.multiple_of((s % parts) * half + start, LANES), size)

    late_cols = LANES

    def ways(s):
        short = half // 2 - late_cols
        return (
            (s % 2 == 0, wide(s, 0, half // 2), wide(s, half // 2, half // 2), None),
            (
                s % 4 == 1,
                wide(s, 0, half // 2),
                wide(s, half // 2, short),
                wide(s, half - late_cols, late_cols),
            ),
            (
                s % 4 == 3,
                wide(s, 0, short),
                wide(s, short, half // 2),
                wide(s, half - late_cols, late_cols),
            ),
        )

    def remote(src, dst, index, s, peer):
        return pltpu.make_async_remote_copy(
            src_ref=src,
            dst_ref=dst,
            send_sem=sems.at[0, index, s % cycle],
            recv_sem=sems.at[1, index, s % cycle],
            device_id=peer,
            device_id_type=mesh_id,
        )

    def own_copy(s):
        unit, cols_now = s // parts, half_of(s)
        return pltpu.make_async_copy(
            own_ref.at[unit, :, cols_now],
            out_ref.at[unit, my_rows, cols_now],
            own_sem.at[s % cycle],
        )

    def rows_at(xx, yy, zz):
        return pl.ds(pl.multiple_of(spread_order(zz, yy, xx, c) * piece, piece), piece)

    def stage_z(s, one, two, late):
        unit, copies = s // parts, []
        size = half if late is None else half - late_cols
        early = wide(s, 0, size)
        here, there = own_ref.at[unit, :, early], out_ref.at[unit, my_rows, early]
        copies = [remote(here, there, k, s, to_z[k]) for k in range(3)]
        if late is not None:
            here, there = own_ref.at[unit, :, late], out_ref.at[unit, my_rows, late]
            copies.append(remote(here, there, 9, s, to_x))
        return copies

    def stage_one(s, one, two, late):
        unit, rows = s // parts, pl.ds(my_line, line)
        one, two = out_ref.at[unit, rows, one], out_ref.at[unit, rows, two]
        copies = [remote(one, one, 3, s, to_y), remote(two, two, 4, s, to_x)]
        if late is not None:
            for i in range(2):
                there = out_ref.at[unit, rows_at(i, y, z), late]
                copies.append(remote(there, there, 10 + i, s, to_y))
        return copies

    def stage_two(s, one, two, late):
        unit = s // parts
        rows = pl.ds(pl.multiple_of((c * 2 + x) * plane, plane), plane)
        there = out_ref.at[unit, rows, one]
        copies = [remote(there, there, 5, s, to_x)]
        for i in range(2):
            rows = pl.ds(pl.multiple_of(((c * 2 + i) * 2 + y) * line, line), line)
            there = out_ref.at[unit, rows, two]
            copies.append(remote(there, there, 6 + i, s, to_y))
        if late is not None:
            for i in range(4):
                there = out_ref.at[unit, rows_at(i // 2, i % 2, z), late]
                copies += [remote(there, there, 12 + 3 * i + k, s, to_z[k]) for k in range(3)]
        return copies

    def stage_core(s):
        rows = pl.ds(pl.multiple_of(c * 2 * plane, 2 * plane), 2 * plane)
        there = out_ref.at[s // parts, rows, half_of(s)]
        return [remote(there, there, 8, s, to_core)]

    stages = (stage_z, stage_one, stage_two, stage_core)

    def each_copy(number, s, act):
        if stages[number] is stage_core:
            for copy in stage_core(s):
                act(copy)
            return
        for kind, one, two, late in ways(s):

            @pl.when(kind)
            def _(one=one, two=two, late=late):
                for copy in stages[number](s, one, two, late):
                    act(copy)


    def unit_copy(unit):
        slot = unit % 2
        return pltpu.make_async_copy(out_ref.at[unit], unit_buf.at[slot], unit_sem.at[slot])

    def save(number, layer, block=None):
        src, dst, sem = bufs[number], saved[number].at[layer], save_sem.at[number, 0]
        if block is not None:
            src, dst, sem = src.at[block], dst.at[block], save_sem.at[number, block]
        return pltpu.make_async_copy(src, dst, sem)

    def free(numbers, layer, block=None):
        @pl.when(layer > 0)
        def _():
            for number in numbers:
                save(number, layer - 1, block).wait()

    def heads(start, stop):
        inputs = [mixed_buf.at[i] for i in range(3)]
        for pair in range(start, stop):
            attend_pair(pair, *inputs, mask_buf, ctx_buf, lse_buf)

    tall = rows // parts
    pairs = width // LANES

    def compute(unit, turn):
        layer, j = unit // per_layer, unit % per_layer
        matrix = unit_buf.at[unit % 2]
        mine = pl.ds(pl.multiple_of(turn * tall, tall), tall)

        def small(i):
            return row_ref[layer, i : i + 1, :]

        def bias(i):
            return bias_buf[pl.ds(layer * (2 + blocks) + i, 1), :]

        def over_rows(body):
            def one(tile, carry):
                body(pl.ds(pl.multiple_of(turn * tall + tile * NORM_ROWS, NORM_ROWS), NORM_ROWS))
                return carry

            lax.fori_loop(0, tall // NORM_ROWS, one, 0)

        @pl.when((j == 0) & (turn == 0))
        def _():
            free((0, 1), layer)

            @pl.when(layer == 0)
            def _():
                x_buf[...] = hidden_ref[...].astype(jnp.float32)

            low_buf[...] = x_buf[...].astype(jnp.bfloat16)
            save(0, layer).start()

        @pl.when(j < 3)
        def _():
            value = dot(low_buf[mine, :], matrix[...], ((1,), (0,)))
            value = value + jnp.where(j == 1, 0.0, bias(j // 2))
            scale = jnp.where(j == 0, HEAD_DIM ** (-0.5), 1.0)
            mixed_buf[j, mine, :] = (value * scale).astype(jnp.bfloat16)

        @pl.when((j == 2) & (turn == 1))
        def _():
            save(1, layer).start()
            free((2, 3), layer)
            heads(0, pairs // 4)

        @pl.when((j == 3) & (turn == 0))
        def _():
            heads(pairs // 4, 3 * pairs // 4)

        @pl.when((j == 3) & (turn == 1))
        def _():
            heads(3 * pairs // 4, pairs)
            save(2, layer).start()
            save(3, layer).start()
            total_buf[...] = dot(ctx_buf[...], matrix[...], ((1,), (1,)))
            free((4, 5, 6), layer)

            def body(tile, carry):
                part = pl.ds(pl.multiple_of(tile * NORM_ROWS, NORM_ROWS), NORM_ROWS)
                value = x_buf[part, :] + total_buf[part, :] + small(0)
                normed, scaled, inverse = norm_rows(value, small(2), small(3))
                normed_buf[part, :] = normed
                nb_buf[part, :] = normed.astype(jnp.bfloat16)
                one_buf[part, :] = scaled
                inv_one_buf[part, :] = jnp.broadcast_to(inverse, (NORM_ROWS, 128))
                return carry

            lax.fori_loop(0, rows // NORM_ROWS, body, 0)
            for number in (4, 5, 6):
                save(number, layer).start()

        @pl.when((j >= 4) & (j < 4 + blocks))
        def _():
            block = j - 4

            @pl.when(turn == 0)
            def _():
                free((7, 8), layer, block)

            value = dot(nb_buf[mine, :], matrix[...], ((1,), (0,)))
            act, slope = gelu_pair(value + bias(2 + block))
            act_buf[block, mine, :] = act.astype(jnp.bfloat16)
            slope_buf[block, mine, :] = slope.astype(jnp.bfloat16)

            @pl.when(turn == 1)
            def _():
                save(7, layer, block).start()
                save(8, layer, block).start()

        @pl.when(j >= 4 + blocks)
        def _():
            block = j - 4 - blocks
            part = dot(act_buf[block, mine, :], matrix[...], ((1,), (1,)))

            @pl.when(block == 0)
            def _():
                total_buf[mine, :] = part

            @pl.when(block > 0)
            def _():
                total_buf[mine, :] += part

        @pl.when(j == per_layer - 1)
        def _():
            @pl.when(turn == 0)
            def _():
                free((9, 10), layer)

            def body(part):
                value = normed_buf[part, :] + total_buf[part, :] + small(1)
                output, scaled, inverse = norm_rows(value, small(4), small(5))
                x_buf[part, :] = output
                two_buf[part, :] = scaled
                inv_two_buf[part, :] = jnp.broadcast_to(inverse, (NORM_ROWS, 128))

            over_rows(body)

            @pl.when(turn == 1)
            def _():
                save(9, layer).start()
                save(10, layer).start()

    steps = parts * units

    def step(s, carry):
        for number in range(len(stages), -1, -1):
            now = s - number * LAG

            if number == 0:
                for turn in range(rounds):
                    last = turn == rounds - 1
                    due = (s == parts * turn) | (last & (s > parts * turn) & (s % parts == 0))

                    @pl.when(due & (s < steps))
                    def _(turn=turn):
                        @pl.when(s == parts * turn)
                        def _():
                            finish_round(turn)

                        if turn + 2 < rounds:
                            start_round(turn + 2)
                        pick(s // parts, turn + 1)

            @pl.when((now >= 0) & (now < steps))
            def _(now=now, number=number):
                if number == 0:
                    own_copy(now).start()
                else:
                    if number == 1:
                        own_copy(now).wait()
                    each_copy(number - 1, now, lambda copy: copy.wait())
                if number < len(stages):
                    each_copy(number, now, lambda copy: copy.start())
                else:

                    @pl.when(now % parts == parts - 1)
                    def _():
                        unit_copy(now // parts).start()

        @pl.when(s == len(stages) * LAG)
        def _():
            for copy in column_copies():
                copy.wait()
            for j in range(4):
                bias_buf[:, j * cols : (j + 1) * cols] = col_got[j]

        done = s - len(stages) * LAG - parts

        @pl.when(done >= 0)
        def _():
            @pl.when(done % parts == 0)
            def _():
                unit_copy(done // parts).wait()

            compute(done // parts, done % parts)

        return carry

    fill_mask(mask_buf, docs_col_ref, docs_row_ref)
    lax.fori_loop(0, steps + len(stages) * LAG + parts, step, 0)
    final_ref[...] = x_buf[...]
    last = LAYERS - 1
    for number in (0, 1, 2, 3, 4, 5, 6, 9, 10):
        save(number, last).wait()
    for block in range(blocks):
        save(7, last, block).wait()
        save(8, last, block).wait()


def forward(unit_slot, masters, hidden_in, docs, col_now, row_now, piece, owners):
    units = unit_slot.shape[0]
    rounds, width, cols = masters.shape
    rows = hidden_in.shape[0]
    blocks = (units // LAYERS - 4) // 2
    low, full = jnp.bfloat16, jnp.float32
    kept = [
        ((rows, width), low),
        ((3, rows, width), low),
        ((rows, width), low),
        ((width // HEAD_DIM, 1, rows), full),
        ((rows, width), full),
        ((rows, 128), full),
        ((rows, width), low),
        ((blocks, rows, width), low),
        ((blocks, rows, width), low),
        ((rows, width), full),
        ((rows, 128), full),
    ]
    any_spec = pl.BlockSpec(memory_space=pl.ANY)
    vmem_spec = pl.BlockSpec(memory_space=pltpu.VMEM)
    smem_spec = pl.BlockSpec(memory_space=pltpu.SMEM)
    dma = pltpu.SemaphoreType.DMA
    return pl.pallas_call(
        forward_kernel,
        out_shape=[
            jax.ShapeDtypeStruct((units, width, width), low),
            jax.ShapeDtypeStruct((rows, width), full),
            jax.ShapeDtypeStruct((rounds * (owners + 2),), jnp.int32),
        ]
        + [jax.ShapeDtypeStruct((LAYERS,) + shape, dtype) for shape, dtype in kept],
        in_specs=[smem_spec] + [any_spec] + [vmem_spec] * 5,
        out_specs=[any_spec, vmem_spec, smem_spec] + [any_spec] * len(kept),
        scratch_shapes=[pltpu.VMEM(shape, dtype) for shape, dtype in kept]
        + [
            pltpu.VMEM((rows, width), full),
            pltpu.VMEM((rows, width), full),
            pltpu.VMEM((rows, width), full),
            pltpu.VMEM((rows, rows), full),
            pltpu.VMEM((2, width, width), low),
            pltpu.VMEM((units, piece, width), low),
            dma((8,)),
            dma((2, 24, 8)),
            dma((2,)),
            dma((len(kept), blocks)),
            dma((rounds,)),
            dma((2, rounds)),
            pltpu.VMEM((rounds, width, cols), full),
            pltpu.VMEM((rounds, width, cols), low),
            pltpu.VMEM((4,) + col_now.shape, full),
            pltpu.VMEM((col_now.shape[0], width), full),
            dma((rounds,)),
            dma((2, 3)),
            pltpu.SMEM((units,), jnp.int32),
            pltpu.SMEM((units,), jnp.int32),
        ]
        + [pltpu.VMEM((width // piece, piece, cols), low)] * rounds,
        compiler_params=pltpu.CompilerParams(
            collective_id=2, has_side_effects=True, vmem_limit_bytes=60 * 1024 * 1024
        ),
        name="gather_forward",
    )(
        unit_slot,
        masters,
        hidden_in,
        docs[:, None],
        docs[None, :],
        col_now,
        row_now,
    )


def run_general(
    unit_slot,
    masters,
    first_moment,
    second_moment,
    hidden_in,
    doc_ids,
    column_state,
    row_state,
    out_grad,
):
    slot_count, width, col_width = masters.shape
    units = unit_slot.shape[0]
    dp_size = lax.axis_size("dp")
    devices = dp_size * lax.axis_size("tensor")
    slots = slot_count * dp_size
    piece = width // devices
    per_layer = units // LAYERS
    blocks = (per_layer - 4) // 2
    tensor_size = lax.axis_size("tensor")
    rows = hidden_in.shape[0]
    seq_len = doc_ids.shape[1]
    heads = width // HEAD_DIM
    share = seq_len // rows
    tensor_index = lax.axis_index("tensor")
    groups = [list(range(i, i + share)) for i in range(0, tensor_size, share)]
    score_scale = HEAD_DIM ** (-0.5)
    sent = masters.astype(jnp.bfloat16).reshape(slot_count, devices, piece, col_width)
    spread = lax.all_to_all(sent.transpose(1, 0, 2, 3), BOTH, 0, 0)
    spread = spread.reshape(dp_size, tensor_size, slot_count, piece, col_width)
    spread = spread.transpose(0, 2, 3, 1, 4).reshape(slots, piece, width)
    mine = spread[unit_slot]
    weights = jnp.concatenate(
        [
            lax.all_gather(
                mine[layer * per_layer : (layer + 1) * per_layer], BOTH, axis=1, tiled=True
            )
            for layer in range(LAYERS)
        ],
        axis=0,
    )

    def matrices(layer):
        unit = weights[layer * per_layer : (layer + 1) * per_layer]
        return (unit[:3], unit[3], unit[4 : 4 + blocks], unit[4 + blocks :])

    row_docs = lax.dynamic_slice_in_dim(doc_ids, tensor_index // share, 1, axis=0)[0]
    my_docs = lax.dynamic_slice_in_dim(row_docs, (tensor_index % share) * rows, rows)
    same_doc = (my_docs[:, None] == row_docs[None, :])[None]

    def whole_row(value):
        if share == 1:
            return value
        return lax.all_gather(value, "tensor", axis=0, tiled=True, axis_index_groups=groups)

    def own_rows(value):
        if share == 1:
            return value
        return lax.psum_scatter(
            value, "tensor", scatter_dimension=0, tiled=True, axis_index_groups=groups
        )

    col_full = lax.all_gather(column_state[0], "tensor", axis=2, tiled=True)
    hidden = hidden_in.astype(jnp.float32)
    saved_layers = []
    for layer in range(LAYERS):
        w_qkv, w_proj, w_in, w_out = matrices(layer)
        row_now = row_state[0, layer]
        col_now = col_full[layer]
        hidden_bf = hidden.astype(jnp.bfloat16)
        query, key, value = (dot(hidden_bf, w_qkv[i], ((1,), (0,))) for i in range(3))
        query = ((query + col_now[0]) * score_scale).astype(jnp.bfloat16)
        key = key.astype(jnp.bfloat16)
        value = (value + col_now[1]).astype(jnp.bfloat16)
        query = query.reshape(rows, heads, HEAD_DIM)
        key = whole_row(key).reshape(seq_len, heads, HEAD_DIM)
        value = whole_row(value).reshape(seq_len, heads, HEAD_DIM)
        scores = jnp.einsum("qhd,khd->hqk", query, key, preferred_element_type=jnp.float32)
        scores = jnp.where(same_doc, scores, -1e30)
        row_top = jnp.max(scores, axis=-1, keepdims=True)
        log_total = row_top + jnp.log(
            jnp.sum(jnp.exp(scores - row_top), axis=-1, keepdims=True)
        )
        soft_bf = jnp.exp(scores - log_total).astype(jnp.bfloat16)
        context = jnp.einsum("hqk,khd->qhd", soft_bf, value, preferred_element_type=jnp.float32)
        context = context.reshape(rows, width).astype(jnp.bfloat16)
        attended = dot(context, w_proj, ((1,), (1,)))
        normed, scaled_one, inverse_one = norm_forward(
            hidden + attended + row_now[0], row_now[2], row_now[3]
        )
        normed_bf = normed.astype(jnp.bfloat16)
        pre_act = jnp.einsum("rd,bdc->brc", normed_bf, w_in, preferred_element_type=jnp.float32)
        activated, slope = gelu_pair(pre_act + col_now[2:, None])
        activated = activated.astype(jnp.bfloat16)
        slope = slope.astype(jnp.bfloat16)
        mlp_out = jnp.einsum(
            "brc,bdc->rd", activated, w_out, preferred_element_type=jnp.float32
        )
        output, scaled_two, inverse_two = norm_forward(
            normed + mlp_out + row_now[1], row_now[4], row_now[5]
        )
        saved_layers.append(
            (hidden_bf, query, key, value, log_total, context, scaled_one, inverse_one, normed_bf)
            + (slope, activated, scaled_two, inverse_two)
        )
        hidden = output
    upstream = out_grad.astype(jnp.float32)
    operands = [None] * LAYERS
    col_parts = [None] * LAYERS
    row_parts = [None] * LAYERS
    for layer in reversed(range(LAYERS)):
        w_qkv, w_proj, w_in, w_out = matrices(layer)
        row_now = row_state[0, layer]
        (
            hidden_bf,
            query,
            key,
            value,
            log_total,
            context,
            scaled_one,
            inverse_one,
            normed_bf,
            slope,
            activated,
            scaled_two,
            inverse_two,
        ) = saved_layers[layer]
        d_two, gain_two, shift_two = norm_backward(upstream, scaled_two, inverse_two, row_now[4])
        grad_bias_two = jnp.sum(d_two, axis=0)
        d_two_bf = d_two.astype(jnp.bfloat16)
        d_act = jnp.einsum("rd,bdc->brc", d_two_bf, w_out, preferred_element_type=jnp.float32)
        d_pre = (d_act * slope).astype(jnp.bfloat16)
        grad_bias_in = jnp.sum(d_pre, axis=1, dtype=jnp.float32)
        d_normed = jnp.einsum("brc,bdc->rd", d_pre, w_in, preferred_element_type=jnp.float32)
        d_normed = d_two + d_normed
        d_one, gain_one, shift_one = norm_backward(d_normed, scaled_one, inverse_one, row_now[2])
        grad_bias_proj = jnp.sum(d_one, axis=0)
        d_one_bf = d_one.astype(jnp.bfloat16)
        d_context = dot(d_one_bf, w_proj, ((1,), (0,))).astype(jnp.bfloat16)
        d_context = d_context.reshape(rows, heads, HEAD_DIM)
        scores = jnp.einsum("qhd,khd->hqk", query, key, preferred_element_type=jnp.float32)
        scores = jnp.where(same_doc, scores, -1e30)
        soft = jnp.exp(scores - log_total)
        d_values = jnp.einsum(
            "hqk,qhd->khd",
            soft.astype(jnp.bfloat16),
            d_context,
            preferred_element_type=jnp.float32,
        )
        d_probs = jnp.einsum(
            "qhd,khd->hqk", d_context, value, preferred_element_type=jnp.float32
        )
        d_scores = (
            soft * (d_probs - jnp.sum(soft * d_probs, axis=-1, keepdims=True))
        ).astype(jnp.bfloat16)
        d_queries = (
            jnp.einsum("hqk,khd->qhd", d_scores, key, preferred_element_type=jnp.float32)
            * score_scale
        )
        d_keys = jnp.einsum("hqk,qhd->khd", d_scores, query, preferred_element_type=jnp.float32)
        d_qkv = jnp.stack(
            [
                d_queries.reshape(rows, width),
                own_rows(d_keys.reshape(seq_len, width)),
                own_rows(d_values.reshape(seq_len, width)),
            ]
        ).astype(jnp.bfloat16)
        grad_bias_qkv = jnp.sum(d_qkv, axis=1, dtype=jnp.float32)
        upstream = d_one + jnp.einsum(
            "brc,bdc->rd", d_qkv, w_qkv, preferred_element_type=jnp.float32
        )
        operands[layer] = (hidden_bf, d_one_bf, normed_bf, d_two_bf)
        operands[layer] += (d_qkv, context[None], d_pre, activated)
        col_parts[layer] = jnp.concatenate(
            [
                grad_bias_qkv[0:1],
                grad_bias_qkv[2:3],
                grad_bias_in,
            ],
            axis=0,
        )
        row_parts[layer] = jnp.stack(
            [grad_bias_proj, grad_bias_two, gain_one, shift_one, gain_two, shift_two]
        )
    small = jnp.stack([jnp.stack(col_parts), jnp.stack(row_parts)])
    summed = []
    for layer in operands:
        whole = jnp.concatenate(
            [
                jnp.einsum(
                    "rd,brc->bdc", layer[i], layer[4 + i], preferred_element_type=jnp.float32
                )
                for i in range(4)
            ],
            axis=0,
        )
        summed.append(
            lax.psum_scatter(whole.astype(jnp.bfloat16), BOTH, scatter_dimension=1, tiled=True)
        )
    summed = jnp.concatenate(summed, axis=0)

    slot_ids = jnp.arange(slots, dtype=jnp.int32)
    named = unit_slot[None, :] == slot_ids[:, None]
    holds = jnp.any(named, axis=1)
    unit_of = jnp.argmax(named, axis=1)
    back = jnp.where(holds[:, None, None], summed[unit_of], jnp.zeros((), jnp.bfloat16))
    back = back.reshape(dp_size, slot_count, piece, tensor_size, col_width)
    back = back.transpose(0, 3, 1, 2, 4).reshape(devices, slot_count, piece, col_width)
    owned = lax.all_to_all(back, BOTH, 0, 0)
    owned = owned.transpose(1, 0, 2, 3)
    owned = owned.reshape(slot_count, width, col_width)
    occupied = lax.dynamic_slice_in_dim(holds, lax.axis_index("dp") * slot_count, slot_count)
    occupied = occupied.astype(jnp.float32)[:, None, None]
    new_master, new_first, new_second = adamw_update(
        masters, owned.astype(jnp.float32), first_moment, second_moment, RATE_UNITS
    )
    updated = (
        new_master * occupied,
        jnp.stack([new_first * occupied, new_second * occupied]),
    )
    return (hidden, upstream, updated, lax.psum(small, BOTH))


def adamw_kernel(table_ref, owned_ref, value_ref, first_ref, second_ref, value_out, state_out):
    taken = table_ref[table_ref.shape[0] - pl.num_programs(0) + pl.program_id(0)] > 0
    gradient = jnp.where(taken, owned_ref[0].astype(jnp.float32), 0.0)
    value, first, second = adamw_update(
        value_ref[0], gradient, first_ref[0], second_ref[0], RATE_UNITS
    )
    value_out[0] = jnp.where(taken, value, 0.0)
    state_out[0, 0] = jnp.where(taken, first, 0.0)
    state_out[1, 0] = jnp.where(taken, second, 0.0)


def adamw_slots(table, owned, masters, first_moment, second_moment):
    count, width, cols = masters.shape
    tall = width // 2
    at = table.shape[0] - 2 * count
    tile = pl.BlockSpec((1, tall, cols), lambda i, j, table: (i, j, 0))
    return pl.pallas_call(
        adamw_kernel,
        grid_spec=pltpu.PrefetchScalarGridSpec(
            num_scalar_prefetch=1,
            grid=(count, width // tall),
            in_specs=[
                pl.BlockSpec((1, tall, cols), lambda i, j, table: (table[at + i], j, 0)),
                tile,
                tile,
                tile,
            ],
            out_specs=(tile, pl.BlockSpec((2, 1, tall, cols), lambda i, j, table: (0, i, j, 0))),
        ),
        out_shape=(
            jax.ShapeDtypeStruct(masters.shape, jnp.float32),
            jax.ShapeDtypeStruct((2,) + masters.shape, jnp.float32),
        ),
        name="adamw",
    )(table, owned, masters, first_moment, second_moment)


def run_kernels(
    unit_slot,
    masters,
    first_moment,
    second_moment,
    hidden_in,
    doc_ids,
    column_state,
    row_state,
    out_grad,
):
    slot_count, width, cols = masters.shape
    blocks = (unit_slot.shape[0] // LAYERS - 4) // 2
    dp_size = lax.axis_size("dp")
    piece = width // (dp_size * lax.axis_size("tensor"))
    docs = lax.dynamic_index_in_dim(doc_ids, lax.axis_index("tensor"), 0, keepdims=False)
    row_now = row_state[0]
    weights, hidden, table, *saved = forward(
        unit_slot,
        masters,
        hidden_in,
        docs,
        column_state[0].reshape(-1, cols),
        row_now,
        piece,
        dp_size,
    )
    upstream, owned, small = backward(table, out_grad, docs, row_now, weights, saved, piece, cols)
    slots = adamw_slots(
        table, owned.reshape(masters.shape), masters, first_moment, second_moment
    )
    return (hidden, upstream, slots, small.reshape(2, LAYERS, 2 + blocks, width))


def local(
    hidden_in,
    doc_ids,
    unit_slot,
    masters,
    first_moment,
    second_moment,
    column_state,
    row_state,
    out_grad,
):
    col_width = masters.shape[2]
    tensor_index = lax.axis_index("tensor")
    kernels = (lax.axis_size("dp"), lax.axis_size("tensor")) == (8, 4)
    kernels = kernels and hidden_in.shape[0] == doc_ids.shape[1]
    run = run_kernels if kernels else run_general
    hidden, upstream, (unit_master, unit_state), small = run(
        unit_slot,
        masters,
        first_moment,
        second_moment,
        hidden_in,
        doc_ids,
        column_state,
        row_state,
        out_grad,
    )
    row_total = small[1]
    col_total = lax.dynamic_slice_in_dim(small[0], tensor_index * col_width, col_width, axis=2)
    new_col, col_first, col_second = adamw_update(
        column_state[0], col_total, column_state[1], column_state[2], RATE_SMALL
    )
    column_out = jnp.stack([col_total, new_col, col_first, col_second])
    new_row, row_first, row_second = adamw_update(
        row_state[0], row_total, row_state[1], row_state[2], RATE_SMALL
    )
    row_out = jnp.stack([row_total, new_row, row_first, row_second])
    return (hidden, upstream, unit_master, unit_state, column_out, row_out)


def solution(mesh):
    return jax.shard_map(
        local,
        mesh=mesh,
        in_specs=(
            P(("dp", "tensor"), None),
            P("dp", None),
            P(),
            P("dp", None, "tensor"),
            P("dp", None, "tensor"),
            P("dp", None, "tensor"),
            P(None, None, None, "tensor"),
            P(),
            P(("dp", "tensor"), None),
        ),
        out_specs=(
            P(("dp", "tensor"), None),
            P(("dp", "tensor"), None),
            P("dp", None, "tensor"),
            P(None, "dp", None, "tensor"),
            P(None, None, None, "tensor"),
            P(),
        ),
        check_vma=False,
    )
```

```python
import functools
import math

import jax
import jax.numpy as jnp
from jax import lax
from jax.experimental import pallas as pl
from jax.experimental.pallas import tpu as pltpu
from jax.sharding import PartitionSpec as P

HEAD_DIM = 64
LAYERS = 2
STEP = 3

EPS_NORM = 1e-06
RATE_UNITS = 0.05
RATE_SMALL = 0.2
WEIGHT_DECAY = 0.01
ADAM_EPS = 1e-08
BETA_MOMENT = 0.5
BOTH = ("dp", "tensor")


def norm_forward(summed, gain, shift):
    row_mean = jnp.mean(summed, axis=1, keepdims=True)
    centred = summed - row_mean
    inverse = lax.rsqrt(jnp.mean(centred * centred, axis=1, keepdims=True) + EPS_NORM)
    scaled = centred * inverse
    return (scaled * gain + shift, scaled, inverse)


def norm_backward(upstream, scaled, inverse, gain):
    d_scaled = upstream * gain
    mean_one = jnp.mean(d_scaled, axis=1, keepdims=True)
    mean_two = jnp.mean(d_scaled * scaled, axis=1, keepdims=True)
    grad_input = inverse * (d_scaled - mean_one - scaled * mean_two)
    return (grad_input, jnp.sum(upstream * scaled, axis=0), jnp.sum(upstream, axis=0))


def gelu_pair(v):
    cdf = 0.5 * (1.0 + lax.erf(v * 2.0 ** (-0.5)))
    bell = jnp.exp(-0.5 * v * v) * (2.0 * math.pi) ** (-0.5)
    return (v * cdf, cdf + v * bell)


def adamw_update(old_value, gradient, first_old, second_old, learn_rate):
    first_new = BETA_MOMENT * first_old + (1.0 - BETA_MOMENT) * gradient
    second_new = BETA_MOMENT * second_old + (1.0 - BETA_MOMENT) * gradient * gradient
    correct = 1.0 - BETA_MOMENT**STEP
    step_size = first_new / correct / (jnp.sqrt(second_new / correct) + ADAM_EPS)
    return (old_value - learn_rate * (step_size + WEIGHT_DECAY * old_value), first_new, second_new)


def dot(left, right, dims):
    return lax.dot_general(left, right, (dims, ((), ())), preferred_element_type=jnp.float32)


LANES = 2 * HEAD_DIM


def head_lanes(value, head):
    lane = lax.broadcasted_iota(jnp.int32, value.shape, 1)
    keep = lane < HEAD_DIM if head == 0 else lane >= HEAD_DIM
    return jnp.where(keep, value, jnp.zeros_like(value))


def pair_lanes(first, second):
    lane = lax.broadcasted_iota(jnp.int32, first.shape, 1)
    return jnp.where(lane < HEAD_DIM, first, second)


def attend_pair(pair, q_ref, k_ref, v_ref, mask_ref, ctx_ref, lse_ref):
    lanes = pl.ds(pl.multiple_of(pair * LANES, LANES), LANES)
    query, key, value = q_ref[:, lanes], k_ref[:, lanes], v_ref[:, lanes]
    value_t = value.T
    parts = []
    for head in range(2):
        scores = dot(head_lanes(key, head), query, ((1,), (1,))) + mask_ref[...]
        top = jnp.max(scores, axis=0, keepdims=True)
        weight = jnp.exp(scores - top)
        total = jnp.sum(weight, axis=0, keepdims=True)
        lse_ref[pair * 2 + head] = top + jnp.log(total)
        mine = value_t[head * HEAD_DIM : (head + 1) * HEAD_DIM]
        mixed = dot(mine, weight.astype(jnp.bfloat16), ((1,), (0,)))
        parts.append(mixed * (1.0 / total))
    ctx_ref[:, lanes] = jnp.concatenate(parts, axis=0).T.astype(ctx_ref.dtype)


def attend_back_pair(pair, q_ref, k_ref, v_ref, d_ref, mask_ref, lse_ref, dq_ref, dk_ref, dv_ref):
    lanes = pl.ds(pl.multiple_of(pair * LANES, LANES), LANES)
    query, key, value = q_ref[:, lanes], k_ref[:, lanes], v_ref[:, lanes]
    grad = d_ref[:, lanes]
    key_t = key.T
    parts, d_keys, d_values = [], [], []
    for head in range(2):
        scores = dot(head_lanes(key, head), query, ((1,), (1,))) + mask_ref[...]
        soft = jnp.exp(scores - lse_ref[pair * 2 + head])
        d_values.append(dot(soft.astype(jnp.bfloat16), grad, ((1,), (0,))))
        d_soft = dot(head_lanes(value, head), grad, ((1,), (1,)))
        both = soft * d_soft
        mean = jnp.sum(both, axis=0, keepdims=True)
        d_scores = (both - soft * mean).astype(jnp.bfloat16)
        d_keys.append(dot(d_scores, query, ((1,), (0,))))
        mine = key_t[head * HEAD_DIM : (head + 1) * HEAD_DIM]
        parts.append(dot(mine, d_scores, ((1,), (0,))))
    scale = HEAD_DIM ** (-0.5)
    dq_ref[:, lanes] = (jnp.concatenate(parts, axis=0).T * scale).astype(dq_ref.dtype)
    dk_ref[:, lanes] = pair_lanes(*d_keys).astype(dk_ref.dtype)
    dv_ref[:, lanes] = pair_lanes(*d_values).astype(dv_ref.dtype)


def fill_mask(mask_ref, docs_col_ref, docs_row_ref):
    same = docs_col_ref[...] == docs_row_ref[...]
    mask_ref[...] = jnp.where(same, 0.0, -1e30).astype(jnp.float32)


LAG = 2


def spread_order(z, y, x, c):
    return ((c * 2 + x) * 2 + y) * 4 + z


def every_other(z, y, x, c, body):
    for step in (2, 1, 3, 0):

        def one(i, carry, step=step):
            body((z + step) % 4, (y + i // 4) % 2, (x + (i // 2) % 2) % 2, (c + i % 2) % 2)
            return carry

        lax.fori_loop(1 if step == 0 else 0, 8, one, 0)


def greet_all(z, y, x, c):
    barrier = pltpu.get_barrier_semaphore()

    def greet(zz, yy, xx, cc):
        pl.semaphore_signal(
            barrier,
            inc=1,
            device_id=(zz * 2 + yy, xx * 2 + cc),
            device_id_type=pl.DeviceIdType.MESH,
        )

    every_other(z, y, x, c, greet)
    return barrier


TILE = 256


def norm_back_rows(upstream, scaled, inverse, gain):
    d_scaled = upstream * gain
    mean_one = jnp.mean(d_scaled, axis=1, keepdims=True)
    mean_two = jnp.mean(d_scaled * scaled, axis=1, keepdims=True)
    return inverse * (d_scaled - mean_one - scaled * mean_two)


def backward_kernel(
    pick_ref,
    out_grad_ref,
    docs_col_ref,
    docs_row_ref,
    row_ref,
    weights_ref,
    low_ref,
    mixed_ref,
    ctx_ref,
    lse_ref,
    one_ref,
    inv_one_ref,
    normed_ref,
    act_ref,
    slope_ref,
    two_ref,
    inv_two_ref,
    owned_ref,
    total_ref,
    small_out,
    out_ref,
    back_buf,
    left_buf,
    right_buf,
    unit_buf,
    scaled_buf,
    inv_buf,
    slope_buf,
    mixed_buf,
    lse_buf,
    mask_buf,
    d_ctx_buf,
    core_out,
    core_in,
    sum_core,
    first_in,
    sum_first,
    second_in,
    sum_second,
    z_in,
    late_in,
    late_sum,
    late_second_in,
    late_pair,
    late_last_in,
    small_sum,
    small_got,
    load_sem,
    core_sems,
    first_sems,
    second_sems,
    z_sems,
    small_sems,
    own_sems,
    round_sems,
):
    units, piece, width = out_ref.shape
    rows = total_ref.shape[0]
    per_layer = units // LAYERS
    blocks = (per_layer - 4) // 2
    at_out, at_query = 2 * blocks, 2 * blocks + 1
    dp, tensor = lax.axis_index("dp"), lax.axis_index("tensor")
    z, y, x, c = dp // 2, dp % 2, tensor // 2, tensor % 2
    half, parts = width // 2, 2
    side_cols = half // 2
    to_core = (dp, x * 2 + 1 - c)
    to_x = (dp, (1 - x) * 2 + c)
    to_y = (z * 2 + 1 - y, tensor)
    to_z = [(((z + k) % 4) * 2 + y, tensor) for k in (1, 2, 3)]
    to_z1 = ((z + 1 - 2 * (z % 2)) * 2 + y, tensor)
    to_z2 = (((z + 2) % 4) * 2 + y, tensor)
    mesh_id = pl.DeviceIdType.MESH

    barrier = greet_all(z, y, x, c)

    def remote(src, dst, sems, send, recv, peer):
        return pltpu.make_async_remote_copy(
            src_ref=src,
            dst_ref=dst,
            send_sem=sems.at[send],
            recv_sem=sems.at[recv],
            device_id=peer,
            device_id_type=mesh_id,
        )

    def place(s):
        return LAYERS - 1 - s // per_layer, s % per_layer

    def unit_of(s):
        layer, j = place(s)
        feed = jnp.where(j % 2 == 0, 4 + blocks + j // 2, 4 + j // 2)
        return layer * per_layer + jnp.where(
            j < at_out, feed, jnp.where(j == at_out, 3, j - at_query)
        )

    def left_of(s):
        j = s % per_layer
        feed = jnp.where(j % 2 == 0, 3, 2)
        return jnp.where(j < at_out, feed, jnp.where(j == at_out, 1, 0))

    def loaded_slot(s):
        return ((s // per_layer) * (blocks + 1) + (s % per_layer) // 2) % 2

    def right_of(s):
        j = s % per_layer
        feed = jnp.where(j % 2 == 0, loaded_slot(s), 2 + (j // 2) % 2)
        return jnp.where(
            j < at_out, feed, jnp.where(j == at_out, loaded_slot(s), 4 + j - at_query)
        )

    local = pltpu.make_async_copy

    def unit_load(s):
        return local(weights_ref.at[unit_of(s)], unit_buf.at[s % 3], load_sem.at[0, s % 3])

    def act_load(layer, block, slot):
        return local(act_ref.at[layer, block], right_buf.at[slot], load_sem.at[1, slot])

    def ctx_load(layer, slot):
        return local(ctx_ref.at[layer], right_buf.at[slot], load_sem.at[1, slot])

    def slope_load(layer, block):
        return local(slope_ref.at[layer, block], slope_buf, load_sem.at[2, 0])

    def norm_loads(layer, which):
        scaled, inv = ((one_ref, inv_one_ref), (two_ref, inv_two_ref))[which]
        return [
            local(scaled.at[layer], scaled_buf, load_sem.at[3, 0]),
            local(inv.at[layer], inv_buf, load_sem.at[3, 1]),
        ]

    def mixed_loads(layer):
        return [
            local(mixed_ref.at[layer], mixed_buf, load_sem.at[4, 0]),
            local(lse_ref.at[layer], lse_buf, load_sem.at[4, 1]),
        ]

    def normed_load(layer):
        return local(normed_ref.at[layer], left_buf.at[2], load_sem.at[2, 1])

    def low_load(layer):
        return local(low_ref.at[layer], left_buf.at[0], load_sem.at[5, 0])

    def begin(*copies):
        for copy in copies:
            copy.start()

    def finish(*copies):
        for copy in copies:
            copy.wait()

    def note(row, value):
        small_sum[0, pl.ds(row, 1), :] = value

    def column(layer, i):
        return layer * (2 + blocks) + i

    def row(layer, i):
        return LAYERS * (2 + blocks) + layer * 6 + i

    def norm_back(layer, gain_row, bias_row, low_slot):
        gain = row_ref[layer, gain_row : gain_row + 1, :]
        size = 128

        def one(tile, carry):
            part = pl.ds(pl.multiple_of(tile * size, size), size)
            upstream = total_ref[part, :]
            scaled = scaled_buf[part, :]
            inside = norm_back_rows(upstream, scaled, inv_buf[part, 0:1], gain)
            total_ref[part, :] = inside
            left_buf[low_slot, part, :] = inside.astype(jnp.bfloat16)
            sums = (upstream * scaled, upstream, inside)
            return tuple(a + jnp.sum(b, axis=0, keepdims=True) for a, b in zip(carry, sums))

        zero = jnp.zeros((1, width), jnp.float32)
        gains, shifts, biases = lax.fori_loop(0, rows // size, one, (zero, zero, zero))
        note(row(layer, gain_row), gains)
        note(row(layer, gain_row + 1), shifts)
        note(row(layer, bias_row), biases)

    def heads(start, stop):
        inputs = [mixed_buf.at[i] for i in range(3)]
        grads = [right_buf.at[4 + i] for i in range(3)]

        def two(step, carry):
            for pair in (start + 2 * step, start + 2 * step + 1):
                attend_back_pair(pair, *inputs, d_ctx_buf, mask_buf, lse_buf, *grads)
            return carry

        lax.fori_loop(0, (stop - start) // 2, two, 0)

    pairs = width // LANES

    def data_gradient(s):
        layer, j = place(s)
        matrix = unit_buf.at[s % 3]
        before = unit_buf.at[(s + 2) % 3]
        slot = loaded_slot(s)

        @pl.when(j == 0)
        def _():
            finish(*norm_loads(layer, 1))

            @pl.when(s == 0)
            def _():
                total_ref[...] = out_grad_ref[...].astype(jnp.float32)

            norm_back(layer, 4, 1, 3)
            begin(*norm_loads(layer, 0), *mixed_loads(layer))

        @pl.when(j == 1)
        def _():
            finish(normed_load(layer))
            begin(low_load(layer))

        @pl.when((j < at_out) & (j % 2 == 0))
        def _():
            block = j // 2
            finish(slope_load(layer, block), act_load(layer, block, slot))

            @pl.when(block < blocks - 1)
            def _():
                act_load(layer, block + 1, 1 - slot).start()

            @pl.when(block == blocks - 1)
            def _():
                ctx_load(layer, 1 - slot).start()

            d_act = dot(left_buf[3], matrix[...], ((1,), (0,)))
            d_pre = (d_act * slope_buf[...].astype(jnp.float32)).astype(jnp.bfloat16)
            right_buf[2 + block % 2] = d_pre
            sums = jnp.sum(d_pre.astype(jnp.float32), axis=0, keepdims=True)
            note(column(layer, 2 + block), sums)

            @pl.when(block < blocks - 1)
            def _():
                slope_load(layer, block + 1).start()

        @pl.when((j < at_out) & (j % 2 == 1))
        def _():
            total_ref[...] += dot(right_buf[2 + (j // 2) % 2], matrix[...], ((1,), (1,)))

        @pl.when(j == at_out)
        def _():
            finish(*norm_loads(layer, 0), *mixed_loads(layer), ctx_load(layer, slot))
            norm_back(layer, 2, 0, 1)

            @pl.when(layer > 0)
            def _():
                act_load(layer - 1, 0, 1 - slot).start()
                begin(*norm_loads(layer - 1, 1))
                slope_load(layer - 1, 0).start()

            d_ctx_buf[...] = dot(left_buf[1], matrix[...], ((1,), (0,))).astype(jnp.bfloat16)

        @pl.when(j == at_query)
        def _():
            finish(low_load(layer))

            @pl.when(layer > 0)
            def _():
                normed_load(layer - 1).start()

            heads(2 * pairs // 8, 4 * pairs // 8)

        @pl.when(j == at_query + 1)
        def _():
            total_ref[...] += dot(right_buf[4], before[...], ((1,), (1,)))

        @pl.when(j == at_query + 2)
        def _():
            total_ref[...] += dot(right_buf[6], matrix[...], ((1,), (1,)))

    def data_gradient_rest(s):
        layer, j = place(s)

        @pl.when(j == at_out)
        def _():
            heads(0, 2 * pairs // 8)

        @pl.when(j == at_query)
        def _():
            heads(4 * pairs // 8, pairs)

        @pl.when(j == at_query + 1)
        def _():
            total_ref[...] += dot(right_buf[5], unit_buf[s % 3], ((1,), (1,)))
            for i, number in ((0, 0), (2, 1)):
                sums = jnp.sum(right_buf[4 + i].astype(jnp.float32), axis=0, keepdims=True)
                note(column(layer, number), sums)

    def product(s, side, tile):
        unit = s // parts
        start = pl.multiple_of(side * half + tile * TILE, TILE)
        left = left_buf[left_of(unit), :, pl.ds(start, TILE)]
        right = right_buf[
            right_of(unit), :, pl.ds(pl.multiple_of((s % parts) * half, half), half)
        ]
        return lax.dot_general(
            left, right, (((0,), (0,)), ((), ())), preferred_element_type=jnp.float32
        )

    def core_copy(s):
        return remote(
            core_out.at[s % 2], core_in.at[s % 4], core_sems, (0, s % 2), (1, s % 4), to_core
        )

    def by_kind(s, body):
        short = side_cols - LANES
        late_end = parts * (units - rounds)
        kinds = (
            ((s % 2 == 0) | (s >= late_end), side_cols, side_cols, False),
            ((s % 4 == 1) & (s < late_end), side_cols, short, True),
            ((s % 4 == 3) & (s < late_end), short, side_cols, True),
        )
        for kind, one, two, late in kinds:

            @pl.when(kind)
            def _(one=one, two=two, late=late):
                body(one, two, late)

    def first_copies(s, one, two, late):
        here, there = sum_core.at[s % 3], first_in.at[s % 4]

        def send(src, dst, number, peer):
            return remote(
                src, dst, first_sems, (0, number, s % 3), (1, number, s % 4), peer
            )

        copies = [
            send(
                here.at[1 - x, :, :, :, pl.ds(0, one)],
                there.at[0, :, :, :, pl.ds(0, one)],
                0,
                to_x,
            ),
            send(
                here.at[:, 1 - y, :, :, pl.ds(one, two)],
                there.at[1, :, :, :, pl.ds(0, two)],
                1,
                to_y,
            ),
        ]
        if late:
            for k in (1, 2, 3):
                src = here.at[:, :, (z + k) % 4, :, pl.ds(one + two, LANES)]
                copies.append(send(src, late_in.at[s % 4, k - 1], 1 + k, to_z[k - 1]))
        return copies

    def second_copies(s, one, two, late):
        here, there = sum_first.at[s % 3], second_in.at[s % 4]

        def send(src, dst, number, peer):
            return remote(
                src, dst, second_sems, (0, number, s % 3), (1, number, s % 4), peer
            )

        copies = [
            send(here.at[0, 1 - y, :, :, pl.ds(0, one)], there.at[0, :, :, pl.ds(0, one)], 0, to_y),
            send(here.at[1, 1 - x, :, :, pl.ds(0, two)], there.at[1, :, :, pl.ds(0, two)], 1, to_x),
        ]
        if late:
            copies.append(send(late_sum.at[s % 3, :, 1 - y], late_second_in.at[s % 4], 2, to_y))
        return copies

    def third_copies(s, one, two, late):
        here, there = sum_second.at[s % 3], z_in.at[s % 4]

        def send(src, dst, number, peer):
            return remote(src, dst, z_sems, (0, number, s % 3), (1, number, s % 4), peer)

        cols_now = pl.ds(0, one + two)
        copies = [
            send(here.at[(z + k) % 4, :, cols_now], there.at[k - 1, :, cols_now], k - 1, to_z[k - 1])
            for k in (1, 2, 3)
        ]
        if late:
            copies.append(send(late_pair.at[s % 3, 1 - x], late_last_in.at[s % 4], 3, to_x))
        return copies

    def plus(value, *others):
        value = value.astype(jnp.float32)
        for other in others:
            value = value + other.astype(jnp.float32)
        return value.astype(jnp.bfloat16)

    def after_z(s, one, two, late):
        for copy in third_copies(s, one, two, late):
            copy.wait()
        unit, here, got = unit_of(s // parts), s % 3, s % 4
        start, size = (half if late else 0), one + two
        base = half if late else pl.multiple_of((s % 2) * half, half)
        out_ref[unit, :, pl.ds(base, size)] = plus(
            sum_second[here, z, :, 0:size], *(z_in[got, k, :, 0:size] for k in range(3))
        )
        if late:
            out_ref[unit, :, start + size : start + half] = plus(
                late_pair[here, x], late_last_in[got]
            )

    def after_second(s, one, two, late):
        for copy in second_copies(s, one, two, late):
            copy.wait()
        here, got = s % 3, s % 4
        sum_second[here, :, :, 0:one] = plus(
            sum_first[here, 0, y, :, :, 0:one], second_in[got, 0, :, :, 0:one]
        )
        sum_second[here, :, :, one : one + two] = plus(
            sum_first[here, 1, x, :, :, 0:two], second_in[got, 1, :, :, 0:two]
        )
        if late:
            late_pair[here] = plus(late_sum[here, :, y], late_second_in[got])
        for copy in third_copies(s, one, two, late):
            copy.start()

    def after_first(s, one, two, late):
        for copy in first_copies(s, one, two, late):
            copy.wait()
        here, got = s % 3, s % 4
        sum_first[here, 0, :, :, :, 0:one] = plus(
            sum_core[here, x, :, :, :, 0:one], first_in[got, 0, :, :, :, 0:one]
        )
        sum_first[here, 1, :, :, :, 0:two] = plus(
            sum_core[here, :, y, :, :, one : one + two], first_in[got, 1, :, :, :, 0:two]
        )
        if late:
            late_sum[here] = plus(
                sum_core[here, :, :, z, :, one + two : half], *(late_in[got, k] for k in range(3))
            )
        for copy in second_copies(s, one, two, late):
            copy.start()

    def start_first(s, one, two, late):
        for copy in first_copies(s, one, two, late):
            copy.start()

    small_peers = (to_core, to_x, to_y, to_z1, to_z2)

    def small_copy(stage):
        return remote(
            small_sum.at[stage],
            small_got.at[stage],
            small_sems,
            (0, stage),
            (1, stage),
            small_peers[stage],
        )

    rounds, owners = back_buf.shape[0], back_buf.shape[1]
    cols = owned_ref.shape[3]
    me = spread_order(z, y, x, c)

    def own_back(number):
        return local(
            back_buf.at[number, dp, :, pl.ds(pl.multiple_of(tensor * cols, cols), cols)],
            owned_ref.at[number, me],
            own_sems.at[number],
        )

    def send_back(number):
        def fill(owner, carry):
            back_buf[number, owner] = out_ref[pick_ref[number * owners + owner]]
            return carry

        lax.fori_loop(0, owners, fill, 0)
        own_back(number).start()

        def send(zz, yy, xx, cc):
            there = xx * 2 + cc
            remote(
                back_buf.at[
                    number, zz * 2 + yy, :, pl.ds(pl.multiple_of(there * cols, cols), cols)
                ],
                owned_ref.at[number, me],
                round_sems,
                (0, number),
                (1, number),
                (zz * 2 + yy, there),
            ).start()

        every_other(z, y, x, c, send)

    def finish_back(number):
        own_back(number).wait()
        most = owned_ref.at[number, pl.ds(0, 31)]
        remote(most, most, round_sems, (0, number), (1, number), to_core).wait()

    top = LAYERS - 1
    steps = parts * units
    begin(
        *norm_loads(top, 1),
        unit_load(jnp.int32(0)),
        slope_load(top, 0),
        act_load(top, 0, 0),
        normed_load(top),
    )
    fill_mask(mask_buf, docs_col_ref, docs_row_ref)
    pl.semaphore_wait(barrier, 31)

    def step(s, carry):
        last = s - 3 * LAG - 1

        @pl.when((last >= 0) & (last < steps))
        def _():
            by_kind(last, functools.partial(after_z, last))

            @pl.when((last // parts >= units - rounds) & (last % parts == parts - 1))
            def _():
                send_back(last // parts - (units - rounds))

        third = s - 2 * LAG - 1

        @pl.when((third >= 0) & (third < steps))
        def _():
            by_kind(third, functools.partial(after_second, third))

        second = s - LAG - 1

        @pl.when((second >= 0) & (second < steps))
        def _():
            by_kind(second, functools.partial(after_first, second))

        @pl.when(s < steps)
        def _():
            unit = s // parts

            @pl.when(s % parts == 0)
            def _():
                unit_load(unit).wait()

                @pl.when(unit + 1 < units)
                def _():
                    unit_load(unit + 1).start()

                data_gradient(unit)

            @pl.when(s % parts == 1)
            def _():
                data_gradient_rest(unit)

            @pl.when(s >= 2)
            def _():
                core_copy(s - 2).wait_send()

            def one(tile, carry):
                part = pl.ds(pl.multiple_of(tile * TILE, TILE), TILE)
                core_out[s % 2, part, :] = product(s, 1 - c, tile).astype(jnp.bfloat16)
                return carry

            lax.fori_loop(0, half // TILE, one, 0)
            core_copy(s).start()

        first = s - 1

        @pl.when((first >= 0) & (first < steps))
        def _():
            core_copy(first).wait_recv()

            def one(tile, carry):
                part = pl.ds(pl.multiple_of(tile * TILE, TILE), TILE)
                total = product(first, c, tile) + core_in[first % 4, part, :].astype(jnp.float32)
                total = total.astype(jnp.bfloat16).reshape(2, 4, piece, half)
                sum_core[first % 3, tile] = total
                return carry

            lax.fori_loop(0, half // TILE, one, 0)
            by_kind(first, functools.partial(start_first, first))

        for stage in range(6):

            @pl.when(s == steps + stage)
            def _(stage=stage):
                if stage > 0:
                    small_copy(stage - 1).wait()
                    total = small_sum[stage - 1] + small_got[stage - 1]
                    if stage < 5:
                        small_sum[stage] = total
                    else:
                        small_out[...] = total
                if stage < 5:
                    small_copy(stage).start()

        return carry

    lax.fori_loop(0, steps + 3 * LAG + 1, step, 0)
    for s in (steps - 2, steps - 1):
        core_copy(s).wait_send()
    for number in range(rounds):
        finish_back(number)


def backward(pick, out_grad, docs, row_now, weights, saved, piece, cols):
    units, width, _ = weights.shape
    rows = out_grad.shape[0]
    blocks = (units // LAYERS - 4) // 2
    half = width // 2
    low, full = jnp.bfloat16, jnp.float32
    rounds = pick.shape[0] // 10
    small = (LAYERS * (8 + blocks), width)
    any_spec = pl.BlockSpec(memory_space=pl.ANY)
    vmem_spec = pl.BlockSpec(memory_space=pltpu.VMEM)
    dma = pltpu.SemaphoreType.DMA
    summed, total, small = pl.pallas_call(
        backward_kernel,
        out_shape=(
            jax.ShapeDtypeStruct((rounds, width // piece, piece, cols), low),
            jax.ShapeDtypeStruct((rows, width), full),
            jax.ShapeDtypeStruct(small, full),
        ),
        in_specs=[pl.BlockSpec(memory_space=pltpu.SMEM)] + [vmem_spec] * 4 + [any_spec] * (1 + len(saved)),
        out_specs=(vmem_spec, vmem_spec, vmem_spec),
        scratch_shapes=[
            pltpu.VMEM((units, piece, width), low),
            pltpu.VMEM((rounds, 8, piece, width), low),
            pltpu.VMEM((4, rows, width), low),
            pltpu.VMEM((7, rows, width), low),
            pltpu.VMEM((3, width, width), low),
            pltpu.VMEM((rows, width), full),
            pltpu.VMEM((rows, 128), full),
            pltpu.VMEM((rows, width), low),
            pltpu.VMEM((3, rows, width), low),
            pltpu.VMEM((width // HEAD_DIM, 1, rows), full),
            pltpu.VMEM((rows, rows), full),
            pltpu.VMEM((rows, width), low),
            pltpu.VMEM((2, half, half), low),
            pltpu.VMEM((4, half, half), low),
            pltpu.VMEM((3, 2, 2, 4, piece, half), low),
            pltpu.VMEM((4, 2, 2, 4, piece, half // 2), low),
            pltpu.VMEM((3, 2, 2, 4, piece, half // 2), low),
            pltpu.VMEM((4, 2, 4, piece, half // 2), low),
            pltpu.VMEM((3, 4, piece, half), low),
            pltpu.VMEM((4, 3, piece, half), low),
            pltpu.VMEM((4, 3, 2, 2, piece, LANES), low),
            pltpu.VMEM((3, 2, 2, piece, LANES), low),
            pltpu.VMEM((4, 2, piece, LANES), low),
            pltpu.VMEM((3, 2, piece, LANES), low),
            pltpu.VMEM((4, piece, LANES), low),
            pltpu.VMEM((5,) + small, full),
            pltpu.VMEM((5,) + small, full),
            dma((6, 3)),
            dma((2, 4)),
            dma((2, 5, 4)),
            dma((2, 3, 4)),
            dma((2, 4, 4)),
            dma((2, 5)),
            dma((rounds,)),
            dma((2, rounds)),
        ],
        compiler_params=pltpu.CompilerParams(
            collective_id=1, has_side_effects=True, vmem_limit_bytes=63 * 1024 * 1024
        ),
        name="backward_reduce",
    )(pick, out_grad, docs[:, None], docs[None, :], row_now, weights, *saved)
    return (total, summed, small)


def norm_rows(value, gain, shift):
    centred = value - jnp.mean(value, axis=1, keepdims=True)
    inverse = lax.rsqrt(jnp.mean(centred * centred, axis=1, keepdims=True) + EPS_NORM)
    scaled = centred * inverse
    return (scaled * gain + shift, scaled, inverse)


NORM_ROWS = 128


def forward_kernel(
    slot_ref,
    masters_ref,
    hidden_ref,
    docs_col_ref,
    docs_row_ref,
    col_ref,
    row_ref,
    out_ref,
    final_ref,
    table_ref,
    *refs,
):
    saved, bufs = refs[:11], refs[11:22]
    rounds = masters_ref.shape[0]
    (x_buf, normed_buf, total_buf, mask_buf, unit_buf, own_ref) = refs[22:28]
    (own_sem, sems, unit_sem, save_sem, got_sem, round_sems) = refs[28:34]
    (masters_buf, sent_ref, col_got, bias_buf, master_sem, col_sems) = refs[34:40]
    rank_ref, back_ref = refs[40:42]
    got = refs[42:]
    (low_buf, mixed_buf, ctx_buf, lse_buf, one_buf, inv_one_buf, nb_buf) = bufs[:7]
    (act_buf, slope_buf, two_buf, inv_two_buf) = bufs[7:]
    units, piece, width = own_ref.shape
    rows = hidden_ref.shape[0]
    per_layer = units // LAYERS
    blocks = (per_layer - 4) // 2
    dp, tensor = lax.axis_index("dp"), lax.axis_index("tensor")
    z, y, x, c = dp // 2, dp % 2, tensor // 2, tensor % 2
    half = width // 2
    line, plane = 4 * piece, 8 * piece
    to_core = (dp, x * 2 + 1 - c)
    to_x = (dp, (1 - x) * 2 + c)
    to_y = (z * 2 + 1 - y, tensor)
    to_z = [(((z + k) % 4) * 2 + y, tensor) for k in (1, 2, 3)]
    mesh_id = pl.DeviceIdType.MESH

    barrier = greet_all(z, y, x, c)
    masters_in = [
        pltpu.make_async_copy(masters_ref.at[i], masters_buf.at[i], master_sem.at[i])
        for i in range(rounds)
    ]
    for copy in masters_in:
        copy.start()
    cols = sent_ref.shape[2]
    owners = table_ref.shape[0] // rounds - 2

    def turn_of(unit):
        layer, j = unit // per_layer, unit % per_layer
        feed = jnp.where(j < 4 + blocks, 2 * (j - 4) + 1, 2 * (j - 4 - blocks))
        place = jnp.where(j < 3, 2 * blocks + 1 + j, jnp.where(j == 3, 2 * blocks, feed))
        return (LAYERS - 1 - layer) * per_layer + place

    def rank_one(unit, carry):
        mine, turn = slot_ref[unit] // rounds, turn_of(unit)
        before, after = 0, 0
        for other in range(units):
            same = jnp.where(slot_ref[other] // rounds == mine, 1, 0)
            before = before + jnp.where(other < unit, same, 0)
            after = after + jnp.where(turn_of(other) > turn, same, 0)
        rank_ref[unit] = before
        back_ref[unit] = rounds - 1 - after
        return carry

    lax.fori_loop(0, units, rank_one, 0)

    def first_of(number):
        found = 0
        for unit in range(units):
            slot = slot_ref[unit]
            here = (slot // rounds == dp) & (rank_ref[unit] == number)
            found = found + jnp.where(here, slot % rounds, 0)
        return found

    def fill_table():
        def spot_one(spot, carry):
            found = (LAYERS - 1) * per_layer + 4 + blocks
            for unit in range(units):
                at = back_ref[unit] * owners + slot_ref[unit] // rounds
                found = jnp.where(at == spot, unit, found)
            table_ref[spot] = found
            return carry

        lax.fori_loop(0, rounds * owners, spot_one, 0)
        for i in range(rounds):
            turn, taken = 0, 0
            for unit in range(units):
                here = slot_ref[unit] == dp * rounds + i
                turn = turn + jnp.where(here, back_ref[unit], 0)
                taken = taken + jnp.where(here, 1, 0)
            table_ref[rounds * owners + i] = turn
            table_ref[rounds * (owners + 1) + i] = taken
    me = dp * 4 + tensor

    def part_for(number, zz, yy, xx, cc):
        start = pl.multiple_of(spread_order(zz, yy, xx, cc) * piece, piece)
        return sent_ref.at[number, pl.ds(start, piece)]

    def keep(number):
        return pltpu.make_async_copy(
            part_for(number, z, y, x, c), got[number].at[me], got_sem.at[number]
        )

    def round_copy(number, src, dst, peer):
        return pltpu.make_async_remote_copy(
            src_ref=src,
            dst_ref=dst,
            send_sem=round_sems.at[0, number],
            recv_sem=round_sems.at[1, number],
            device_id=peer,
            device_id_type=mesh_id,
        )

    def start_round(number):
        keep(number).start()

        def send(zz, yy, xx, cc):
            src = part_for(number, zz, yy, xx, cc)
            round_copy(number, src, got[number].at[me], (zz * 2 + yy, xx * 2 + cc)).start()

        every_other(z, y, x, c, send)

    def finish_round(number):
        keep(number).wait()
        most = got[number].at[pl.ds(0, 31)]
        round_copy(number, most, most, to_core).wait()

    def pick(unit, there):
        rank, owner = rank_ref[unit], slot_ref[unit] // rounds
        for j in range(4):
            value = got[0][owner * 4 + j]
            for number in range(1, there):
                value = jnp.where(rank == number, got[number][owner * 4 + j], value)
            own_ref[unit, :, j * cols : (j + 1) * cols] = value

    def column_copies():
        return [
            pltpu.make_async_remote_copy(
                src_ref=col_ref,
                dst_ref=col_got.at[tensor],
                send_sem=col_sems.at[0, k],
                recv_sem=col_sems.at[1, k],
                device_id=(dp, (tensor + k + 1) % 4),
                device_id_type=mesh_id,
            )
            for k in range(3)
        ]

    for copy in masters_in:
        copy.wait()
    sent_ref[0] = masters_buf[first_of(0)].astype(sent_ref.dtype)
    pl.semaphore_wait(barrier, 31)
    start_round(0)
    for number in range(1, rounds):
        sent_ref[number] = masters_buf[first_of(number)].astype(sent_ref.dtype)
    start_round(1)
    col_got[tensor] = col_ref[...]
    for copy in column_copies():
        copy.start()
    fill_table()

    my_line = pl.multiple_of(((c * 2 + x) * 2 + y) * line, line)
    my_rows = pl.ds(pl.multiple_of(my_line + z * piece, piece), piece)
    parts, cycle = 2, sems.shape[2]

    def half_of(s):
        return pl.ds(pl.multiple_of((s % parts) * half, half), half)

    def wide(s, start, size):
        return pl.ds(pl.multiple_of((s % parts) * half + start, LANES), size)

    late_cols = LANES

    def ways(s):
        short = half // 2 - late_cols
        return (
            (s % 2 == 0, wide(s, 0, half // 2), wide(s, half // 2, half // 2), None),
            (
                s % 4 == 1,
                wide(s, 0, half // 2),
                wide(s, half // 2, short),
                wide(s, half - late_cols, late_cols),
            ),
            (
                s % 4 == 3,
                wide(s, 0, short),
                wide(s, short, half // 2),
                wide(s, half - late_cols, late_cols),
            ),
        )

    def remote(src, dst, index, s, peer):
        return pltpu.make_async_remote_copy(
            src_ref=src,
            dst_ref=dst,
            send_sem=sems.at[0, index, s % cycle],
            recv_sem=sems.at[1, index, s % cycle],
            device_id=peer,
            device_id_type=mesh_id,
        )

    def own_copy(s):
        unit, cols_now = s // parts, half_of(s)
        return pltpu.make_async_copy(
            own_ref.at[unit, :, cols_now],
            out_ref.at[unit, my_rows, cols_now],
            own_sem.at[s % cycle],
        )

    def rows_at(xx, yy, zz):
        return pl.ds(pl.multiple_of(spread_order(zz, yy, xx, c) * piece, piece), piece)

    def stage_z(s, one, two, late):
        unit, copies = s // parts, []
        size = half if late is None else half - late_cols
        early = wide(s, 0, size)
        here, there = own_ref.at[unit, :, early], out_ref.at[unit, my_rows, early]
        copies = [remote(here, there, k, s, to_z[k]) for k in range(3)]
        if late is not None:
            here, there = own_ref.at[unit, :, late], out_ref.at[unit, my_rows, late]
            copies.append(remote(here, there, 9, s, to_x))
        return copies

    def stage_one(s, one, two, late):
        unit, rows = s // parts, pl.ds(my_line, line)
        one, two = out_ref.at[unit, rows, one], out_ref.at[unit, rows, two]
        copies = [remote(one, one, 3, s, to_y), remote(two, two, 4, s, to_x)]
        if late is not None:
            for i in range(2):
                there = out_ref.at[unit, rows_at(i, y, z), late]
                copies.append(remote(there, there, 10 + i, s, to_y))
        return copies

    def stage_two(s, one, two, late):
        unit = s // parts
        rows = pl.ds(pl.multiple_of((c * 2 + x) * plane, plane), plane)
        there = out_ref.at[unit, rows, one]
        copies = [remote(there, there, 5, s, to_x)]
        for i in range(2):
            rows = pl.ds(pl.multiple_of(((c * 2 + i) * 2 + y) * line, line), line)
            there = out_ref.at[unit, rows, two]
            copies.append(remote(there, there, 6 + i, s, to_y))
        if late is not None:
            for i in range(4):
                there = out_ref.at[unit, rows_at(i // 2, i % 2, z), late]
                copies += [remote(there, there, 12 + 3 * i + k, s, to_z[k]) for k in range(3)]
        return copies

    def stage_core(s):
        rows = pl.ds(pl.multiple_of(c * 2 * plane, 2 * plane), 2 * plane)
        there = out_ref.at[s // parts, rows, half_of(s)]
        return [remote(there, there, 8, s, to_core)]

    stages = (stage_z, stage_one, stage_two, stage_core)

    def each_copy(number, s, act):
        if stages[number] is stage_core:
            for copy in stage_core(s):
                act(copy)
            return
        for kind, one, two, late in ways(s):

            @pl.when(kind)
            def _(one=one, two=two, late=late):
                for copy in stages[number](s, one, two, late):
                    act(copy)


    def unit_copy(unit):
        slot = unit % 2
        return pltpu.make_async_copy(out_ref.at[unit], unit_buf.at[slot], unit_sem.at[slot])

    def save(number, layer, block=None):
        src, dst, sem = bufs[number], saved[number].at[layer], save_sem.at[number, 0]
        if block is not None:
            src, dst, sem = src.at[block], dst.at[block], save_sem.at[number, block]
        return pltpu.make_async_copy(src, dst, sem)

    def free(numbers, layer, block=None):
        @pl.when(layer > 0)
        def _():
            for number in numbers:
                save(number, layer - 1, block).wait()

    def heads(start, stop):
        inputs = [mixed_buf.at[i] for i in range(3)]
        for pair in range(start, stop):
            attend_pair(pair, *inputs, mask_buf, ctx_buf, lse_buf)

    tall = rows // parts
    pairs = width // LANES

    def compute(unit, turn):
        layer, j = unit // per_layer, unit % per_layer
        matrix = unit_buf.at[unit % 2]
        mine = pl.ds(pl.multiple_of(turn * tall, tall), tall)

        def small(i):
            return row_ref[layer, i : i + 1, :]

        def bias(i):
            return bias_buf[pl.ds(layer * (2 + blocks) + i, 1), :]

        def over_rows(body):
            def one(tile, carry):
                body(pl.ds(pl.multiple_of(turn * tall + tile * NORM_ROWS, NORM_ROWS), NORM_ROWS))
                return carry

            lax.fori_loop(0, tall // NORM_ROWS, one, 0)

        @pl.when((j == 0) & (turn == 0))
        def _():
            free((0, 1), layer)

            @pl.when(layer == 0)
            def _():
                x_buf[...] = hidden_ref[...].astype(jnp.float32)

            low_buf[...] = x_buf[...].astype(jnp.bfloat16)
            save(0, layer).start()

        @pl.when(j < 3)
        def _():
            value = dot(low_buf[mine, :], matrix[...], ((1,), (0,)))
            value = value + jnp.where(j == 1, 0.0, bias(j // 2))
            scale = jnp.where(j == 0, HEAD_DIM ** (-0.5), 1.0)
            mixed_buf[j, mine, :] = (value * scale).astype(jnp.bfloat16)

        @pl.when((j == 2) & (turn == 1))
        def _():
            save(1, layer).start()
            free((2, 3), layer)
            heads(0, pairs // 4)

        @pl.when((j == 3) & (turn == 0))
        def _():
            heads(pairs // 4, 3 * pairs // 4)

        @pl.when((j == 3) & (turn == 1))
        def _():
            heads(3 * pairs // 4, pairs)
            save(2, layer).start()
            save(3, layer).start()
            total_buf[...] = dot(ctx_buf[...], matrix[...], ((1,), (1,)))
            free((4, 5, 6), layer)

            def body(tile, carry):
                part = pl.ds(pl.multiple_of(tile * NORM_ROWS, NORM_ROWS), NORM_ROWS)
                value = x_buf[part, :] + total_buf[part, :] + small(0)
                normed, scaled, inverse = norm_rows(value, small(2), small(3))
                normed_buf[part, :] = normed
                nb_buf[part, :] = normed.astype(jnp.bfloat16)
                one_buf[part, :] = scaled
                inv_one_buf[part, :] = jnp.broadcast_to(inverse, (NORM_ROWS, 128))
                return carry

            lax.fori_loop(0, rows // NORM_ROWS, body, 0)
            for number in (4, 5, 6):
                save(number, layer).start()

        @pl.when((j >= 4) & (j < 4 + blocks))
        def _():
            block = j - 4

            @pl.when(turn == 0)
            def _():
                free((7, 8), layer, block)

            value = dot(nb_buf[mine, :], matrix[...], ((1,), (0,)))
            act, slope = gelu_pair(value + bias(2 + block))
            act_buf[block, mine, :] = act.astype(jnp.bfloat16)
            slope_buf[block, mine, :] = slope.astype(jnp.bfloat16)

            @pl.when(turn == 1)
            def _():
                save(7, layer, block).start()
                save(8, layer, block).start()

        @pl.when(j >= 4 + blocks)
        def _():
            block = j - 4 - blocks
            part = dot(act_buf[block, mine, :], matrix[...], ((1,), (1,)))

            @pl.when(block == 0)
            def _():
                total_buf[mine, :] = part

            @pl.when(block > 0)
            def _():
                total_buf[mine, :] += part

        @pl.when(j == per_layer - 1)
        def _():
            @pl.when(turn == 0)
            def _():
                free((9, 10), layer)

            def body(part):
                value = normed_buf[part, :] + total_buf[part, :] + small(1)
                output, scaled, inverse = norm_rows(value, small(4), small(5))
                x_buf[part, :] = output
                two_buf[part, :] = scaled
                inv_two_buf[part, :] = jnp.broadcast_to(inverse, (NORM_ROWS, 128))

            over_rows(body)

            @pl.when(turn == 1)
            def _():
                save(9, layer).start()
                save(10, layer).start()

    steps = parts * units

    def step(s, carry):
        for number in range(len(stages), -1, -1):
            now = s - number * LAG

            if number == 0:
                for turn in range(rounds):
                    last = turn == rounds - 1
                    due = (s == parts * turn) | (last & (s > parts * turn) & (s % parts == 0))

                    @pl.when(due & (s < steps))
                    def _(turn=turn):
                        @pl.when(s == parts * turn)
                        def _():
                            finish_round(turn)

                        if turn + 2 < rounds:
                            start_round(turn + 2)
                        pick(s // parts, turn + 1)

            @pl.when((now >= 0) & (now < steps))
            def _(now=now, number=number):
                if number == 0:
                    own_copy(now).start()
                else:
                    if number == 1:
                        own_copy(now).wait()
                    each_copy(number - 1, now, lambda copy: copy.wait())
                if number < len(stages):
                    each_copy(number, now, lambda copy: copy.start())
                else:

                    @pl.when(now % parts == parts - 1)
                    def _():
                        unit_copy(now // parts).start()

        @pl.when(s == len(stages) * LAG)
        def _():
            for copy in column_copies():
                copy.wait()
            for j in range(4):
                bias_buf[:, j * cols : (j + 1) * cols] = col_got[j]

        done = s - len(stages) * LAG - parts

        @pl.when(done >= 0)
        def _():
            @pl.when(done % parts == 0)
            def _():
                unit_copy(done // parts).wait()

            compute(done // parts, done % parts)

        return carry

    fill_mask(mask_buf, docs_col_ref, docs_row_ref)
    lax.fori_loop(0, steps + len(stages) * LAG + parts, step, 0)
    final_ref[...] = x_buf[...]
    last = LAYERS - 1
    for number in (0, 1, 2, 3, 4, 5, 6, 9, 10):
        save(number, last).wait()
    for block in range(blocks):
        save(7, last, block).wait()
        save(8, last, block).wait()


def forward(unit_slot, masters, hidden_in, docs, col_now, row_now, piece, owners):
    units = unit_slot.shape[0]
    rounds, width, cols = masters.shape
    rows = hidden_in.shape[0]
    blocks = (units // LAYERS - 4) // 2
    low, full = jnp.bfloat16, jnp.float32
    kept = [
        ((rows, width), low),
        ((3, rows, width), low),
        ((rows, width), low),
        ((width // HEAD_DIM, 1, rows), full),
        ((rows, width), full),
        ((rows, 128), full),
        ((rows, width), low),
        ((blocks, rows, width), low),
        ((blocks, rows, width), low),
        ((rows, width), full),
        ((rows, 128), full),
    ]
    any_spec = pl.BlockSpec(memory_space=pl.ANY)
    vmem_spec = pl.BlockSpec(memory_space=pltpu.VMEM)
    smem_spec = pl.BlockSpec(memory_space=pltpu.SMEM)
    dma = pltpu.SemaphoreType.DMA
    return pl.pallas_call(
        forward_kernel,
        out_shape=[
            jax.ShapeDtypeStruct((units, width, width), low),
            jax.ShapeDtypeStruct((rows, width), full),
            jax.ShapeDtypeStruct((rounds * (owners + 2),), jnp.int32),
        ]
        + [jax.ShapeDtypeStruct((LAYERS,) + shape, dtype) for shape, dtype in kept],
        in_specs=[smem_spec] + [any_spec] + [vmem_spec] * 5,
        out_specs=[any_spec, vmem_spec, smem_spec] + [any_spec] * len(kept),
        scratch_shapes=[pltpu.VMEM(shape, dtype) for shape, dtype in kept]
        + [
            pltpu.VMEM((rows, width), full),
            pltpu.VMEM((rows, width), full),
            pltpu.VMEM((rows, width), full),
            pltpu.VMEM((rows, rows), full),
            pltpu.VMEM((2, width, width), low),
            pltpu.VMEM((units, piece, width), low),
            dma((8,)),
            dma((2, 24, 8)),
            dma((2,)),
            dma((len(kept), blocks)),
            dma((rounds,)),
            dma((2, rounds)),
            pltpu.VMEM((rounds, width, cols), full),
            pltpu.VMEM((rounds, width, cols), low),
            pltpu.VMEM((4,) + col_now.shape, full),
            pltpu.VMEM((col_now.shape[0], width), full),
            dma((rounds,)),
            dma((2, 3)),
            pltpu.SMEM((units,), jnp.int32),
            pltpu.SMEM((units,), jnp.int32),
        ]
        + [pltpu.VMEM((width // piece, piece, cols), low)] * rounds,
        compiler_params=pltpu.CompilerParams(
            collective_id=2, has_side_effects=True, vmem_limit_bytes=60 * 1024 * 1024
        ),
        name="gather_forward",
    )(
        unit_slot,
        masters,
        hidden_in,
        docs[:, None],
        docs[None, :],
        col_now,
        row_now,
    )


def run_general(
    unit_slot,
    masters,
    first_moment,
    second_moment,
    hidden_in,
    doc_ids,
    column_state,
    row_state,
    out_grad,
):
    slot_count, width, col_width = masters.shape
    units = unit_slot.shape[0]
    dp_size = lax.axis_size("dp")
    devices = dp_size * lax.axis_size("tensor")
    slots = slot_count * dp_size
    piece = width // devices
    per_layer = units // LAYERS
    blocks = (per_layer - 4) // 2
    tensor_size = lax.axis_size("tensor")
    rows = hidden_in.shape[0]
    seq_len = doc_ids.shape[1]
    heads = width // HEAD_DIM
    share = seq_len // rows
    tensor_index = lax.axis_index("tensor")
    groups = [list(range(i, i + share)) for i in range(0, tensor_size, share)]
    score_scale = HEAD_DIM ** (-0.5)
    sent = masters.astype(jnp.bfloat16).reshape(slot_count, devices, piece, col_width)
    spread = lax.all_to_all(sent.transpose(1, 0, 2, 3), BOTH, 0, 0)
    spread = spread.reshape(dp_size, tensor_size, slot_count, piece, col_width)
    spread = spread.transpose(0, 2, 3, 1, 4).reshape(slots, piece, width)
    mine = spread[unit_slot]
    weights = jnp.concatenate(
        [
            lax.all_gather(
                mine[layer * per_layer : (layer + 1) * per_layer], BOTH, axis=1, tiled=True
            )
            for layer in range(LAYERS)
        ],
        axis=0,
    )

    def matrices(layer):
        unit = weights[layer * per_layer : (layer + 1) * per_layer]
        return (unit[:3], unit[3], unit[4 : 4 + blocks], unit[4 + blocks :])

    row_docs = lax.dynamic_slice_in_dim(doc_ids, tensor_index // share, 1, axis=0)[0]
    my_docs = lax.dynamic_slice_in_dim(row_docs, (tensor_index % share) * rows, rows)
    same_doc = (my_docs[:, None] == row_docs[None, :])[None]

    def whole_row(value):
        if share == 1:
            return value
        return lax.all_gather(value, "tensor", axis=0, tiled=True, axis_index_groups=groups)

    def own_rows(value):
        if share == 1:
            return value
        return lax.psum_scatter(
            value, "tensor", scatter_dimension=0, tiled=True, axis_index_groups=groups
        )

    col_full = lax.all_gather(column_state[0], "tensor", axis=2, tiled=True)
    hidden = hidden_in.astype(jnp.float32)
    saved_layers = []
    for layer in range(LAYERS):
        w_qkv, w_proj, w_in, w_out = matrices(layer)
        row_now = row_state[0, layer]
        col_now = col_full[layer]
        hidden_bf = hidden.astype(jnp.bfloat16)
        query, key, value = (dot(hidden_bf, w_qkv[i], ((1,), (0,))) for i in range(3))
        query = ((query + col_now[0]) * score_scale).astype(jnp.bfloat16)
        key = key.astype(jnp.bfloat16)
        value = (value + col_now[1]).astype(jnp.bfloat16)
        query = query.reshape(rows, heads, HEAD_DIM)
        key = whole_row(key).reshape(seq_len, heads, HEAD_DIM)
        value = whole_row(value).reshape(seq_len, heads, HEAD_DIM)
        scores = jnp.einsum("qhd,khd->hqk", query, key, preferred_element_type=jnp.float32)
        scores = jnp.where(same_doc, scores, -1e30)
        row_top = jnp.max(scores, axis=-1, keepdims=True)
        log_total = row_top + jnp.log(
            jnp.sum(jnp.exp(scores - row_top), axis=-1, keepdims=True)
        )
        soft_bf = jnp.exp(scores - log_total).astype(jnp.bfloat16)
        context = jnp.einsum("hqk,khd->qhd", soft_bf, value, preferred_element_type=jnp.float32)
        context = context.reshape(rows, width).astype(jnp.bfloat16)
        attended = dot(context, w_proj, ((1,), (1,)))
        normed, scaled_one, inverse_one = norm_forward(
            hidden + attended + row_now[0], row_now[2], row_now[3]
        )
        normed_bf = normed.astype(jnp.bfloat16)
        pre_act = jnp.einsum("rd,bdc->brc", normed_bf, w_in, preferred_element_type=jnp.float32)
        activated, slope = gelu_pair(pre_act + col_now[2:, None])
        activated = activated.astype(jnp.bfloat16)
        slope = slope.astype(jnp.bfloat16)
        mlp_out = jnp.einsum(
            "brc,bdc->rd", activated, w_out, preferred_element_type=jnp.float32
        )
        output, scaled_two, inverse_two = norm_forward(
            normed + mlp_out + row_now[1], row_now[4], row_now[5]
        )
        saved_layers.append(
            (hidden_bf, query, key, value, log_total, context, scaled_one, inverse_one, normed_bf)
            + (slope, activated, scaled_two, inverse_two)
        )
        hidden = output
    upstream = out_grad.astype(jnp.float32)
    operands = [None] * LAYERS
    col_parts = [None] * LAYERS
    row_parts = [None] * LAYERS
    for layer in reversed(range(LAYERS)):
        w_qkv, w_proj, w_in, w_out = matrices(layer)
        row_now = row_state[0, layer]
        (
            hidden_bf,
            query,
            key,
            value,
            log_total,
            context,
            scaled_one,
            inverse_one,
            normed_bf,
            slope,
            activated,
            scaled_two,
            inverse_two,
        ) = saved_layers[layer]
        d_two, gain_two, shift_two = norm_backward(upstream, scaled_two, inverse_two, row_now[4])
        grad_bias_two = jnp.sum(d_two, axis=0)
        d_two_bf = d_two.astype(jnp.bfloat16)
        d_act = jnp.einsum("rd,bdc->brc", d_two_bf, w_out, preferred_element_type=jnp.float32)
        d_pre = (d_act * slope).astype(jnp.bfloat16)
        grad_bias_in = jnp.sum(d_pre, axis=1, dtype=jnp.float32)
        d_normed = jnp.einsum("brc,bdc->rd", d_pre, w_in, preferred_element_type=jnp.float32)
        d_normed = d_two + d_normed
        d_one, gain_one, shift_one = norm_backward(d_normed, scaled_one, inverse_one, row_now[2])
        grad_bias_proj = jnp.sum(d_one, axis=0)
        d_one_bf = d_one.astype(jnp.bfloat16)
        d_context = dot(d_one_bf, w_proj, ((1,), (0,))).astype(jnp.bfloat16)
        d_context = d_context.reshape(rows, heads, HEAD_DIM)
        scores = jnp.einsum("qhd,khd->hqk", query, key, preferred_element_type=jnp.float32)
        scores = jnp.where(same_doc, scores, -1e30)
        soft = jnp.exp(scores - log_total)
        d_values = jnp.einsum(
            "hqk,qhd->khd",
            soft.astype(jnp.bfloat16),
            d_context,
            preferred_element_type=jnp.float32,
        )
        d_probs = jnp.einsum(
            "qhd,khd->hqk", d_context, value, preferred_element_type=jnp.float32
        )
        d_scores = (
            soft * (d_probs - jnp.sum(soft * d_probs, axis=-1, keepdims=True))
        ).astype(jnp.bfloat16)
        d_queries = (
            jnp.einsum("hqk,khd->qhd", d_scores, key, preferred_element_type=jnp.float32)
            * score_scale
        )
        d_keys = jnp.einsum("hqk,qhd->khd", d_scores, query, preferred_element_type=jnp.float32)
        d_qkv = jnp.stack(
            [
                d_queries.reshape(rows, width),
                own_rows(d_keys.reshape(seq_len, width)),
                own_rows(d_values.reshape(seq_len, width)),
            ]
        ).astype(jnp.bfloat16)
        grad_bias_qkv = jnp.sum(d_qkv, axis=1, dtype=jnp.float32)
        upstream = d_one + jnp.einsum(
            "brc,bdc->rd", d_qkv, w_qkv, preferred_element_type=jnp.float32
        )
        operands[layer] = (hidden_bf, d_one_bf, normed_bf, d_two_bf)
        operands[layer] += (d_qkv, context[None], d_pre, activated)
        col_parts[layer] = jnp.concatenate(
            [
                grad_bias_qkv[0:1],
                grad_bias_qkv[2:3],
                grad_bias_in,
            ],
            axis=0,
        )
        row_parts[layer] = jnp.stack(
            [grad_bias_proj, grad_bias_two, gain_one, shift_one, gain_two, shift_two]
        )
    small = jnp.stack([jnp.stack(col_parts), jnp.stack(row_parts)])
    summed = []
    for layer in operands:
        whole = jnp.concatenate(
            [
                jnp.einsum(
                    "rd,brc->bdc", layer[i], layer[4 + i], preferred_element_type=jnp.float32
                )
                for i in range(4)
            ],
            axis=0,
        )
        summed.append(
            lax.psum_scatter(whole.astype(jnp.bfloat16), BOTH, scatter_dimension=1, tiled=True)
        )
    summed = jnp.concatenate(summed, axis=0)

    slot_ids = jnp.arange(slots, dtype=jnp.int32)
    named = unit_slot[None, :] == slot_ids[:, None]
    holds = jnp.any(named, axis=1)
    unit_of = jnp.argmax(named, axis=1)
    back = jnp.where(holds[:, None, None], summed[unit_of], jnp.zeros((), jnp.bfloat16))
    back = back.reshape(dp_size, slot_count, piece, tensor_size, col_width)
    back = back.transpose(0, 3, 1, 2, 4).reshape(devices, slot_count, piece, col_width)
    owned = lax.all_to_all(back, BOTH, 0, 0)
    owned = owned.transpose(1, 0, 2, 3)
    owned = owned.reshape(slot_count, width, col_width)
    occupied = lax.dynamic_slice_in_dim(holds, lax.axis_index("dp") * slot_count, slot_count)
    occupied = occupied.astype(jnp.float32)[:, None, None]
    new_master, new_first, new_second = adamw_update(
        masters, owned.astype(jnp.float32), first_moment, second_moment, RATE_UNITS
    )
    updated = (
        new_master * occupied,
        jnp.stack([new_first * occupied, new_second * occupied]),
    )
    return (hidden, upstream, updated, lax.psum(small, BOTH))


def adamw_kernel(table_ref, owned_ref, value_ref, first_ref, second_ref, value_out, state_out):
    taken = table_ref[table_ref.shape[0] - pl.num_programs(0) + pl.program_id(0)] > 0
    gradient = jnp.where(taken, owned_ref[0].astype(jnp.float32), 0.0)
    value, first, second = adamw_update(
        value_ref[0], gradient, first_ref[0], second_ref[0], RATE_UNITS
    )
    value_out[0] = jnp.where(taken, value, 0.0)
    state_out[0, 0] = jnp.where(taken, first, 0.0)
    state_out[1, 0] = jnp.where(taken, second, 0.0)


def adamw_slots(table, owned, masters, first_moment, second_moment):
    count, width, cols = masters.shape
    tall = width
    at = table.shape[0] - 2 * count
    tile = pl.BlockSpec((1, tall, cols), lambda i, j, table: (i, j, 0))
    return pl.pallas_call(
        adamw_kernel,
        grid_spec=pltpu.PrefetchScalarGridSpec(
            num_scalar_prefetch=1,
            grid=(count, width // tall),
            in_specs=[
                pl.BlockSpec((1, tall, cols), lambda i, j, table: (table[at + i], j, 0)),
                tile,
                tile,
                tile,
            ],
            out_specs=(tile, pl.BlockSpec((2, 1, tall, cols), lambda i, j, table: (0, i, j, 0))),
        ),
        out_shape=(
            jax.ShapeDtypeStruct(masters.shape, jnp.float32),
            jax.ShapeDtypeStruct((2,) + masters.shape, jnp.float32),
        ),
        name="adamw",
    )(table, owned, masters, first_moment, second_moment)


def run_kernels(
    unit_slot,
    masters,
    first_moment,
    second_moment,
    hidden_in,
    doc_ids,
    column_state,
    row_state,
    out_grad,
):
    slot_count, width, cols = masters.shape
    blocks = (unit_slot.shape[0] // LAYERS - 4) // 2
    dp_size = lax.axis_size("dp")
    piece = width // (dp_size * lax.axis_size("tensor"))
    docs = lax.dynamic_index_in_dim(doc_ids, lax.axis_index("tensor"), 0, keepdims=False)
    row_now = row_state[0]
    weights, hidden, table, *saved = forward(
        unit_slot,
        masters,
        hidden_in,
        docs,
        column_state[0].reshape(-1, cols),
        row_now,
        piece,
        dp_size,
    )
    upstream, owned, small = backward(table, out_grad, docs, row_now, weights, saved, piece, cols)
    slots = adamw_slots(
        table, owned.reshape(masters.shape), masters, first_moment, second_moment
    )
    return (hidden, upstream, slots, small.reshape(2, LAYERS, 2 + blocks, width))


def local(
    hidden_in,
    doc_ids,
    unit_slot,
    masters,
    first_moment,
    second_moment,
    column_state,
    row_state,
    out_grad,
):
    col_width = masters.shape[2]
    tensor_index = lax.axis_index("tensor")
    kernels = (lax.axis_size("dp"), lax.axis_size("tensor")) == (8, 4)
    kernels = kernels and hidden_in.shape[0] == doc_ids.shape[1]
    run = run_kernels if kernels else run_general
    hidden, upstream, (unit_master, unit_state), small = run(
        unit_slot,
        masters,
        first_moment,
        second_moment,
        hidden_in,
        doc_ids,
        column_state,
        row_state,
        out_grad,
    )
    row_total = small[1]
    col_total = lax.dynamic_slice_in_dim(small[0], tensor_index * col_width, col_width, axis=2)
    new_col, col_first, col_second = adamw_update(
        column_state[0], col_total, column_state[1], column_state[2], RATE_SMALL
    )
    column_out = jnp.stack([col_total, new_col, col_first, col_second])
    new_row, row_first, row_second = adamw_update(
        row_state[0], row_total, row_state[1], row_state[2], RATE_SMALL
    )
    row_out = jnp.stack([row_total, new_row, row_first, row_second])
    return (hidden, upstream, unit_master, unit_state, column_out, row_out)


def solution(mesh):
    return jax.shard_map(
        local,
        mesh=mesh,
        in_specs=(
            P(("dp", "tensor"), None),
            P("dp", None),
            P(),
            P("dp", None, "tensor"),
            P("dp", None, "tensor"),
            P("dp", None, "tensor"),
            P(None, None, None, "tensor"),
            P(),
            P(("dp", "tensor"), None),
        ),
        out_specs=(
            P(("dp", "tensor"), None),
            P(("dp", "tensor"), None),
            P("dp", None, "tensor"),
            P(None, "dp", None, "tensor"),
            P(None, None, None, "tensor"),
            P(),
        ),
        check_vma=False,
    )
```
